32 devices in a mesh: dp: 8 (over z, x), tensor: 4 (over y, core).
Axes of the slice: x: 2, y: 2, z: 4, core: 2. Of those that a mesh axis runs over, the one named last changes fastest.
Arguments:
- hidden_in: bfloat16 [4096, 2048], P('dp'), may hold values from -40 to 40
- seq_lens: int32 [8, 8], P('dp'), may hold values from 0 to 512, as said below
- norm1_gain: float32 [2048], replicated, may hold values from 0.5 to 1.5
- query_weight: bfloat16 [2048, 4096], P(None, 'tensor'), may hold values from -0.125 to 0.125
- key_weight: bfloat16 [2048, 512], P(None, 'tensor'), may hold values from -0.125 to 0.125
- value_weight: bfloat16 [2048, 512], P(None, 'tensor'), may hold values from -0.125 to 0.125
- query_gain: float32 [128], replicated, may hold values from 0.5 to 1.5
- key_gain: float32 [128], replicated, may hold values from 0.5 to 1.5
- out_weight: bfloat16 [4096, 2048], P('tensor'), may hold values from -0.75 to 0.75
- norm2_gain: float32 [2048], replicated, may hold values from 0.5 to 1.5
- w_gate_up: bfloat16 [16, 2048, 2, 768], P('dp', None, None, 'tensor'), may hold values from -0.125 to 0.125
- w_down: bfloat16 [16, 768, 2048], P('dp', 'tensor'), may hold values from -0.875 to 0.875
- routes: int32 [4096, 8], P('dp'), may hold values from 0 to 15, all different within a row; in each aligned block of 512 rows (0 to 511, 512 to 1023, ...) at most 384 rows name the same one
- route_weights: float32 [4096, 8], P('dp'), may hold values from 0.05 to 0.25
- out_grad: bfloat16 [4096, 2048], P('dp'), may hold values from -6 to 6
Outputs:
- hidden_out: bfloat16 [4096, 2048], P('dp')
- hidden_grad: bfloat16 [4096, 2048], P('dp')
- grad_norm1_gain: float32 [2048], replicated
- grad_query_weight: float32 [2048, 4096], P(None, 'tensor')
- grad_key_weight: float32 [2048, 512], P(None, 'tensor')
- grad_value_weight: float32 [2048, 512], P(None, 'tensor')
- grad_query_gain: float32 [128], replicated
- grad_key_gain: float32 [128], replicated
- grad_out_weight: float32 [4096, 2048], P('tensor')
- grad_norm2_gain: float32 [2048], replicated
- grad_w_gate_up: float32 [16, 2048, 2, 768], P('dp', None, None, 'tensor')
- grad_w_down: float32 [16, 768, 2048], P('dp', 'tensor')
The draws below stay inside these ranges and needn't reach their ends.
Inputs may be any that keep to these rules, and one draw needn't show every extreme that they name: `seq_lens`: each row sums to 512; zeros are empty slots; some row holds a single sequence of 512. `routes`: A row names 8 different experts. In the rows of one index of dp no expert is named by more than 384 rows, a bound that some block reaches.
All inputs are finite; a program needn't handle non-finite values.
Results may differ from the reference program's by a relative error of at most 0.028.
Values may be sent and summed in bfloat16 or wider, within the bound.
A program may use at most 384 MiB of HBM per device.

```python
import math
import jax
import jax.numpy as jnp
import numpy as np
from jax import lax

D = 2048
HEADS = 32
KV_HEADS = 4
HEAD_DIM = 128
FF = 768
TOPK = 8
SEQ_SLOTS = 8
TOK_DEV = 512
TOKENS = 4096
EXPERTS = 16
CAP = 384
N_DP = 8
N_TENSOR = 4


def draw_hidden_in(key, part):
    key_list = jax.random.split(key, 3)
    row_scale = jnp.exp(jax.random.uniform(key_list[0], (TOKENS, 1), jnp.float32, 0.0, math.log(10.0)))
    column_scale = jnp.exp(jax.random.uniform(key_list[1], (1, D), jnp.float32, 0.0, math.log(10.0)))
    base_values = jnp.clip(jax.random.normal(key_list[2], (TOKENS, D), jnp.float32), -4.0, 4.0)
    return (base_values * row_scale * column_scale / 20.0).astype(jnp.bfloat16)


def draw_seq_lens(key, part):
    first_key, second_key = jax.random.split(key)
    counts = jax.random.randint(first_key, (N_DP,), 1, SEQ_SLOTS + 1).astype(jnp.int32)
    counts = counts.at[0].set(1)
    cutpoints = jax.random.randint(second_key, (N_DP, SEQ_SLOTS - 1), 1, TOK_DEV).astype(jnp.int32)
    active = jnp.arange(SEQ_SLOTS - 1, dtype=jnp.int32)[None, :] < (counts - 1)[:, None]
    cutpoints = jnp.sort(jnp.where(active, cutpoints, TOK_DEV), axis=1).astype(jnp.int32)
    bounds = jnp.concatenate([jnp.zeros((N_DP, 1), jnp.int32), cutpoints, jnp.full((N_DP, 1), TOK_DEV, jnp.int32)], axis=1)
    return (bounds[:, 1:] - bounds[:, :-1]).astype(jnp.int32)


def block_scale(rng, dims, cuts, smallest, top_value):
    def one(dim, blocks):
        heights = jax.random.uniform(jax.random.fold_in(jax.random.fold_in(rng, 6), dim), (blocks,), jnp.float32, smallest / len(cuts), top_value / len(cuts))
        return jnp.repeat(jnp.exp(heights), dims[dim] // blocks).reshape((-1,) + (1,) * (len(dims) - dim - 1))

    loudness = one(*cuts[0])
    for cut in cuts[1:]:
        loudness = loudness * one(*cut)
    return loudness


def assign_block(own_key, own, number, rows, number_of, top, bound, lean):
    sequence = jax.random.permutation(own_key, number_of)
    crowded, usual = load_shares(number_of, rows * top, bound, lean, True), load_shares(number_of, rows * top, bound, lean, False)
    places = jnp.arange(number_of)

    def named(sizes, rotation):
        used = int((sizes > 0).sum())
        fixed = max(1, used // 4)
        passed = fixed + (places - fixed + rotation * (used - fixed)) % max(1, number_of - fixed)
        return jnp.zeros((number_of,), jnp.int32).at[sequence[jnp.where(places < fixed, places, passed)]].set(jnp.asarray(sizes, jnp.int32))

    sizes = jnp.where(number % 4 == 0, named(crowded, number // 4), named(usual, number - number // 4 - 1))
    mixed = jax.random.permutation(jax.random.fold_in(own, 3), number_of)
    donor, sink = mixed[0:number_of // 2 * 2:2], mixed[1:number_of // 2 * 2:2]
    margin = jnp.minimum(sizes[donor] - 1, bound - sizes[sink]) // 2
    margin = jnp.where((donor == sequence[0]) | (sink == sequence[0]) | (sizes[sink] == 0), 0, jnp.maximum(margin, 0))
    passed = jax.random.randint(jax.random.fold_in(own, 4), (number_of // 2,), 0, 1 << 20) % (margin + 1)
    sizes = sizes.at[donor].add(-passed).at[sink].add(passed)
    members = jnp.searchsorted(jnp.cumsum(sizes), jnp.arange(rows * top), side="right").astype(jnp.int32)
    grid = members.reshape(top, rows).T
    grid = grid[jax.random.permutation(jax.random.fold_in(own, 1), rows)]
    rotation = jax.random.randint(jax.random.fold_in(own, 2), (rows, 1), 0, top)
    return jnp.take_along_axis(grid, (jnp.arange(top)[None, :] + rotation) % top, axis=1)


def load_shares(count, total, reach, lean, full):
    loads = [(1 << 20) // math.isqrt(rank ** lean) + 1 for rank in range(1, count + 1)]
    largest = reach if full else min(reach, max(-(-total // count), total * loads[0] // sum(loads)))
    least = 1 if total - largest >= count - 1 else 0
    given, spare = [largest] + [least] * (count - 1), total - largest - least * (count - 1)
    while spare > 0:
        free = [i for i in range(1, count) if given[i] < largest] or [i for i in range(1, count) if given[i] < reach]
        mass, left = sum([loads[i] for i in free]), spare
        for i in free:
            more = min(reach - given[i], max(1, left * loads[i] // mass), spare)
            given[i] = given[i] + more
            spare = spare - more
    return np.array(given)


def normal_values(own_key, extent, spread, limit, cuts=(), kind=jnp.bfloat16):
    values = jax.random.normal(own_key, extent, jnp.float32) * spread
    if len(cuts) > 0:
        values = block_scale(own_key, extent, cuts, -0.22, 0.18) * values
    return jnp.clip(values, min=-limit, max=limit).astype(kind)


def setup_inputs(seed: int = 0) -> dict:
    seeds = jax.random.split(jax.random.key(seed), 16)
    hidden_in = draw_hidden_in(jax.random.fold_in(seeds[15], 71), 0)
    seq_lens = draw_seq_lens(jax.random.fold_in(seeds[15], 71), 0)
    norm1_gain = jnp.clip(1.0 + 0.1 * jax.random.normal(seeds[2], (D,), jnp.float32), 0.5, 1.5)
    query_weight = normal_values(seeds[3], (D, HEADS * HEAD_DIM), D ** -0.5, 0.125, ((1, 4),))
    key_weight = normal_values(seeds[4], (D, KV_HEADS * HEAD_DIM), D ** -0.5, 0.125, ((1, 4),))
    value_weight = normal_values(seeds[5], (D, KV_HEADS * HEAD_DIM), D ** -0.5, 0.125, ((1, 4),))
    query_gain = jnp.clip(1.0 + 0.1 * jax.random.normal(seeds[6], (HEAD_DIM,), jnp.float32), 0.5, 1.5)
    key_gain = jnp.clip(1.0 + 0.1 * jax.random.normal(seeds[7], (HEAD_DIM,), jnp.float32), 0.5, 1.5)
    out_weight = normal_values(seeds[8], (HEADS * HEAD_DIM, D), (max(HEADS * HEAD_DIM // 64, 1)) ** -0.5, 0.75, ((0, 4),))
    norm2_gain = jnp.clip(1.0 + 0.1 * jax.random.normal(seeds[9], (D,), jnp.float32), 0.5, 1.5)
    w_gate_up = normal_values(seeds[10], (EXPERTS, D, 2, FF), D ** -0.5, 0.125, ((0, 8), (3, 4)))
    w_down = normal_values(seeds[11], (EXPERTS, FF, D), (FF // 16) ** -0.5, 0.875, ((0, 8), (1, 4)))
    routes_keys = jax.random.split(jax.random.fold_in(seeds[12], 1), TOKENS // TOK_DEV)
    routes_turns = jax.random.permutation(jax.random.fold_in(seeds[12], 3), TOKENS // TOK_DEV)
    routes = jax.vmap(lambda own, number: assign_block(jax.random.fold_in(seeds[12], 2), own, number, TOK_DEV, EXPERTS, TOPK, CAP, 1))(routes_keys, routes_turns).reshape((TOKENS, TOPK))
    route_weights = jnp.clip(0.05 + 0.2 * jax.random.uniform(seeds[13], (TOKENS, TOPK), jnp.float32) ** block_scale(seeds[13], (TOKENS, TOPK), ((0, 8),), -0.2, 0.2), 0.05, 0.25)
    out_grad = normal_values(seeds[14], (TOKENS, D), 1.0, 6.0, ((0, 8),))
    return dict(hidden_in=hidden_in, seq_lens=seq_lens, norm1_gain=norm1_gain, query_weight=query_weight, key_weight=key_weight, value_weight=value_weight, query_gain=query_gain, key_gain=key_gain, out_weight=out_weight, norm2_gain=norm2_gain, w_gate_up=w_gate_up, w_down=w_down, routes=routes, route_weights=route_weights, out_grad=out_grad)


EPSILON = 1e-06
ROPE_BASE = 1000000.0
HIGHEST = lax.Precision.HIGHEST

@jax.custom_vjp
def low(v):
    return lax.optimization_barrier(v.astype(jnp.bfloat16)).astype(jnp.float32)

@jax.custom_vjp
def low_back(v):
    return v

def low_keep(v):
    return (low(v), None)

def low_pass(kept, grad):
    return (grad,)

def back_keep(v):
    return (v, None)

def back_low(kept, grad):
    return (low(grad),)
low.defvjp(low_keep, low_pass)
low_back.defvjp(back_keep, back_low)

def matmul(left, right):
    return jnp.dot(left, right, precision=HIGHEST)

def rms_scale(values):
    return values * lax.rsqrt(lax.optimization_barrier(jnp.mean(values * values, axis=-1, keepdims=True)) + EPSILON)

def rotary_tables(positions):
    halves = jnp.arange(HEAD_DIM // 2, dtype=jnp.float32)
    inverse = jnp.exp(halves * (-2.0 * math.log(ROPE_BASE) / HEAD_DIM))
    angles = positions.astype(jnp.float32)[:, None] * inverse[None, :]
    return (jnp.cos(angles), jnp.sin(angles))

def rotate(values, cosine_table, sine_table):
    middle_index = values.shape[-1] // 2
    first_half = values[..., :middle_index]
    second = values[..., middle_index:]
    return jnp.concatenate([first_half * cosine_table - second * sine_table, second * cosine_table + first_half * sine_table], axis=-1)

def sequence_layout(lengths, token_count):
    lengths = lengths.astype(jnp.int32)
    endings = jnp.cumsum(lengths).astype(jnp.int32)
    places = jnp.arange(token_count, dtype=jnp.int32)
    starts = lax.optimization_barrier(jnp.sum(jnp.where(endings[None, :] <= places[:, None], lengths[None, :], 0), axis=1)).astype(jnp.int32)
    return (places, starts)

def attend(projected, lengths, query_gain, key_gain):
    query_rows, key_rows, value_rows = projected
    places, starts = sequence_layout(lengths, TOK_DEV)
    cosine_table, sine_table = rotary_tables(places - starts)
    cosine_table = cosine_table[:, None, :]
    sine_table = sine_table[:, None, :]
    query_rows = query_rows.reshape(TOK_DEV, HEADS, HEAD_DIM)
    key_rows = key_rows.reshape(TOK_DEV, KV_HEADS, HEAD_DIM)
    value_rows = low(value_rows.reshape(TOK_DEV, KV_HEADS, HEAD_DIM))
    query_rows = low(rotate(rms_scale(query_rows) * query_gain, cosine_table, sine_table))
    key_rows = low(rotate(rms_scale(key_rows) * key_gain, cosine_table, sine_table))
    sharing = HEADS // KV_HEADS
    query_rows = query_rows.reshape(TOK_DEV, KV_HEADS, sharing, HEAD_DIM)
    scores = jnp.einsum('tkgd,skd->kgts', query_rows, key_rows, precision=HIGHEST) * HEAD_DIM ** (-0.5)
    scores = low_back(scores)
    visible = (places[None, :] <= places[:, None]) & (places[None, :] >= starts[:, None])
    exponent = jnp.where(visible, jnp.exp(scores), 0.0)
    soft_weights = low(exponent / lax.optimization_barrier(jnp.sum(exponent, axis=-1, keepdims=True)))
    mixed = jnp.einsum('kgts,skd->tkgd', soft_weights, value_rows, precision=HIGHEST)
    return low(low_back(mixed.reshape(TOK_DEV, HEADS * HEAD_DIM)))

def mixture(normed_two, w_gate_up, w_down, routes, route_weights):
    padded = jnp.concatenate([normed_two, jnp.zeros((1, D), jnp.float32)], axis=0)
    expert_ids = jnp.arange(EXPERTS, dtype=jnp.int32)
    group_size = FF // N_TENSOR
    rows_most = N_DP * CAP

    def one_expert(running, inputs):
        gate_up, down_proj, expert_id = inputs
        hits = routes == expert_id
        token_weight = lax.optimization_barrier(jnp.sum(jnp.where(hits, route_weights, 0.0), axis=1))
        chosen = jnp.any(hits, axis=1)
        picked = jnp.nonzero(chosen, size=rows_most, fill_value=TOKENS)[0].astype(jnp.int32)
        taken = padded[picked]
        weight_rows = jnp.concatenate([token_weight, jnp.zeros((1,), jnp.float32)], axis=0)[picked]
        result = jnp.zeros((rows_most, D), jnp.float32)
        for member in range(N_TENSOR):
            lower = member * group_size
            upper = lower + group_size
            source_rows = low_back(taken)
            gate_act = low_back(matmul(source_rows, gate_up[:, 0, lower:upper]))
            up_act = low_back(matmul(source_rows, gate_up[:, 1, lower:upper]))
            active = low(jax.nn.silu(gate_act) * up_act)
            result = result + low(low_back(matmul(active, down_proj[lower:upper, :])))
        return (running.at[picked].add(weight_rows[:, None] * result), None)
    running, _ = lax.scan(jax.checkpoint(one_expert), jnp.zeros((TOKENS + 1, D), jnp.float32), (w_gate_up, w_down, expert_ids))
    return running[:TOKENS]

def forward(hidden, norm1_gain, query_weight, key_weight, value_weight, query_gain, key_gain, out_weight, norm2_gain, w_gate_up, w_down, seq_lens, routes, route_weights):
    normed = low(rms_scale(hidden) * norm1_gain)
    query_rows = low_back(matmul(normed, query_weight))
    key_rows = low_back(matmul(normed, key_weight))
    value_rows = low_back(matmul(normed, value_weight))
    blocked = (query_rows.reshape(N_DP, TOK_DEV, HEADS * HEAD_DIM), key_rows.reshape(N_DP, TOK_DEV, KV_HEADS * HEAD_DIM), value_rows.reshape(N_DP, TOK_DEV, KV_HEADS * HEAD_DIM))

    def per_block(inputs):
        projected, lengths = inputs
        return attend(projected, lengths, query_gain, key_gain)
    mixed = lax.map(jax.checkpoint(per_block), (blocked, seq_lens))
    attention = low_back(matmul(mixed.reshape(TOKENS, HEADS * HEAD_DIM), out_weight))
    middle = hidden + attention
    normed_two = low(rms_scale(middle) * norm2_gain)
    return middle + mixture(normed_two, w_gate_up, w_down, routes, route_weights)

def reference(hidden_in, seq_lens, norm1_gain, query_weight, key_weight, value_weight, query_gain, key_gain, out_weight, norm2_gain, w_gate_up, w_down, routes, route_weights, out_grad):
    primals = (hidden_in.astype(jnp.float32), norm1_gain, query_weight.astype(jnp.float32), key_weight.astype(jnp.float32), value_weight.astype(jnp.float32), query_gain, key_gain, out_weight.astype(jnp.float32), norm2_gain, w_gate_up.astype(jnp.float32), w_down.astype(jnp.float32))

    def layer(*params):
        return forward(*params, seq_lens, routes, route_weights)
    result, pullback = jax.vjp(layer, *primals)
    grads = pullback(out_grad.astype(jnp.float32))
    return (result.astype(jnp.bfloat16), grads[0].astype(jnp.bfloat16), grads[1], grads[2], grads[3], grads[4], grads[5], grads[6], grads[7], grads[8], grads[9], grads[10])
```

```python
import math

import jax
import jax.numpy as jnp
from jax import lax
from jax.sharding import PartitionSpec as P

EPSILON = 1e-06
ROPE_BASE = 1000000.0


def rms_parts(values):
    inverse = lax.rsqrt(jnp.mean(values * values, axis=-1, keepdims=True) + EPSILON)
    return (values * inverse, inverse)


def rms_back(grad_hat, normal_hat, inverse):
    return inverse * (
        grad_hat - normal_hat * jnp.mean(grad_hat * normal_hat, axis=-1, keepdims=True)
    )


def rotary_tables(positions, head_dim):
    halves = jnp.arange(head_dim // 2, dtype=jnp.float32)
    inverse = jnp.exp(halves * (-2.0 * math.log(ROPE_BASE) / head_dim))
    angles = positions.astype(jnp.float32)[:, None] * inverse[None, :]
    return (jnp.cos(angles), jnp.sin(angles))


def rotate(values, cosine_table, sine_table):
    middle_index = values.shape[-1] // 2
    first_half = values[..., :middle_index]
    second = values[..., middle_index:]
    return jnp.concatenate(
        [
            first_half * cosine_table - second * sine_table,
            second * cosine_table + first_half * sine_table,
        ],
        axis=-1,
    )


def rotate_back(gradient, cosine_table, sine_table):
    middle_index = gradient.shape[-1] // 2
    first_half = gradient[..., :middle_index]
    second = gradient[..., middle_index:]
    return jnp.concatenate(
        [
            first_half * cosine_table + second * sine_table,
            second * cosine_table - first_half * sine_table,
        ],
        axis=-1,
    )


def sequence_layout(lengths, token_count):
    endings = jnp.cumsum(lengths)
    places = jnp.arange(token_count, dtype=jnp.int32)
    starts = jnp.sum(jnp.where(endings[None, :] <= places[:, None], lengths[None, :], 0), axis=1)
    return (places, starts)


def local(
    hidden_in,
    seq_lens,
    norm1_gain,
    query_weight,
    key_weight,
    value_weight,
    query_gain,
    key_gain,
    out_weight,
    norm2_gain,
    w_gate_up,
    w_down,
    routes,
    route_weights,
    out_grad,
):
    bf = jnp.bfloat16
    f32 = jnp.float32
    tokens, model_width = hidden_in.shape
    local_experts = w_gate_up.shape[0]
    hidden_part = w_gate_up.shape[3]
    head_dim = query_gain.shape[0]
    local_heads = query_weight.shape[1] // head_dim
    data_size = lax.axis_size("dp")
    tensor_size = lax.axis_size("tensor")
    quarter = tokens // tensor_size
    experts = local_experts * data_size
    score_scale = head_dim ** (-0.5)
    row0 = lax.axis_index("tensor") * quarter

    def mine(array):
        return lax.dynamic_slice_in_dim(array, row0, quarter, 0)

    expert_ids = jnp.arange(experts, dtype=jnp.int32)
    dense = jnp.sum(
        jnp.where(mine(routes)[:, :, None] == expert_ids[None, None, :], mine(route_weights)[:, :, None], 0.0),
        axis=1,
    )
    dense_high = dense.astype(bf)
    dense_low = (dense - dense_high.astype(f32)).astype(bf)
    packed = jnp.concatenate([mine(out_grad), dense_high, dense_low], axis=1)
    gathered = lax.all_gather(packed, "dp", tiled=True)
    grads_all = gathered[:, :model_width]
    dense_all = gathered[:, model_width : model_width + experts].astype(f32) + gathered[
        :, model_width + experts :
    ].astype(f32)
    weight_all = lax.dynamic_slice_in_dim(
        dense_all, lax.axis_index("dp") * local_experts, local_experts, 1
    )
    rows = data_size * quarter
    units = local_experts * hidden_part
    own_weights = jnp.concatenate(
        [
            jnp.transpose(w_gate_up, (2, 0, 3, 1)).reshape(2, units, model_width),
            w_down.reshape(1, units, model_width),
        ],
        axis=0,
    )
    all_weights = lax.all_gather(own_weights, "tensor")
    weight_cols = jnp.broadcast_to(
        weight_all[:, None, :, None], (rows, tensor_size, local_experts, hidden_part)
    ).reshape(rows, tensor_size, units)

    hidden = hidden_in.astype(f32)
    hat_one, inv_one = rms_parts(hidden)
    normed = (hat_one * norm1_gain).astype(bf)
    query_proj = jnp.dot(normed, query_weight, preferred_element_type=f32).reshape(
        tokens, local_heads, head_dim
    )
    key_proj = jnp.dot(normed, key_weight, preferred_element_type=f32)
    value_low = jnp.dot(normed, value_weight, preferred_element_type=f32).astype(bf)
    places, starts = sequence_layout(seq_lens[0], tokens)
    cosine_table, sine_table = rotary_tables(places - starts, head_dim)
    query_hat, query_inv = rms_parts(query_proj)
    query_low = rotate(
        query_hat * query_gain, cosine_table[:, None, :], sine_table[:, None, :]
    ).astype(bf)
    key_hat, key_inv = rms_parts(key_proj)
    key_low = rotate(key_hat * key_gain, cosine_table, sine_table).astype(bf)
    visible = (places[None, :] <= places[:, None]) & (places[None, :] >= starts[:, None])
    scores = jnp.einsum("thd,sd->hts", query_low, key_low, preferred_element_type=f32) * score_scale
    exponent = jnp.where(visible[None], jnp.exp(scores), 0.0)
    totals = jnp.sum(exponent, axis=-1, keepdims=True)
    log_totals = jnp.log(totals)
    soft_low = (exponent / totals).astype(bf)
    mixed_low = (
        jnp.einsum("hts,sd->thd", soft_low, value_low, preferred_element_type=f32)
        .reshape(tokens, local_heads * head_dim)
        .astype(bf)
    )
    attention = lax.psum_scatter(
        jnp.dot(mixed_low, out_weight, preferred_element_type=f32).astype(bf), "tensor", tiled=True
    ).astype(f32)
    hidden_q = mine(hidden_in).astype(f32)
    hat_one_q, inv_one_q = rms_parts(hidden_q)
    middle = hidden_q + attention
    hat_two, inv_two = rms_parts(middle)
    normed_two = (hat_two * norm2_gain).astype(bf)
    inputs = lax.all_gather(normed_two, "dp", tiled=True)

    def project(left, which):
        return jnp.einsum("td,rud->tru", left, all_weights[:, which], preferred_element_type=f32)

    gate_act = project(inputs, 0)
    upward = project(inputs, 1)
    sigmoid_gate = jax.nn.sigmoid(gate_act)
    active = gate_act * sigmoid_gate * upward
    weighted_low = (weight_cols * active).astype(bf)
    mixture_part = jnp.einsum(
        "tru,rud->td", weighted_low, all_weights[:, 2], preferred_element_type=f32
    ).astype(bf)
    mixture = lax.psum_scatter(mixture_part, "dp", tiled=True).astype(f32)
    hidden_out = (middle + mixture).astype(bf)
    grad_active = weight_cols * project(grads_all, 2)
    grad_gate = (
        grad_active * upward * sigmoid_gate * (1.0 + gate_act * (1.0 - sigmoid_gate))
    ).astype(bf)
    grad_up = (grad_active * gate_act * sigmoid_gate).astype(bf)
    grad_normed_part = jnp.einsum(
        "tru,rud->td", grad_gate, all_weights[:, 0], preferred_element_type=f32
    ) + jnp.einsum("tru,rud->td", grad_up, all_weights[:, 1], preferred_element_type=f32)
    grad_normed_two = lax.psum_scatter(grad_normed_part.astype(bf), "dp", tiled=True).astype(f32)
    weight_grads = jnp.stack(
        [
            jnp.einsum("tru,td->rud", grad_gate, inputs, preferred_element_type=f32).astype(bf),
            jnp.einsum("tru,td->rud", grad_up, inputs, preferred_element_type=f32).astype(bf),
            jnp.einsum("tru,td->rud", weighted_low, grads_all, preferred_element_type=f32).astype(bf),
        ],
        axis=1,
    )
    own_grads = (
        lax.psum_scatter(weight_grads.reshape(-1, model_width), "tensor", tiled=True)
        .astype(f32)
        .reshape(3, units, model_width)
    )
    grad_w_gate_up = jnp.transpose(
        own_grads[:2].reshape(2, local_experts, hidden_part, model_width), (1, 3, 0, 2)
    )
    grad_w_down = own_grads[2].reshape(local_experts, hidden_part, model_width)

    grad_out = mine(out_grad).astype(f32)
    grad_gain_two = jnp.sum(grad_normed_two * hat_two, axis=0)
    grad_middle = grad_out + rms_back(grad_normed_two * norm2_gain, hat_two, inv_two)
    grad_mid_low = lax.all_gather(grad_middle.astype(bf), "tensor", tiled=True)
    grad_out_weight = jnp.einsum("ti,td->id", mixed_low, grad_mid_low, preferred_element_type=f32)
    grad_mixed = (
        jnp.einsum("td,id->ti", grad_mid_low, out_weight, preferred_element_type=f32)
        .astype(bf)
        .reshape(tokens, local_heads, head_dim)
    )
    scores_again = (
        jnp.einsum("thd,sd->hts", query_low, key_low, preferred_element_type=f32) * score_scale
    )
    soft_again = jnp.where(visible[None], jnp.exp(scores_again - log_totals), 0.0)
    grad_soft = jnp.einsum("thd,sd->hts", grad_mixed, value_low, preferred_element_type=f32)
    grad_scores = (
        soft_again * (grad_soft - jnp.sum(soft_again * grad_soft, axis=-1, keepdims=True))
    ).astype(bf)
    grad_values = jnp.einsum(
        "hts,thd->sd", soft_again.astype(bf), grad_mixed, preferred_element_type=f32
    ).astype(bf)
    grad_query_rot = score_scale * jnp.einsum(
        "hts,sd->thd", grad_scores, key_low, preferred_element_type=f32
    )
    grad_key_rot = score_scale * jnp.einsum(
        "hts,thd->sd", grad_scores, query_low, preferred_element_type=f32
    )
    grad_query_norm = rotate_back(grad_query_rot, cosine_table[:, None, :], sine_table[:, None, :])
    grad_query_gain = jnp.sum(grad_query_norm * query_hat, axis=(0, 1))
    grad_query_low = (
        rms_back(grad_query_norm * query_gain, query_hat, query_inv)
        .reshape(tokens, local_heads * head_dim)
        .astype(bf)
    )
    grad_key_norm = rotate_back(grad_key_rot, cosine_table, sine_table)
    grad_key_gain = jnp.sum(grad_key_norm * key_hat, axis=0)
    grad_key_low = rms_back(grad_key_norm * key_gain, key_hat, key_inv).astype(bf)
    grad_query_weight = jnp.einsum("ti,tj->ij", normed, grad_query_low, preferred_element_type=f32)
    grad_key_weight = jnp.einsum("ti,tj->ij", normed, grad_key_low, preferred_element_type=f32)
    grad_value_weight = jnp.einsum("ti,tj->ij", normed, grad_values, preferred_element_type=f32)
    grad_normed_one = jnp.einsum("tj,ij->ti", grad_query_low, query_weight, preferred_element_type=f32)
    grad_normed_one = grad_normed_one + jnp.einsum(
        "tj,ij->ti", grad_key_low, key_weight, preferred_element_type=f32
    )
    grad_normed_one = grad_normed_one + jnp.einsum(
        "tj,ij->ti", grad_values, value_weight, preferred_element_type=f32
    )
    grad_normed_one = lax.psum_scatter(grad_normed_one.astype(bf), "tensor", tiled=True).astype(f32)
    grad_gain_one = jnp.sum(grad_normed_one * hat_one_q, axis=0)
    grad_hidden = grad_middle + rms_back(grad_normed_one * norm1_gain, hat_one_q, inv_one_q)
    both = lax.all_gather(
        jnp.stack([hidden_out, grad_hidden.astype(bf)], axis=0), "tensor", axis=1, tiled=True
    )
    grad_out_sum = lax.psum(grad_out_weight.astype(bf), "dp").astype(f32)
    summed = (
        lax.psum(grad_query_weight.astype(bf), "dp").astype(f32),
        lax.psum(grad_key_weight.astype(bf), "dp").astype(f32),
        lax.psum(grad_value_weight.astype(bf), "dp").astype(f32),
    )
    gains = lax.psum(
        jnp.concatenate([grad_gain_one, grad_gain_two, grad_query_gain, grad_key_gain]),
        ("dp", "tensor"),
    )
    return (
        both[0],
        both[1],
        gains[:model_width],
        summed[0],
        summed[1],
        summed[2],
        gains[2 * model_width : 2 * model_width + head_dim],
        gains[2 * model_width + head_dim :],
        grad_out_sum,
        gains[model_width : 2 * model_width],
        grad_w_gate_up,
        grad_w_down,
    )


def solution(mesh):
    in_specs = (
        P("dp", None),
        P("dp", None),
        P(),
        P(None, "tensor"),
        P(None, "tensor"),
        P(None, "tensor"),
        P(),
        P(),
        P("tensor", None),
        P(),
        P("dp", None, None, "tensor"),
        P("dp", "tensor", None),
        P("dp", None),
        P("dp", None),
        P("dp", None),
    )
    out_specs = (
        P("dp", None),
        P("dp", None),
        P(),
        P(None, "tensor"),
        P(None, "tensor"),
        P(None, "tensor"),
        P(),
        P(),
        P("tensor", None),
        P(),
        P("dp", None, None, "tensor"),
        P("dp", "tensor", None),
    )
    return jax.shard_map(local, mesh=mesh, in_specs=in_specs, out_specs=out_specs, check_vma=False)
```

```python
import functools
import math

import jax
import jax.numpy as jnp
from jax import lax
from jax.experimental import pallas as pl
from jax.experimental.pallas import tpu as pltpu
from jax.sharding import PartitionSpec as P

EPSILON = 1e-06
ROPE_BASE = 1000000.0


def rms_parts(values):
    inverse = lax.rsqrt(jnp.mean(values * values, axis=-1, keepdims=True) + EPSILON)
    return (values * inverse, inverse)


def rms_back(grad_hat, normal_hat, inverse):
    return inverse * (
        grad_hat - normal_hat * jnp.mean(grad_hat * normal_hat, axis=-1, keepdims=True)
    )


def rotary_tables(positions, head_dim):
    halves = jnp.arange(head_dim // 2, dtype=jnp.float32)
    inverse = jnp.exp(halves * (-2.0 * math.log(ROPE_BASE) / head_dim))
    angles = positions.astype(jnp.float32)[:, None] * inverse[None, :]
    return (jnp.cos(angles), jnp.sin(angles))


def rotate(values, cosine_table, sine_table):
    middle_index = values.shape[-1] // 2
    first_half = values[..., :middle_index]
    second = values[..., middle_index:]
    return jnp.concatenate(
        [
            first_half * cosine_table - second * sine_table,
            second * cosine_table + first_half * sine_table,
        ],
        axis=-1,
    )


def rotate_back(gradient, cosine_table, sine_table):
    middle_index = gradient.shape[-1] // 2
    first_half = gradient[..., :middle_index]
    second = gradient[..., middle_index:]
    return jnp.concatenate(
        [
            first_half * cosine_table + second * sine_table,
            second * cosine_table - first_half * sine_table,
        ],
        axis=-1,
    )


def sequence_layout(lengths, token_count):
    endings = jnp.cumsum(lengths)
    places = jnp.arange(token_count, dtype=jnp.int32)
    starts = jnp.sum(jnp.where(endings[None, :] <= places[:, None], lengths[None, :], 0), axis=1)
    return (places, starts)


LANES = 128
MESH = pl.DeviceIdType.MESH
VMEM_LIMIT = 60 * 1024 * 1024


def ring_place(index, size):
    return jnp.where(index % 2 == 0, index // 2, size - (index + 1) // 2)


def ring_index(place, size):
    place = place % size
    return jnp.where(place < size // 2, 2 * place, 2 * size - 1 - 2 * place)


def tensor_peers():
    own = lax.axis_index("tensor")
    partner = own + 1 - 2 * (own % 2)
    across = (own + 2) % 4
    return own, partner, across


def greet(devices):
    barrier = pltpu.get_barrier_semaphore()
    for device in devices:
        pl.semaphore_signal(barrier, inc=1, device_id=device, device_id_type=MESH)
    pl.semaphore_wait(barrier, len(devices))


def push(source, target, sems, device):
    return pltpu.make_async_remote_copy(
        src_ref=source,
        dst_ref=target,
        send_sem=sems[0],
        recv_sem=sems[1],
        device_id=device,
        device_id_type=MESH,
    )


class GatherRing:
    def __init__(self, size, blocks, sems, key, parts=2):
        self.size, self.blocks, self.sems, self.key, self.parts = size, blocks, sems, key, parts
        self.place = ring_place(lax.axis_index("dp"), size)
        self.sent = []
        self.live = {}

    def send(self, step):
        size, half = self.size, self.blocks.shape[1] // 2
        piece = half // self.parts
        for part in range(self.parts):
            for way in (0, 1):
                sign = 1 - 2 * way
                block = self.key(ring_index(self.place + size * 2 - sign * step, size))
                rows = pl.ds(way * half + part * piece, piece)
                ref = self.blocks.at[block, rows]
                device = (ring_index(self.place + size + sign, size), lax.axis_index("tensor"))
                copy = push(
                    ref,
                    ref,
                    (self.sems.at[0, way, step, part], self.sems.at[1, way, step, part]),
                    device,
                )
                if step > 0:
                    self.live[step - 1, part, way].wait_recv()
                copy.start()
                self.live[step, part, way] = copy
                self.sent.append(copy)

    def step(self, step):
        if step + 1 < self.size - 1:
            self.send(step + 1)
        else:
            for part in range(self.parts):
                for way in (0, 1):
                    self.live[step, part, way].wait_recv()

    def finish(self):
        for copy in self.sent:
            copy.wait_send()


def row_loop(total, rows, body):
    def run(index, carry):
        body(pl.ds(pl.multiple_of(index * rows, rows), rows))
        return carry

    lax.fori_loop(0, total // rows, run, 0)


def exchange_tokens_body(
    size,
    part_ref,
    token_ref,
    pack_ref,
    gain_ref,
    middle_ref,
    inputs_ref,
    packs_ref,
    from_partner,
    from_across,
    joined,
    ring_sems,
    pack_sems,
    side_sems,
    local_sem,
):
    f32 = jnp.float32
    dp = lax.axis_index("dp")
    own, partner, across = tensor_peers()
    far_partner = (partner + 2) % 4
    quarter = token_ref.shape[0]
    place = ring_place(dp, size)
    neighbours = [(ring_index(place + 1, size), own), (ring_index(place + size - 1, size), own)]
    greet(neighbours + [(dp, partner), (dp, across)])

    def part_rows(index):
        return pl.ds(pl.multiple_of(index * quarter, quarter), quarter)

    def side(index):
        return (side_sems.at[0, index], side_sems.at[1, index])

    first = push(part_ref.at[part_rows(far_partner)], from_partner.at[1], side(0), (dp, partner))
    second = push(part_ref.at[part_rows(partner)], from_partner.at[0], side(1), (dp, partner))
    first.start()
    second.start()
    keep = pltpu.make_async_copy(pack_ref, packs_ref.at[dp], local_sem)
    keep.start()
    keep.wait()
    packs = GatherRing(size, packs_ref, pack_sems, lambda index: index)
    packs.send(0)
    first.wait_recv()
    base = across * quarter

    def join(rows):
        there = pl.ds(pl.multiple_of(base + rows.start, 16), rows.size)
        joined[rows, :] = (
            part_ref[there, :].astype(f32) + from_partner[1, rows, :].astype(f32)
        ).astype(jnp.bfloat16)

    row_loop(quarter, 16, join)
    third = push(joined, from_across, side(2), (dp, across))
    third.start()
    packs.step(0)
    second.wait_recv()
    third.wait_recv()
    mine = own * quarter

    def norm(rows):
        there = pl.ds(pl.multiple_of(mine + rows.start, 16), rows.size)
        middle = (
            token_ref[rows, :].astype(f32)
            + part_ref[there, :].astype(f32)
            + from_partner[0, rows, :].astype(f32)
            + from_across[rows, :].astype(f32)
        )
        middle_ref[rows, :] = middle
        inverse = lax.rsqrt(jnp.mean(middle * middle, axis=-1, keepdims=True) + EPSILON)
        inputs_ref[dp, rows, :] = (middle * inverse * gain_ref[...]).astype(jnp.bfloat16)

    row_loop(quarter, 16, norm)
    tokens = GatherRing(size, inputs_ref, ring_sems, lambda index: index)
    tokens.send(0)
    for step in range(1, size - 1):
        packs.step(step)
        tokens.step(step - 1)
    tokens.step(size - 2)
    packs.finish()
    tokens.finish()
    first.wait_send()
    second.wait_send()
    third.wait_send()


def exchange_tokens(size, partial, token_rows, packed, gain):
    quarter, width = token_rows.shape
    columns = packed.shape[1]
    bf = jnp.bfloat16
    vmem = pl.BlockSpec(memory_space=pltpu.VMEM)
    dma = pltpu.SemaphoreType.DMA
    return pl.pallas_call(
        functools.partial(exchange_tokens_body, size),
        out_shape=(
            jax.ShapeDtypeStruct((quarter, width), jnp.float32),
            jax.ShapeDtypeStruct((size, quarter, width), bf),
            jax.ShapeDtypeStruct((size, quarter, columns), bf),
        ),
        in_specs=[vmem] * 4,
        out_specs=(vmem,) * 3,
        scratch_shapes=[
            pltpu.VMEM((2, quarter, width), bf),
            pltpu.VMEM((quarter, width), bf),
            pltpu.VMEM((quarter, width), bf),
            dma((2, 2, size - 1, 2)),
            dma((2, 2, size - 1, 2)),
            dma((2, 3)),
            dma(()),
        ],
        compiler_params=pltpu.CompilerParams(
            collective_id=0, has_side_effects=True, vmem_limit_bytes=VMEM_LIMIT
        ),
        name="exchange_tokens",
    )(partial, token_rows, packed, gain.reshape(1, -1))


def finish_sums_body(
    size,
    lead,
    qkv_ref,
    out_ref,
    normed_ref,
    middle_ref,
    token_ref,
    hidden_ref,
    gain_ref,
    gains_ref,
    hidden_all,
    grad_all,
    query_out,
    key_out,
    value_out,
    outer_out,
    gains_out,
    slots_a,
    slots_b,
    gather_a,
    gather_b,
    wide_a,
    wide_b,
    from_partner,
    from_across,
    joined,
    totals,
    pair_gains,
    ring_gains,
    sems_a,
    sems_b,
    ring_sems,
    side_sems,
    store_sems,
    local_sems,
):
    f32, bf = jnp.float32, jnp.bfloat16
    dp = lax.axis_index("dp")
    own, partner, across = tensor_peers()
    far_partner = (partner + 2) % 4
    quarter, width = token_ref.shape
    place = ring_place(dp, size)
    forward = (ring_index(place + 1, size), own)
    backward = (ring_index(place + size - 1, size), own)
    ways = ((forward, 1), (backward, -1))
    greet([forward, backward, (dp, partner), (dp, across)])
    waits = []

    def start(copy):
        copy.start()
        waits.append(copy)
        return copy

    sets = (
        (qkv_ref, slots_a, gather_a, wide_a, sems_a),
        (out_ref, slots_b, gather_b, wide_b, sems_b),
    )

    def block_of(ref, block, way):
        rows = ref.shape[0] // size
        cut = ref.shape[1] // 2
        return (pl.ds(pl.multiple_of(block * rows, rows), rows), pl.ds(way * cut, cut))

    def wrap(value):
        return (value + 2 * size) % size

    live = {}

    def reduce_send(step):
        for which, (ref, slots, _, _, sems) in enumerate(sets):
            for way, (device, sign) in enumerate(ways):
                if step == 0:
                    source = ref.at[block_of(ref, wrap(place - sign), way)]
                else:
                    add_own(which, way, step - 1)
                    source = slots.at[way, step - 1]
                live[which, way, step] = start(
                    push(
                        source,
                        slots.at[way, step],
                        (sems.at[0, way, step], sems.at[1, way, step]),
                        device,
                    )
                )

    def add_own(which, way, step):
        ref, slots, _, _, _ = sets[which]
        live[which, way, step].wait_recv()
        sign = ways[way][1]
        rows, columns = block_of(ref, wrap(place - sign * (2 + step)), way)
        base = rows.start

        def add(inner):
            there = pl.ds(pl.multiple_of(base + inner.start, 16), inner.size)
            slots[way, step, inner, :] = (
                slots[way, step, inner, :].astype(f32) + ref[there, columns].astype(f32)
            ).astype(bf)

        row_loop(ref.shape[0] // size, 16, add)

    gather = {}

    def gather_send(step):
        for which, (ref, slots, blocks, _, sems) in enumerate(sets):
            cut = ref.shape[1] // 2
            for way, (device, sign) in enumerate(ways):
                columns = pl.ds(way * cut, cut)
                block = wrap(place - sign * step)
                if step == 0:
                    add_own(which, way, size - 2)
                    source = slots.at[way, size - 2]
                else:
                    gather[which, way, step - 1].wait_recv()
                    source = blocks.at[block, :, columns]
                gather[which, way, step] = start(
                    push(
                        source,
                        blocks.at[block, :, columns],
                        (sems.at[0, way, size - 1 + step], sems.at[1, way, size - 1 + step]),
                        device,
                    )
                )
                store(which, way, block, source)

    pending = {}

    def store(which, way, block, source):
        ref, _, _, wide, _ = sets[which]
        rows_total = ref.shape[0] // size
        cut = ref.shape[1] // 2
        for copy in pending.pop((which, way), []):
            copy.wait()

        def widen(inner):
            wide[way, inner, :] = source[inner, :].astype(f32)

        row_loop(rows_total, 16, widen)
        rows = pl.ds(pl.multiple_of(block * rows_total, rows_total), rows_total)
        if which == 1:
            targets = [(outer_out.at[rows, pl.ds(way * cut, cut)], 0, cut)]
        elif way == 0:
            targets = [(query_out.at[rows, pl.ds(0, cut)], 0, cut)]
        else:
            rest = lead - cut
            tail = key_out.shape[1]
            targets = [
                (query_out.at[rows, pl.ds(cut, rest)], 0, rest),
                (key_out.at[rows], rest, tail),
                (value_out.at[rows], rest + tail, tail),
            ]
        copies = []
        for index, (target, first, count) in enumerate(targets):
            copy = pltpu.make_async_copy(
                wide.at[way, :, pl.ds(first, count)], target, store_sems.at[which, way, index]
            )
            copy.start()
            copies.append(copy)
        pending[which, way] = copies

    def part_rows(index):
        return pl.ds(pl.multiple_of(index * quarter, quarter), quarter)

    def side(index):
        return (side_sems.at[0, index], side_sems.at[1, index])

    reduce_send(0)
    first = start(
        push(normed_ref.at[part_rows(far_partner)], from_partner.at[1], side(0), (dp, partner))
    )
    second = start(
        push(normed_ref.at[part_rows(partner)], from_partner.at[0], side(1), (dp, partner))
    )
    mine = part_rows(own)
    spread = []
    spread.append(start(push(hidden_ref, hidden_all.at[mine], side(3), (dp, across))))
    spread.append(start(push(hidden_ref, hidden_all.at[mine], side(4), (dp, partner))))
    keep = pltpu.make_async_copy(hidden_ref, hidden_all.at[mine], local_sems.at[0])
    keep.start()
    reduce_send(1)
    first.wait_recv()
    away = across * quarter

    def join(rows):
        there = pl.ds(pl.multiple_of(away + rows.start, 16), rows.size)
        joined[rows, :] = (
            normed_ref[there, :].astype(f32) + from_partner[1, rows, :].astype(f32)
        ).astype(bf)

    row_loop(quarter, 16, join)
    third = start(push(joined, from_across, side(2), (dp, across)))
    reduce_send(2)
    second.wait_recv()
    third.wait_recv()
    home = own * quarter
    totals[...] = jnp.zeros_like(totals)

    def finish(rows):
        there = pl.ds(pl.multiple_of(home + rows.start, 16), rows.size)
        grads = (
            normed_ref[there, :].astype(f32)
            + from_partner[0, rows, :].astype(f32)
            + from_across[rows, :].astype(f32)
        )
        hidden = token_ref[rows, :].astype(f32)
        inverse = lax.rsqrt(jnp.mean(hidden * hidden, axis=-1, keepdims=True) + EPSILON)
        hat = hidden * inverse
        product = grads * hat
        totals[:, :width] += jnp.sum(product.reshape(-1, 8, width), axis=0)
        scaled = grads * gain_ref[...]
        back = inverse * (scaled - hat * jnp.mean(scaled * hat, axis=-1, keepdims=True))
        joined_grad = (middle_ref[rows, :] + back).astype(bf)
        grad_all[there, :] = joined_grad

    row_loop(quarter, 16, finish)
    spread.append(start(push(grad_all.at[mine], grad_all.at[mine], side(5), (dp, across))))
    spread.append(start(push(grad_all.at[mine], grad_all.at[mine], side(6), (dp, partner))))
    pair_gains[0, :, :width] = jnp.sum(totals[:, :width], axis=0, keepdims=True)
    pair_gains[0, :, width:] = gains_ref[...]
    swap = start(push(pair_gains.at[0], pair_gains.at[1], side(7), (dp, partner)))
    reduce_send(3)
    far = part_rows(across)
    spread[0].wait_recv()
    spread.append(start(push(hidden_all.at[far], hidden_all.at[far], side(8), (dp, partner))))
    spread[2].wait_recv()
    spread.append(start(push(grad_all.at[far], grad_all.at[far], side(9), (dp, partner))))
    swap.wait_recv()
    pair_gains[2] = pair_gains[0] + pair_gains[1]
    swap = start(push(pair_gains.at[2], pair_gains.at[3], side(10), (dp, across)))
    for step in range(4, size - 1):
        reduce_send(step)
    swap.wait_recv()
    ring_gains[place] = pair_gains[2] + pair_gains[3]
    gather_send(0)
    small = None
    for step in range(size - 1):
        if small is not None:
            small.wait_recv()
        ref = ring_gains.at[wrap(place - step)]
        small = start(push(ref, ref, (ring_sems.at[0, step], ring_sems.at[1, step]), forward))
        if step > 0:
            gather_send(step)
    small.wait_recv()
    for which, (ref, _, blocks, _, _) in enumerate(sets):
        cut = ref.shape[1] // 2
        for way, (_, sign) in enumerate(ways):
            gather[which, way, size - 2].wait_recv()
            block = wrap(place - sign * (size - 1))
            store(which, way, block, blocks.at[block, :, pl.ds(way * cut, cut)])
    gains_out[...] = jnp.sum(ring_gains[...], axis=0)
    for copies in pending.values():
        for copy in copies:
            copy.wait()
    keep.wait()
    for index in (1, 3, 4, 5):
        spread[index].wait_recv()
    for copy in waits:
        copy.wait_send()


def finish_sums(
    size, grad_in, grad_out, grad_normed, grad_middle, token_rows, hidden_rows, gain, gains, head_dim
):
    bf, f32 = jnp.bfloat16, jnp.float32
    quarter, width = token_rows.shape
    tokens = grad_normed.shape[0]
    lead = grad_in.shape[1] - 2 * head_dim
    vmem = pl.BlockSpec(memory_space=pltpu.VMEM)
    anywhere = pl.BlockSpec(memory_space=pl.ANY)
    dma = pltpu.SemaphoreType.DMA
    rows_a, rows_b = grad_in.shape[0] // size, grad_out.shape[0] // size
    cut_a, cut_b = grad_in.shape[1] // 2, grad_out.shape[1] // 2
    count = width + gains.shape[1]
    return pl.pallas_call(
        functools.partial(finish_sums_body, size, lead),
        out_shape=(
            jax.ShapeDtypeStruct((tokens, width), bf),
            jax.ShapeDtypeStruct((tokens, width), bf),
            jax.ShapeDtypeStruct((width, lead), f32),
            jax.ShapeDtypeStruct((width, head_dim), f32),
            jax.ShapeDtypeStruct((width, head_dim), f32),
            jax.ShapeDtypeStruct(grad_out.shape, f32),
            jax.ShapeDtypeStruct((1, count), f32),
        ),
        in_specs=[vmem] * 8,
        out_specs=(vmem, vmem, anywhere, anywhere, anywhere, anywhere, vmem),
        scratch_shapes=[
            pltpu.VMEM((2, size - 1, rows_a, cut_a), bf),
            pltpu.VMEM((2, size - 1, rows_b, cut_b), bf),
            pltpu.VMEM((size, rows_a, 2 * cut_a), bf),
            pltpu.VMEM((size, rows_b, 2 * cut_b), bf),
            pltpu.VMEM((2, rows_a, cut_a), f32),
            pltpu.VMEM((2, rows_b, cut_b), f32),
            pltpu.VMEM((2, quarter, width), bf),
            pltpu.VMEM((quarter, width), bf),
            pltpu.VMEM((quarter, width), bf),
            pltpu.VMEM((8, width), f32),
            pltpu.VMEM((4, 1, count), f32),
            pltpu.VMEM((size, 1, count), f32),
            dma((2, 2, 2 * size - 2)),
            dma((2, 2, 2 * size - 2)),
            dma((2, size - 1)),
            dma((2, 11)),
            dma((2, 2, 3)),
            dma((1,)),
        ],
        compiler_params=pltpu.CompilerParams(
            collective_id=1, has_side_effects=True, vmem_limit_bytes=VMEM_LIMIT
        ),
        name="finish_sums",
    )(
        grad_in,
        grad_out,
        grad_normed,
        grad_middle,
        token_rows,
        hidden_rows,
        gain.reshape(1, -1),
        gains,
    )


def local(
    hidden_in,
    seq_lens,
    norm1_gain,
    query_weight,
    key_weight,
    value_weight,
    query_gain,
    key_gain,
    out_weight,
    norm2_gain,
    w_gate_up,
    w_down,
    routes,
    route_weights,
    out_grad,
):
    bf = jnp.bfloat16
    f32 = jnp.float32
    tokens, model_width = hidden_in.shape
    local_experts = w_gate_up.shape[0]
    hidden_part = w_gate_up.shape[3]
    head_dim = query_gain.shape[0]
    local_heads = query_weight.shape[1] // head_dim
    data_size = lax.axis_size("dp")
    tensor_size = lax.axis_size("tensor")
    quarter = tokens // tensor_size
    experts = local_experts * data_size
    score_scale = head_dim ** (-0.5)
    row0 = lax.axis_index("tensor") * quarter

    def mine(array):
        return lax.dynamic_slice_in_dim(array, row0, quarter, 0)

    expert_ids = jnp.arange(experts, dtype=jnp.int32)
    dense = jnp.sum(
        jnp.where(mine(routes)[:, :, None] == expert_ids[None, None, :], mine(route_weights)[:, :, None], 0.0),
        axis=1,
    )
    dense_high = dense.astype(bf)
    dense_low = (dense - dense_high.astype(f32)).astype(bf)
    spare = -2 * experts % LANES
    packed = jnp.concatenate(
        [mine(out_grad), dense_high, dense_low, jnp.zeros((quarter, spare), bf)], axis=1
    )
    rows = data_size * quarter
    units = local_experts * hidden_part
    own_weights = jnp.concatenate(
        [
            jnp.transpose(w_gate_up, (2, 0, 3, 1)).reshape(2, units, model_width),
            w_down.reshape(1, units, model_width),
        ],
        axis=0,
    )
    all_weights = lax.all_gather(own_weights, "tensor")
    hidden = hidden_in.astype(f32)
    hat_one, inv_one = rms_parts(hidden)
    normed = (hat_one * norm1_gain).astype(bf)
    query_proj = jnp.dot(normed, query_weight, preferred_element_type=f32).reshape(
        tokens, local_heads, head_dim
    )
    key_proj = jnp.dot(normed, key_weight, preferred_element_type=f32)
    value_low = jnp.dot(normed, value_weight, preferred_element_type=f32).astype(bf)
    places, starts = sequence_layout(seq_lens[0], tokens)
    cosine_table, sine_table = rotary_tables(places - starts, head_dim)
    query_hat, query_inv = rms_parts(query_proj)
    query_low = rotate(
        query_hat * query_gain, cosine_table[:, None, :], sine_table[:, None, :]
    ).astype(bf)
    key_hat, key_inv = rms_parts(key_proj)
    key_low = rotate(key_hat * key_gain, cosine_table, sine_table).astype(bf)
    visible = (places[None, :] <= places[:, None]) & (places[None, :] >= starts[:, None])
    scores = jnp.einsum("thd,sd->hts", query_low, key_low, preferred_element_type=f32) * score_scale
    exponent = jnp.where(visible[None], jnp.exp(scores), 0.0)
    totals = jnp.sum(exponent, axis=-1, keepdims=True)
    log_totals = jnp.log(totals)
    soft_low = (exponent / totals).astype(bf)
    mixed_low = (
        jnp.einsum("hts,sd->thd", soft_low, value_low, preferred_element_type=f32)
        .reshape(tokens, local_heads * head_dim)
        .astype(bf)
    )
    hidden_q = mine(hidden_in)
    hat_one_q, inv_one_q = rms_parts(hidden_q.astype(f32))
    partial = jnp.dot(mixed_low, out_weight, preferred_element_type=f32).astype(bf)
    middle, inputs, gathered = exchange_tokens(
        data_size, partial, hidden_q, packed, norm2_gain
    )
    inputs = inputs.reshape(rows, model_width)
    gathered = gathered.reshape(rows, -1)
    grads_all = gathered[:, :model_width]
    dense_all = gathered[:, model_width : model_width + experts].astype(f32) + gathered[
        :, model_width + experts : model_width + 2 * experts
    ].astype(f32)
    weight_all = lax.dynamic_slice_in_dim(
        dense_all, lax.axis_index("dp") * local_experts, local_experts, 1
    )
    weight_cols = jnp.broadcast_to(
        weight_all[:, None, :, None], (rows, tensor_size, local_experts, hidden_part)
    ).reshape(rows, tensor_size, units)
    hat_two, inv_two = rms_parts(middle)

    def project(left, which):
        return jnp.einsum("td,rud->tru", left, all_weights[:, which], preferred_element_type=f32)

    gate_act = project(inputs, 0)
    upward = project(inputs, 1)
    sigmoid_gate = jax.nn.sigmoid(gate_act)
    active = gate_act * sigmoid_gate * upward
    weighted_low = (weight_cols * active).astype(bf)
    mixture_part = jnp.einsum(
        "tru,rud->td", weighted_low, all_weights[:, 2], preferred_element_type=f32
    ).astype(bf)
    mixture = lax.psum_scatter(mixture_part, "dp", tiled=True).astype(f32)
    hidden_out = (middle + mixture).astype(bf)
    grad_active = weight_cols * project(grads_all, 2)
    grad_gate = (
        grad_active * upward * sigmoid_gate * (1.0 + gate_act * (1.0 - sigmoid_gate))
    ).astype(bf)
    grad_up = (grad_active * gate_act * sigmoid_gate).astype(bf)
    grad_normed_part = jnp.einsum(
        "tru,rud->td", grad_gate, all_weights[:, 0], preferred_element_type=f32
    ) + jnp.einsum("tru,rud->td", grad_up, all_weights[:, 1], preferred_element_type=f32)
    grad_normed_two = lax.psum_scatter(grad_normed_part.astype(bf), "dp", tiled=True).astype(f32)
    weight_grads = jnp.stack(
        [
            jnp.einsum("tru,td->rud", grad_gate, inputs, preferred_element_type=f32).astype(bf),
            jnp.einsum("tru,td->rud", grad_up, inputs, preferred_element_type=f32).astype(bf),
            jnp.einsum("tru,td->rud", weighted_low, grads_all, preferred_element_type=f32).astype(bf),
        ],
        axis=1,
    )
    own_grads = (
        lax.psum_scatter(weight_grads.reshape(-1, model_width), "tensor", tiled=True)
        .astype(f32)
        .reshape(3, units, model_width)
    )
    grad_w_gate_up = jnp.transpose(
        own_grads[:2].reshape(2, local_experts, hidden_part, model_width), (1, 3, 0, 2)
    )
    grad_w_down = own_grads[2].reshape(local_experts, hidden_part, model_width)

    grad_out = mine(out_grad).astype(f32)
    grad_gain_two = jnp.sum(grad_normed_two * hat_two, axis=0)
    grad_middle = grad_out + rms_back(grad_normed_two * norm2_gain, hat_two, inv_two)
    grad_mid_low = lax.all_gather(grad_middle.astype(bf), "tensor", tiled=True)
    grad_out_weight = jnp.einsum("ti,td->id", mixed_low, grad_mid_low, preferred_element_type=f32)
    grad_mixed = (
        jnp.einsum("td,id->ti", grad_mid_low, out_weight, preferred_element_type=f32)
        .astype(bf)
        .reshape(tokens, local_heads, head_dim)
    )
    scores_again = (
        jnp.einsum("thd,sd->hts", query_low, key_low, preferred_element_type=f32) * score_scale
    )
    soft_again = jnp.where(visible[None], jnp.exp(scores_again - log_totals), 0.0)
    grad_soft = jnp.einsum("thd,sd->hts", grad_mixed, value_low, preferred_element_type=f32)
    grad_scores = (
        soft_again * (grad_soft - jnp.sum(soft_again * grad_soft, axis=-1, keepdims=True))
    ).astype(bf)
    grad_values = jnp.einsum(
        "hts,thd->sd", soft_again.astype(bf), grad_mixed, preferred_element_type=f32
    ).astype(bf)
    grad_query_rot = score_scale * jnp.einsum(
        "hts,sd->thd", grad_scores, key_low, preferred_element_type=f32
    )
    grad_key_rot = score_scale * jnp.einsum(
        "hts,thd->sd", grad_scores, query_low, preferred_element_type=f32
    )
    grad_query_norm = rotate_back(grad_query_rot, cosine_table[:, None, :], sine_table[:, None, :])
    grad_query_gain = jnp.sum(grad_query_norm * query_hat, axis=(0, 1))
    grad_query_low = (
        rms_back(grad_query_norm * query_gain, query_hat, query_inv)
        .reshape(tokens, local_heads * head_dim)
        .astype(bf)
    )
    grad_key_norm = rotate_back(grad_key_rot, cosine_table, sine_table)
    grad_key_gain = jnp.sum(grad_key_norm * key_hat, axis=0)
    grad_key_low = rms_back(grad_key_norm * key_gain, key_hat, key_inv).astype(bf)
    grad_all_low = jnp.concatenate([grad_query_low, grad_key_low, grad_values], axis=1)
    grad_in_weights = jnp.einsum(
        "ti,tj->ij", normed, grad_all_low, preferred_element_type=f32
    ).astype(bf)
    grad_normed_one = jnp.einsum("tj,ij->ti", grad_query_low, query_weight, preferred_element_type=f32)
    grad_normed_one = grad_normed_one + jnp.einsum(
        "tj,ij->ti", grad_key_low, key_weight, preferred_element_type=f32
    )
    grad_normed_one = grad_normed_one + jnp.einsum(
        "tj,ij->ti", grad_values, value_weight, preferred_element_type=f32
    )
    gains = jnp.concatenate([grad_gain_two, grad_query_gain, grad_key_gain]).reshape(1, -1)
    final = finish_sums(
        data_size,
        grad_in_weights,
        grad_out_weight.astype(bf),
        grad_normed_one.astype(bf),
        grad_middle,
        hidden_q,
        hidden_out,
        norm1_gain,
        gains,
        head_dim,
    )
    gains = final[6].reshape(-1)
    return (
        final[0],
        final[1],
        gains[:model_width],
        final[2],
        final[3],
        final[4],
        gains[2 * model_width : 2 * model_width + head_dim],
        gains[2 * model_width + head_dim :],
        final[5],
        gains[model_width : 2 * model_width],
        grad_w_gate_up,
        grad_w_down,
    )


def solution(mesh):
    in_specs = (
        P("dp", None),
        P("dp", None),
        P(),
        P(None, "tensor"),
        P(None, "tensor"),
        P(None, "tensor"),
        P(),
        P(),
        P("tensor", None),
        P(),
        P("dp", None, None, "tensor"),
        P("dp", "tensor", None),
        P("dp", None),
        P("dp", None),
        P("dp", None),
    )
    out_specs = (
        P("dp", None),
        P("dp", None),
        P(),
        P(None, "tensor"),
        P(None, "tensor"),
        P(None, "tensor"),
        P(),
        P(),
        P("tensor", None),
        P(),
        P("dp", None, None, "tensor"),
        P("dp", "tensor", None),
    )
    return jax.shard_map(local, mesh=mesh, in_specs=in_specs, out_specs=out_specs, check_vma=False)
```

```python
import functools
import math

import jax
import jax.numpy as jnp
from jax import lax
from jax.experimental import pallas as pl
from jax.experimental.pallas import tpu as pltpu
from jax.sharding import PartitionSpec as P

EPSILON = 1e-06
ROPE_BASE = 1000000.0


def rms_parts(values):
    inverse = lax.rsqrt(jnp.mean(values * values, axis=-1, keepdims=True) + EPSILON)
    return (values * inverse, inverse)


def rms_back(grad_hat, normal_hat, inverse):
    return inverse * (
        grad_hat - normal_hat * jnp.mean(grad_hat * normal_hat, axis=-1, keepdims=True)
    )


def rotary_tables(positions, head_dim):
    halves = jnp.arange(head_dim // 2, dtype=jnp.float32)
    inverse = jnp.exp(halves * (-2.0 * math.log(ROPE_BASE) / head_dim))
    angles = positions.astype(jnp.float32)[:, None] * inverse[None, :]
    return (jnp.cos(angles), jnp.sin(angles))


def rotate(values, cosine_table, sine_table):
    middle_index = values.shape[-1] // 2
    first_half = values[..., :middle_index]
    second = values[..., middle_index:]
    return jnp.concatenate(
        [
            first_half * cosine_table - second * sine_table,
            second * cosine_table + first_half * sine_table,
        ],
        axis=-1,
    )


def rotate_back(gradient, cosine_table, sine_table):
    middle_index = gradient.shape[-1] // 2
    first_half = gradient[..., :middle_index]
    second = gradient[..., middle_index:]
    return jnp.concatenate(
        [
            first_half * cosine_table + second * sine_table,
            second * cosine_table - first_half * sine_table,
        ],
        axis=-1,
    )


def sequence_layout(lengths, token_count):
    endings = jnp.cumsum(lengths)
    places = jnp.arange(token_count, dtype=jnp.int32)
    starts = jnp.sum(jnp.where(endings[None, :] <= places[:, None], lengths[None, :], 0), axis=1)
    return (places, starts)


LANES = 128
MESH = pl.DeviceIdType.MESH
VMEM_LIMIT = 60 * 1024 * 1024


def ring_place(index, size):
    return jnp.where(index % 2 == 0, index // 2, size - (index + 1) // 2)


def ring_index(place, size):
    place = place % size
    return jnp.where(place < size // 2, 2 * place, 2 * size - 1 - 2 * place)


def tensor_peers():
    own = lax.axis_index("tensor")
    partner = own + 1 - 2 * (own % 2)
    across = (own + 2) % 4
    return own, partner, across


def greet(devices):
    barrier = pltpu.get_barrier_semaphore()
    for device in devices:
        pl.semaphore_signal(barrier, inc=1, device_id=device, device_id_type=MESH)
    pl.semaphore_wait(barrier, len(devices))


def push(source, target, sems, device):
    return pltpu.make_async_remote_copy(
        src_ref=source,
        dst_ref=target,
        send_sem=sems[0],
        recv_sem=sems[1],
        device_id=device,
        device_id_type=MESH,
    )


def slot_of(delta, size):
    delta = (delta + size // 2 - 1) % size - (size // 2 - 1)
    if delta == 0:
        return size - 1
    if delta == size // 2:
        return size - 2
    return 2 * delta - 1 if delta > 0 else -2 * delta - 2


class GatherRing:
    def __init__(self, size, blocks, sems, parts=2):
        self.size, self.blocks, self.sems, self.parts = size, blocks, sems, parts
        self.place = ring_place(lax.axis_index("dp"), size)
        self.sent = []
        self.live = {}

    def send(self, step):
        size, half = self.size, self.blocks.shape[1] // 2
        piece = half // self.parts
        for part in range(self.parts):
            for way in (0, 1):
                sign = 1 - 2 * way
                rows = pl.ds(way * half + part * piece, piece)
                source = self.blocks.at[slot_of(-sign * step, size), rows]
                target = self.blocks.at[slot_of(-sign * (step + 1), size), rows]
                device = (ring_index(self.place + size + sign, size), lax.axis_index("tensor"))
                copy = push(
                    source,
                    target,
                    (self.sems.at[0, way, step, part], self.sems.at[1, way, step, part]),
                    device,
                )
                if step > 0:
                    self.live[step - 1, part, way].wait_recv()
                copy.start()
                self.live[step, part, way] = copy
                self.sent.append(copy)

    def step(self, step):
        if step + 1 < self.size - 1:
            self.send(step + 1)
        else:
            for part in range(self.parts):
                for way in (0, 1):
                    self.live[step, part, way].wait_recv()

    def finish(self):
        for copy in self.sent:
            copy.wait_send()


def row_loop(total, rows, body):
    def run(index, carry):
        body(pl.ds(pl.multiple_of(index * rows, rows), rows))
        return carry

    lax.fori_loop(0, total // rows, run, 0)


def exchange_tokens_body(
    size,
    part_ref,
    token_ref,
    pack_ref,
    gain_ref,
    middle_ref,
    inputs_ref,
    packs_ref,
    from_partner,
    from_across,
    joined,
    ring_sems,
    pack_sems,
    side_sems,
    local_sem,
):
    f32 = jnp.float32
    dp = lax.axis_index("dp")
    own, partner, across = tensor_peers()
    far_partner = (partner + 2) % 4
    quarter = token_ref.shape[0]
    place = ring_place(dp, size)
    neighbours = [(ring_index(place + 1, size), own), (ring_index(place + size - 1, size), own)]
    greet(neighbours + [(dp, partner), (dp, across)])

    def part_rows(index):
        return pl.ds(pl.multiple_of(index * quarter, quarter), quarter)

    def side(index):
        return (side_sems.at[0, index], side_sems.at[1, index])

    first = push(part_ref.at[part_rows(far_partner)], from_partner.at[1], side(0), (dp, partner))
    second = push(part_ref.at[part_rows(partner)], from_partner.at[0], side(1), (dp, partner))
    first.start()
    second.start()
    keep = pltpu.make_async_copy(pack_ref, packs_ref.at[size - 1], local_sem)
    keep.start()
    keep.wait()
    packs = GatherRing(size, packs_ref, pack_sems)
    packs.send(0)
    first.wait_recv()
    base = across * quarter

    def join(rows):
        there = pl.ds(pl.multiple_of(base + rows.start, 16), rows.size)
        joined[rows, :] = (
            part_ref[there, :].astype(f32) + from_partner[1, rows, :].astype(f32)
        ).astype(jnp.bfloat16)

    row_loop(quarter, 16, join)
    third = push(joined, from_across, side(2), (dp, across))
    third.start()
    packs.step(0)
    second.wait_recv()
    third.wait_recv()
    mine = own * quarter

    def norm(rows):
        there = pl.ds(pl.multiple_of(mine + rows.start, 16), rows.size)
        middle = (
            token_ref[rows, :].astype(f32)
            + part_ref[there, :].astype(f32)
            + from_partner[0, rows, :].astype(f32)
            + from_across[rows, :].astype(f32)
        )
        middle_ref[rows, :] = middle
        inverse = lax.rsqrt(jnp.mean(middle * middle, axis=-1, keepdims=True) + EPSILON)
        inputs_ref[size - 1, rows, :] = (middle * inverse * gain_ref[...]).astype(jnp.bfloat16)

    row_loop(quarter, 16, norm)
    tokens = GatherRing(size, inputs_ref, ring_sems)
    tokens.send(0)
    for step in range(1, size - 1):
        packs.step(step)
        tokens.step(step - 1)
    tokens.step(size - 2)
    packs.finish()
    tokens.finish()
    first.wait_send()
    second.wait_send()
    third.wait_send()


def exchange_tokens(size, partial, token_rows, packed, gain):
    quarter, width = token_rows.shape
    columns = packed.shape[1]
    bf = jnp.bfloat16
    vmem = pl.BlockSpec(memory_space=pltpu.VMEM)
    dma = pltpu.SemaphoreType.DMA
    return pl.pallas_call(
        functools.partial(exchange_tokens_body, size),
        out_shape=(
            jax.ShapeDtypeStruct((quarter, width), jnp.float32),
            jax.ShapeDtypeStruct((size, quarter, width), bf),
            jax.ShapeDtypeStruct((size, quarter, columns), bf),
        ),
        in_specs=[vmem] * 4,
        out_specs=(vmem,) * 3,
        scratch_shapes=[
            pltpu.VMEM((2, quarter, width), bf),
            pltpu.VMEM((quarter, width), bf),
            pltpu.VMEM((quarter, width), bf),
            dma((2, 2, size - 1, 2)),
            dma((2, 2, size - 1, 2)),
            dma((2, 3)),
            dma(()),
        ],
        compiler_params=pltpu.CompilerParams(
            collective_id=0, has_side_effects=True, vmem_limit_bytes=VMEM_LIMIT
        ),
        name="exchange_tokens",
    )(partial, token_rows, packed, gain.reshape(1, -1))


def matmul_nt(left, right):
    return lax.dot_general(left, right, (((1,), (1,)), ((), ())), preferred_element_type=jnp.float32)


def matmul(left, right):
    return lax.dot_general(left, right, (((1,), (0,)), ((), ())), preferred_element_type=jnp.float32)


def run_experts_body(
    size,
    local_experts,
    experts,
    inputs_ref,
    packs_ref,
    weights_ref,
    member_ref,
    middle_ref,
    gain_ref,
    mix_ref,
    wgrad_ref,
    gmid_ref,
    gmid_all,
    gain_out,
    weights,
    hidden,
    parts,
    slots,
    turned,
    stage,
    totals,
    load_sems,
    ring_sems,
    side_sems,
    store_sems,
):
    f32, bf = jnp.float32, jnp.bfloat16
    dp = lax.axis_index("dp")
    own, partner, across = tensor_peers()
    width = inputs_ref.shape[1]
    quarter = inputs_ref.shape[0] // size
    pair = 2 * quarter
    half = size // 2
    units = weights.shape[1]
    members = weights_ref.shape[0]
    span = units // members
    cut = width // 2
    wide = 512
    place = ring_place(dp, size)
    forward = (ring_index(place + 1, size), own)
    backward = (ring_index(place + size - 1, size), own)
    greet([forward, backward, (dp, partner), (dp, across)])
    pieces = units // LANES
    each = pieces // members

    def load(piece):
        source = weights_ref.at[piece // each, :, pl.ds((piece % each) * LANES, LANES), :]
        target = weights.at[:, pl.ds(piece * LANES, LANES), :]
        return pltpu.make_async_copy(source, target, load_sems.at[piece])

    for piece in range(pieces):
        load(piece).start()

    def ring_copy(way, step, source):
        device = forward if way == 0 else backward
        return push(
            source, slots.at[way, step], (ring_sems.at[0, way, step], ring_sems.at[1, way, step]), device
        )

    def columns_of(way):
        return pl.ds(way * cut, cut)

    def ring_step(step, blocks, first=False):
        for way in (0, 1):
            if first:
                source = parts.at[blocks[way], :, columns_of(way)]
            else:
                source = slots.at[way, step - 1]
                ring_copy(way, step - 1, source).wait_recv()

                def add(rows):
                    slots[way, step - 1, rows, :] = (
                        slots[way, step - 1, rows, :].astype(f32)
                        + parts[blocks[way], rows, columns_of(way)].astype(f32)
                    ).astype(bf)

                row_loop(quarter, 16, add)
            ring_copy(way, step, source).start()

    def do_pair(index, carry):
        rows = pl.ds(pl.multiple_of(index * pair, pair), pair)
        tail = packs_ref[rows, width:].astype(f32)
        lane = lax.broadcasted_iota(jnp.int32, tail.shape, 1)
        shares = []
        for expert in range(local_experts):
            name = dp * local_experts + expert
            picked = (lane == name) | (lane == experts + name)
            shares.append(jnp.sum(jnp.where(picked, tail, 0.0), axis=1, keepdims=True))

        def do_units(tile, carry):
            here = pl.ds(pl.multiple_of(tile * wide, wide), wide)

            @pl.when(index == 0)
            def _():
                for piece in range(wide // LANES):
                    load(tile * (wide // LANES) + piece).wait()

            scale = shares[0] * member_ref[0:1, here]
            for expert in range(1, local_experts):
                scale = scale + shares[expert] * member_ref[expert : expert + 1, here]
            tokens = inputs_ref[rows, :]
            gate = matmul_nt(tokens, weights[0, here, :])
            upward = matmul_nt(tokens, weights[1, here, :])
            grads = scale * matmul_nt(packs_ref[rows, :width], weights[2, here, :])
            share = jax.nn.sigmoid(gate)
            silu = gate * share
            hidden[0, rows, here] = (grads * upward * share * (1.0 + gate * (1.0 - share))).astype(bf)
            hidden[1, rows, here] = (grads * silu).astype(bf)
            hidden[2, rows, here] = (scale * silu * upward).astype(bf)
            return carry

        lax.fori_loop(0, units // wide, do_units, 0)

        def do_columns(tile, carry):
            here = pl.ds(pl.multiple_of(tile * wide, wide), wide)
            sums = matmul(hidden[0, rows, :], weights[0, :, here]) + matmul(
                hidden[1, rows, :], weights[1, :, here]
            )
            low = sums.astype(bf)
            parts[2 * index, :, here] = low[:quarter]
            parts[2 * index + 1, :, here] = low[quarter:]
            return carry

        lax.fori_loop(0, width // wide, do_columns, 0)

        @pl.when(index == 0)
        def _():
            ring_step(0, (0, 1), first=True)

        @pl.when(index > 0)
        def _():
            ring_step(index, (2 * index, 2 * index + 1 - index // (half - 1)))

        return carry

    lax.fori_loop(0, half, do_pair, 0)

    def mix_pairs(first, last):
        def run(index, carry):
            rows = pl.ds(pl.multiple_of(index * pair, pair), pair)
            left = ring_index(place + size - 1 - index, size)
            right = ring_index(place + (index + 1) % half, size)

            def do_columns(tile, carry):
                here = pl.ds(pl.multiple_of(tile * wide, wide), wide)
                low = matmul(hidden[2, rows, :], weights[2, :, here]).astype(bf)
                mix_ref[left, :, here] = low[:quarter]
                mix_ref[right, :, here] = low[quarter:]
                return carry

            lax.fori_loop(0, width // wide, do_columns, 0)
            return carry

        lax.fori_loop(first, last, run, 0)

    def store(kind, member, slot):
        return pltpu.make_async_copy(stage.at[slot], wgrad_ref.at[member, kind], store_sems.at[slot])

    def weight_grads(first, last):
        def run(index, carry):
            kind = index // members
            member = index % members
            slot = index % 2

            @pl.when(index >= 2)
            def _():
                store(kind, member, slot).wait()

            rows = pl.ds(pl.multiple_of(member * span, span), span)
            for chunk in range(half):
                some = pl.ds(chunk * pair, pair)
                turned[:, some] = hidden[kind, some, rows].T

            def do_columns(tile, carry):
                here = pl.ds(pl.multiple_of(tile * wide, wide), wide)
                source = inputs_ref if first < 2 * members else packs_ref
                stage[slot, :, here] = matmul(turned[...], source[:, here]).astype(bf)
                return carry

            lax.fori_loop(0, width // wide, do_columns, 0)
            store(kind, member, slot).start()
            return carry

        lax.fori_loop(first, last, run, 0)

    def final_sum():
        totals[...] = jnp.zeros_like(totals)
        for way in (0, 1):
            ring_copy(way, size - 2, slots.at[way, size - 2]).wait_recv()
        base = own * quarter

        def finish(rows):
            sums = jnp.concatenate(
                [slots[0, size - 2, rows, :].astype(f32), slots[1, size - 2, rows, :].astype(f32)],
                axis=-1,
            ) + parts[size - 1, rows, :].astype(f32)
            middle = middle_ref[rows, :]
            inverse = lax.rsqrt(jnp.mean(middle * middle, axis=-1, keepdims=True) + EPSILON)
            hat = middle * inverse
            product = sums * hat
            totals[...] += product[:8] + product[8:]
            scaled = sums * gain_ref[...]
            back = inverse * (scaled - hat * jnp.mean(scaled * hat, axis=-1, keepdims=True))
            above = packs_ref[
                pl.ds(pl.multiple_of((size - 1) * quarter + rows.start, 16), rows.size), :width
            ]
            grad = above.astype(f32) + back
            gmid_ref[rows, :] = grad
            gmid_all[pl.ds(pl.multiple_of(base + rows.start, 16), rows.size), :] = grad.astype(bf)

        row_loop(quarter, 16, finish)
        gain_out[...] = jnp.sum(totals[...], axis=0, keepdims=True)

    def rows_of(index):
        return pl.ds(pl.multiple_of(index * quarter, quarter), quarter)

    def spread(index, whose, device):
        ref = gmid_all.at[rows_of(whose)]
        return push(ref, ref, (side_sems.at[0, index], side_sems.at[1, index]), device)

    def first_spread():
        spread(0, own, (dp, across)).start()
        spread(1, own, (dp, partner)).start()

    def second_spread():
        spread(0, own, (dp, across)).wait_recv()
        spread(2, across, (dp, partner)).start()

    events = []
    for step in range(half, size - 1):
        delta = -(1 + step)
        blocks = (slot_of(delta, size), slot_of(-delta, size))
        events.append(functools.partial(ring_step, step, blocks))

    def closing():
        final_sum()
        first_spread()

    events.append(closing)
    events.append(second_spread)
    work = [functools.partial(mix_pairs, 0, half // 2), functools.partial(mix_pairs, half // 2, half)]
    for first in range(0, 3 * members, 2):
        work.append(functools.partial(weight_grads, first, first + 2))
    done = 0
    for number, piece in enumerate(work):
        piece()
        upto = min(len(events), -(-(number + 1) * len(events) // (len(work) - 2)))
        while done < upto:
            events[done]()
            done += 1
    for slot in (0, 1):
        store(0, 0, slot).wait()
    spread(1, own, (dp, partner)).wait_recv()
    spread(2, across, (dp, partner)).wait_recv()
    for index, device in ((0, across), (1, partner), (2, partner)):
        spread(index, own, (dp, device)).wait_send()
    for way in (0, 1):
        for step in range(size - 1):
            ring_copy(way, step, slots.at[way, step]).wait_send()


def run_experts(size, inputs, packs, weights, middle, gain, experts):
    bf, f32 = jnp.bfloat16, jnp.float32
    members, _, span, width = weights.shape
    local_experts = experts // size
    rows = inputs.shape[0]
    quarter = rows // size
    units = members * span
    expert_of = (jnp.arange(units, dtype=jnp.int32) // (span // local_experts)) % local_experts
    member = (expert_of[None, :] == jnp.arange(local_experts, dtype=jnp.int32)[:, None]).astype(f32)
    vmem = pl.BlockSpec(memory_space=pltpu.VMEM)
    anywhere = pl.BlockSpec(memory_space=pl.ANY)
    dma = pltpu.SemaphoreType.DMA
    return pl.pallas_call(
        functools.partial(run_experts_body, size, local_experts, experts),
        out_shape=(
            jax.ShapeDtypeStruct((size, quarter, width), bf),
            jax.ShapeDtypeStruct((members, 3, span, width), bf),
            jax.ShapeDtypeStruct((quarter, width), f32),
            jax.ShapeDtypeStruct((members * quarter, width), bf),
            jax.ShapeDtypeStruct((1, width), f32),
        ),
        in_specs=[vmem, vmem, anywhere, vmem, vmem, vmem],
        out_specs=(vmem, anywhere, vmem, vmem, vmem),
        scratch_shapes=[
            pltpu.VMEM((3, units, width), bf),
            pltpu.VMEM((3, rows, units), bf),
            pltpu.VMEM((size, quarter, width), bf),
            pltpu.VMEM((2, size - 1, quarter, width // 2), bf),
            pltpu.VMEM((span, rows), bf),
            pltpu.VMEM((2, span, width), bf),
            pltpu.VMEM((8, width), f32),
            dma((units // LANES,)),
            dma((2, 2, size - 1)),
            dma((2, 3)),
            dma((2,)),
        ],
        compiler_params=pltpu.CompilerParams(
            collective_id=2, has_side_effects=True, vmem_limit_bytes=VMEM_LIMIT
        ),
        name="run_experts",
    )(inputs, packs, weights, member, middle, gain.reshape(1, -1))


def finish_sums_body(
    size,
    qkv_ref,
    out_ref,
    normed_ref,
    middle_ref,
    token_ref,
    gain_ref,
    gains_ref,
    grad_all,
    gather_a,
    gather_b,
    gains_out,
    slots_a,
    slots_b,
    from_partner,
    from_across,
    joined,
    totals,
    pair_gains,
    ring_gains,
    sems_a,
    sems_b,
    ring_sems,
    side_sems,
):
    f32, bf = jnp.float32, jnp.bfloat16
    dp = lax.axis_index("dp")
    own, partner, across = tensor_peers()
    far_partner = (partner + 2) % 4
    quarter, width = token_ref.shape
    place = ring_place(dp, size)
    forward = (ring_index(place + 1, size), own)
    backward = (ring_index(place + size - 1, size), own)
    ways = ((forward, 1), (backward, -1))
    greet([forward, backward, (dp, partner), (dp, across)])
    waits = []

    def start(copy):
        copy.start()
        waits.append(copy)
        return copy

    sets = (
        (qkv_ref, slots_a, gather_a, sems_a),
        (out_ref, slots_b, gather_b, sems_b),
    )

    def block_of(ref, block, way):
        rows = ref.shape[0] // size
        cut = ref.shape[1] // 2
        return (pl.ds(pl.multiple_of(block * rows, rows), rows), pl.ds(way * cut, cut))

    def wrap(value):
        return (value + 2 * size) % size

    live = {}

    def reduce_send(step):
        for which, (ref, slots, _, sems) in enumerate(sets):
            for way, (device, sign) in enumerate(ways):
                if step == 0:
                    source = ref.at[block_of(ref, wrap(place - sign), way)]
                else:
                    add_own(which, way, step - 1)
                    source = slots.at[way, step - 1]
                live[which, way, step] = start(
                    push(
                        source,
                        slots.at[way, step],
                        (sems.at[0, way, step], sems.at[1, way, step]),
                        device,
                    )
                )

    def add_own(which, way, step):
        ref, slots, blocks, _ = sets[which]
        live[which, way, step].wait_recv()
        sign = ways[way][1]
        rows, columns = block_of(ref, wrap(place - sign * (2 + step)), way)
        base = rows.start

        def add(inner):
            there = pl.ds(pl.multiple_of(base + inner.start, 16), inner.size)
            sums = (slots[way, step, inner, :].astype(f32) + ref[there, columns].astype(f32)).astype(bf)
            if step == size - 2:
                blocks[place, inner, columns] = sums
            else:
                slots[way, step, inner, :] = sums

        row_loop(ref.shape[0] // size, 16, add)

    gather = {}

    def gather_send(step):
        for which, (ref, _, blocks, sems) in enumerate(sets):
            cut = ref.shape[1] // 2
            for way, (device, sign) in enumerate(ways):
                if step == 0:
                    add_own(which, way, size - 2)
                else:
                    gather[which, way, step - 1].wait_recv()
                source = blocks.at[wrap(place - sign * step), :, pl.ds(way * cut, cut)]
                gather[which, way, step] = start(
                    push(
                        source,
                        source,
                        (sems.at[0, way, size - 1 + step], sems.at[1, way, size - 1 + step]),
                        device,
                    )
                )

    def part_rows(index):
        return pl.ds(pl.multiple_of(index * quarter, quarter), quarter)

    def side(index):
        return (side_sems.at[0, index], side_sems.at[1, index])

    reduce_send(0)
    first = start(
        push(normed_ref.at[part_rows(far_partner)], from_partner.at[1], side(0), (dp, partner))
    )
    second = start(
        push(normed_ref.at[part_rows(partner)], from_partner.at[0], side(1), (dp, partner))
    )
    mine = part_rows(own)
    spread = []
    reduce_send(1)
    first.wait_recv()
    away = across * quarter

    def join(rows):
        there = pl.ds(pl.multiple_of(away + rows.start, 16), rows.size)
        joined[rows, :] = (
            normed_ref[there, :].astype(f32) + from_partner[1, rows, :].astype(f32)
        ).astype(bf)

    row_loop(quarter, 16, join)
    third = start(push(joined, from_across, side(2), (dp, across)))
    reduce_send(2)
    second.wait_recv()
    third.wait_recv()
    home = own * quarter
    totals[...] = jnp.zeros_like(totals)

    def finish(rows):
        there = pl.ds(pl.multiple_of(home + rows.start, 16), rows.size)
        grads = (
            normed_ref[there, :].astype(f32)
            + from_partner[0, rows, :].astype(f32)
            + from_across[rows, :].astype(f32)
        )
        hidden = token_ref[rows, :].astype(f32)
        inverse = lax.rsqrt(jnp.mean(hidden * hidden, axis=-1, keepdims=True) + EPSILON)
        hat = hidden * inverse
        product = grads * hat
        totals[:, :width] += jnp.sum(product.reshape(-1, 8, width), axis=0)
        scaled = grads * gain_ref[...]
        back = inverse * (scaled - hat * jnp.mean(scaled * hat, axis=-1, keepdims=True))
        joined_grad = (middle_ref[rows, :] + back).astype(bf)
        grad_all[there, :] = joined_grad

    row_loop(quarter, 16, finish)
    spread.append(start(push(grad_all.at[mine], grad_all.at[mine], side(3), (dp, across))))
    spread.append(start(push(grad_all.at[mine], grad_all.at[mine], side(4), (dp, partner))))
    pair_gains[0, :, :width] = jnp.sum(totals[:, :width], axis=0, keepdims=True)
    pair_gains[0, :, width:] = gains_ref[...]
    swap = start(push(pair_gains.at[0], pair_gains.at[1], side(5), (dp, partner)))
    reduce_send(3)
    far = part_rows(across)
    spread[0].wait_recv()
    spread.append(start(push(grad_all.at[far], grad_all.at[far], side(6), (dp, partner))))
    swap.wait_recv()
    pair_gains[2] = pair_gains[0] + pair_gains[1]
    swap = start(push(pair_gains.at[2], pair_gains.at[3], side(7), (dp, across)))
    for step in range(4, size - 1):
        reduce_send(step)
    swap.wait_recv()
    ring_gains[place] = pair_gains[2] + pair_gains[3]
    gather_send(0)
    small = None
    for step in range(size - 1):
        if small is not None:
            small.wait_recv()
        ref = ring_gains.at[wrap(place - step)]
        small = start(push(ref, ref, (ring_sems.at[0, step], ring_sems.at[1, step]), forward))
        if step > 0:
            gather_send(step)
    small.wait_recv()
    for copy in (gather[which, way, size - 2] for which in (0, 1) for way in (0, 1)):
        copy.wait_recv()
    gains_out[...] = jnp.sum(ring_gains[...], axis=0)
    spread[1].wait_recv()
    spread[2].wait_recv()
    for copy in waits:
        copy.wait_send()


def finish_sums(size, grad_in, grad_out, grad_normed, grad_middle, token_rows, gain, gains):
    bf, f32 = jnp.bfloat16, jnp.float32
    quarter, width = token_rows.shape
    tokens = grad_normed.shape[0]
    vmem = pl.BlockSpec(memory_space=pltpu.VMEM)
    dma = pltpu.SemaphoreType.DMA
    rows_a, rows_b = grad_in.shape[0] // size, grad_out.shape[0] // size
    cut_a, cut_b = grad_in.shape[1] // 2, grad_out.shape[1] // 2
    count = width + gains.shape[1]
    return pl.pallas_call(
        functools.partial(finish_sums_body, size),
        out_shape=(
            jax.ShapeDtypeStruct((tokens, width), bf),
            jax.ShapeDtypeStruct((size, rows_a, 2 * cut_a), bf),
            jax.ShapeDtypeStruct((size, rows_b, 2 * cut_b), bf),
            jax.ShapeDtypeStruct((1, count), f32),
        ),
        in_specs=[vmem] * 7,
        out_specs=(vmem,) * 4,
        scratch_shapes=[
            pltpu.VMEM((2, size - 1, rows_a, cut_a), bf),
            pltpu.VMEM((2, size - 1, rows_b, cut_b), bf),
            pltpu.VMEM((2, quarter, width), bf),
            pltpu.VMEM((quarter, width), bf),
            pltpu.VMEM((quarter, width), bf),
            pltpu.VMEM((8, width), f32),
            pltpu.VMEM((4, 1, count), f32),
            pltpu.VMEM((size, 1, count), f32),
            dma((2, 2, 2 * size - 2)),
            dma((2, 2, 2 * size - 2)),
            dma((2, size - 1)),
            dma((2, 8)),
        ],
        compiler_params=pltpu.CompilerParams(
            collective_id=1, has_side_effects=True, vmem_limit_bytes=VMEM_LIMIT
        ),
        name="finish_sums",
    )(
        grad_in,
        grad_out,
        grad_normed,
        grad_middle,
        token_rows,
        gain.reshape(1, -1),
        gains,
    )


def large_experts(size, inputs, packs, all_weights, middle, gain, experts, out_rows):
    f32, bf = jnp.float32, jnp.bfloat16
    members, _, units, model_width = all_weights.shape
    local_experts = experts // size
    indices = jnp.arange(size, dtype=jnp.int32)
    half = size // 2
    delta = (ring_place(indices, size) - ring_place(lax.axis_index("dp"), size)) % size
    ahead = jnp.where(delta == half, size - 2, jnp.where(delta == 0, size - 1, 2 * delta - 1))
    slots = jnp.where(delta > half, 2 * (size - delta) - 2, ahead)
    inputs = inputs[slots].reshape(-1, model_width)
    packs = packs[slots].reshape(inputs.shape[0], -1)
    grads_all = packs[:, :model_width]
    shares = packs[:, model_width : model_width + 2 * experts].astype(f32)
    shares = shares[:, :experts] + shares[:, experts:]
    shares = lax.dynamic_slice_in_dim(
        shares, lax.axis_index("dp") * local_experts, local_experts, 1
    )
    weight_cols = jnp.broadcast_to(
        shares[:, None, :, None],
        (shares.shape[0], members, local_experts, units // local_experts),
    ).reshape(-1, members, units)

    def project(left, which):
        return jnp.einsum("td,rud->tru", left, all_weights[:, which], preferred_element_type=f32)

    gate_act = project(inputs, 0)
    upward = project(inputs, 1)
    sigmoid_gate = jax.nn.sigmoid(gate_act)
    active = gate_act * sigmoid_gate * upward
    weighted_low = (weight_cols * active).astype(bf)
    mixture_part = jnp.einsum(
        "tru,rud->td", weighted_low, all_weights[:, 2], preferred_element_type=f32
    ).astype(bf)
    grad_active = weight_cols * project(grads_all, 2)
    grad_gate = (
        grad_active * upward * sigmoid_gate * (1.0 + gate_act * (1.0 - sigmoid_gate))
    ).astype(bf)
    grad_up = (grad_active * gate_act * sigmoid_gate).astype(bf)
    grad_normed_part = jnp.einsum(
        "tru,rud->td", grad_gate, all_weights[:, 0], preferred_element_type=f32
    ) + jnp.einsum("tru,rud->td", grad_up, all_weights[:, 1], preferred_element_type=f32)
    grad_normed_two = lax.psum_scatter(grad_normed_part.astype(bf), "dp", tiled=True).astype(f32)
    weight_grads = jnp.stack(
        [
            jnp.einsum("tru,td->rud", grad_gate, inputs, preferred_element_type=f32).astype(bf),
            jnp.einsum("tru,td->rud", grad_up, inputs, preferred_element_type=f32).astype(bf),
            jnp.einsum("tru,td->rud", weighted_low, grads_all, preferred_element_type=f32).astype(bf),
        ],
        axis=1,
    )
    hat_two, inv_two = rms_parts(middle)
    grad_gain_two = jnp.sum(grad_normed_two * hat_two, axis=0)
    grad_middle = out_rows.astype(f32) + rms_back(grad_normed_two * gain, hat_two, inv_two)
    grad_mid_low = lax.all_gather(grad_middle.astype(bf), "tensor", tiled=True)
    return (mixture_part, weight_grads, grad_middle, grad_mid_low, grad_gain_two)


def local(
    hidden_in,
    seq_lens,
    norm1_gain,
    query_weight,
    key_weight,
    value_weight,
    query_gain,
    key_gain,
    out_weight,
    norm2_gain,
    w_gate_up,
    w_down,
    routes,
    route_weights,
    out_grad,
):
    bf = jnp.bfloat16
    f32 = jnp.float32
    tokens, model_width = hidden_in.shape
    local_experts = w_gate_up.shape[0]
    hidden_part = w_gate_up.shape[3]
    head_dim = query_gain.shape[0]
    local_heads = query_weight.shape[1] // head_dim
    data_size = lax.axis_size("dp")
    tensor_size = lax.axis_size("tensor")
    quarter = tokens // tensor_size
    experts = local_experts * data_size
    score_scale = head_dim ** (-0.5)
    row0 = lax.axis_index("tensor") * quarter

    def mine(array):
        return lax.dynamic_slice_in_dim(array, row0, quarter, 0)

    expert_ids = jnp.arange(experts, dtype=jnp.int32)
    dense = jnp.sum(
        jnp.where(mine(routes)[:, :, None] == expert_ids[None, None, :], mine(route_weights)[:, :, None], 0.0),
        axis=1,
    )
    dense_high = dense.astype(bf)
    dense_low = (dense - dense_high.astype(f32)).astype(bf)
    spare = -2 * experts % LANES
    packed = jnp.concatenate(
        [mine(out_grad), dense_high, dense_low, jnp.zeros((quarter, spare), bf)], axis=1
    )
    rows = data_size * quarter
    units = local_experts * hidden_part
    own_weights = jnp.concatenate(
        [
            jnp.transpose(w_gate_up, (2, 0, 3, 1)).reshape(2, units, model_width),
            w_down.reshape(1, units, model_width),
        ],
        axis=0,
    )
    all_weights = lax.all_gather(own_weights, "tensor")
    hidden = hidden_in.astype(f32)
    hat_one, inv_one = rms_parts(hidden)
    normed = (hat_one * norm1_gain).astype(bf)
    query_proj = jnp.dot(normed, query_weight, preferred_element_type=f32).reshape(
        tokens, local_heads, head_dim
    )
    key_proj = jnp.dot(normed, key_weight, preferred_element_type=f32)
    value_low = jnp.dot(normed, value_weight, preferred_element_type=f32).astype(bf)
    places, starts = sequence_layout(seq_lens[0], tokens)
    cosine_table, sine_table = rotary_tables(places - starts, head_dim)
    query_hat, query_inv = rms_parts(query_proj)
    query_low = rotate(
        query_hat * query_gain, cosine_table[:, None, :], sine_table[:, None, :]
    ).astype(bf)
    key_hat, key_inv = rms_parts(key_proj)
    key_low = rotate(key_hat * key_gain, cosine_table, sine_table).astype(bf)
    visible = (places[None, :] <= places[:, None]) & (places[None, :] >= starts[:, None])
    scores = jnp.einsum("thd,sd->hts", query_low, key_low, preferred_element_type=f32) * score_scale
    exponent = jnp.where(visible[None], jnp.exp(scores), 0.0)
    totals = jnp.sum(exponent, axis=-1, keepdims=True)
    log_totals = jnp.log(totals)
    soft_low = (exponent / totals).astype(bf)
    mixed_low = (
        jnp.einsum("hts,sd->thd", soft_low, value_low, preferred_element_type=f32)
        .reshape(tokens, local_heads * head_dim)
        .astype(bf)
    )
    hidden_q = mine(hidden_in)
    partial = jnp.dot(mixed_low, out_weight, preferred_element_type=f32).astype(bf)
    middle, inputs, gathered = exchange_tokens(data_size, partial, hidden_q, packed, norm2_gain)
    if data_size <= 8:
        mixture_part, weight_grads, grad_middle, grad_mid_low, grad_gain_two = run_experts(
            data_size,
            inputs.reshape(rows, model_width),
            gathered.reshape(rows, -1),
            all_weights,
            middle,
            norm2_gain,
            experts,
        )
        grad_gain_two = grad_gain_two.reshape(-1)
        mixture_part = mixture_part.reshape(rows, model_width)
    else:
        mixture_part, weight_grads, grad_middle, grad_mid_low, grad_gain_two = large_experts(
            data_size, inputs, gathered, all_weights, middle, norm2_gain, experts, mine(out_grad)
        )
    mixture = lax.psum_scatter(mixture_part, "dp", tiled=True).astype(f32)
    hidden_out = lax.all_gather((middle + mixture).astype(bf), "tensor", tiled=True)
    own_grads = (
        lax.psum_scatter(weight_grads.reshape(-1, model_width), "tensor", tiled=True)
        .astype(f32)
        .reshape(3, units, model_width)
    )
    grad_w_gate_up = jnp.transpose(
        own_grads[:2].reshape(2, local_experts, hidden_part, model_width), (1, 3, 0, 2)
    )
    grad_w_down = own_grads[2].reshape(local_experts, hidden_part, model_width)
    grad_out_weight = jnp.einsum("ti,td->id", mixed_low, grad_mid_low, preferred_element_type=f32)
    grad_mixed = (
        jnp.einsum("td,id->ti", grad_mid_low, out_weight, preferred_element_type=f32)
        .astype(bf)
        .reshape(tokens, local_heads, head_dim)
    )
    scores_again = (
        jnp.einsum("thd,sd->hts", query_low, key_low, preferred_element_type=f32) * score_scale
    )
    soft_again = jnp.where(visible[None], jnp.exp(scores_again - log_totals), 0.0)
    grad_soft = jnp.einsum("thd,sd->hts", grad_mixed, value_low, preferred_element_type=f32)
    grad_scores = (
        soft_again * (grad_soft - jnp.sum(soft_again * grad_soft, axis=-1, keepdims=True))
    ).astype(bf)
    grad_values = jnp.einsum(
        "hts,thd->sd", soft_again.astype(bf), grad_mixed, preferred_element_type=f32
    ).astype(bf)
    grad_query_rot = score_scale * jnp.einsum(
        "hts,sd->thd", grad_scores, key_low, preferred_element_type=f32
    )
    grad_key_rot = score_scale * jnp.einsum(
        "hts,thd->sd", grad_scores, query_low, preferred_element_type=f32
    )
    grad_query_norm = rotate_back(grad_query_rot, cosine_table[:, None, :], sine_table[:, None, :])
    grad_query_gain = jnp.sum(grad_query_norm * query_hat, axis=(0, 1))
    grad_query_low = (
        rms_back(grad_query_norm * query_gain, query_hat, query_inv)
        .reshape(tokens, local_heads * head_dim)
        .astype(bf)
    )
    grad_key_norm = rotate_back(grad_key_rot, cosine_table, sine_table)
    grad_key_gain = jnp.sum(grad_key_norm * key_hat, axis=0)
    grad_key_low = rms_back(grad_key_norm * key_gain, key_hat, key_inv).astype(bf)
    grad_all_low = jnp.concatenate([grad_query_low, grad_key_low, grad_values], axis=1)
    grad_in_weights = jnp.einsum(
        "ti,tj->ij", normed, grad_all_low, preferred_element_type=f32
    ).astype(bf)
    grad_normed_one = jnp.einsum("tj,ij->ti", grad_query_low, query_weight, preferred_element_type=f32)
    grad_normed_one = grad_normed_one + jnp.einsum(
        "tj,ij->ti", grad_key_low, key_weight, preferred_element_type=f32
    )
    grad_normed_one = grad_normed_one + jnp.einsum(
        "tj,ij->ti", grad_values, value_weight, preferred_element_type=f32
    )
    gains = jnp.concatenate([grad_gain_two, grad_query_gain, grad_key_gain]).reshape(1, -1)
    grad_hidden, in_low, out_low, gains = finish_sums(
        data_size,
        grad_in_weights,
        grad_out_weight.astype(bf),
        grad_normed_one.astype(bf),
        grad_middle,
        hidden_q,
        norm1_gain,
        gains,
    )
    in_low = in_low.reshape(model_width, -1)
    lead = local_heads * head_dim
    gains = gains.reshape(-1)
    return (
        hidden_out,
        grad_hidden,
        gains[:model_width],
        in_low[:, :lead].astype(f32),
        in_low[:, lead : lead + head_dim].astype(f32),
        in_low[:, lead + head_dim :].astype(f32),
        gains[2 * model_width : 2 * model_width + head_dim],
        gains[2 * model_width + head_dim :],
        out_low.reshape(-1, model_width).astype(f32),
        gains[model_width : 2 * model_width],
        grad_w_gate_up,
        grad_w_down,
    )


def solution(mesh):
    in_specs = (
        P("dp", None),
        P("dp", None),
        P(),
        P(None, "tensor"),
        P(None, "tensor"),
        P(None, "tensor"),
        P(),
        P(),
        P("tensor", None),
        P(),
        P("dp", None, None, "tensor"),
        P("dp", "tensor", None),
        P("dp", None),
        P("dp", None),
        P("dp", None),
    )
    out_specs = (
        P("dp", None),
        P("dp", None),
        P(),
        P(None, "tensor"),
        P(None, "tensor"),
        P(None, "tensor"),
        P(),
        P(),
        P("tensor", None),
        P(),
        P("dp", None, None, "tensor"),
        P("dp", "tensor", None),
    )
    return jax.shard_map(local, mesh=mesh, in_specs=in_specs, out_specs=out_specs, check_vma=False)
```

```python
import functools
import math

import jax
import jax.numpy as jnp
from jax import lax
from jax.experimental import pallas as pl
from jax.experimental.pallas import tpu as pltpu
from jax.sharding import PartitionSpec as P

EPSILON = 1e-06
ROPE_BASE = 1000000.0


def rms_parts(values):
    inverse = lax.rsqrt(jnp.mean(values * values, axis=-1, keepdims=True) + EPSILON)
    return (values * inverse, inverse)


def rms_back(grad_hat, normal_hat, inverse):
    return inverse * (
        grad_hat - normal_hat * jnp.mean(grad_hat * normal_hat, axis=-1, keepdims=True)
    )


def rotary_tables(positions, head_dim):
    halves = jnp.arange(head_dim // 2, dtype=jnp.float32)
    inverse = jnp.exp(halves * (-2.0 * math.log(ROPE_BASE) / head_dim))
    angles = positions.astype(jnp.float32)[:, None] * inverse[None, :]
    return (jnp.cos(angles), jnp.sin(angles))


def rotate(values, cosine_table, sine_table):
    middle_index = values.shape[-1] // 2
    first_half = values[..., :middle_index]
    second = values[..., middle_index:]
    return jnp.concatenate(
        [
            first_half * cosine_table - second * sine_table,
            second * cosine_table + first_half * sine_table,
        ],
        axis=-1,
    )


def rotate_back(gradient, cosine_table, sine_table):
    middle_index = gradient.shape[-1] // 2
    first_half = gradient[..., :middle_index]
    second = gradient[..., middle_index:]
    return jnp.concatenate(
        [
            first_half * cosine_table + second * sine_table,
            second * cosine_table - first_half * sine_table,
        ],
        axis=-1,
    )


def sequence_layout(lengths, token_count):
    endings = jnp.cumsum(lengths)
    places = jnp.arange(token_count, dtype=jnp.int32)
    starts = jnp.sum(jnp.where(endings[None, :] <= places[:, None], lengths[None, :], 0), axis=1)
    return (places, starts)


LANES = 128
MESH = pl.DeviceIdType.MESH
VMEM_LIMIT = 127 * 512 * 1024


def ring_place(index, size):
    return jnp.where(index % 2 == 0, index // 2, size - (index + 1) // 2)


def ring_index(place, size):
    place = place % size
    return jnp.where(place < size // 2, 2 * place, 2 * size - 1 - 2 * place)


def tensor_peers():
    own = lax.axis_index("tensor")
    partner = own + 1 - 2 * (own % 2)
    across = (own + 2) % 4
    return own, partner, across


def greet(devices):
    barrier = pltpu.get_barrier_semaphore()
    for device in devices:
        pl.semaphore_signal(barrier, inc=1, device_id=device, device_id_type=MESH)
    pl.semaphore_wait(barrier, len(devices))


def push(source, target, sems, device):
    return pltpu.make_async_remote_copy(
        src_ref=source,
        dst_ref=target,
        send_sem=sems[0],
        recv_sem=sems[1],
        device_id=device,
        device_id_type=MESH,
    )


def slot_of(delta, size):
    delta = (delta + size // 2 - 1) % size - (size // 2 - 1)
    if delta == 0:
        return size - 1
    if delta == size // 2:
        return size - 2
    return 2 * delta - 1 if delta > 0 else -2 * delta - 2


class GatherRing:
    def __init__(self, size, blocks, sems, parts=2):
        self.size, self.blocks, self.sems, self.parts = size, blocks, sems, parts
        self.place = ring_place(lax.axis_index("dp"), size)
        self.sent = []
        self.live = {}

    def send(self, step):
        size, half = self.size, self.blocks.shape[1] // 2
        piece = half // self.parts
        for part in range(self.parts):
            for way in (0, 1):
                sign = 1 - 2 * way
                rows = pl.ds(way * half + part * piece, piece)
                source = self.blocks.at[slot_of(-sign * step, size), rows]
                target = self.blocks.at[slot_of(-sign * (step + 1), size), rows]
                device = (ring_index(self.place + size + sign, size), lax.axis_index("tensor"))
                copy = push(
                    source,
                    target,
                    (self.sems.at[0, way, step, part], self.sems.at[1, way, step, part]),
                    device,
                )
                if step > 0:
                    self.live[step - 1, part, way].wait_recv()
                copy.start()
                self.live[step, part, way] = copy
                self.sent.append(copy)

    def step(self, step):
        if step + 1 < self.size - 1:
            self.send(step + 1)
        else:
            for part in range(self.parts):
                for way in (0, 1):
                    self.live[step, part, way].wait_recv()

    def finish(self):
        for copy in self.sent:
            copy.wait_send()


def row_loop(total, rows, body):
    def run(index, carry):
        body(pl.ds(pl.multiple_of(index * rows, rows), rows))
        return carry

    lax.fori_loop(0, total // rows, run, 0)


def exchange_tokens_body(
    size,
    part_ref,
    token_ref,
    pack_ref,
    gain_ref,
    middle_ref,
    inputs_ref,
    packs_ref,
    from_partner,
    from_across,
    joined,
    ring_sems,
    pack_sems,
    side_sems,
    local_sem,
):
    f32 = jnp.float32
    dp = lax.axis_index("dp")
    own, partner, across = tensor_peers()
    far_partner = (partner + 2) % 4
    quarter = token_ref.shape[0]
    place = ring_place(dp, size)
    neighbours = [(ring_index(place + 1, size), own), (ring_index(place + size - 1, size), own)]
    greet(neighbours + [(dp, partner), (dp, across)])

    def part_rows(index):
        return pl.ds(pl.multiple_of(index * quarter, quarter), quarter)

    def side(index):
        return (side_sems.at[0, index], side_sems.at[1, index])

    first = push(part_ref.at[part_rows(far_partner)], from_partner.at[1], side(0), (dp, partner))
    second = push(part_ref.at[part_rows(partner)], from_partner.at[0], side(1), (dp, partner))
    first.start()
    second.start()
    keep = pltpu.make_async_copy(pack_ref, packs_ref.at[size - 1], local_sem)
    keep.start()
    keep.wait()
    packs = GatherRing(size, packs_ref, pack_sems)
    packs.send(0)
    first.wait_recv()
    base = across * quarter

    def join(rows):
        there = pl.ds(pl.multiple_of(base + rows.start, 16), rows.size)
        joined[rows, :] = (
            part_ref[there, :].astype(f32) + from_partner[1, rows, :].astype(f32)
        ).astype(jnp.bfloat16)

    row_loop(quarter, 16, join)
    third = push(joined, from_across, side(2), (dp, across))
    third.start()
    packs.step(0)
    second.wait_recv()
    third.wait_recv()
    mine = own * quarter

    def norm(rows):
        there = pl.ds(pl.multiple_of(mine + rows.start, 16), rows.size)
        middle = (
            token_ref[rows, :].astype(f32)
            + part_ref[there, :].astype(f32)
            + from_partner[0, rows, :].astype(f32)
            + from_across[rows, :].astype(f32)
        )
        middle_ref[rows, :] = middle
        inverse = lax.rsqrt(jnp.mean(middle * middle, axis=-1, keepdims=True) + EPSILON)
        inputs_ref[size - 1, rows, :] = (middle * inverse * gain_ref[...]).astype(jnp.bfloat16)

    row_loop(quarter, 16, norm)
    tokens = GatherRing(size, inputs_ref, ring_sems)
    tokens.send(0)
    for step in range(1, size - 1):
        packs.step(step)
        tokens.step(step - 1)
    tokens.step(size - 2)
    packs.finish()
    tokens.finish()
    first.wait_send()
    second.wait_send()
    third.wait_send()


def exchange_tokens(size, partial, token_rows, packed, gain):
    quarter, width = token_rows.shape
    columns = packed.shape[1]
    bf = jnp.bfloat16
    vmem = pl.BlockSpec(memory_space=pltpu.VMEM)
    dma = pltpu.SemaphoreType.DMA
    return pl.pallas_call(
        functools.partial(exchange_tokens_body, size),
        out_shape=(
            jax.ShapeDtypeStruct((quarter, width), jnp.float32),
            jax.ShapeDtypeStruct((size, quarter, width), bf),
            jax.ShapeDtypeStruct((size, quarter, columns), bf),
        ),
        in_specs=[vmem] * 4,
        out_specs=(vmem,) * 3,
        scratch_shapes=[
            pltpu.VMEM((2, quarter, width), bf),
            pltpu.VMEM((quarter, width), bf),
            pltpu.VMEM((quarter, width), bf),
            dma((2, 2, size - 1, 2)),
            dma((2, 2, size - 1, 2)),
            dma((2, 3)),
            dma(()),
        ],
        compiler_params=pltpu.CompilerParams(
            collective_id=0, has_side_effects=True, vmem_limit_bytes=VMEM_LIMIT
        ),
        name="exchange_tokens",
    )(partial, token_rows, packed, gain.reshape(1, -1))


def matmul_nt(left, right):
    return lax.dot_general(left, right, (((1,), (1,)), ((), ())), preferred_element_type=jnp.float32)


def matmul(left, right):
    return lax.dot_general(left, right, (((1,), (0,)), ((), ())), preferred_element_type=jnp.float32)


def run_experts_body(
    size,
    local_experts,
    experts,
    inputs_ref,
    packs_ref,
    weights_ref,
    member_ref,
    middle_ref,
    gain_ref,
    hidden_out,
    kept_ref,
    given_ref,
    gmid_ref,
    gmid_all,
    gain_out,
    weights,
    hidden,
    grad_parts,
    mix_parts,
    grad_slots,
    mix_slots,
    turned,
    stage,
    totals,
    load_sems,
    grad_sems,
    mix_sems,
    side_sems,
    store_sems,
    give_sems,
):
    f32, bf = jnp.float32, jnp.bfloat16
    dp = lax.axis_index("dp")
    own, partner, across = tensor_peers()
    width = inputs_ref.shape[1]
    quarter = inputs_ref.shape[0] // size
    pair = 2 * quarter
    half = size // 2
    units = weights.shape[1]
    members = weights_ref.shape[0]
    span = units // members
    cut = width // 2
    wide = 512
    place = ring_place(dp, size)
    forward = (ring_index(place + 1, size), own)
    backward = (ring_index(place + size - 1, size), own)
    greet([forward, backward, (dp, partner), (dp, across)])
    pieces = units // LANES
    each = pieces // members

    def load(piece):
        source = weights_ref.at[piece // each, :, pl.ds((piece % each) * LANES, LANES), :]
        target = weights.at[:, pl.ds(piece * LANES, LANES), :]
        return pltpu.make_async_copy(source, target, load_sems.at[piece])

    for piece in range(pieces):
        load(piece).start()

    grad_ring = (grad_parts, grad_slots, grad_sems)
    mix_ring = (mix_parts, mix_slots, mix_sems)

    def ring_copy(ring, way, step, source):
        device = forward if way == 0 else backward
        _, slots, sems = ring
        return push(
            source, slots.at[way, step], (sems.at[0, way, step], sems.at[1, way, step]), device
        )

    def columns_of(way):
        return pl.ds(way * cut, cut)

    def ring_step(ring, step, blocks, first=False):
        parts, slots, _ = ring
        for way in (0, 1):
            if first:
                source = parts.at[blocks[way], :, columns_of(way)]
            else:
                source = slots.at[way, step - 1]
                ring_copy(ring, way, step - 1, source).wait_recv()

                def add(rows):
                    slots[way, step - 1, rows, :] = (
                        slots[way, step - 1, rows, :].astype(f32)
                        + parts[blocks[way], rows, columns_of(way)].astype(f32)
                    ).astype(bf)

                row_loop(quarter, 16, add)
            ring_copy(ring, way, step, source).start()

    def do_pair(index, carry):
        rows = pl.ds(pl.multiple_of(index * pair, pair), pair)
        tail = packs_ref[rows, width:].astype(f32)
        lane = lax.broadcasted_iota(jnp.int32, tail.shape, 1)
        shares = []
        for expert in range(local_experts):
            name = dp * local_experts + expert
            picked = (lane == name) | (lane == experts + name)
            shares.append(jnp.sum(jnp.where(picked, tail, 0.0), axis=1, keepdims=True))

        def do_units(tile, carry):
            here = pl.ds(pl.multiple_of(tile * wide, wide), wide)

            @pl.when(index == 0)
            def _():
                for piece in range(wide // LANES):
                    load(tile * (wide // LANES) + piece).wait()

            scale = shares[0] * member_ref[0:1, here]
            for expert in range(1, local_experts):
                scale = scale + shares[expert] * member_ref[expert : expert + 1, here]
            tokens = inputs_ref[rows, :]
            gate = matmul_nt(tokens, weights[0, here, :])
            upward = matmul_nt(tokens, weights[1, here, :])
            grads = scale * matmul_nt(packs_ref[rows, :width], weights[2, here, :])
            share = jax.nn.sigmoid(gate)
            silu = gate * share
            hidden[0, rows, here] = (grads * upward * share * (1.0 + gate * (1.0 - share))).astype(bf)
            hidden[1, rows, here] = (grads * silu).astype(bf)
            hidden[2, rows, here] = (scale * silu * upward).astype(bf)
            return carry

        lax.fori_loop(0, units // wide, do_units, 0)

        def do_columns(tile, carry):
            here = pl.ds(pl.multiple_of(tile * wide, wide), wide)
            sums = matmul(hidden[0, rows, :], weights[0, :, here]) + matmul(
                hidden[1, rows, :], weights[1, :, here]
            )
            low = sums.astype(bf)
            grad_parts[2 * index, :, here] = low[:quarter]
            grad_parts[2 * index + 1, :, here] = low[quarter:]
            return carry

        def do_mix(tile, carry):
            here = pl.ds(pl.multiple_of(tile * wide, wide), wide)
            low = matmul(hidden[2, rows, :], weights[2, :, here]).astype(bf)
            mix_parts[2 * index, :, here] = low[:quarter]
            mix_parts[2 * index + 1, :, here] = low[quarter:]
            return carry

        lax.fori_loop(0, width // wide, do_columns, 0)

        def go_on(ring):
            @pl.when(index == 0)
            def _():
                ring_step(ring, 0, (0, 1), first=True)

            @pl.when(index > 0)
            def _():
                ring_step(ring, index, (2 * index, 2 * index + 1 - index // (half - 1)))

        go_on(grad_ring)
        lax.fori_loop(0, width // wide, do_mix, 0)
        go_on(mix_ring)
        return carry

    lax.fori_loop(0, half, do_pair, 0)
    far_partner = (partner + 2) % 4

    def keep(index, slot):
        target = kept_ref.at[index % members - 2, index // members]
        return pltpu.make_async_copy(stage.at[slot], target, store_sems.at[slot])

    def give(index, slot):
        target = given_ref.at[index % members, index // members]
        number = 2 * (index // members) + index % members
        return push(
            stage.at[slot], target, (give_sems.at[0, number], give_sems.at[1, number]), (dp, partner)
        )

    def weight_grads(first, last):
        def run(index, carry):
            kind = index // members
            whose = index % members
            slot = index % 2
            member = jnp.where(whose < 2, partner + 2 * whose, own + 2 * (3 - whose)) % members

            @pl.when((index >= 2) & (whose < 2))
            def _():
                keep(index - 2, slot).wait()

            @pl.when(whose >= 2)
            def _():
                give(index - 2, slot).wait_send()

            rows = pl.ds(pl.multiple_of(member * span, span), span)
            for chunk in range(half):
                some = pl.ds(chunk * pair, pair)
                turned[:, some] = hidden[kind, some, rows].T

            def do_columns(tile, carry):
                here = pl.ds(pl.multiple_of(tile * wide, wide), wide)
                source = inputs_ref if first < 2 * members else packs_ref
                stage[slot, :, here] = matmul(turned[...], source[:, here]).astype(bf)
                return carry

            lax.fori_loop(0, width // wide, do_columns, 0)

            @pl.when(whose < 2)
            def _():
                give(index, slot).start()

            @pl.when(whose >= 2)
            def _():
                keep(index, slot).start()

            return carry

        lax.fori_loop(first, last, run, 0)

    def final_sum():
        totals[...] = jnp.zeros_like(totals)
        for way in (0, 1):
            ring_copy(grad_ring, way, size - 2, grad_slots.at[way, size - 2]).wait_recv()
        base = own * quarter

        def finish(rows):
            sums = jnp.concatenate(
                [
                    grad_slots[0, size - 2, rows, :].astype(f32),
                    grad_slots[1, size - 2, rows, :].astype(f32),
                ],
                axis=-1,
            ) + grad_parts[size - 1, rows, :].astype(f32)
            middle = middle_ref[rows, :]
            inverse = lax.rsqrt(jnp.mean(middle * middle, axis=-1, keepdims=True) + EPSILON)
            hat = middle * inverse
            product = sums * hat
            totals[...] += product[:8] + product[8:]
            scaled = sums * gain_ref[...]
            back = inverse * (scaled - hat * jnp.mean(scaled * hat, axis=-1, keepdims=True))
            above = packs_ref[
                pl.ds(pl.multiple_of((size - 1) * quarter + rows.start, 16), rows.size), :width
            ]
            grad = above.astype(f32) + back
            gmid_ref[rows, :] = grad
            gmid_all[pl.ds(pl.multiple_of(base + rows.start, 16), rows.size), :] = grad.astype(bf)

        row_loop(quarter, 16, finish)
        gain_out[...] = jnp.sum(totals[...], axis=0, keepdims=True)

    def rows_of(index):
        return pl.ds(pl.multiple_of(index * quarter, quarter), quarter)

    def spread(index, whose, device):
        ref = gmid_all.at[rows_of(whose)]
        return push(ref, ref, (side_sems.at[0, index], side_sems.at[1, index]), device)

    def first_spread():
        spread(0, own, (dp, across)).start()
        spread(1, own, (dp, partner)).start()

    def second_spread():
        spread(0, own, (dp, across)).wait_recv()
        spread(2, across, (dp, partner)).start()

    def final_mix():
        for way in (0, 1):
            ring_copy(mix_ring, way, size - 2, mix_slots.at[way, size - 2]).wait_recv()

        def finish(rows):
            for way in (0, 1):
                columns = columns_of(way)
                hidden_out[rows, columns] = (
                    middle_ref[rows, columns]
                    + mix_slots[way, size - 2, rows, :].astype(f32)
                    + mix_parts[size - 1, rows, columns].astype(f32)
                ).astype(bf)

        row_loop(quarter, 16, finish)

    def closing():
        final_sum()
        first_spread()

    grad_events, mix_events = [], []
    for step in range(half, size - 1):
        delta = -(1 + step)
        blocks = (slot_of(delta, size), slot_of(-delta, size))
        grad_events.append(functools.partial(ring_step, grad_ring, step, blocks))
        mix_events.append(functools.partial(ring_step, mix_ring, step, blocks))
    events = grad_events[:-1]
    events += [grad_events[-1], mix_events[0], closing] + mix_events[1:2] + [second_spread]
    events += mix_events[2:] + [final_mix]
    work = [functools.partial(weight_grads, first, first + 2) for first in range(0, 3 * members, 2)]
    done = 0
    for number, piece in enumerate(work):
        piece()
        upto = -(-(number + 1) * len(events) // len(work))
        while done < upto:
            events[done]()
            done += 1
    for slot in (0, 1):
        keep(3 * members - 2 + slot, slot).wait()
    for kind in range(3):
        for whose in (0, 1):
            give(kind * members + whose, 0).wait_recv()
    spread(1, own, (dp, partner)).wait_recv()
    spread(2, across, (dp, partner)).wait_recv()
    for index, device in ((0, across), (1, partner), (2, partner)):
        spread(index, own, (dp, device)).wait_send()
    for ring in (grad_ring, mix_ring):
        for way in (0, 1):
            for step in range(size - 1):
                ring_copy(ring, way, step, ring[1].at[way, step]).wait_send()


def run_experts(size, inputs, packs, weights, middle, gain, experts):
    bf, f32 = jnp.bfloat16, jnp.float32
    members, _, span, width = weights.shape
    local_experts = experts // size
    rows = inputs.shape[0]
    quarter = rows // size
    units = members * span
    expert_of = (jnp.arange(units, dtype=jnp.int32) // (span // local_experts)) % local_experts
    member = (expert_of[None, :] == jnp.arange(local_experts, dtype=jnp.int32)[:, None]).astype(f32)
    vmem = pl.BlockSpec(memory_space=pltpu.VMEM)
    anywhere = pl.BlockSpec(memory_space=pl.ANY)
    dma = pltpu.SemaphoreType.DMA
    return pl.pallas_call(
        functools.partial(run_experts_body, size, local_experts, experts),
        out_shape=(
            jax.ShapeDtypeStruct((quarter, width), bf),
            jax.ShapeDtypeStruct((2, 3, span, width), bf),
            jax.ShapeDtypeStruct((2, 3, span, width), bf),
            jax.ShapeDtypeStruct((quarter, width), f32),
            jax.ShapeDtypeStruct((members * quarter, width), bf),
            jax.ShapeDtypeStruct((1, width), f32),
        ),
        in_specs=[vmem, vmem, anywhere, vmem, vmem, vmem],
        out_specs=(vmem, anywhere, anywhere, vmem, vmem, vmem),
        scratch_shapes=[
            pltpu.VMEM((3, units, width), bf),
            pltpu.VMEM((3, rows, units), bf),
            pltpu.VMEM((size, quarter, width), bf),
            pltpu.VMEM((size, quarter, width), bf),
            pltpu.VMEM((2, size - 1, quarter, width // 2), bf),
            pltpu.VMEM((2, size - 1, quarter, width // 2), bf),
            pltpu.VMEM((span, rows), bf),
            pltpu.VMEM((2, span, width), bf),
            pltpu.VMEM((8, width), f32),
            dma((units // LANES,)),
            dma((2, 2, size - 1)),
            dma((2, 2, size - 1)),
            dma((2, 3)),
            dma((2,)),
            dma((2, 6)),
        ],
        compiler_params=pltpu.CompilerParams(
            collective_id=2, has_side_effects=True, vmem_limit_bytes=VMEM_LIMIT
        ),
        name="run_experts",
    )(inputs, packs, weights, member, middle, gain.reshape(1, -1))


def finish_sums_body(
    size,
    qkv_ref,
    out_ref,
    normed_ref,
    middle_ref,
    token_ref,
    hidden_ref,
    cross_ref,
    gain_ref,
    gains_ref,
    hidden_all,
    crossed_ref,
    grad_all,
    gather_a,
    gather_b,
    gains_out,
    slots_a,
    slots_b,
    from_partner,
    from_across,
    joined,
    totals,
    pair_gains,
    ring_gains,
    sems_a,
    sems_b,
    ring_sems,
    side_sems,
):
    f32, bf = jnp.float32, jnp.bfloat16
    dp = lax.axis_index("dp")
    own, partner, across = tensor_peers()
    far_partner = (partner + 2) % 4
    quarter, width = token_ref.shape
    place = ring_place(dp, size)
    forward = (ring_index(place + 1, size), own)
    backward = (ring_index(place + size - 1, size), own)
    ways = ((forward, 1), (backward, -1))
    greet([forward, backward, (dp, partner), (dp, across)])
    waits = []

    def start(copy):
        copy.start()
        waits.append(copy)
        return copy

    sets = (
        (qkv_ref, slots_a, gather_a, sems_a),
        (out_ref, slots_b, gather_b, sems_b),
    )

    def block_of(ref, block, way):
        rows = ref.shape[0] // size
        cut = ref.shape[1] // 2
        return (pl.ds(pl.multiple_of(block * rows, rows), rows), pl.ds(way * cut, cut))

    def wrap(value):
        return (value + 2 * size) % size

    live = {}

    def reduce_send(step):
        for which, (ref, slots, _, sems) in enumerate(sets):
            for way, (device, sign) in enumerate(ways):
                if step == 0:
                    source = ref.at[block_of(ref, wrap(place - sign), way)]
                else:
                    add_own(which, way, step - 1)
                    source = slots.at[way, step - 1]
                live[which, way, step] = start(
                    push(
                        source,
                        slots.at[way, step],
                        (sems.at[0, way, step], sems.at[1, way, step]),
                        device,
                    )
                )

    def add_own(which, way, step):
        ref, slots, blocks, _ = sets[which]
        live[which, way, step].wait_recv()
        sign = ways[way][1]
        rows, columns = block_of(ref, wrap(place - sign * (2 + step)), way)
        base = rows.start

        def add(inner):
            there = pl.ds(pl.multiple_of(base + inner.start, 16), inner.size)
            sums = (slots[way, step, inner, :].astype(f32) + ref[there, columns].astype(f32)).astype(bf)
            if step == size - 2:
                blocks[place, inner, columns] = sums
            else:
                slots[way, step, inner, :] = sums

        row_loop(ref.shape[0] // size, 16, add)

    gather = {}

    def gather_send(step):
        for which, (ref, _, blocks, sems) in enumerate(sets):
            cut = ref.shape[1] // 2
            for way, (device, sign) in enumerate(ways):
                if step == 0:
                    add_own(which, way, size - 2)
                else:
                    gather[which, way, step - 1].wait_recv()
                source = blocks.at[wrap(place - sign * step), :, pl.ds(way * cut, cut)]
                gather[which, way, step] = start(
                    push(
                        source,
                        source,
                        (sems.at[0, way, size - 1 + step], sems.at[1, way, size - 1 + step]),
                        device,
                    )
                )

    def part_rows(index):
        return pl.ds(pl.multiple_of(index * quarter, quarter), quarter)

    def side(index):
        return (side_sems.at[0, index], side_sems.at[1, index])

    reduce_send(0)
    first = start(
        push(normed_ref.at[part_rows(far_partner)], from_partner.at[1], side(0), (dp, partner))
    )
    second = start(
        push(normed_ref.at[part_rows(partner)], from_partner.at[0], side(1), (dp, partner))
    )
    mine = part_rows(own)
    crossing = start(push(cross_ref, crossed_ref, side(8), (dp, across)))
    home = own * quarter

    def keep(rows):
        hidden_all[pl.ds(pl.multiple_of(home + rows.start, 16), rows.size), :] = hidden_ref[rows, :]

    row_loop(quarter, 16, keep)
    spread = []
    shown = [start(push(hidden_ref, hidden_all.at[mine], side(9), (dp, across)))]
    shown.append(start(push(hidden_ref, hidden_all.at[mine], side(10), (dp, partner))))
    reduce_send(1)
    first.wait_recv()
    away = across * quarter

    def join(rows):
        there = pl.ds(pl.multiple_of(away + rows.start, 16), rows.size)
        joined[rows, :] = (
            normed_ref[there, :].astype(f32) + from_partner[1, rows, :].astype(f32)
        ).astype(bf)

    row_loop(quarter, 16, join)
    third = start(push(joined, from_across, side(2), (dp, across)))
    reduce_send(2)
    second.wait_recv()
    third.wait_recv()
    totals[...] = jnp.zeros_like(totals)

    def finish(rows):
        there = pl.ds(pl.multiple_of(home + rows.start, 16), rows.size)
        grads = (
            normed_ref[there, :].astype(f32)
            + from_partner[0, rows, :].astype(f32)
            + from_across[rows, :].astype(f32)
        )
        hidden = token_ref[rows, :].astype(f32)
        inverse = lax.rsqrt(jnp.mean(hidden * hidden, axis=-1, keepdims=True) + EPSILON)
        hat = hidden * inverse
        product = grads * hat
        totals[:, :width] += jnp.sum(product.reshape(-1, 8, width), axis=0)
        scaled = grads * gain_ref[...]
        back = inverse * (scaled - hat * jnp.mean(scaled * hat, axis=-1, keepdims=True))
        joined_grad = (middle_ref[rows, :] + back).astype(bf)
        grad_all[there, :] = joined_grad

    row_loop(quarter, 16, finish)
    spread.append(start(push(grad_all.at[mine], grad_all.at[mine], side(3), (dp, across))))
    spread.append(start(push(grad_all.at[mine], grad_all.at[mine], side(4), (dp, partner))))
    pair_gains[0, :, :width] = jnp.sum(totals[:, :width], axis=0, keepdims=True)
    pair_gains[0, :, width:] = gains_ref[...]
    swap = start(push(pair_gains.at[0], pair_gains.at[1], side(5), (dp, partner)))
    reduce_send(3)
    far = part_rows(across)
    shown[0].wait_recv()
    shown.append(start(push(hidden_all.at[far], hidden_all.at[far], side(11), (dp, partner))))
    spread[0].wait_recv()
    spread.append(start(push(grad_all.at[far], grad_all.at[far], side(6), (dp, partner))))
    swap.wait_recv()
    pair_gains[2] = pair_gains[0] + pair_gains[1]
    swap = start(push(pair_gains.at[2], pair_gains.at[3], side(7), (dp, across)))
    for step in range(4, size - 1):
        reduce_send(step)
    swap.wait_recv()
    ring_gains[place] = pair_gains[2] + pair_gains[3]
    gather_send(0)
    small = None
    for step in range(size - 1):
        if small is not None:
            small.wait_recv()
        ref = ring_gains.at[wrap(place - step)]
        small = start(push(ref, ref, (ring_sems.at[0, step], ring_sems.at[1, step]), forward))
        if step > 0:
            gather_send(step)
    small.wait_recv()
    for copy in (gather[which, way, size - 2] for which in (0, 1) for way in (0, 1)):
        copy.wait_recv()
    gains_out[...] = jnp.sum(ring_gains[...], axis=0)
    for copy in (spread[1], spread[2], shown[1], shown[2], crossing):
        copy.wait_recv()
    for copy in waits:
        copy.wait_send()


def finish_sums(
    size, grad_in, grad_out, grad_normed, grad_middle, token_rows, hidden_rows, cross, gain, gains
):
    bf, f32 = jnp.bfloat16, jnp.float32
    quarter, width = token_rows.shape
    tokens = grad_normed.shape[0]
    vmem = pl.BlockSpec(memory_space=pltpu.VMEM)
    anywhere = pl.BlockSpec(memory_space=pl.ANY)
    dma = pltpu.SemaphoreType.DMA
    rows_a, rows_b = grad_in.shape[0] // size, grad_out.shape[0] // size
    cut_a, cut_b = grad_in.shape[1] // 2, grad_out.shape[1] // 2
    count = width + gains.shape[1]
    return pl.pallas_call(
        functools.partial(finish_sums_body, size),
        out_shape=(
            jax.ShapeDtypeStruct((tokens, width), bf),
            jax.ShapeDtypeStruct(cross.shape, bf),
            jax.ShapeDtypeStruct((tokens, width), bf),
            jax.ShapeDtypeStruct((size, rows_a, 2 * cut_a), bf),
            jax.ShapeDtypeStruct((size, rows_b, 2 * cut_b), bf),
            jax.ShapeDtypeStruct((1, count), f32),
        ),
        in_specs=[vmem] * 6 + [anywhere, vmem, vmem],
        out_specs=(vmem, anywhere) + (vmem,) * 4,
        scratch_shapes=[
            pltpu.VMEM((2, size - 1, rows_a, cut_a), bf),
            pltpu.VMEM((2, size - 1, rows_b, cut_b), bf),
            pltpu.VMEM((2, quarter, width), bf),
            pltpu.VMEM((quarter, width), bf),
            pltpu.VMEM((quarter, width), bf),
            pltpu.VMEM((8, width), f32),
            pltpu.VMEM((4, 1, count), f32),
            pltpu.VMEM((size, 1, count), f32),
            dma((2, 2, 2 * size - 2)),
            dma((2, 2, 2 * size - 2)),
            dma((2, size - 1)),
            dma((2, 12)),
        ],
        compiler_params=pltpu.CompilerParams(
            collective_id=1, has_side_effects=True, vmem_limit_bytes=VMEM_LIMIT
        ),
        name="finish_sums",
    )(
        grad_in,
        grad_out,
        grad_normed,
        grad_middle,
        token_rows,
        hidden_rows,
        cross,
        gain.reshape(1, -1),
        gains,
    )


def large_experts(size, inputs, packs, all_weights, middle, gain, experts):
    f32, bf = jnp.float32, jnp.bfloat16
    members, _, units, model_width = all_weights.shape
    local_experts = experts // size
    indices = jnp.arange(size, dtype=jnp.int32)
    half = size // 2
    delta = (ring_place(indices, size) - ring_place(lax.axis_index("dp"), size)) % size
    ahead = jnp.where(delta == half, size - 2, jnp.where(delta == 0, size - 1, 2 * delta - 1))
    slots = jnp.where(delta > half, 2 * (size - delta) - 2, ahead)
    quarter = middle.shape[0]
    out_rows = packs[-quarter:, :model_width]
    inputs = inputs.reshape(size, quarter, -1)[slots].reshape(-1, model_width)
    packs = packs.reshape(size, quarter, -1)[slots].reshape(inputs.shape[0], -1)
    grads_all = packs[:, :model_width]
    shares = packs[:, model_width : model_width + 2 * experts].astype(f32)
    shares = shares[:, :experts] + shares[:, experts:]
    shares = lax.dynamic_slice_in_dim(
        shares, lax.axis_index("dp") * local_experts, local_experts, 1
    )
    weight_cols = jnp.broadcast_to(
        shares[:, None, :, None],
        (shares.shape[0], members, local_experts, units // local_experts),
    ).reshape(-1, members, units)

    def project(left, which):
        return jnp.einsum("td,rud->tru", left, all_weights[:, which], preferred_element_type=f32)

    gate_act = project(inputs, 0)
    upward = project(inputs, 1)
    sigmoid_gate = jax.nn.sigmoid(gate_act)
    active = gate_act * sigmoid_gate * upward
    weighted_low = (weight_cols * active).astype(bf)
    mixture_part = jnp.einsum(
        "tru,rud->td", weighted_low, all_weights[:, 2], preferred_element_type=f32
    ).astype(bf)
    grad_active = weight_cols * project(grads_all, 2)
    grad_gate = (
        grad_active * upward * sigmoid_gate * (1.0 + gate_act * (1.0 - sigmoid_gate))
    ).astype(bf)
    grad_up = (grad_active * gate_act * sigmoid_gate).astype(bf)
    grad_normed_part = jnp.einsum(
        "tru,rud->td", grad_gate, all_weights[:, 0], preferred_element_type=f32
    ) + jnp.einsum("tru,rud->td", grad_up, all_weights[:, 1], preferred_element_type=f32)
    grad_normed_two = lax.psum_scatter(grad_normed_part.astype(bf), "dp", tiled=True).astype(f32)
    weight_grads = jnp.stack(
        [
            jnp.einsum("tru,td->rud", grad_gate, inputs, preferred_element_type=f32).astype(bf),
            jnp.einsum("tru,td->rud", grad_up, inputs, preferred_element_type=f32).astype(bf),
            jnp.einsum("tru,td->rud", weighted_low, grads_all, preferred_element_type=f32).astype(bf),
        ],
        axis=1,
    )
    hat_two, inv_two = rms_parts(middle)
    grad_gain_two = jnp.sum(grad_normed_two * hat_two, axis=0)
    grad_middle = out_rows.astype(f32) + rms_back(grad_normed_two * gain, hat_two, inv_two)
    grad_mid_low = lax.all_gather(grad_middle.astype(bf), "tensor", tiled=True)
    mixture = lax.psum_scatter(mixture_part, "dp", tiled=True).astype(f32)
    hidden_out = (middle + mixture).astype(bf)
    zero = jnp.zeros(weight_grads.shape[1:], bf)
    sums = lax.psum_scatter(weight_grads.reshape(-1, model_width), "tensor", tiled=True)
    kept = jnp.stack([zero, sums.reshape(zero.shape)])
    given = jnp.stack([zero, zero])
    return (hidden_out, kept, given, grad_middle, grad_mid_low, grad_gain_two)


def local(
    hidden_in,
    seq_lens,
    norm1_gain,
    query_weight,
    key_weight,
    value_weight,
    query_gain,
    key_gain,
    out_weight,
    norm2_gain,
    w_gate_up,
    w_down,
    routes,
    route_weights,
    out_grad,
):
    bf = jnp.bfloat16
    f32 = jnp.float32
    tokens, model_width = hidden_in.shape
    local_experts = w_gate_up.shape[0]
    hidden_part = w_gate_up.shape[3]
    head_dim = query_gain.shape[0]
    local_heads = query_weight.shape[1] // head_dim
    data_size = lax.axis_size("dp")
    tensor_size = lax.axis_size("tensor")
    quarter = tokens // tensor_size
    experts = local_experts * data_size
    score_scale = head_dim ** (-0.5)
    row0 = lax.axis_index("tensor") * quarter

    def mine(array):
        return lax.dynamic_slice_in_dim(array, row0, quarter, 0)

    expert_ids = jnp.arange(experts, dtype=jnp.int32)
    dense = jnp.sum(
        jnp.where(mine(routes)[:, :, None] == expert_ids[None, None, :], mine(route_weights)[:, :, None], 0.0),
        axis=1,
    )
    dense_high = dense.astype(bf)
    dense_low = (dense - dense_high.astype(f32)).astype(bf)
    spare = -2 * experts % LANES
    packed = jnp.concatenate(
        [mine(out_grad), dense_high, dense_low, jnp.zeros((quarter, spare), bf)], axis=1
    )
    rows = data_size * quarter
    units = local_experts * hidden_part
    own_weights = jnp.concatenate(
        [
            jnp.transpose(w_gate_up, (2, 0, 3, 1)).reshape(2, units, model_width),
            w_down.reshape(1, units, model_width),
        ],
        axis=0,
    )
    all_weights = lax.all_gather(own_weights, "tensor")
    hidden = hidden_in.astype(f32)
    hat_one, inv_one = rms_parts(hidden)
    normed = (hat_one * norm1_gain).astype(bf)
    query_proj = jnp.dot(normed, query_weight, preferred_element_type=f32).reshape(
        tokens, local_heads, head_dim
    )
    key_proj = jnp.dot(normed, key_weight, preferred_element_type=f32)
    value_low = jnp.dot(normed, value_weight, preferred_element_type=f32).astype(bf)
    places, starts = sequence_layout(seq_lens[0], tokens)
    cosine_table, sine_table = rotary_tables(places - starts, head_dim)
    query_hat, query_inv = rms_parts(query_proj)
    query_low = rotate(
        query_hat * query_gain, cosine_table[:, None, :], sine_table[:, None, :]
    ).astype(bf)
    key_hat, key_inv = rms_parts(key_proj)
    key_low = rotate(key_hat * key_gain, cosine_table, sine_table).astype(bf)
    visible = (places[None, :] <= places[:, None]) & (places[None, :] >= starts[:, None])
    scores = jnp.einsum("thd,sd->hts", query_low, key_low, preferred_element_type=f32) * score_scale
    exponent = jnp.where(visible[None], jnp.exp(scores), 0.0)
    totals = jnp.sum(exponent, axis=-1, keepdims=True)
    log_totals = jnp.log(totals)
    soft_low = (exponent / totals).astype(bf)
    mixed_low = (
        jnp.einsum("hts,sd->thd", soft_low, value_low, preferred_element_type=f32)
        .reshape(tokens, local_heads * head_dim)
        .astype(bf)
    )
    hidden_q = mine(hidden_in)
    partial = jnp.dot(mixed_low, out_weight, preferred_element_type=f32).astype(bf)
    middle, inputs, gathered = exchange_tokens(data_size, partial, hidden_q, packed, norm2_gain)
    stage = run_experts if data_size <= 8 else large_experts
    hidden_out, kept, given, grad_middle, grad_mid_low, grad_gain_two = stage(
        data_size,
        inputs.reshape(rows, model_width),
        gathered.reshape(rows, -1),
        all_weights,
        middle,
        norm2_gain,
        experts,
    )
    grad_gain_two = grad_gain_two.reshape(-1)
    joined = (kept[0].astype(f32) + given[1].astype(f32)).astype(bf)
    grad_out_weight = jnp.einsum("ti,td->id", mixed_low, grad_mid_low, preferred_element_type=f32)
    grad_mixed = (
        jnp.einsum("td,id->ti", grad_mid_low, out_weight, preferred_element_type=f32)
        .astype(bf)
        .reshape(tokens, local_heads, head_dim)
    )
    scores_again = (
        jnp.einsum("thd,sd->hts", query_low, key_low, preferred_element_type=f32) * score_scale
    )
    soft_again = jnp.where(visible[None], jnp.exp(scores_again - log_totals), 0.0)
    grad_soft = jnp.einsum("thd,sd->hts", grad_mixed, value_low, preferred_element_type=f32)
    grad_scores = (
        soft_again * (grad_soft - jnp.sum(soft_again * grad_soft, axis=-1, keepdims=True))
    ).astype(bf)
    grad_values = jnp.einsum(
        "hts,thd->sd", soft_again.astype(bf), grad_mixed, preferred_element_type=f32
    ).astype(bf)
    grad_query_rot = score_scale * jnp.einsum(
        "hts,sd->thd", grad_scores, key_low, preferred_element_type=f32
    )
    grad_key_rot = score_scale * jnp.einsum(
        "hts,thd->sd", grad_scores, query_low, preferred_element_type=f32
    )
    grad_query_norm = rotate_back(grad_query_rot, cosine_table[:, None, :], sine_table[:, None, :])
    grad_query_gain = jnp.sum(grad_query_norm * query_hat, axis=(0, 1))
    grad_query_low = (
        rms_back(grad_query_norm * query_gain, query_hat, query_inv)
        .reshape(tokens, local_heads * head_dim)
        .astype(bf)
    )
    grad_key_norm = rotate_back(grad_key_rot, cosine_table, sine_table)
    grad_key_gain = jnp.sum(grad_key_norm * key_hat, axis=0)
    grad_key_low = rms_back(grad_key_norm * key_gain, key_hat, key_inv).astype(bf)
    grad_all_low = jnp.concatenate([grad_query_low, grad_key_low, grad_values], axis=1)
    grad_in_weights = jnp.einsum(
        "ti,tj->ij", normed, grad_all_low, preferred_element_type=f32
    ).astype(bf)
    grad_normed_one = jnp.einsum("tj,ij->ti", grad_query_low, query_weight, preferred_element_type=f32)
    grad_normed_one = grad_normed_one + jnp.einsum(
        "tj,ij->ti", grad_key_low, key_weight, preferred_element_type=f32
    )
    grad_normed_one = grad_normed_one + jnp.einsum(
        "tj,ij->ti", grad_values, value_weight, preferred_element_type=f32
    )
    gains = jnp.concatenate([grad_gain_two, grad_query_gain, grad_key_gain]).reshape(1, -1)
    hidden_out, crossed, grad_hidden, in_low, out_low, gains = finish_sums(
        data_size,
        grad_in_weights,
        grad_out_weight.astype(bf),
        grad_normed_one.astype(bf),
        grad_middle,
        hidden_q,
        hidden_out,
        joined,
        norm1_gain,
        gains,
    )
    own_grads = kept[1].astype(f32) + given[0].astype(f32) + crossed.astype(f32)
    grad_w_gate_up = jnp.transpose(
        own_grads[:2].reshape(2, local_experts, hidden_part, model_width), (1, 3, 0, 2)
    )
    grad_w_down = own_grads[2].reshape(local_experts, hidden_part, model_width)
    in_low = in_low.reshape(model_width, -1)
    lead = local_heads * head_dim
    gains = gains.reshape(-1)
    return (
        hidden_out,
        grad_hidden,
        gains[:model_width],
        in_low[:, :lead].astype(f32),
        in_low[:, lead : lead + head_dim].astype(f32),
        in_low[:, lead + head_dim :].astype(f32),
        gains[2 * model_width : 2 * model_width + head_dim],
        gains[2 * model_width + head_dim :],
        out_low.reshape(-1, model_width).astype(f32),
        gains[model_width : 2 * model_width],
        grad_w_gate_up,
        grad_w_down,
    )


def solution(mesh):
    in_specs = (
        P("dp", None),
        P("dp", None),
        P(),
        P(None, "tensor"),
        P(None, "tensor"),
        P(None, "tensor"),
        P(),
        P(),
        P("tensor", None),
        P(),
        P("dp", None, None, "tensor"),
        P("dp", "tensor", None),
        P("dp", None),
        P("dp", None),
        P("dp", None),
    )
    out_specs = (
        P("dp", None),
        P("dp", None),
        P(),
        P(None, "tensor"),
        P(None, "tensor"),
        P(None, "tensor"),
        P(),
        P(),
        P("tensor", None),
        P(),
        P("dp", None, None, "tensor"),
        P("dp", "tensor", None),
    )
    return jax.shard_map(local, mesh=mesh, in_specs=in_specs, out_specs=out_specs, check_vma=False)
```

```python
import functools
import math

import jax
import jax.numpy as jnp
from jax import lax
from jax.experimental import pallas as pl
from jax.experimental.pallas import tpu as pltpu
from jax.sharding import PartitionSpec as P

EPSILON = 1e-06
ROPE_BASE = 1000000.0


def rms_parts(values):
    inverse = lax.rsqrt(jnp.mean(values * values, axis=-1, keepdims=True) + EPSILON)
    return (values * inverse, inverse)


def rms_back(grad_hat, normal_hat, inverse):
    return inverse * (
        grad_hat - normal_hat * jnp.mean(grad_hat * normal_hat, axis=-1, keepdims=True)
    )


def rotary_tables(positions, head_dim):
    halves = jnp.arange(head_dim // 2, dtype=jnp.float32)
    inverse = jnp.exp(halves * (-2.0 * math.log(ROPE_BASE) / head_dim))
    angles = positions.astype(jnp.float32)[:, None] * inverse[None, :]
    return (jnp.cos(angles), jnp.sin(angles))


def rotate(values, cosine_table, sine_table):
    middle_index = values.shape[-1] // 2
    first_half = values[..., :middle_index]
    second = values[..., middle_index:]
    return jnp.concatenate(
        [
            first_half * cosine_table - second * sine_table,
            second * cosine_table + first_half * sine_table,
        ],
        axis=-1,
    )


def sequence_layout(lengths, token_count):
    endings = jnp.cumsum(lengths)
    places = jnp.arange(token_count, dtype=jnp.int32)
    starts = jnp.sum(jnp.where(endings[None, :] <= places[:, None], lengths[None, :], 0), axis=1)
    return (places, starts)


LANES = 128
MESH = pl.DeviceIdType.MESH
VMEM_LIMIT = 127 * 512 * 1024


def ring_place(index, size):
    return jnp.where(index % 2 == 0, index // 2, size - (index + 1) // 2)


def ring_index(place, size):
    place = place % size
    return jnp.where(place < size // 2, 2 * place, 2 * size - 1 - 2 * place)


def tensor_peers():
    own = lax.axis_index("tensor")
    partner = own + 1 - 2 * (own % 2)
    across = (own + 2) % 4
    return own, partner, across


def greet(devices):
    barrier = pltpu.get_barrier_semaphore()
    for device in devices:
        pl.semaphore_signal(barrier, inc=1, device_id=device, device_id_type=MESH)
    pl.semaphore_wait(barrier, len(devices))


def push(source, target, sems, device):
    return pltpu.make_async_remote_copy(
        src_ref=source,
        dst_ref=target,
        send_sem=sems[0],
        recv_sem=sems[1],
        device_id=device,
        device_id_type=MESH,
    )


def slot_of(delta, size):
    delta = (delta + size // 2 - 1) % size - (size // 2 - 1)
    if delta == 0:
        return size - 1
    if delta == size // 2:
        return size - 2
    return 2 * delta - 1 if delta > 0 else -2 * delta - 2


class GatherRing:
    def __init__(self, size, blocks, sems, parts=2):
        self.size, self.blocks, self.sems, self.parts = size, blocks, sems, parts
        self.place = ring_place(lax.axis_index("dp"), size)
        self.sent = []
        self.live = {}

    def send(self, step):
        size, half = self.size, self.blocks.shape[1] // 2
        piece = half // self.parts
        for part in range(self.parts):
            for way in (0, 1):
                sign = 1 - 2 * way
                rows = pl.ds(way * half + part * piece, piece)
                source = self.blocks.at[slot_of(-sign * step, size), rows]
                target = self.blocks.at[slot_of(-sign * (step + 1), size), rows]
                device = (ring_index(self.place + size + sign, size), lax.axis_index("tensor"))
                copy = push(
                    source,
                    target,
                    (self.sems.at[0, way, step, part], self.sems.at[1, way, step, part]),
                    device,
                )
                if step > 0:
                    self.live[step - 1, part, way].wait_recv()
                copy.start()
                self.live[step, part, way] = copy
                self.sent.append(copy)

    def step(self, step):
        if step + 1 < self.size - 1:
            self.send(step + 1)
        else:
            for part in range(self.parts):
                for way in (0, 1):
                    self.live[step, part, way].wait_recv()

    def finish(self):
        for copy in self.sent:
            copy.wait_send()


def row_loop(total, rows, body):
    def run(index, carry):
        body(pl.ds(pl.multiple_of(index * rows, rows), rows))
        return carry

    lax.fori_loop(0, total // rows, run, 0)


def exchange_tokens_body(
    size,
    part_ref,
    token_ref,
    pack_ref,
    gain_ref,
    middle_ref,
    inputs_ref,
    packs_ref,
    from_partner,
    from_across,
    joined,
    ring_sems,
    pack_sems,
    side_sems,
    local_sem,
):
    f32 = jnp.float32
    dp = lax.axis_index("dp")
    own, partner, across = tensor_peers()
    far_partner = (partner + 2) % 4
    quarter = token_ref.shape[0]
    place = ring_place(dp, size)
    neighbours = [(ring_index(place + 1, size), own), (ring_index(place + size - 1, size), own)]
    greet(neighbours + [(dp, partner), (dp, across)])

    def part_rows(index):
        return pl.ds(pl.multiple_of(index * quarter, quarter), quarter)

    def side(index):
        return (side_sems.at[0, index], side_sems.at[1, index])

    first = push(part_ref.at[part_rows(far_partner)], from_partner.at[1], side(0), (dp, partner))
    second = push(part_ref.at[part_rows(partner)], from_partner.at[0], side(1), (dp, partner))
    first.start()
    second.start()
    keep = pltpu.make_async_copy(pack_ref, packs_ref.at[size - 1], local_sem)
    keep.start()
    keep.wait()
    packs = GatherRing(size, packs_ref, pack_sems)
    packs.send(0)
    first.wait_recv()
    base = across * quarter

    def join(rows):
        there = pl.ds(pl.multiple_of(base + rows.start, 16), rows.size)
        joined[rows, :] = (
            part_ref[there, :].astype(f32) + from_partner[1, rows, :].astype(f32)
        ).astype(jnp.bfloat16)

    row_loop(quarter, 16, join)
    third = push(joined, from_across, side(2), (dp, across))
    third.start()
    packs.step(0)
    second.wait_recv()
    third.wait_recv()
    mine = own * quarter

    def norm(rows):
        there = pl.ds(pl.multiple_of(mine + rows.start, 16), rows.size)
        middle = (
            token_ref[rows, :].astype(f32)
            + part_ref[there, :].astype(f32)
            + from_partner[0, rows, :].astype(f32)
            + from_across[rows, :].astype(f32)
        )
        middle_ref[rows, :] = middle
        inverse = lax.rsqrt(jnp.mean(middle * middle, axis=-1, keepdims=True) + EPSILON)
        inputs_ref[size - 1, rows, :] = (middle * inverse * gain_ref[...]).astype(jnp.bfloat16)

    row_loop(quarter, 16, norm)
    tokens = GatherRing(size, inputs_ref, ring_sems)
    tokens.send(0)
    for step in range(1, size - 1):
        packs.step(step)
        tokens.step(step - 1)
    tokens.step(size - 2)
    packs.finish()
    tokens.finish()
    first.wait_send()
    second.wait_send()
    third.wait_send()


def exchange_tokens(size, partial, token_rows, packed, gain):
    quarter, width = token_rows.shape
    columns = packed.shape[1]
    bf = jnp.bfloat16
    vmem = pl.BlockSpec(memory_space=pltpu.VMEM)
    dma = pltpu.SemaphoreType.DMA
    return pl.pallas_call(
        functools.partial(exchange_tokens_body, size),
        out_shape=(
            jax.ShapeDtypeStruct((quarter, width), jnp.float32),
            jax.ShapeDtypeStruct((size, quarter, width), bf),
            jax.ShapeDtypeStruct((size, quarter, columns), bf),
        ),
        in_specs=[vmem] * 4,
        out_specs=(vmem,) * 3,
        scratch_shapes=[
            pltpu.VMEM((2, quarter, width), bf),
            pltpu.VMEM((quarter, width), bf),
            pltpu.VMEM((quarter, width), bf),
            dma((2, 2, size - 1, 2)),
            dma((2, 2, size - 1, 2)),
            dma((2, 3)),
            dma(()),
        ],
        compiler_params=pltpu.CompilerParams(
            collective_id=0, has_side_effects=True, vmem_limit_bytes=VMEM_LIMIT
        ),
        name="exchange_tokens",
    )(partial, token_rows, packed, gain.reshape(1, -1))


def matmul_nt(left, right):
    return lax.dot_general(left, right, (((1,), (1,)), ((), ())), preferred_element_type=jnp.float32)


def matmul(left, right):
    return lax.dot_general(left, right, (((1,), (0,)), ((), ())), preferred_element_type=jnp.float32)


def run_experts_body(
    size,
    local_experts,
    experts,
    inputs_ref,
    packs_ref,
    weights_ref,
    member_ref,
    middle_ref,
    gain_ref,
    hidden_out,
    kept_ref,
    given_ref,
    gmid_ref,
    gmid_all,
    gain_out,
    weights,
    hidden,
    grad_parts,
    mix_parts,
    grad_slots,
    mix_slots,
    turned,
    stage,
    totals,
    load_sems,
    grad_sems,
    mix_sems,
    side_sems,
    store_sems,
    give_sems,
):
    f32, bf = jnp.float32, jnp.bfloat16
    dp = lax.axis_index("dp")
    own, partner, across = tensor_peers()
    width = inputs_ref.shape[1]
    quarter = inputs_ref.shape[0] // size
    pair = 2 * quarter
    half = size // 2
    units = weights.shape[1]
    members = weights_ref.shape[0]
    span = units // members
    cut = width // 2
    wide = 512
    place = ring_place(dp, size)
    forward = (ring_index(place + 1, size), own)
    backward = (ring_index(place + size - 1, size), own)
    greet([forward, backward, (dp, partner), (dp, across)])
    pieces = units // LANES
    each = pieces // members

    def load(piece):
        source = weights_ref.at[piece // each, :, pl.ds((piece % each) * LANES, LANES), :]
        target = weights.at[:, pl.ds(piece * LANES, LANES), :]
        return pltpu.make_async_copy(source, target, load_sems.at[piece])

    for piece in range(pieces):
        load(piece).start()

    grad_ring = (grad_parts, grad_slots, grad_sems)
    mix_ring = (mix_parts, mix_slots, mix_sems)

    def ring_copy(ring, way, step, source):
        device = forward if way == 0 else backward
        _, slots, sems = ring
        return push(
            source, slots.at[way, step], (sems.at[0, way, step], sems.at[1, way, step]), device
        )

    def columns_of(way):
        return pl.ds(way * cut, cut)

    def ring_step(ring, step, blocks, first=False):
        parts, slots, _ = ring
        for way in (0, 1):
            if first:
                source = parts.at[blocks[way], :, columns_of(way)]
            else:
                source = slots.at[way, step - 1]
                ring_copy(ring, way, step - 1, source).wait_recv()

                def add(rows):
                    slots[way, step - 1, rows, :] = (
                        slots[way, step - 1, rows, :].astype(f32)
                        + parts[blocks[way], rows, columns_of(way)].astype(f32)
                    ).astype(bf)

                row_loop(quarter, 16, add)
            ring_copy(ring, way, step, source).start()

    def do_pair(index, carry):
        rows = pl.ds(pl.multiple_of(index * pair, pair), pair)
        tail = packs_ref[rows, width:].astype(f32)
        lane = lax.broadcasted_iota(jnp.int32, tail.shape, 1)
        shares = []
        for expert in range(local_experts):
            name = dp * local_experts + expert
            picked = (lane == name) | (lane == experts + name)
            shares.append(jnp.sum(jnp.where(picked, tail, 0.0), axis=1, keepdims=True))

        def do_units(tile, carry):
            here = pl.ds(pl.multiple_of(tile * wide, wide), wide)

            @pl.when(index == 0)
            def _():
                for piece in range(wide // LANES):
                    load(tile * (wide // LANES) + piece).wait()

            scale = shares[0] * member_ref[0:1, here]
            for expert in range(1, local_experts):
                scale = scale + shares[expert] * member_ref[expert : expert + 1, here]
            tokens = inputs_ref[rows, :]
            gate = matmul_nt(tokens, weights[0, here, :])
            upward = matmul_nt(tokens, weights[1, here, :])
            grads = scale * matmul_nt(packs_ref[rows, :width], weights[2, here, :])
            share = jax.nn.sigmoid(gate)
            silu = gate * share
            hidden[0, rows, here] = (grads * upward * share * (1.0 + gate * (1.0 - share))).astype(bf)
            hidden[1, rows, here] = (grads * silu).astype(bf)
            hidden[2, rows, here] = (scale * silu * upward).astype(bf)
            return carry

        lax.fori_loop(0, units // wide, do_units, 0)

        def do_columns(tile, carry):
            here = pl.ds(pl.multiple_of(tile * wide, wide), wide)
            sums = matmul(hidden[0, rows, :], weights[0, :, here]) + matmul(
                hidden[1, rows, :], weights[1, :, here]
            )
            low = sums.astype(bf)
            grad_parts[2 * index, :, here] = low[:quarter]
            grad_parts[2 * index + 1, :, here] = low[quarter:]
            return carry

        def do_mix(tile, carry):
            here = pl.ds(pl.multiple_of(tile * wide, wide), wide)
            low = matmul(hidden[2, rows, :], weights[2, :, here]).astype(bf)
            mix_parts[2 * index, :, here] = low[:quarter]
            mix_parts[2 * index + 1, :, here] = low[quarter:]
            return carry

        lax.fori_loop(0, width // wide, do_columns, 0)

        def go_on(ring):
            @pl.when(index == 0)
            def _():
                ring_step(ring, 0, (0, 1), first=True)

            @pl.when(index > 0)
            def _():
                ring_step(ring, index, (2 * index, 2 * index + 1 - index // (half - 1)))

        go_on(grad_ring)
        lax.fori_loop(0, width // wide, do_mix, 0)
        go_on(mix_ring)
        return carry

    lax.fori_loop(0, half, do_pair, 0)
    far_partner = (partner + 2) % 4

    def keep(index, slot):
        target = kept_ref.at[index % members - 2, index // members]
        return pltpu.make_async_copy(stage.at[slot], target, store_sems.at[slot])

    def give(index, slot):
        target = given_ref.at[index % members, index // members]
        number = 2 * (index // members) + index % members
        return push(
            stage.at[slot], target, (give_sems.at[0, number], give_sems.at[1, number]), (dp, partner)
        )

    def weight_grads(first, last):
        def run(index, carry):
            kind = index // members
            whose = index % members
            slot = index % 2
            member = jnp.where(whose < 2, partner + 2 * whose, own + 2 * (3 - whose)) % members

            @pl.when((index >= 2) & (whose < 2))
            def _():
                keep(index - 2, slot).wait()

            @pl.when(whose >= 2)
            def _():
                give(index - 2, slot).wait_send()

            rows = pl.ds(pl.multiple_of(member * span, span), span)
            for chunk in range(half):
                some = pl.ds(chunk * pair, pair)
                turned[:, some] = hidden[kind, some, rows].T

            def do_columns(tile, carry):
                here = pl.ds(pl.multiple_of(tile * wide, wide), wide)
                source = inputs_ref if first < 2 * members else packs_ref
                stage[slot, :, here] = matmul(turned[...], source[:, here]).astype(bf)
                return carry

            lax.fori_loop(0, width // wide, do_columns, 0)

            @pl.when(whose < 2)
            def _():
                give(index, slot).start()

            @pl.when(whose >= 2)
            def _():
                keep(index, slot).start()

            return carry

        lax.fori_loop(first, last, run, 0)

    def final_sum():
        totals[...] = jnp.zeros_like(totals)
        for way in (0, 1):
            ring_copy(grad_ring, way, size - 2, grad_slots.at[way, size - 2]).wait_recv()
        base = own * quarter

        def finish(rows):
            sums = jnp.concatenate(
                [
                    grad_slots[0, size - 2, rows, :].astype(f32),
                    grad_slots[1, size - 2, rows, :].astype(f32),
                ],
                axis=-1,
            ) + grad_parts[size - 1, rows, :].astype(f32)
            middle = middle_ref[rows, :]
            inverse = lax.rsqrt(jnp.mean(middle * middle, axis=-1, keepdims=True) + EPSILON)
            hat = middle * inverse
            product = sums * hat
            totals[...] += product[:8] + product[8:]
            scaled = sums * gain_ref[...]
            back = inverse * (scaled - hat * jnp.mean(scaled * hat, axis=-1, keepdims=True))
            above = packs_ref[
                pl.ds(pl.multiple_of((size - 1) * quarter + rows.start, 16), rows.size), :width
            ]
            grad = above.astype(f32) + back
            gmid_ref[rows, :] = grad
            gmid_all[pl.ds(pl.multiple_of(base + rows.start, 16), rows.size), :] = grad.astype(bf)

        row_loop(quarter, 16, finish)
        gain_out[...] = jnp.sum(totals[...], axis=0, keepdims=True)

    def rows_of(index):
        return pl.ds(pl.multiple_of(index * quarter, quarter), quarter)

    def spread(index, whose, device):
        ref = gmid_all.at[rows_of(whose)]
        return push(ref, ref, (side_sems.at[0, index], side_sems.at[1, index]), device)

    def first_spread():
        spread(0, own, (dp, across)).start()
        spread(1, own, (dp, partner)).start()

    def second_spread():
        spread(0, own, (dp, across)).wait_recv()
        spread(2, across, (dp, partner)).start()

    def final_mix():
        for way in (0, 1):
            ring_copy(mix_ring, way, size - 2, mix_slots.at[way, size - 2]).wait_recv()

        def finish(rows):
            for way in (0, 1):
                columns = columns_of(way)
                hidden_out[rows, columns] = (
                    middle_ref[rows, columns]
                    + mix_slots[way, size - 2, rows, :].astype(f32)
                    + mix_parts[size - 1, rows, columns].astype(f32)
                ).astype(bf)

        row_loop(quarter, 16, finish)

    def closing():
        final_sum()
        first_spread()

    grad_events, mix_events = [], []
    for step in range(half, size - 1):
        delta = -(1 + step)
        blocks = (slot_of(delta, size), slot_of(-delta, size))
        grad_events.append(functools.partial(ring_step, grad_ring, step, blocks))
        mix_events.append(functools.partial(ring_step, mix_ring, step, blocks))
    events = grad_events[:-1]
    events += [grad_events[-1], mix_events[0], closing] + mix_events[1:2] + [second_spread]
    events += mix_events[2:] + [final_mix]
    work = [functools.partial(weight_grads, first, first + 2) for first in range(0, 3 * members, 2)]
    done = 0
    for number, piece in enumerate(work):
        piece()
        upto = -(-(number + 1) * len(events) // len(work))
        while done < upto:
            events[done]()
            done += 1
    for slot in (0, 1):
        keep(3 * members - 2 + slot, slot).wait()
    for kind in range(3):
        for whose in (0, 1):
            give(kind * members + whose, 0).wait_recv()
    spread(1, own, (dp, partner)).wait_recv()
    spread(2, across, (dp, partner)).wait_recv()
    for index, device in ((0, across), (1, partner), (2, partner)):
        spread(index, own, (dp, device)).wait_send()
    for ring in (grad_ring, mix_ring):
        for way in (0, 1):
            for step in range(size - 1):
                ring_copy(ring, way, step, ring[1].at[way, step]).wait_send()


def run_experts(size, inputs, packs, weights, middle, gain, experts):
    bf, f32 = jnp.bfloat16, jnp.float32
    members, _, span, width = weights.shape
    local_experts = experts // size
    rows = inputs.shape[0]
    quarter = rows // size
    units = members * span
    expert_of = (jnp.arange(units, dtype=jnp.int32) // (span // local_experts)) % local_experts
    member = (expert_of[None, :] == jnp.arange(local_experts, dtype=jnp.int32)[:, None]).astype(f32)
    vmem = pl.BlockSpec(memory_space=pltpu.VMEM)
    anywhere = pl.BlockSpec(memory_space=pl.ANY)
    dma = pltpu.SemaphoreType.DMA
    return pl.pallas_call(
        functools.partial(run_experts_body, size, local_experts, experts),
        out_shape=(
            jax.ShapeDtypeStruct((quarter, width), bf),
            jax.ShapeDtypeStruct((2, 3, span, width), bf),
            jax.ShapeDtypeStruct((2, 3, span, width), bf),
            jax.ShapeDtypeStruct((quarter, width), f32),
            jax.ShapeDtypeStruct((members * quarter, width), bf),
            jax.ShapeDtypeStruct((1, width), f32),
        ),
        in_specs=[vmem, vmem, anywhere, vmem, vmem, vmem],
        out_specs=(vmem, anywhere, anywhere, vmem, vmem, vmem),
        scratch_shapes=[
            pltpu.VMEM((3, units, width), bf),
            pltpu.VMEM((3, rows, units), bf),
            pltpu.VMEM((size, quarter, width), bf),
            pltpu.VMEM((size, quarter, width), bf),
            pltpu.VMEM((2, size - 1, quarter, width // 2), bf),
            pltpu.VMEM((2, size - 1, quarter, width // 2), bf),
            pltpu.VMEM((span, rows), bf),
            pltpu.VMEM((2, span, width), bf),
            pltpu.VMEM((8, width), f32),
            dma((units // LANES,)),
            dma((2, 2, size - 1)),
            dma((2, 2, size - 1)),
            dma((2, 3)),
            dma((2,)),
            dma((2, 6)),
        ],
        compiler_params=pltpu.CompilerParams(
            collective_id=2, has_side_effects=True, vmem_limit_bytes=VMEM_LIMIT
        ),
        name="run_experts",
    )(inputs, packs, weights, member, middle, gain.reshape(1, -1))


def back_through_head(grads, raw, gain, cosine, sine):
    hat_grads = grads * cosine - pltpu.roll(grads, grads.shape[1] // 2, 1) * sine
    inverse = lax.rsqrt(jnp.mean(raw * raw, axis=-1, keepdims=True) + EPSILON)
    hat = raw * inverse
    terms = hat_grads * hat
    scaled = hat_grads * gain
    back = inverse * (scaled - hat * jnp.mean(scaled * hat, axis=-1, keepdims=True))
    return back.astype(jnp.bfloat16), terms


def finish_layer_body(
    size,
    gmid_low_ref,
    out_weight_ref,
    mixed_ref,
    query_ref,
    key_ref,
    value_ref,
    raw_query_ref,
    raw_key_ref,
    normed_ref,
    query_weight_ref,
    key_weight_ref,
    value_weight_ref,
    cosine_ref,
    sine_ref,
    start_ref,
    query_gain_ref,
    key_gain_ref,
    middle_ref,
    token_ref,
    hidden_ref,
    cross_ref,
    gain_ref,
    gains_ref,
    hidden_all,
    crossed_ref,
    grad_all,
    gather_a,
    gather_b,
    gains_out,
    qkv_ref,
    out_ref,
    slots_a,
    slots_b,
    grad_mixed,
    grad_heads,
    key_sums,
    value_sums,
    turned,
    partial,
    from_partner,
    from_across,
    joined,
    totals,
    head_totals,
    pair_gains,
    ring_gains,
    sems_a,
    sems_b,
    ring_sems,
    side_sems,
):
    f32, bf = jnp.float32, jnp.bfloat16
    dp = lax.axis_index("dp")
    own, partner, across = tensor_peers()
    far_partner = (partner + 2) % 4
    quarter, width = token_ref.shape
    tokens = normed_ref.shape[0]
    head_dim = key_ref.shape[1]
    lead = query_ref.shape[1]
    heads = lead // head_dim
    scale = head_dim**-0.5
    place = ring_place(dp, size)
    forward = (ring_index(place + 1, size), own)
    backward = (ring_index(place + size - 1, size), own)
    ways = ((forward, 1), (backward, -1))
    greet([forward, backward, (dp, partner), (dp, across)])
    waits = []

    def start(copy):
        copy.start()
        waits.append(copy)
        return copy

    sets = (
        (qkv_ref, slots_a, gather_a, sems_a),
        (out_ref, slots_b, gather_b, sems_b),
    )

    def block_of(ref, block, way):
        rows = ref.shape[0] // size
        cut = ref.shape[1] // 2
        return (pl.ds(pl.multiple_of(block * rows, rows), rows), pl.ds(way * cut, cut))

    def wrap(value):
        return (value + 2 * size) % size

    live = {}

    def add_own(which, way, step):
        ref, slots, blocks, _ = sets[which]
        live[which, way, step].wait_recv()
        sign = ways[way][1]
        rows, columns = block_of(ref, wrap(place - sign * (2 + step)), way)
        base = rows.start

        def add(inner):
            there = pl.ds(pl.multiple_of(base + inner.start, 16), inner.size)
            sums = (slots[way, step, inner, :].astype(f32) + ref[there, columns].astype(f32)).astype(bf)
            if step == size - 2:
                blocks[place, inner, columns] = sums
            else:
                slots[way, step, inner, :] = sums

        row_loop(ref.shape[0] // size, 16, add)

    def ring_event(which, step):
        ref, slots, blocks, sems = sets[which]
        cut = ref.shape[1] // 2
        for way, (device, sign) in enumerate(ways):
            if step == 0:
                source = ref.at[block_of(ref, wrap(place - sign), way)]
            elif step < size:
                add_own(which, way, step - 1)
                source = slots.at[way, step - 1] if step < size - 1 else None
            else:
                live[which, way, step - 1].wait_recv()
            if step >= 2 * size - 2:
                continue
            if step >= size - 1:
                block = wrap(place - sign * (step - size + 1))
                source = blocks.at[block, :, pl.ds(way * cut, cut)]
                target = source
            else:
                target = slots.at[way, step]
            sem = (sems.at[0, way, step], sems.at[1, way, step])
            live[which, way, step] = start(push(source, target, sem, device))

    def part_rows(index):
        return pl.ds(pl.multiple_of(index * quarter, quarter), quarter)

    def side(index):
        return (side_sems.at[0, index], side_sems.at[1, index])

    mine = part_rows(own)
    home = own * quarter

    step_rows = 2 * LANES
    wide = 4 * LANES

    def out_rows(index, carry):
        rows = pl.ds(pl.multiple_of(index * step_rows, step_rows), step_rows)
        turned[...] = mixed_ref[:, rows].T

        def columns(tile, carry):
            here = pl.ds(pl.multiple_of(tile * wide, wide), wide)
            out_ref[rows, here] = matmul(turned[...], gmid_low_ref[:, here]).astype(bf)
            return carry

        return lax.fori_loop(0, width // wide, columns, carry)

    lax.fori_loop(0, lead // step_rows, out_rows, 0)
    ring_event(1, 0)

    def keep(rows):
        hidden_all[pl.ds(pl.multiple_of(home + rows.start, 16), rows.size), :] = hidden_ref[rows, :]

    row_loop(quarter, 16, keep)
    shown = [start(push(hidden_ref, hidden_all.at[mine], side(9), (dp, across)))]
    shown.append(start(push(hidden_ref, hidden_all.at[mine], side(10), (dp, partner))))

    def mixed_columns(tile, carry):
        here = pl.ds(pl.multiple_of(tile * wide, wide), wide)
        grad_mixed[:, here] = matmul_nt(gmid_low_ref[...], out_weight_ref[here, :]).astype(bf)
        return carry

    lax.fori_loop(0, lead // wide, mixed_columns, 0)
    key_sums[...] = jnp.zeros_like(key_sums)
    value_sums[...] = jnp.zeros_like(value_sums)
    head_totals[...] = jnp.zeros_like(head_totals)
    block = tokens // 2

    def do_head(head, carry):
        lanes = pl.ds(pl.multiple_of(head * head_dim, head_dim), head_dim)
        for part in (0, 1):
            rows = pl.ds(part * block, block)
            count = (part + 1) * block
            keys = pl.ds(0, count)
            queries = query_ref[rows, lanes]
            outer = grad_mixed[rows, lanes]
            scores = matmul_nt(key_ref[keys, :], queries)
            key_at = lax.broadcasted_iota(jnp.int32, scores.shape, 0)
            query_at = lax.broadcasted_iota(jnp.int32, scores.shape, 1) + part * block
            seen = (key_at <= query_at) & (key_at >= start_ref[:, rows])
            exponent = jnp.where(seen, jnp.exp(scores * scale), 0.0)
            soft = exponent * (1.0 / jnp.sum(exponent, axis=0, keepdims=True))
            grad_soft = matmul_nt(value_ref[keys, :], outer)
            inner = jnp.sum(soft * grad_soft, axis=0, keepdims=True)
            grad_scores = (soft * (grad_soft - inner)).astype(bf)
            value_sums[keys, :] += matmul(soft.astype(bf), outer)
            key_sums[keys, :] += matmul(grad_scores, queries)
            grad_query = scale * lax.dot_general(
                grad_scores, key_ref[keys, :], (((0,), (0,)), ((), ())), preferred_element_type=f32
            )
            low, terms = back_through_head(
                grad_query, raw_query_ref[rows, lanes], query_gain_ref[...], cosine_ref[rows, :], sine_ref[rows, :]
            )
            grad_heads[rows, lanes] = low
            head_totals[0] += jnp.sum(terms.reshape(-1, 8, head_dim), axis=0)
        return carry

    lax.fori_loop(0, heads // 2, do_head, 0)
    ring_event(1, 1)
    lax.fori_loop(heads // 2, heads, do_head, 0)
    ring_event(1, 2)
    low, terms = back_through_head(
        scale * key_sums[...], raw_key_ref[...], key_gain_ref[...], cosine_ref[...], sine_ref[...]
    )
    grad_heads[:, pl.ds(lead, head_dim)] = low
    head_totals[1] += jnp.sum(terms.reshape(-1, 8, head_dim), axis=0)
    grad_heads[:, pl.ds(lead + head_dim, head_dim)] = value_sums[...].astype(bf)

    def in_rows(index, carry):
        rows = pl.ds(pl.multiple_of(index * step_rows, step_rows), step_rows)
        turned[...] = normed_ref[:, rows].T
        qkv_ref[rows, :] = matmul(turned[...], grad_heads[...]).astype(bf)
        return carry

    lax.fori_loop(0, width // step_rows, in_rows, 0)
    ring_event(1, 3)
    ring_event(0, 0)

    def token_columns(tile, carry):
        here = pl.ds(pl.multiple_of(tile * wide, wide), wide)
        sums = matmul_nt(grad_heads[:, :lead], query_weight_ref[here, :])
        sums = sums + matmul_nt(grad_heads[:, lead : lead + head_dim], key_weight_ref[here, :])
        sums = sums + matmul_nt(grad_heads[:, lead + head_dim :], value_weight_ref[here, :])
        partial[:, here] = sums.astype(bf)
        return carry

    lax.fori_loop(0, width // wide, token_columns, 0)
    first = start(push(partial.at[part_rows(far_partner)], from_partner.at[1], side(0), (dp, partner)))
    second = start(push(partial.at[part_rows(partner)], from_partner.at[0], side(1), (dp, partner)))
    ring_event(1, 4)
    first.wait_recv()
    away = across * quarter

    def join(rows):
        there = pl.ds(pl.multiple_of(away + rows.start, 16), rows.size)
        joined[rows, :] = (partial[there, :].astype(f32) + from_partner[1, rows, :].astype(f32)).astype(bf)

    row_loop(quarter, 16, join)
    third = start(push(joined, from_across, side(2), (dp, across)))
    ring_event(0, 1)
    ring_event(1, 5)
    second.wait_recv()
    third.wait_recv()
    totals[...] = jnp.zeros_like(totals)

    def finish(rows):
        there = pl.ds(pl.multiple_of(home + rows.start, 16), rows.size)
        grads = (
            partial[there, :].astype(f32)
            + from_partner[0, rows, :].astype(f32)
            + from_across[rows, :].astype(f32)
        )
        hidden = token_ref[rows, :].astype(f32)
        inverse = lax.rsqrt(jnp.mean(hidden * hidden, axis=-1, keepdims=True) + EPSILON)
        hat = hidden * inverse
        product = grads * hat
        totals[...] += product[:8] + product[8:]
        scaled = grads * gain_ref[...]
        back = inverse * (scaled - hat * jnp.mean(scaled * hat, axis=-1, keepdims=True))
        grad_all[there, :] = (middle_ref[rows, :] + back).astype(bf)

    row_loop(quarter, 16, finish)
    spread = [start(push(grad_all.at[mine], grad_all.at[mine], side(3), (dp, across)))]
    spread.append(start(push(grad_all.at[mine], grad_all.at[mine], side(4), (dp, partner))))
    pair_gains[0, :, :width] = jnp.sum(totals[...], axis=0, keepdims=True)
    pair_gains[0, :, width : 2 * width] = gains_ref[...]
    pair_gains[0, :, 2 * width : 2 * width + head_dim] = jnp.sum(head_totals[0], axis=0, keepdims=True)
    pair_gains[0, :, 2 * width + head_dim :] = jnp.sum(head_totals[1], axis=0, keepdims=True)
    swap = start(push(pair_gains.at[0], pair_gains.at[1], side(5), (dp, partner)))
    ring_event(0, 2)
    ring_event(1, 6)
    far = part_rows(across)
    shown[0].wait_recv()
    shown.append(start(push(hidden_all.at[far], hidden_all.at[far], side(11), (dp, partner))))
    spread[0].wait_recv()
    spread.append(start(push(grad_all.at[far], grad_all.at[far], side(6), (dp, partner))))
    swap.wait_recv()
    pair_gains[2] = pair_gains[0] + pair_gains[1]
    swap = start(push(pair_gains.at[2], pair_gains.at[3], side(7), (dp, across)))
    ring_event(0, 3)
    ring_event(1, 7)
    swap.wait_recv()
    crossing = start(push(cross_ref, crossed_ref, side(8), (dp, across)))
    ring_gains[place] = pair_gains[2] + pair_gains[3]
    small = None
    for step in range(4, 2 * size - 1):
        ring_event(0, step)
        if step + 4 < 2 * size - 1:
            ring_event(1, step + 4)
        if step - 4 < size - 1:
            if small is not None:
                small.wait_recv()
            ref = ring_gains.at[wrap(place - step + 4)]
            sem = (ring_sems.at[0, step - 4], ring_sems.at[1, step - 4])
            small = start(push(ref, ref, sem, forward))
    small.wait_recv()
    gains_out[...] = jnp.sum(ring_gains[...], axis=0)
    for copy in (spread[1], spread[2], shown[1], shown[2], crossing):
        copy.wait_recv()
    for copy in waits:
        copy.wait_send()


def finish_layer(size, *arguments):
    bf, f32 = jnp.bfloat16, jnp.float32
    (
        _, out_weight, mixed, query, key, _, _, _, normed, query_weight, _, _, _, _, _, _, _, _, token_rows, _,
        cross, _, _,
    ) = arguments
    quarter, width = token_rows.shape
    tokens = normed.shape[0]
    lead, head_dim = query.shape[1], key.shape[1]
    vmem = pl.BlockSpec(memory_space=pltpu.VMEM)
    anywhere = pl.BlockSpec(memory_space=pl.ANY)
    dma = pltpu.SemaphoreType.DMA
    columns = lead + 2 * head_dim
    rows_a, rows_b = width // size, lead // size
    count = 2 * width + 2 * head_dim
    return pl.pallas_call(
        functools.partial(finish_layer_body, size),
        out_shape=(
            jax.ShapeDtypeStruct((tokens, width), bf),
            jax.ShapeDtypeStruct(cross.shape, bf),
            jax.ShapeDtypeStruct((tokens, width), bf),
            jax.ShapeDtypeStruct((size, rows_a, columns), bf),
            jax.ShapeDtypeStruct((size, rows_b, width), bf),
            jax.ShapeDtypeStruct((1, count), f32),
        ),
        in_specs=[anywhere if argument is cross else vmem for argument in arguments],
        out_specs=(vmem, anywhere) + (vmem,) * 4,
        scratch_shapes=[
            pltpu.VMEM((width, columns), bf),
            pltpu.VMEM((lead, width), bf),
            pltpu.VMEM((2, size - 1, rows_a, columns // 2), bf),
            pltpu.VMEM((2, size - 1, rows_b, width // 2), bf),
            pltpu.VMEM((tokens, lead), bf),
            pltpu.VMEM((tokens, columns), bf),
            pltpu.VMEM((tokens, head_dim), f32),
            pltpu.VMEM((tokens, head_dim), f32),
            pltpu.VMEM((2 * LANES, tokens), bf),
            pltpu.VMEM((tokens, width), bf),
            pltpu.VMEM((2, quarter, width), bf),
            pltpu.VMEM((quarter, width), bf),
            pltpu.VMEM((quarter, width), bf),
            pltpu.VMEM((8, width), f32),
            pltpu.VMEM((2, 8, head_dim), f32),
            pltpu.VMEM((4, 1, count), f32),
            pltpu.VMEM((size, 1, count), f32),
            dma((2, 2, 2 * size - 2)),
            dma((2, 2, 2 * size - 2)),
            dma((2, size - 1)),
            dma((2, 12)),
        ],
        compiler_params=pltpu.CompilerParams(
            collective_id=1, has_side_effects=True, vmem_limit_bytes=VMEM_LIMIT
        ),
        name="finish_layer",
    )(*arguments)


def large_experts(size, inputs, packs, all_weights, middle, gain, experts):
    f32, bf = jnp.float32, jnp.bfloat16
    members, _, units, model_width = all_weights.shape
    local_experts = experts // size
    indices = jnp.arange(size, dtype=jnp.int32)
    half = size // 2
    delta = (ring_place(indices, size) - ring_place(lax.axis_index("dp"), size)) % size
    ahead = jnp.where(delta == half, size - 2, jnp.where(delta == 0, size - 1, 2 * delta - 1))
    slots = jnp.where(delta > half, 2 * (size - delta) - 2, ahead)
    quarter = middle.shape[0]
    out_rows = packs[-quarter:, :model_width]
    inputs = inputs.reshape(size, quarter, -1)[slots].reshape(-1, model_width)
    packs = packs.reshape(size, quarter, -1)[slots].reshape(inputs.shape[0], -1)
    grads_all = packs[:, :model_width]
    shares = packs[:, model_width : model_width + 2 * experts].astype(f32)
    shares = shares[:, :experts] + shares[:, experts:]
    shares = lax.dynamic_slice_in_dim(
        shares, lax.axis_index("dp") * local_experts, local_experts, 1
    )
    weight_cols = jnp.broadcast_to(
        shares[:, None, :, None],
        (shares.shape[0], members, local_experts, units // local_experts),
    ).reshape(-1, members, units)

    def project(left, which):
        return jnp.einsum("td,rud->tru", left, all_weights[:, which], preferred_element_type=f32)

    gate_act = project(inputs, 0)
    upward = project(inputs, 1)
    sigmoid_gate = jax.nn.sigmoid(gate_act)
    active = gate_act * sigmoid_gate * upward
    weighted_low = (weight_cols * active).astype(bf)
    mixture_part = jnp.einsum(
        "tru,rud->td", weighted_low, all_weights[:, 2], preferred_element_type=f32
    ).astype(bf)
    grad_active = weight_cols * project(grads_all, 2)
    grad_gate = (
        grad_active * upward * sigmoid_gate * (1.0 + gate_act * (1.0 - sigmoid_gate))
    ).astype(bf)
    grad_up = (grad_active * gate_act * sigmoid_gate).astype(bf)
    grad_normed_part = jnp.einsum(
        "tru,rud->td", grad_gate, all_weights[:, 0], preferred_element_type=f32
    ) + jnp.einsum("tru,rud->td", grad_up, all_weights[:, 1], preferred_element_type=f32)
    grad_normed_two = lax.psum_scatter(grad_normed_part.astype(bf), "dp", tiled=True).astype(f32)
    weight_grads = jnp.stack(
        [
            jnp.einsum("tru,td->rud", grad_gate, inputs, preferred_element_type=f32).astype(bf),
            jnp.einsum("tru,td->rud", grad_up, inputs, preferred_element_type=f32).astype(bf),
            jnp.einsum("tru,td->rud", weighted_low, grads_all, preferred_element_type=f32).astype(bf),
        ],
        axis=1,
    )
    hat_two, inv_two = rms_parts(middle)
    grad_gain_two = jnp.sum(grad_normed_two * hat_two, axis=0)
    grad_middle = out_rows.astype(f32) + rms_back(grad_normed_two * gain, hat_two, inv_two)
    grad_mid_low = lax.all_gather(grad_middle.astype(bf), "tensor", tiled=True)
    mixture = lax.psum_scatter(mixture_part, "dp", tiled=True).astype(f32)
    hidden_out = (middle + mixture).astype(bf)
    zero = jnp.zeros(weight_grads.shape[1:], bf)
    sums = lax.psum_scatter(weight_grads.reshape(-1, model_width), "tensor", tiled=True)
    kept = jnp.stack([zero, sums.reshape(zero.shape)])
    given = jnp.stack([zero, zero])
    return (hidden_out, kept, given, grad_middle, grad_mid_low, grad_gain_two)


def local(
    hidden_in,
    seq_lens,
    norm1_gain,
    query_weight,
    key_weight,
    value_weight,
    query_gain,
    key_gain,
    out_weight,
    norm2_gain,
    w_gate_up,
    w_down,
    routes,
    route_weights,
    out_grad,
):
    bf = jnp.bfloat16
    f32 = jnp.float32
    tokens, model_width = hidden_in.shape
    local_experts = w_gate_up.shape[0]
    hidden_part = w_gate_up.shape[3]
    head_dim = query_gain.shape[0]
    local_heads = query_weight.shape[1] // head_dim
    data_size = lax.axis_size("dp")
    tensor_size = lax.axis_size("tensor")
    quarter = tokens // tensor_size
    experts = local_experts * data_size
    score_scale = head_dim ** (-0.5)
    row0 = lax.axis_index("tensor") * quarter

    def mine(array):
        return lax.dynamic_slice_in_dim(array, row0, quarter, 0)

    expert_ids = jnp.arange(experts, dtype=jnp.int32)
    dense = jnp.sum(
        jnp.where(mine(routes)[:, :, None] == expert_ids[None, None, :], mine(route_weights)[:, :, None], 0.0),
        axis=1,
    )
    dense_high = dense.astype(bf)
    dense_low = (dense - dense_high.astype(f32)).astype(bf)
    spare = -2 * experts % LANES
    packed = jnp.concatenate(
        [mine(out_grad), dense_high, dense_low, jnp.zeros((quarter, spare), bf)], axis=1
    )
    rows = data_size * quarter
    units = local_experts * hidden_part
    own_weights = jnp.concatenate(
        [
            jnp.transpose(w_gate_up, (2, 0, 3, 1)).reshape(2, units, model_width),
            w_down.reshape(1, units, model_width),
        ],
        axis=0,
    )
    all_weights = lax.all_gather(own_weights, "tensor")
    hidden = hidden_in.astype(f32)
    hat_one, _ = rms_parts(hidden)
    normed = (hat_one * norm1_gain).astype(bf)
    query_proj = jnp.dot(normed, query_weight, preferred_element_type=f32).reshape(
        tokens, local_heads, head_dim
    )
    key_proj = jnp.dot(normed, key_weight, preferred_element_type=f32)
    value_low = jnp.dot(normed, value_weight, preferred_element_type=f32).astype(bf)
    places, starts = sequence_layout(seq_lens[0], tokens)
    cosine_table, sine_table = rotary_tables(places - starts, head_dim)
    query_hat, _ = rms_parts(query_proj)
    query_low = rotate(
        query_hat * query_gain, cosine_table[:, None, :], sine_table[:, None, :]
    ).astype(bf)
    key_hat, _ = rms_parts(key_proj)
    key_low = rotate(key_hat * key_gain, cosine_table, sine_table).astype(bf)
    visible = (places[None, :] <= places[:, None]) & (places[None, :] >= starts[:, None])
    scores = jnp.einsum("thd,sd->hts", query_low, key_low, preferred_element_type=f32) * score_scale
    exponent = jnp.where(visible[None], jnp.exp(scores), 0.0)
    totals = jnp.sum(exponent, axis=-1, keepdims=True)
    soft_low = (exponent / totals).astype(bf)
    mixed_low = (
        jnp.einsum("hts,sd->thd", soft_low, value_low, preferred_element_type=f32)
        .reshape(tokens, local_heads * head_dim)
        .astype(bf)
    )
    hidden_q = mine(hidden_in)
    partial = jnp.dot(mixed_low, out_weight, preferred_element_type=f32).astype(bf)
    middle, inputs, gathered = exchange_tokens(data_size, partial, hidden_q, packed, norm2_gain)
    stage = run_experts if data_size <= 8 else large_experts
    hidden_out, kept, given, grad_middle, grad_mid_low, grad_gain_two = stage(
        data_size,
        inputs.reshape(rows, model_width),
        gathered.reshape(rows, -1),
        all_weights,
        middle,
        norm2_gain,
        experts,
    )
    joined = (kept[0].astype(f32) + given[1].astype(f32)).astype(bf)
    both = jnp.concatenate([cosine_table, cosine_table], axis=1)
    signed = jnp.concatenate([-sine_table, sine_table], axis=1)
    hidden_out, crossed, grad_hidden, in_low, out_low, gains = finish_layer(
        data_size,
        grad_mid_low,
        out_weight,
        mixed_low,
        query_low.reshape(tokens, -1),
        key_low,
        value_low,
        query_proj.reshape(tokens, -1),
        key_proj,
        normed,
        query_weight,
        key_weight,
        value_weight,
        both,
        signed,
        starts.reshape(1, -1).astype(jnp.int32),
        query_gain.reshape(1, -1),
        key_gain.reshape(1, -1),
        grad_middle,
        hidden_q,
        hidden_out,
        joined,
        norm1_gain.reshape(1, -1),
        grad_gain_two.reshape(1, -1),
    )
    own_grads = kept[1].astype(f32) + given[0].astype(f32) + crossed.astype(f32)
    grad_w_gate_up = jnp.transpose(
        own_grads[:2].reshape(2, local_experts, hidden_part, model_width), (1, 3, 0, 2)
    )
    grad_w_down = own_grads[2].reshape(local_experts, hidden_part, model_width)
    in_low = in_low.reshape(model_width, -1)
    lead = local_heads * head_dim
    gains = gains.reshape(-1)
    return (
        hidden_out,
        grad_hidden,
        gains[:model_width],
        in_low[:, :lead].astype(f32),
        in_low[:, lead : lead + head_dim].astype(f32),
        in_low[:, lead + head_dim :].astype(f32),
        gains[2 * model_width : 2 * model_width + head_dim],
        gains[2 * model_width + head_dim :],
        out_low.reshape(-1, model_width).astype(f32),
        gains[model_width : 2 * model_width],
        grad_w_gate_up,
        grad_w_down,
    )


def solution(mesh):
    in_specs = (
        P("dp", None),
        P("dp", None),
        P(),
        P(None, "tensor"),
        P(None, "tensor"),
        P(None, "tensor"),
        P(),
        P(),
        P("tensor", None),
        P(),
        P("dp", None, None, "tensor"),
        P("dp", "tensor", None),
        P("dp", None),
        P("dp", None),
        P("dp", None),
    )
    out_specs = (
        P("dp", None),
        P("dp", None),
        P(),
        P(None, "tensor"),
        P(None, "tensor"),
        P(None, "tensor"),
        P(),
        P(),
        P("tensor", None),
        P(),
        P("dp", None, None, "tensor"),
        P("dp", "tensor", None),
    )
    return jax.shard_map(local, mesh=mesh, in_specs=in_specs, out_specs=out_specs, check_vma=False)
```

```python
import functools
import math

import jax
import jax.numpy as jnp
from jax import lax
from jax.experimental import pallas as pl
from jax.experimental.pallas import tpu as pltpu
from jax.sharding import PartitionSpec as P

EPSILON = 1e-06
ROPE_BASE = 1000000.0


def rms_parts(values):
    inverse = lax.rsqrt(jnp.mean(values * values, axis=-1, keepdims=True) + EPSILON)
    return (values * inverse, inverse)


def rms_back(grad_hat, normal_hat, inverse):
    return inverse * (
        grad_hat - normal_hat * jnp.mean(grad_hat * normal_hat, axis=-1, keepdims=True)
    )


def rotary_tables(positions, head_dim):
    halves = jnp.arange(head_dim // 2, dtype=jnp.float32)
    inverse = jnp.exp(halves * (-2.0 * math.log(ROPE_BASE) / head_dim))
    angles = positions.astype(jnp.float32)[:, None] * inverse[None, :]
    return (jnp.cos(angles), jnp.sin(angles))


def sequence_layout(lengths, token_count):
    endings = jnp.cumsum(lengths)
    places = jnp.arange(token_count, dtype=jnp.int32)
    starts = jnp.sum(jnp.where(endings[None, :] <= places[:, None], lengths[None, :], 0), axis=1)
    return (places, starts)


LANES = 128
MESH = pl.DeviceIdType.MESH
VMEM_LIMIT = 127 * 512 * 1024


def ring_place(index, size):
    return jnp.where(index % 2 == 0, index // 2, size - (index + 1) // 2)


def ring_index(place, size):
    place = place % size
    return jnp.where(place < size // 2, 2 * place, 2 * size - 1 - 2 * place)


def tensor_peers():
    own = lax.axis_index("tensor")
    partner = own + 1 - 2 * (own % 2)
    across = (own + 2) % 4
    return own, partner, across


def greet(devices):
    barrier = pltpu.get_barrier_semaphore()
    for device in devices:
        pl.semaphore_signal(barrier, inc=1, device_id=device, device_id_type=MESH)
    pl.semaphore_wait(barrier, len(devices))


def push(source, target, sems, device):
    return pltpu.make_async_remote_copy(
        src_ref=source,
        dst_ref=target,
        send_sem=sems[0],
        recv_sem=sems[1],
        device_id=device,
        device_id_type=MESH,
    )


def slot_of(delta, size):
    delta = (delta + size // 2 - 1) % size - (size // 2 - 1)
    if delta == 0:
        return size - 1
    if delta == size // 2:
        return size - 2
    return 2 * delta - 1 if delta > 0 else -2 * delta - 2


class GatherRing:
    def __init__(self, size, blocks, sems, parts=2):
        self.size, self.blocks, self.sems, self.parts = size, blocks, sems, parts
        self.place = ring_place(lax.axis_index("dp"), size)
        self.sent = []
        self.live = {}

    def send(self, step):
        size, half = self.size, self.blocks.shape[1] // 2
        piece = half // self.parts
        for part in range(self.parts):
            for way in (0, 1):
                sign = 1 - 2 * way
                rows = pl.ds(way * half + part * piece, piece)
                source = self.blocks.at[slot_of(-sign * step, size), rows]
                target = self.blocks.at[slot_of(-sign * (step + 1), size), rows]
                device = (ring_index(self.place + size + sign, size), lax.axis_index("tensor"))
                copy = push(
                    source,
                    target,
                    (self.sems.at[0, way, step, part], self.sems.at[1, way, step, part]),
                    device,
                )
                if step > 0:
                    self.live[step - 1, part, way].wait_recv()
                copy.start()
                self.live[step, part, way] = copy
                self.sent.append(copy)

    def step(self, step):
        if step + 1 < self.size - 1:
            self.send(step + 1)
        else:
            for part in range(self.parts):
                for way in (0, 1):
                    self.live[step, part, way].wait_recv()

    def finish(self):
        for copy in self.sent:
            copy.wait_send()


def row_loop(total, rows, body):
    def run(index, carry):
        body(pl.ds(pl.multiple_of(index * rows, rows), rows))
        return carry

    lax.fori_loop(0, total // rows, run, 0)


def matmul_nt(left, right):
    return lax.dot_general(left, right, (((1,), (1,)), ((), ())), preferred_element_type=jnp.float32)


def matmul(left, right):
    return lax.dot_general(left, right, (((1,), (0,)), ((), ())), preferred_element_type=jnp.float32)


def rms_rows(values):
    return lax.rsqrt(jnp.mean(values * values, axis=-1, keepdims=True) + EPSILON)


def turn(values, cosine, sine):
    return values * cosine + pltpu.roll(values, values.shape[1] // 2, 1) * sine


def start_layer_body(
    size,
    experts,
    token_ref,
    above_ref,
    route_ref,
    share_ref,
    query_weight_ref,
    key_weight_ref,
    value_weight_ref,
    out_weight_ref,
    gate_up_ref,
    down_ref,
    cosine_ref,
    sine_ref,
    start_ref,
    first_gain_ref,
    second_gain_ref,
    query_gain_ref,
    key_gain_ref,
    middle_ref,
    inputs_ref,
    packs_ref,
    others_ref,
    mixed_ref,
    query_ref,
    key_ref,
    value_ref,
    raw_query_ref,
    raw_key_ref,
    normed_ref,
    query_weight,
    key_weight,
    value_weight,
    out_weight,
    part_ref,
    from_partner,
    from_across,
    joined,
    ring_sems,
    pack_sems,
    side_sems,
    load_sems,
    near_sems,
    far_sems,
    pass_sems,
):
    f32, bf = jnp.float32, jnp.bfloat16
    dp = lax.axis_index("dp")
    own, partner, across = tensor_peers()
    far_partner = (partner + 2) % 4
    quarter, width = middle_ref.shape
    tokens = token_ref.shape[0]
    head_dim = key_ref.shape[1]
    lead = query_ref.shape[1]
    heads = lead // head_dim
    place = ring_place(dp, size)
    loads = []
    for index, (source, target) in enumerate(
        (
            (query_weight_ref, query_weight),
            (key_weight_ref, key_weight),
            (value_weight_ref, value_weight),
            (out_weight_ref, out_weight),
        )
    ):
        copy = pltpu.make_async_copy(source, target, load_sems.at[index])
        copy.start()
        loads.append(copy)
    mine = pl.ds(pl.multiple_of(own * quarter, quarter), quarter)
    base = own * quarter
    above = pltpu.make_async_copy(
        above_ref.at[mine], packs_ref.at[size - 1, :, pl.ds(0, width)], load_sems.at[4]
    )
    above.start()
    neighbours = [(ring_index(place + 1, size), own), (ring_index(place + size - 1, size), own)]
    greet(neighbours + [(dp, partner), (dp, across)])

    halves = 2
    pieces = []
    for kind in range(3):
        for expert in range(gate_up_ref.shape[0]):
            for half in range(halves):
                pieces.append((kind, expert, half))
    span = gate_up_ref.shape[2] // halves

    def piece_of(number):
        kind, expert, half = pieces[number]
        rows = pl.ds(half * span, span)
        source = gate_up_ref.at[expert, kind, rows] if kind < 2 else down_ref.at[expert, rows]
        return source, (kind, expert, rows)

    near = []
    for kind in range(3):
        for expert in range(gate_up_ref.shape[0]):
            number = len(near)
            source = gate_up_ref.at[expert, kind] if kind < 2 else down_ref.at[expert]
            copy = push(
                source,
                others_ref.at[0, kind, expert],
                (near_sems.at[0, number], near_sems.at[1, number]),
                (dp, partner),
            )
            copy.start()
            near.append(copy)
    far, passed = [], []

    def pump(passing=True):
        number = len(far)
        if number >= 2:
            old = far[number - 2]
            if number - 2 < len(pieces):
                old.wait_recv()
                kind, expert, rows = piece_of(number - 2)[1]
                copy = push(
                    others_ref.at[1, kind, expert, rows],
                    others_ref.at[2, kind, expert, rows],
                    (pass_sems.at[0, number - 2], pass_sems.at[1, number - 2]),
                    (dp, partner),
                )
                copy.start()
                passed.append(copy)
                old.wait_send()
        if number < len(pieces):
            source, (kind, expert, rows) = piece_of(number)
            copy = push(
                source,
                others_ref.at[1, kind, expert, rows],
                (far_sems.at[0, number], far_sems.at[1, number]),
                (dp, across),
            )
            copy.start()
            far.append(copy)
        else:
            far.append(None)

    pump()
    pump()

    tail = packs_ref.shape[2] - width
    lane = lax.broadcasted_iota(jnp.int32, (quarter, tail), 1)
    name = jnp.where(lane < experts, lane, lane - experts)
    dense = jnp.zeros((quarter, tail), f32)
    for choice in range(route_ref.shape[1]):
        named = route_ref[mine, choice : choice + 1]
        dense = dense + jnp.where(named == name, share_ref[mine, choice : choice + 1], 0.0)
    high = dense.astype(bf)
    low = (dense - high.astype(f32)).astype(bf)
    packs_ref[size - 1, :, width:] = jnp.where(
        lane < experts, high.astype(f32), jnp.where(lane < 2 * experts, low.astype(f32), 0.0)
    ).astype(bf)
    above.wait()
    packs = GatherRing(size, packs_ref, pack_sems)
    packs.send(0)

    def norm_first(rows):
        hidden = token_ref[rows, :].astype(f32)
        normed_ref[rows, :] = (hidden * rms_rows(hidden) * first_gain_ref[...]).astype(bf)

    row_loop(tokens, 16, norm_first)
    loads[0].wait()
    wide = 4 * LANES

    def project(tile, carry):
        here = pl.ds(pl.multiple_of(tile * wide, wide), wide)
        raw_query_ref[:, here] = matmul(normed_ref[...], query_weight[:, here])
        return carry

    lax.fori_loop(0, lead // wide, project, 0)
    loads[1].wait()
    loads[2].wait()
    raw_key = matmul(normed_ref[...], key_weight[...])
    raw_key_ref[...] = raw_key
    key_ref[...] = turn(
        raw_key * rms_rows(raw_key) * key_gain_ref[...], cosine_ref[...], sine_ref[...]
    ).astype(bf)
    value_ref[...] = matmul(normed_ref[...], value_weight[...]).astype(bf)
    packs.step(0)
    scale = head_dim**-0.5
    block = tokens // 2

    def do_head(head, carry):
        lanes = pl.ds(pl.multiple_of(head * head_dim, head_dim), head_dim)
        for part in (0, 1):
            rows = pl.ds(part * block, block)
            keys = pl.ds(0, (part + 1) * block)
            raw = raw_query_ref[rows, lanes]
            queries = turn(
                raw * rms_rows(raw) * query_gain_ref[...], cosine_ref[rows, :], sine_ref[rows, :]
            ).astype(bf)
            query_ref[rows, lanes] = queries
            scores = matmul_nt(key_ref[keys, :], queries)
            key_at = lax.broadcasted_iota(jnp.int32, scores.shape, 0)
            query_at = lax.broadcasted_iota(jnp.int32, scores.shape, 1) + part * block
            seen = (key_at <= query_at) & (key_at >= start_ref[:, rows])
            exponent = jnp.where(seen, jnp.exp(scores * scale), 0.0)
            soft = (exponent * (1.0 / jnp.sum(exponent, axis=0, keepdims=True))).astype(bf)
            mixed_ref[rows, lanes] = lax.dot_general(
                soft, value_ref[keys, :], (((0,), (0,)), ((), ())), preferred_element_type=f32
            ).astype(bf)
        return carry

    lax.fori_loop(0, heads // 2, do_head, 0)
    packs.step(1)
    pump()
    lax.fori_loop(heads // 2, heads, do_head, 0)
    packs.step(2)
    loads[3].wait()

    def share(tile, carry):
        here = pl.ds(pl.multiple_of(tile * wide, wide), wide)
        part_ref[:, here] = matmul(mixed_ref[...], out_weight[:, here]).astype(bf)
        return carry

    lax.fori_loop(0, width // wide, share, 0)

    def part_rows(index):
        return pl.ds(pl.multiple_of(index * quarter, quarter), quarter)

    def side(index):
        return (side_sems.at[0, index], side_sems.at[1, index])

    first = push(part_ref.at[part_rows(far_partner)], from_partner.at[1], side(0), (dp, partner))
    second = push(part_ref.at[part_rows(partner)], from_partner.at[0], side(1), (dp, partner))
    first.start()
    second.start()
    packs.step(3)
    first.wait_recv()
    away = across * quarter

    def join(rows):
        there = pl.ds(pl.multiple_of(away + rows.start, 16), rows.size)
        joined[rows, :] = (part_ref[there, :].astype(f32) + from_partner[1, rows, :].astype(f32)).astype(bf)

    row_loop(quarter, 16, join)
    third = push(joined, from_across, side(2), (dp, across))
    third.start()
    pump()
    second.wait_recv()
    third.wait_recv()

    def norm_second(rows):
        there = pl.ds(pl.multiple_of(base + rows.start, 16), rows.size)
        middle = (
            token_ref[there, :].astype(f32)
            + part_ref[there, :].astype(f32)
            + from_partner[0, rows, :].astype(f32)
            + from_across[rows, :].astype(f32)
        )
        middle_ref[rows, :] = middle
        inputs_ref[size - 1, rows, :] = (middle * rms_rows(middle) * second_gain_ref[...]).astype(bf)

    row_loop(quarter, 16, norm_second)
    ring = GatherRing(size, inputs_ref, ring_sems)
    ring.send(0)
    for step in range(size - 1):
        if step + 4 < size - 1:
            packs.step(step + 4)
        pump()
        ring.step(step)
    while len(far) < len(pieces) + 2:
        pump()
    packs.finish()
    ring.finish()
    first.wait_send()
    second.wait_send()
    third.wait_send()
    for copy in near + passed:
        copy.wait()


def start_layer(size, experts, *arguments):
    tokens_rows, _, _, _, query_weight, key_weight, value_weight, out_weight, gate_up = arguments[:9]
    bf, f32 = jnp.bfloat16, jnp.float32
    tokens, width = tokens_rows.shape
    quarter = tokens // 4
    lead, head_dim = query_weight.shape[1], key_weight.shape[1]
    columns = width + -(-2 * experts // LANES) * LANES
    local, _, units, _ = gate_up.shape
    vmem = pl.BlockSpec(memory_space=pltpu.VMEM)
    anywhere = pl.BlockSpec(memory_space=pl.ANY)
    dma = pltpu.SemaphoreType.DMA
    return pl.pallas_call(
        functools.partial(start_layer_body, size, experts),
        out_shape=(
            jax.ShapeDtypeStruct((quarter, width), f32),
            jax.ShapeDtypeStruct((size, quarter, width), bf),
            jax.ShapeDtypeStruct((size, quarter, columns), bf),
            jax.ShapeDtypeStruct((3, 3, local, units, width), bf),
            jax.ShapeDtypeStruct((tokens, lead), bf),
            jax.ShapeDtypeStruct((tokens, lead), bf),
            jax.ShapeDtypeStruct((tokens, head_dim), bf),
            jax.ShapeDtypeStruct((tokens, head_dim), bf),
            jax.ShapeDtypeStruct((tokens, lead), f32),
            jax.ShapeDtypeStruct((tokens, head_dim), f32),
            jax.ShapeDtypeStruct((tokens, width), bf),
        ),
        in_specs=[vmem, anywhere, vmem, vmem] + [anywhere] * 6 + [vmem] * 7,
        out_specs=(vmem, vmem, vmem, anywhere) + (vmem,) * 7,
        scratch_shapes=[
            pltpu.VMEM(query_weight.shape, bf),
            pltpu.VMEM(key_weight.shape, bf),
            pltpu.VMEM(value_weight.shape, bf),
            pltpu.VMEM(out_weight.shape, bf),
            pltpu.VMEM((tokens, width), bf),
            pltpu.VMEM((2, quarter, width), bf),
            pltpu.VMEM((quarter, width), bf),
            pltpu.VMEM((quarter, width), bf),
            dma((2, 2, size - 1, 2)),
            dma((2, 2, size - 1, 2)),
            dma((2, 3)),
            dma((5,)),
            dma((2, 3 * local)),
            dma((2, 6 * local)),
            dma((2, 6 * local)),
        ],
        compiler_params=pltpu.CompilerParams(
            collective_id=0, has_side_effects=True, vmem_limit_bytes=VMEM_LIMIT
        ),
        name="start_layer",
    )(*arguments)


def run_experts_body(
    size,
    local_experts,
    experts,
    inputs_ref,
    packs_ref,
    gate_up_ref,
    down_ref,
    others_ref,
    member_ref,
    middle_ref,
    gain_ref,
    hidden_out,
    kept_ref,
    given_ref,
    gmid_ref,
    gmid_all,
    gain_out,
    weights,
    hidden,
    grad_parts,
    mix_parts,
    grad_slots,
    mix_slots,
    turned,
    stage,
    totals,
    load_sems,
    grad_sems,
    mix_sems,
    side_sems,
    store_sems,
    give_sems,
):
    f32, bf = jnp.float32, jnp.bfloat16
    dp = lax.axis_index("dp")
    own, partner, across = tensor_peers()
    width = inputs_ref.shape[1]
    quarter = inputs_ref.shape[0] // size
    pair = 2 * quarter
    half = size // 2
    units = weights.shape[1]
    members = others_ref.shape[0] + 1
    span = units // members
    cut = width // 2
    wide = 512
    place = ring_place(dp, size)
    forward = (ring_index(place + 1, size), own)
    backward = (ring_index(place + size - 1, size), own)
    greet([forward, backward, (dp, partner), (dp, across)])
    part_units = span // local_experts
    loads = []
    for expert in range(local_experts):
        rows = pl.ds(expert * part_units, part_units)
        for kind in range(3):
            source = gate_up_ref.at[expert, kind] if kind < 2 else down_ref.at[expert]
            loads.append((expert * part_units, source, weights.at[kind, rows]))
    for other in range(members - 1):
        for first in range(0, span, LANES):
            at = (other + 1) * span + first
            source = others_ref.at[other, :, pl.ds(first, LANES)]
            loads.append((at, source, weights.at[:, pl.ds(at, LANES)]))
    loads = [
        (at, pltpu.make_async_copy(source, target, load_sems.at[number]))
        for number, (at, source, target) in enumerate(loads)
    ]
    for _, copy in loads:
        copy.start()

    grad_ring = (grad_parts, grad_slots, grad_sems)
    mix_ring = (mix_parts, mix_slots, mix_sems)

    def ring_copy(ring, way, step, source):
        device = forward if way == 0 else backward
        _, slots, sems = ring
        return push(
            source, slots.at[way, step], (sems.at[0, way, step], sems.at[1, way, step]), device
        )

    def columns_of(way):
        return pl.ds(way * cut, cut)

    def ring_step(ring, step, blocks, first=False):
        parts, slots, _ = ring
        for way in (0, 1):
            if first:
                source = parts.at[blocks[way], :, columns_of(way)]
            else:
                source = slots.at[way, step - 1]
                ring_copy(ring, way, step - 1, source).wait_recv()

                def add(rows):
                    slots[way, step - 1, rows, :] = (
                        slots[way, step - 1, rows, :].astype(f32)
                        + parts[blocks[way], rows, columns_of(way)].astype(f32)
                    ).astype(bf)

                row_loop(quarter, 16, add)
            ring_copy(ring, way, step, source).start()

    def do_pair(index, carry):
        rows = pl.ds(pl.multiple_of(index * pair, pair), pair)
        tail = packs_ref[rows, width:].astype(f32)
        lane = lax.broadcasted_iota(jnp.int32, tail.shape, 1)
        shares = []
        for expert in range(local_experts):
            name = dp * local_experts + expert
            picked = (lane == name) | (lane == experts + name)
            shares.append(jnp.sum(jnp.where(picked, tail, 0.0), axis=1, keepdims=True))

        def do_units(tile, carry):
            here = pl.ds(pl.multiple_of(tile * wide, wide), wide)

            for number in range(units // wide):

                @pl.when((index == 0) & (tile == number))
                def _():
                    for at, copy in loads:
                        if at // wide == number:
                            copy.wait()

            scale = shares[0] * member_ref[0:1, here]
            for expert in range(1, local_experts):
                scale = scale + shares[expert] * member_ref[expert : expert + 1, here]
            tokens = inputs_ref[rows, :]
            gate = matmul_nt(tokens, weights[0, here, :])
            upward = matmul_nt(tokens, weights[1, here, :])
            grads = scale * matmul_nt(packs_ref[rows, :width], weights[2, here, :])
            share = jax.nn.sigmoid(gate)
            silu = gate * share
            hidden[0, rows, here] = (grads * upward * share * (1.0 + gate * (1.0 - share))).astype(bf)
            hidden[1, rows, here] = (grads * silu).astype(bf)
            hidden[2, rows, here] = (scale * silu * upward).astype(bf)
            return carry

        lax.fori_loop(0, units // wide, do_units, 0)

        def do_columns(tile, carry):
            here = pl.ds(pl.multiple_of(tile * wide, wide), wide)
            sums = matmul(hidden[0, rows, :], weights[0, :, here]) + matmul(
                hidden[1, rows, :], weights[1, :, here]
            )
            low = sums.astype(bf)
            grad_parts[2 * index, :, here] = low[:quarter]
            grad_parts[2 * index + 1, :, here] = low[quarter:]
            return carry

        def do_mix(tile, carry):
            here = pl.ds(pl.multiple_of(tile * wide, wide), wide)
            low = matmul(hidden[2, rows, :], weights[2, :, here]).astype(bf)
            mix_parts[2 * index, :, here] = low[:quarter]
            mix_parts[2 * index + 1, :, here] = low[quarter:]
            return carry

        lax.fori_loop(0, width // wide, do_columns, 0)

        def go_on(ring):
            @pl.when(index == 0)
            def _():
                ring_step(ring, 0, (0, 1), first=True)

            @pl.when(index > 0)
            def _():
                ring_step(ring, index, (2 * index, 2 * index + 1 - index // (half - 1)))

        go_on(grad_ring)
        lax.fori_loop(0, width // wide, do_mix, 0)
        go_on(mix_ring)
        return carry

    lax.fori_loop(0, half, do_pair, 0)
    def keep(index, slot):
        target = kept_ref.at[index % members - 2, index // members]
        return pltpu.make_async_copy(stage.at[slot], target, store_sems.at[slot])

    def give(index, slot):
        target = given_ref.at[index % members, index // members]
        number = 2 * (index // members) + index % members
        return push(
            stage.at[slot], target, (give_sems.at[0, number], give_sems.at[1, number]), (dp, partner)
        )

    def weight_grads(first, last):
        def run(index, carry):
            kind = index // members
            whose = index % members
            slot = index % 2
            member = jnp.where(whose < 2, 1 + 2 * whose, 2 * (3 - whose))

            @pl.when((index >= 2) & (whose < 2))
            def _():
                keep(index - 2, slot).wait()

            @pl.when(whose >= 2)
            def _():
                give(index - 2, slot).wait_send()

            rows = pl.ds(pl.multiple_of(member * span, span), span)
            for chunk in range(half):
                some = pl.ds(chunk * pair, pair)
                turned[:, some] = hidden[kind, some, rows].T

            def do_columns(tile, carry):
                here = pl.ds(pl.multiple_of(tile * wide, wide), wide)
                source = inputs_ref if first < 2 * members else packs_ref
                stage[slot, :, here] = matmul(turned[...], source[:, here]).astype(bf)
                return carry

            lax.fori_loop(0, width // wide, do_columns, 0)

            @pl.when(whose < 2)
            def _():
                give(index, slot).start()

            @pl.when(whose >= 2)
            def _():
                keep(index, slot).start()

            return carry

        lax.fori_loop(first, last, run, 0)

    def final_sum():
        totals[...] = jnp.zeros_like(totals)
        for way in (0, 1):
            ring_copy(grad_ring, way, size - 2, grad_slots.at[way, size - 2]).wait_recv()
        base = own * quarter

        def finish(rows):
            sums = jnp.concatenate(
                [
                    grad_slots[0, size - 2, rows, :].astype(f32),
                    grad_slots[1, size - 2, rows, :].astype(f32),
                ],
                axis=-1,
            ) + grad_parts[size - 1, rows, :].astype(f32)
            middle = middle_ref[rows, :]
            inverse = lax.rsqrt(jnp.mean(middle * middle, axis=-1, keepdims=True) + EPSILON)
            hat = middle * inverse
            product = sums * hat
            totals[...] += product[:8] + product[8:]
            scaled = sums * gain_ref[...]
            back = inverse * (scaled - hat * jnp.mean(scaled * hat, axis=-1, keepdims=True))
            above = packs_ref[
                pl.ds(pl.multiple_of((size - 1) * quarter + rows.start, 16), rows.size), :width
            ]
            grad = above.astype(f32) + back
            gmid_ref[rows, :] = grad
            gmid_all[pl.ds(pl.multiple_of(base + rows.start, 16), rows.size), :] = grad.astype(bf)

        row_loop(quarter, 16, finish)
        gain_out[...] = jnp.sum(totals[...], axis=0, keepdims=True)

    def rows_of(index):
        return pl.ds(pl.multiple_of(index * quarter, quarter), quarter)

    def spread(index, whose, device):
        ref = gmid_all.at[rows_of(whose)]
        return push(ref, ref, (side_sems.at[0, index], side_sems.at[1, index]), device)

    def first_spread():
        spread(0, own, (dp, across)).start()
        spread(1, own, (dp, partner)).start()

    def second_spread():
        spread(0, own, (dp, across)).wait_recv()
        spread(2, across, (dp, partner)).start()

    def final_mix():
        for way in (0, 1):
            ring_copy(mix_ring, way, size - 2, mix_slots.at[way, size - 2]).wait_recv()

        def finish(rows):
            for way in (0, 1):
                columns = columns_of(way)
                hidden_out[rows, columns] = (
                    middle_ref[rows, columns]
                    + mix_slots[way, size - 2, rows, :].astype(f32)
                    + mix_parts[size - 1, rows, columns].astype(f32)
                ).astype(bf)

        row_loop(quarter, 16, finish)

    def closing():
        final_sum()
        first_spread()

    grad_events, mix_events = [], []
    for step in range(half, size - 1):
        delta = -(1 + step)
        blocks = (slot_of(delta, size), slot_of(-delta, size))
        grad_events.append(functools.partial(ring_step, grad_ring, step, blocks))
        mix_events.append(functools.partial(ring_step, mix_ring, step, blocks))
    events = grad_events[:-1]
    events += [grad_events[-1], mix_events[0], closing] + mix_events[1:2] + [second_spread]
    events += mix_events[2:] + [final_mix]
    work = [functools.partial(weight_grads, first, first + 2) for first in range(0, 3 * members, 2)]
    done = 0
    for number, piece in enumerate(work):
        piece()
        upto = -(-(number + 1) * len(events) // len(work))
        while done < upto:
            events[done]()
            done += 1
    for slot in (0, 1):
        keep(3 * members - 2 + slot, slot).wait()
    for kind in range(3):
        for whose in (0, 1):
            give(kind * members + whose, 0).wait_recv()
    spread(1, own, (dp, partner)).wait_recv()
    spread(2, across, (dp, partner)).wait_recv()
    for index, device in ((0, across), (1, partner), (2, partner)):
        spread(index, own, (dp, device)).wait_send()
    for ring in (grad_ring, mix_ring):
        for way in (0, 1):
            for step in range(size - 1):
                ring_copy(ring, way, step, ring[1].at[way, step]).wait_send()


def run_experts(size, inputs, packs, gate_up, down, others, middle, gain, experts):
    bf, f32 = jnp.bfloat16, jnp.float32
    local_experts, _, part_units, width = gate_up.shape
    others = others.reshape(3, 3, local_experts * part_units, width)
    members, span = 4, local_experts * part_units
    rows = inputs.shape[0]
    quarter = rows // size
    units = members * span
    expert_of = (jnp.arange(units, dtype=jnp.int32) // (span // local_experts)) % local_experts
    member = (expert_of[None, :] == jnp.arange(local_experts, dtype=jnp.int32)[:, None]).astype(f32)
    vmem = pl.BlockSpec(memory_space=pltpu.VMEM)
    anywhere = pl.BlockSpec(memory_space=pl.ANY)
    dma = pltpu.SemaphoreType.DMA
    return pl.pallas_call(
        functools.partial(run_experts_body, size, local_experts, experts),
        out_shape=(
            jax.ShapeDtypeStruct((quarter, width), bf),
            jax.ShapeDtypeStruct((2, 3, span, width), bf),
            jax.ShapeDtypeStruct((2, 3, span, width), bf),
            jax.ShapeDtypeStruct((quarter, width), f32),
            jax.ShapeDtypeStruct((members * quarter, width), bf),
            jax.ShapeDtypeStruct((1, width), f32),
        ),
        in_specs=[vmem, vmem, anywhere, anywhere, anywhere, vmem, vmem, vmem],
        out_specs=(vmem, anywhere, anywhere, vmem, vmem, vmem),
        scratch_shapes=[
            pltpu.VMEM((3, units, width), bf),
            pltpu.VMEM((3, rows, units), bf),
            pltpu.VMEM((size, quarter, width), bf),
            pltpu.VMEM((size, quarter, width), bf),
            pltpu.VMEM((2, size - 1, quarter, width // 2), bf),
            pltpu.VMEM((2, size - 1, quarter, width // 2), bf),
            pltpu.VMEM((span, rows), bf),
            pltpu.VMEM((2, span, width), bf),
            pltpu.VMEM((8, width), f32),
            dma((3 * local_experts + 3 * span // LANES,)),
            dma((2, 2, size - 1)),
            dma((2, 2, size - 1)),
            dma((2, 3)),
            dma((2,)),
            dma((2, 6)),
        ],
        compiler_params=pltpu.CompilerParams(
            collective_id=2, has_side_effects=True, vmem_limit_bytes=VMEM_LIMIT
        ),
        name="run_experts",
    )(inputs, packs, gate_up, down, others, member, middle, gain.reshape(1, -1))


def back_through_head(grads, raw, gain, cosine, sine):
    hat_grads = grads * cosine - pltpu.roll(grads, grads.shape[1] // 2, 1) * sine
    inverse = lax.rsqrt(jnp.mean(raw * raw, axis=-1, keepdims=True) + EPSILON)
    hat = raw * inverse
    terms = hat_grads * hat
    scaled = hat_grads * gain
    back = inverse * (scaled - hat * jnp.mean(scaled * hat, axis=-1, keepdims=True))
    return back.astype(jnp.bfloat16), terms


def finish_layer_body(
    size,
    gmid_low_ref,
    out_weight_ref,
    mixed_ref,
    query_ref,
    key_ref,
    value_ref,
    raw_query_ref,
    raw_key_ref,
    normed_ref,
    query_weight_ref,
    key_weight_ref,
    value_weight_ref,
    cosine_ref,
    sine_ref,
    start_ref,
    query_gain_ref,
    key_gain_ref,
    middle_ref,
    token_ref,
    hidden_ref,
    cross_ref,
    gain_ref,
    gains_ref,
    hidden_all,
    crossed_ref,
    grad_all,
    gather_a,
    gather_b,
    gains_out,
    qkv_ref,
    out_ref,
    slots_a,
    slots_b,
    grad_mixed,
    grad_heads,
    key_sums,
    value_sums,
    turned,
    partial,
    from_partner,
    from_across,
    joined,
    totals,
    head_totals,
    pair_gains,
    ring_gains,
    sems_a,
    sems_b,
    ring_sems,
    side_sems,
):
    f32, bf = jnp.float32, jnp.bfloat16
    dp = lax.axis_index("dp")
    own, partner, across = tensor_peers()
    far_partner = (partner + 2) % 4
    quarter, width = token_ref.shape
    tokens = normed_ref.shape[0]
    head_dim = key_ref.shape[1]
    lead = query_ref.shape[1]
    heads = lead // head_dim
    scale = head_dim**-0.5
    place = ring_place(dp, size)
    forward = (ring_index(place + 1, size), own)
    backward = (ring_index(place + size - 1, size), own)
    ways = ((forward, 1), (backward, -1))
    greet([forward, backward, (dp, partner), (dp, across)])
    waits = []

    def start(copy):
        copy.start()
        waits.append(copy)
        return copy

    sets = (
        (qkv_ref, slots_a, gather_a, sems_a),
        (out_ref, slots_b, gather_b, sems_b),
    )

    def block_of(ref, block, way):
        rows = ref.shape[0] // size
        cut = ref.shape[1] // 2
        return (pl.ds(pl.multiple_of(block * rows, rows), rows), pl.ds(way * cut, cut))

    def wrap(value):
        return (value + 2 * size) % size

    live = {}

    def add_own(which, way, step):
        ref, slots, blocks, _ = sets[which]
        live[which, way, step].wait_recv()
        sign = ways[way][1]
        rows, columns = block_of(ref, wrap(place - sign * (2 + step)), way)
        base = rows.start

        def add(inner):
            there = pl.ds(pl.multiple_of(base + inner.start, 16), inner.size)
            sums = (slots[way, step, inner, :].astype(f32) + ref[there, columns].astype(f32)).astype(bf)
            if step == size - 2:
                blocks[place, inner, columns] = sums
            else:
                slots[way, step, inner, :] = sums

        row_loop(ref.shape[0] // size, 16, add)

    def ring_event(which, step):
        ref, slots, blocks, sems = sets[which]
        cut = ref.shape[1] // 2
        for way, (device, sign) in enumerate(ways):
            if step == 0:
                source = ref.at[block_of(ref, wrap(place - sign), way)]
            elif step < size:
                add_own(which, way, step - 1)
                source = slots.at[way, step - 1] if step < size - 1 else None
            else:
                live[which, way, step - 1].wait_recv()
            if step >= 2 * size - 2:
                continue
            if step >= size - 1:
                block = wrap(place - sign * (step - size + 1))
                source = blocks.at[block, :, pl.ds(way * cut, cut)]
                target = source
            else:
                target = slots.at[way, step]
            sem = (sems.at[0, way, step], sems.at[1, way, step])
            live[which, way, step] = start(push(source, target, sem, device))

    def part_rows(index):
        return pl.ds(pl.multiple_of(index * quarter, quarter), quarter)

    def side(index):
        return (side_sems.at[0, index], side_sems.at[1, index])

    mine = part_rows(own)
    home = own * quarter

    step_rows = 2 * LANES
    wide = 4 * LANES

    def out_rows(index, carry):
        rows = pl.ds(pl.multiple_of(index * step_rows, step_rows), step_rows)
        turned[...] = mixed_ref[:, rows].T

        def columns(tile, carry):
            here = pl.ds(pl.multiple_of(tile * wide, wide), wide)
            out_ref[rows, here] = matmul(turned[...], gmid_low_ref[:, here]).astype(bf)
            return carry

        return lax.fori_loop(0, width // wide, columns, carry)

    lax.fori_loop(0, lead // step_rows, out_rows, 0)
    ring_event(1, 0)

    def keep(rows):
        hidden_all[pl.ds(pl.multiple_of(home + rows.start, 16), rows.size), :] = hidden_ref[rows, :]

    row_loop(quarter, 16, keep)
    shown = [start(push(hidden_ref, hidden_all.at[mine], side(9), (dp, across)))]
    shown.append(start(push(hidden_ref, hidden_all.at[mine], side(10), (dp, partner))))

    def mixed_columns(tile, carry):
        here = pl.ds(pl.multiple_of(tile * wide, wide), wide)
        grad_mixed[:, here] = matmul_nt(gmid_low_ref[...], out_weight_ref[here, :]).astype(bf)
        return carry

    lax.fori_loop(0, lead // wide, mixed_columns, 0)
    key_sums[...] = jnp.zeros_like(key_sums)
    value_sums[...] = jnp.zeros_like(value_sums)
    head_totals[...] = jnp.zeros_like(head_totals)
    block = tokens // 2

    def do_head(head, carry):
        lanes = pl.ds(pl.multiple_of(head * head_dim, head_dim), head_dim)
        for part in (0, 1):
            rows = pl.ds(part * block, block)
            count = (part + 1) * block
            keys = pl.ds(0, count)
            queries = query_ref[rows, lanes]
            outer = grad_mixed[rows, lanes]
            scores = matmul_nt(key_ref[keys, :], queries)
            key_at = lax.broadcasted_iota(jnp.int32, scores.shape, 0)
            query_at = lax.broadcasted_iota(jnp.int32, scores.shape, 1) + part * block
            seen = (key_at <= query_at) & (key_at >= start_ref[:, rows])
            exponent = jnp.where(seen, jnp.exp(scores * scale), 0.0)
            soft = exponent * (1.0 / jnp.sum(exponent, axis=0, keepdims=True))
            grad_soft = matmul_nt(value_ref[keys, :], outer)
            inner = jnp.sum(soft * grad_soft, axis=0, keepdims=True)
            grad_scores = (soft * (grad_soft - inner)).astype(bf)
            value_sums[keys, :] += matmul(soft.astype(bf), outer)
            key_sums[keys, :] += matmul(grad_scores, queries)
            grad_query = scale * lax.dot_general(
                grad_scores, key_ref[keys, :], (((0,), (0,)), ((), ())), preferred_element_type=f32
            )
            low, terms = back_through_head(
                grad_query, raw_query_ref[rows, lanes], query_gain_ref[...], cosine_ref[rows, :], sine_ref[rows, :]
            )
            grad_heads[rows, lanes] = low
            head_totals[0] += jnp.sum(terms.reshape(-1, 8, head_dim), axis=0)
        return carry

    lax.fori_loop(0, heads // 2, do_head, 0)
    ring_event(1, 1)
    lax.fori_loop(heads // 2, heads, do_head, 0)
    ring_event(1, 2)
    low, terms = back_through_head(
        scale * key_sums[...], raw_key_ref[...], key_gain_ref[...], cosine_ref[...], sine_ref[...]
    )
    grad_heads[:, pl.ds(lead, head_dim)] = low
    head_totals[1] += jnp.sum(terms.reshape(-1, 8, head_dim), axis=0)
    grad_heads[:, pl.ds(lead + head_dim, head_dim)] = value_sums[...].astype(bf)

    def in_rows(index, carry):
        rows = pl.ds(pl.multiple_of(index * step_rows, step_rows), step_rows)
        turned[...] = normed_ref[:, rows].T
        qkv_ref[rows, :] = matmul(turned[...], grad_heads[...]).astype(bf)
        return carry

    lax.fori_loop(0, width // step_rows, in_rows, 0)
    ring_event(1, 3)
    ring_event(0, 0)

    def token_columns(tile, carry):
        here = pl.ds(pl.multiple_of(tile * wide, wide), wide)
        sums = matmul_nt(grad_heads[:, :lead], query_weight_ref[here, :])
        sums = sums + matmul_nt(grad_heads[:, lead : lead + head_dim], key_weight_ref[here, :])
        sums = sums + matmul_nt(grad_heads[:, lead + head_dim :], value_weight_ref[here, :])
        partial[:, here] = sums.astype(bf)
        return carry

    lax.fori_loop(0, width // wide, token_columns, 0)
    first = start(push(partial.at[part_rows(far_partner)], from_partner.at[1], side(0), (dp, partner)))
    second = start(push(partial.at[part_rows(partner)], from_partner.at[0], side(1), (dp, partner)))
    ring_event(1, 4)
    first.wait_recv()
    away = across * quarter

    def join(rows):
        there = pl.ds(pl.multiple_of(away + rows.start, 16), rows.size)
        joined[rows, :] = (partial[there, :].astype(f32) + from_partner[1, rows, :].astype(f32)).astype(bf)

    row_loop(quarter, 16, join)
    third = start(push(joined, from_across, side(2), (dp, across)))
    ring_event(0, 1)
    ring_event(1, 5)
    second.wait_recv()
    third.wait_recv()
    totals[...] = jnp.zeros_like(totals)

    def finish(rows):
        there = pl.ds(pl.multiple_of(home + rows.start, 16), rows.size)
        grads = (
            partial[there, :].astype(f32)
            + from_partner[0, rows, :].astype(f32)
            + from_across[rows, :].astype(f32)
        )
        hidden = token_ref[rows, :].astype(f32)
        inverse = lax.rsqrt(jnp.mean(hidden * hidden, axis=-1, keepdims=True) + EPSILON)
        hat = hidden * inverse
        product = grads * hat
        totals[...] += product[:8] + product[8:]
        scaled = grads * gain_ref[...]
        back = inverse * (scaled - hat * jnp.mean(scaled * hat, axis=-1, keepdims=True))
        grad_all[there, :] = (middle_ref[rows, :] + back).astype(bf)

    row_loop(quarter, 16, finish)
    spread = [start(push(grad_all.at[mine], grad_all.at[mine], side(3), (dp, across)))]
    spread.append(start(push(grad_all.at[mine], grad_all.at[mine], side(4), (dp, partner))))
    pair_gains[0, :, :width] = jnp.sum(totals[...], axis=0, keepdims=True)
    pair_gains[0, :, width : 2 * width] = gains_ref[...]
    pair_gains[0, :, 2 * width : 2 * width + head_dim] = jnp.sum(head_totals[0], axis=0, keepdims=True)
    pair_gains[0, :, 2 * width + head_dim :] = jnp.sum(head_totals[1], axis=0, keepdims=True)
    swap = start(push(pair_gains.at[0], pair_gains.at[1], side(5), (dp, partner)))
    ring_event(0, 2)
    ring_event(1, 6)
    far = part_rows(across)
    shown[0].wait_recv()
    shown.append(start(push(hidden_all.at[far], hidden_all.at[far], side(11), (dp, partner))))
    spread[0].wait_recv()
    spread.append(start(push(grad_all.at[far], grad_all.at[far], side(6), (dp, partner))))
    swap.wait_recv()
    pair_gains[2] = pair_gains[0] + pair_gains[1]
    swap = start(push(pair_gains.at[2], pair_gains.at[3], side(7), (dp, across)))
    ring_event(0, 3)
    ring_event(1, 7)
    swap.wait_recv()
    crossing = start(push(cross_ref, crossed_ref, side(8), (dp, across)))
    ring_gains[place] = pair_gains[2] + pair_gains[3]
    small = None
    for step in range(4, 2 * size - 1):
        ring_event(0, step)
        if step + 4 < 2 * size - 1:
            ring_event(1, step + 4)
        if step - 4 < size - 1:
            if small is not None:
                small.wait_recv()
            ref = ring_gains.at[wrap(place - step + 4)]
            sem = (ring_sems.at[0, step - 4], ring_sems.at[1, step - 4])
            small = start(push(ref, ref, sem, forward))
    small.wait_recv()
    gains_out[...] = jnp.sum(ring_gains[...], axis=0)
    for copy in (spread[1], spread[2], shown[1], shown[2], crossing):
        copy.wait_recv()
    for copy in waits:
        copy.wait_send()


def finish_layer(size, *arguments):
    bf, f32 = jnp.bfloat16, jnp.float32
    (
        _, out_weight, mixed, query, key, _, _, _, normed, query_weight, _, _, _, _, _, _, _, _, token_rows, _,
        cross, _, _,
    ) = arguments
    quarter, width = token_rows.shape
    tokens = normed.shape[0]
    lead, head_dim = query.shape[1], key.shape[1]
    vmem = pl.BlockSpec(memory_space=pltpu.VMEM)
    anywhere = pl.BlockSpec(memory_space=pl.ANY)
    dma = pltpu.SemaphoreType.DMA
    columns = lead + 2 * head_dim
    rows_a, rows_b = width // size, lead // size
    count = 2 * width + 2 * head_dim
    return pl.pallas_call(
        functools.partial(finish_layer_body, size),
        out_shape=(
            jax.ShapeDtypeStruct((tokens, width), bf),
            jax.ShapeDtypeStruct(cross.shape, bf),
            jax.ShapeDtypeStruct((tokens, width), bf),
            jax.ShapeDtypeStruct((size, rows_a, columns), bf),
            jax.ShapeDtypeStruct((size, rows_b, width), bf),
            jax.ShapeDtypeStruct((1, count), f32),
        ),
        in_specs=[anywhere if argument is cross else vmem for argument in arguments],
        out_specs=(vmem, anywhere) + (vmem,) * 4,
        scratch_shapes=[
            pltpu.VMEM((width, columns), bf),
            pltpu.VMEM((lead, width), bf),
            pltpu.VMEM((2, size - 1, rows_a, columns // 2), bf),
            pltpu.VMEM((2, size - 1, rows_b, width // 2), bf),
            pltpu.VMEM((tokens, lead), bf),
            pltpu.VMEM((tokens, columns), bf),
            pltpu.VMEM((tokens, head_dim), f32),
            pltpu.VMEM((tokens, head_dim), f32),
            pltpu.VMEM((2 * LANES, tokens), bf),
            pltpu.VMEM((tokens, width), bf),
            pltpu.VMEM((2, quarter, width), bf),
            pltpu.VMEM((quarter, width), bf),
            pltpu.VMEM((quarter, width), bf),
            pltpu.VMEM((8, width), f32),
            pltpu.VMEM((2, 8, head_dim), f32),
            pltpu.VMEM((4, 1, count), f32),
            pltpu.VMEM((size, 1, count), f32),
            dma((2, 2, 2 * size - 2)),
            dma((2, 2, 2 * size - 2)),
            dma((2, size - 1)),
            dma((2, 12)),
        ],
        compiler_params=pltpu.CompilerParams(
            collective_id=1, has_side_effects=True, vmem_limit_bytes=VMEM_LIMIT
        ),
        name="finish_layer",
    )(*arguments)


def large_experts(size, inputs, packs, gate_up, down, others, middle, gain, experts):
    f32, bf = jnp.float32, jnp.bfloat16
    model_width = inputs.shape[1]
    own_weights = jnp.stack([gate_up[:, 0], gate_up[:, 1], down])
    all_weights = jnp.concatenate([own_weights[None], others])
    members = all_weights.shape[0]
    order = jnp.arange(members, dtype=jnp.int32) ^ lax.axis_index("tensor")
    all_weights = all_weights.reshape(members, 3, -1, model_width)[order]
    units = all_weights.shape[2]
    local_experts = experts // size
    indices = jnp.arange(size, dtype=jnp.int32)
    half = size // 2
    delta = (ring_place(indices, size) - ring_place(lax.axis_index("dp"), size)) % size
    ahead = jnp.where(delta == half, size - 2, jnp.where(delta == 0, size - 1, 2 * delta - 1))
    slots = jnp.where(delta > half, 2 * (size - delta) - 2, ahead)
    quarter = middle.shape[0]
    out_rows = packs[-quarter:, :model_width]
    inputs = inputs.reshape(size, quarter, -1)[slots].reshape(-1, model_width)
    packs = packs.reshape(size, quarter, -1)[slots].reshape(inputs.shape[0], -1)
    grads_all = packs[:, :model_width]
    shares = packs[:, model_width : model_width + 2 * experts].astype(f32)
    shares = shares[:, :experts] + shares[:, experts:]
    shares = lax.dynamic_slice_in_dim(
        shares, lax.axis_index("dp") * local_experts, local_experts, 1
    )
    weight_cols = jnp.broadcast_to(
        shares[:, None, :, None],
        (shares.shape[0], members, local_experts, units // local_experts),
    ).reshape(-1, members, units)

    def project(left, which):
        return jnp.einsum("td,rud->tru", left, all_weights[:, which], preferred_element_type=f32)

    gate_act = project(inputs, 0)
    upward = project(inputs, 1)
    sigmoid_gate = jax.nn.sigmoid(gate_act)
    active = gate_act * sigmoid_gate * upward
    weighted_low = (weight_cols * active).astype(bf)
    mixture_part = jnp.einsum(
        "tru,rud->td", weighted_low, all_weights[:, 2], preferred_element_type=f32
    ).astype(bf)
    grad_active = weight_cols * project(grads_all, 2)
    grad_gate = (
        grad_active * upward * sigmoid_gate * (1.0 + gate_act * (1.0 - sigmoid_gate))
    ).astype(bf)
    grad_up = (grad_active * gate_act * sigmoid_gate).astype(bf)
    grad_normed_part = jnp.einsum(
        "tru,rud->td", grad_gate, all_weights[:, 0], preferred_element_type=f32
    ) + jnp.einsum("tru,rud->td", grad_up, all_weights[:, 1], preferred_element_type=f32)
    grad_normed_two = lax.psum_scatter(grad_normed_part.astype(bf), "dp", tiled=True).astype(f32)
    weight_grads = jnp.stack(
        [
            jnp.einsum("tru,td->rud", grad_gate, inputs, preferred_element_type=f32).astype(bf),
            jnp.einsum("tru,td->rud", grad_up, inputs, preferred_element_type=f32).astype(bf),
            jnp.einsum("tru,td->rud", weighted_low, grads_all, preferred_element_type=f32).astype(bf),
        ],
        axis=1,
    )
    hat_two, inv_two = rms_parts(middle)
    grad_gain_two = jnp.sum(grad_normed_two * hat_two, axis=0)
    grad_middle = out_rows.astype(f32) + rms_back(grad_normed_two * gain, hat_two, inv_two)
    grad_mid_low = lax.all_gather(grad_middle.astype(bf), "tensor", tiled=True)
    mixture = lax.psum_scatter(mixture_part, "dp", tiled=True).astype(f32)
    hidden_out = (middle + mixture).astype(bf)
    zero = jnp.zeros(weight_grads.shape[1:], bf)
    sums = lax.psum_scatter(weight_grads.reshape(-1, model_width), "tensor", tiled=True)
    kept = jnp.stack([zero, sums.reshape(zero.shape)])
    given = jnp.stack([zero, zero])
    return (hidden_out, kept, given, grad_middle, grad_mid_low, grad_gain_two)


def local(
    hidden_in,
    seq_lens,
    norm1_gain,
    query_weight,
    key_weight,
    value_weight,
    query_gain,
    key_gain,
    out_weight,
    norm2_gain,
    w_gate_up,
    w_down,
    routes,
    route_weights,
    out_grad,
):
    bf = jnp.bfloat16
    f32 = jnp.float32
    tokens, model_width = hidden_in.shape
    local_experts = w_gate_up.shape[0]
    hidden_part = w_gate_up.shape[3]
    head_dim = query_gain.shape[0]
    data_size = lax.axis_size("dp")
    quarter = tokens // lax.axis_size("tensor")
    experts = local_experts * data_size
    rows = data_size * quarter
    places, starts = sequence_layout(seq_lens[0], tokens)
    cosine_table, sine_table = rotary_tables(places - starts, head_dim)
    cosines = jnp.concatenate([cosine_table, cosine_table], axis=1)
    sines = jnp.concatenate([-sine_table, sine_table], axis=1)
    starts = starts.reshape(1, -1).astype(jnp.int32)
    gate_up = jnp.transpose(w_gate_up, (0, 2, 3, 1))
    (
        middle,
        inputs,
        gathered,
        others,
        mixed_low,
        query_low,
        key_low,
        value_low,
        raw_query,
        raw_key,
        normed,
    ) = start_layer(
        data_size,
        experts,
        hidden_in,
        out_grad,
        routes,
        route_weights,
        query_weight,
        key_weight,
        value_weight,
        out_weight,
        gate_up,
        w_down,
        cosines,
        sines,
        starts,
        norm1_gain.reshape(1, -1),
        norm2_gain.reshape(1, -1),
        query_gain.reshape(1, -1),
        key_gain.reshape(1, -1),
    )
    stage = run_experts if data_size <= 8 else large_experts
    hidden_out, kept, given, grad_middle, grad_mid_low, grad_gain_two = stage(
        data_size,
        inputs.reshape(rows, model_width),
        gathered.reshape(rows, -1),
        gate_up,
        w_down,
        others,
        middle,
        norm2_gain,
        experts,
    )
    joined = (kept[0].astype(f32) + given[1].astype(f32)).astype(bf)
    hidden_q = lax.dynamic_slice_in_dim(hidden_in, lax.axis_index("tensor") * quarter, quarter, 0)
    hidden_out, crossed, grad_hidden, in_low, out_low, gains = finish_layer(
        data_size,
        grad_mid_low,
        out_weight,
        mixed_low,
        query_low,
        key_low,
        value_low,
        raw_query,
        raw_key,
        normed,
        query_weight,
        key_weight,
        value_weight,
        cosines,
        sines,
        starts,
        query_gain.reshape(1, -1),
        key_gain.reshape(1, -1),
        grad_middle,
        hidden_q,
        hidden_out,
        joined,
        norm1_gain.reshape(1, -1),
        grad_gain_two.reshape(1, -1),
    )
    own_grads = kept[1].astype(f32) + given[0].astype(f32) + crossed.astype(f32)
    grad_w_gate_up = jnp.transpose(
        own_grads[:2].reshape(2, local_experts, hidden_part, model_width), (1, 3, 0, 2)
    )
    grad_w_down = own_grads[2].reshape(local_experts, hidden_part, model_width)
    in_low = in_low.reshape(model_width, -1)
    lead = query_weight.shape[1]
    gains = gains.reshape(-1)
    return (
        hidden_out,
        grad_hidden,
        gains[:model_width],
        in_low[:, :lead].astype(f32),
        in_low[:, lead : lead + head_dim].astype(f32),
        in_low[:, lead + head_dim :].astype(f32),
        gains[2 * model_width : 2 * model_width + head_dim],
        gains[2 * model_width + head_dim :],
        out_low.reshape(-1, model_width).astype(f32),
        gains[model_width : 2 * model_width],
        grad_w_gate_up,
        grad_w_down,
    )


def solution(mesh):
    in_specs = (
        P("dp", None),
        P("dp", None),
        P(),
        P(None, "tensor"),
        P(None, "tensor"),
        P(None, "tensor"),
        P(),
        P(),
        P("tensor", None),
        P(),
        P("dp", None, None, "tensor"),
        P("dp", "tensor", None),
        P("dp", None),
        P("dp", None),
        P("dp", None),
    )
    out_specs = (
        P("dp", None),
        P("dp", None),
        P(),
        P(None, "tensor"),
        P(None, "tensor"),
        P(None, "tensor"),
        P(),
        P(),
        P("tensor", None),
        P(),
        P("dp", None, None, "tensor"),
        P("dp", "tensor", None),
    )
    return jax.shard_map(local, mesh=mesh, in_specs=in_specs, out_specs=out_specs, check_vma=False)
```

```python
import functools
import math

import jax
import jax.numpy as jnp
from jax import lax
from jax.experimental import pallas as pl
from jax.experimental.pallas import tpu as pltpu
from jax.sharding import PartitionSpec as P

EPSILON = 1e-06
ROPE_BASE = 1000000.0


def rms_parts(values):
    inverse = lax.rsqrt(jnp.mean(values * values, axis=-1, keepdims=True) + EPSILON)
    return (values * inverse, inverse)


def rms_back(grad_hat, normal_hat, inverse):
    return inverse * (
        grad_hat - normal_hat * jnp.mean(grad_hat * normal_hat, axis=-1, keepdims=True)
    )


def rotary_tables(positions, head_dim):
    halves = jnp.arange(head_dim // 2, dtype=jnp.float32)
    inverse = jnp.exp(halves * (-2.0 * math.log(ROPE_BASE) / head_dim))
    angles = positions.astype(jnp.float32)[:, None] * inverse[None, :]
    return (jnp.cos(angles), jnp.sin(angles))


def sequence_layout(lengths, token_count):
    endings = jnp.cumsum(lengths)
    places = jnp.arange(token_count, dtype=jnp.int32)
    starts = jnp.sum(jnp.where(endings[None, :] <= places[:, None], lengths[None, :], 0), axis=1)
    return (places, starts)


LANES = 128
MESH = pl.DeviceIdType.MESH
VMEM_LIMIT = 127 * 512 * 1024


def ring_place(index, size):
    return jnp.where(index % 2 == 0, index // 2, size - (index + 1) // 2)


def ring_index(place, size):
    place = place % size
    return jnp.where(place < size // 2, 2 * place, 2 * size - 1 - 2 * place)


def tensor_peers():
    own = lax.axis_index("tensor")
    partner = own + 1 - 2 * (own % 2)
    across = (own + 2) % 4
    return own, partner, across


def greet(devices):
    barrier = pltpu.get_barrier_semaphore()
    for device in devices:
        pl.semaphore_signal(barrier, inc=1, device_id=device, device_id_type=MESH)
    pl.semaphore_wait(barrier, len(devices))


def push(source, target, sems, device):
    return pltpu.make_async_remote_copy(
        src_ref=source,
        dst_ref=target,
        send_sem=sems[0],
        recv_sem=sems[1],
        device_id=device,
        device_id_type=MESH,
    )


def slot_of(delta, size):
    delta = (delta + size // 2 - 1) % size - (size // 2 - 1)
    if delta == 0:
        return size - 1
    if delta == size // 2:
        return size - 2
    return 2 * delta - 1 if delta > 0 else -2 * delta - 2


class GatherRing:
    def __init__(self, size, blocks, sems, parts=2):
        self.size, self.blocks, self.sems, self.parts = size, blocks, sems, parts
        self.place = ring_place(lax.axis_index("dp"), size)
        self.sent = []
        self.live = {}

    def send(self, step):
        size, half = self.size, self.blocks.shape[1] // 2
        piece = half // self.parts
        for part in range(self.parts):
            for way in (0, 1):
                sign = 1 - 2 * way
                rows = pl.ds(way * half + part * piece, piece)
                source = self.blocks.at[slot_of(-sign * step, size), rows]
                target = self.blocks.at[slot_of(-sign * (step + 1), size), rows]
                device = (ring_index(self.place + size + sign, size), lax.axis_index("tensor"))
                copy = push(
                    source,
                    target,
                    (self.sems.at[0, way, step, part], self.sems.at[1, way, step, part]),
                    device,
                )
                if step > 0:
                    self.live[step - 1, part, way].wait_recv()
                copy.start()
                self.live[step, part, way] = copy
                self.sent.append(copy)

    def step(self, step):
        if step + 1 < self.size - 1:
            self.send(step + 1)
        else:
            for part in range(self.parts):
                for way in (0, 1):
                    self.live[step, part, way].wait_recv()

    def finish(self):
        for copy in self.sent:
            copy.wait_send()


def row_loop(total, rows, body):
    def run(index, carry):
        body(pl.ds(pl.multiple_of(index * rows, rows), rows))
        return carry

    lax.fori_loop(0, total // rows, run, 0)


def matmul_nt(left, right):
    return lax.dot_general(left, right, (((1,), (1,)), ((), ())), preferred_element_type=jnp.float32)


def matmul(left, right):
    return lax.dot_general(left, right, (((1,), (0,)), ((), ())), preferred_element_type=jnp.float32)


def rms_rows(values):
    return lax.rsqrt(jnp.mean(values * values, axis=-1, keepdims=True) + EPSILON)


def turn(values, cosine, sine):
    return values * cosine + pltpu.roll(values, values.shape[1] // 2, 1) * sine


def start_layer_body(
    size,
    experts,
    token_ref,
    above_ref,
    route_ref,
    share_ref,
    query_weight_ref,
    key_weight_ref,
    value_weight_ref,
    out_weight_ref,
    gate_up_ref,
    down_ref,
    cosine_ref,
    sine_ref,
    start_ref,
    first_gain_ref,
    second_gain_ref,
    query_gain_ref,
    key_gain_ref,
    middle_ref,
    inputs_ref,
    packs_ref,
    others_ref,
    mixed_ref,
    query_ref,
    key_ref,
    value_ref,
    raw_query_ref,
    raw_key_ref,
    normed_ref,
    query_weight,
    key_weight,
    value_weight,
    out_weight,
    part_ref,
    from_partner,
    from_across,
    joined,
    ring_sems,
    pack_sems,
    side_sems,
    load_sems,
    near_sems,
    far_sems,
    pass_sems,
):
    f32, bf = jnp.float32, jnp.bfloat16
    dp = lax.axis_index("dp")
    own, partner, across = tensor_peers()
    far_partner = (partner + 2) % 4
    quarter, width = middle_ref.shape
    tokens = token_ref.shape[0]
    head_dim = key_ref.shape[1]
    lead = query_ref.shape[1]
    heads = lead // head_dim
    place = ring_place(dp, size)
    loads = []
    for index, (source, target) in enumerate(
        (
            (query_weight_ref, query_weight),
            (key_weight_ref, key_weight),
            (value_weight_ref, value_weight),
            (out_weight_ref, out_weight),
        )
    ):
        copy = pltpu.make_async_copy(source, target, load_sems.at[index])
        copy.start()
        loads.append(copy)
    mine = pl.ds(pl.multiple_of(own * quarter, quarter), quarter)
    base = own * quarter
    above = pltpu.make_async_copy(
        above_ref.at[mine], packs_ref.at[size - 1, :, pl.ds(0, width)], load_sems.at[4]
    )
    above.start()
    neighbours = [(ring_index(place + 1, size), own), (ring_index(place + size - 1, size), own)]
    greet(neighbours + [(dp, partner), (dp, across)])

    halves = 2
    pieces = []
    for kind in range(3):
        for expert in range(gate_up_ref.shape[0]):
            for half in range(halves):
                pieces.append((kind, expert, half))
    span = gate_up_ref.shape[2] // halves

    def piece_of(number):
        kind, expert, half = pieces[number]
        rows = pl.ds(half * span, span)
        source = gate_up_ref.at[expert, kind, rows] if kind < 2 else down_ref.at[expert, rows]
        return source, (kind, expert, rows)

    near = []
    for kind in range(3):
        for expert in range(gate_up_ref.shape[0]):
            number = len(near)
            source = gate_up_ref.at[expert, kind] if kind < 2 else down_ref.at[expert]
            copy = push(
                source,
                others_ref.at[0, kind, expert],
                (near_sems.at[0, number], near_sems.at[1, number]),
                (dp, partner),
            )
            copy.start()
            near.append(copy)
    far, passed = [], []

    def pump(passing=True):
        number = len(far)
        if number >= 3:
            old = far[number - 3]
            if number - 3 < len(pieces):
                old.wait_recv()
                kind, expert, rows = piece_of(number - 3)[1]
                copy = push(
                    others_ref.at[1, kind, expert, rows],
                    others_ref.at[2, kind, expert, rows],
                    (pass_sems.at[0, number - 3], pass_sems.at[1, number - 3]),
                    (dp, partner),
                )
                copy.start()
                passed.append(copy)
                old.wait_send()
        if number < len(pieces):
            source, (kind, expert, rows) = piece_of(number)
            copy = push(
                source,
                others_ref.at[1, kind, expert, rows],
                (far_sems.at[0, number], far_sems.at[1, number]),
                (dp, across),
            )
            copy.start()
            far.append(copy)
        else:
            far.append(None)

    pump()
    pump()
    pump()

    tail = packs_ref.shape[2] - width
    lane = lax.broadcasted_iota(jnp.int32, (quarter, tail), 1)
    name = jnp.where(lane < experts, lane, lane - experts)
    dense = jnp.zeros((quarter, tail), f32)
    for choice in range(route_ref.shape[1]):
        named = route_ref[mine, choice : choice + 1]
        dense = dense + jnp.where(named == name, share_ref[mine, choice : choice + 1], 0.0)
    high = dense.astype(bf)
    low = (dense - high.astype(f32)).astype(bf)
    packs_ref[size - 1, :, width:] = jnp.where(
        lane < experts, high.astype(f32), jnp.where(lane < 2 * experts, low.astype(f32), 0.0)
    ).astype(bf)
    above.wait()
    packs = GatherRing(size, packs_ref, pack_sems)
    packs.send(0)

    def norm_first(rows):
        hidden = token_ref[rows, :].astype(f32)
        normed_ref[rows, :] = (hidden * rms_rows(hidden) * first_gain_ref[...]).astype(bf)

    row_loop(tokens, 16, norm_first)
    loads[0].wait()
    wide = 4 * LANES

    def project(tile, carry):
        here = pl.ds(pl.multiple_of(tile * wide, wide), wide)
        raw_query_ref[:, here] = matmul(normed_ref[...], query_weight[:, here])
        return carry

    lax.fori_loop(0, lead // wide, project, 0)
    loads[1].wait()
    loads[2].wait()
    raw_key = matmul(normed_ref[...], key_weight[...])
    raw_key_ref[...] = raw_key
    key_ref[...] = turn(
        raw_key * rms_rows(raw_key) * key_gain_ref[...], cosine_ref[...], sine_ref[...]
    ).astype(bf)
    value_ref[...] = matmul(normed_ref[...], value_weight[...]).astype(bf)
    packs.step(0)
    scale = head_dim**-0.5
    block = tokens // 2

    def do_head(head, carry):
        lanes = pl.ds(pl.multiple_of(head * head_dim, head_dim), head_dim)
        for part in (0, 1):
            rows = pl.ds(part * block, block)
            keys = pl.ds(0, (part + 1) * block)
            raw = raw_query_ref[rows, lanes]
            queries = turn(
                raw * rms_rows(raw) * query_gain_ref[...], cosine_ref[rows, :], sine_ref[rows, :]
            ).astype(bf)
            query_ref[rows, lanes] = queries
            scores = matmul_nt(key_ref[keys, :], queries)
            key_at = lax.broadcasted_iota(jnp.int32, scores.shape, 0)
            query_at = lax.broadcasted_iota(jnp.int32, scores.shape, 1) + part * block
            seen = (key_at <= query_at) & (key_at >= start_ref[:, rows])
            exponent = jnp.where(seen, jnp.exp(scores * scale), 0.0)
            soft = (exponent * (1.0 / jnp.sum(exponent, axis=0, keepdims=True))).astype(bf)
            mixed_ref[rows, lanes] = lax.dot_general(
                soft, value_ref[keys, :], (((0,), (0,)), ((), ())), preferred_element_type=f32
            ).astype(bf)
        return carry

    lax.fori_loop(0, heads // 2, do_head, 0)
    packs.step(1)
    pump()
    lax.fori_loop(heads // 2, heads, do_head, 0)
    packs.step(2)
    loads[3].wait()

    def share(tile, carry):
        here = pl.ds(pl.multiple_of(tile * wide, wide), wide)
        part_ref[:, here] = matmul(mixed_ref[...], out_weight[:, here]).astype(bf)
        return carry

    lax.fori_loop(0, width // wide, share, 0)

    def part_rows(index):
        return pl.ds(pl.multiple_of(index * quarter, quarter), quarter)

    def side(index):
        return (side_sems.at[0, index], side_sems.at[1, index])

    first = push(part_ref.at[part_rows(far_partner)], from_partner.at[1], side(0), (dp, partner))
    second = push(part_ref.at[part_rows(partner)], from_partner.at[0], side(1), (dp, partner))
    first.start()
    second.start()
    packs.step(3)
    first.wait_recv()
    away = across * quarter

    def join(rows):
        there = pl.ds(pl.multiple_of(away + rows.start, 16), rows.size)
        joined[rows, :] = (part_ref[there, :].astype(f32) + from_partner[1, rows, :].astype(f32)).astype(bf)

    row_loop(quarter, 16, join)
    third = push(joined, from_across, side(2), (dp, across))
    third.start()
    pump()
    second.wait_recv()
    third.wait_recv()

    def norm_second(rows):
        there = pl.ds(pl.multiple_of(base + rows.start, 16), rows.size)
        middle = (
            token_ref[there, :].astype(f32)
            + part_ref[there, :].astype(f32)
            + from_partner[0, rows, :].astype(f32)
            + from_across[rows, :].astype(f32)
        )
        middle_ref[rows, :] = middle
        inputs_ref[size - 1, rows, :] = (middle * rms_rows(middle) * second_gain_ref[...]).astype(bf)

    row_loop(quarter, 16, norm_second)
    ring = GatherRing(size, inputs_ref, ring_sems)
    ring.send(0)
    for step in range(size - 1):
        if step + 4 < size - 1:
            packs.step(step + 4)
        pump()
        ring.step(step)
        if step % 2 == 1:
            pump()
    while len(far) < len(pieces) + 3:
        pump()
    packs.finish()
    ring.finish()
    first.wait_send()
    second.wait_send()
    third.wait_send()
    for copy in near + passed:
        copy.wait()


def start_layer(size, experts, *arguments):
    tokens_rows, _, _, _, query_weight, key_weight, value_weight, out_weight, gate_up = arguments[:9]
    bf, f32 = jnp.bfloat16, jnp.float32
    tokens, width = tokens_rows.shape
    quarter = tokens // 4
    lead, head_dim = query_weight.shape[1], key_weight.shape[1]
    columns = width + -(-2 * experts // LANES) * LANES
    local, _, units, _ = gate_up.shape
    vmem = pl.BlockSpec(memory_space=pltpu.VMEM)
    anywhere = pl.BlockSpec(memory_space=pl.ANY)
    dma = pltpu.SemaphoreType.DMA
    return pl.pallas_call(
        functools.partial(start_layer_body, size, experts),
        out_shape=(
            jax.ShapeDtypeStruct((quarter, width), f32),
            jax.ShapeDtypeStruct((size, quarter, width), bf),
            jax.ShapeDtypeStruct((size, quarter, columns), bf),
            jax.ShapeDtypeStruct((3, 3, local, units, width), bf),
            jax.ShapeDtypeStruct((tokens, lead), bf),
            jax.ShapeDtypeStruct((tokens, lead), bf),
            jax.ShapeDtypeStruct((tokens, head_dim), bf),
            jax.ShapeDtypeStruct((tokens, head_dim), bf),
            jax.ShapeDtypeStruct((tokens, lead), f32),
            jax.ShapeDtypeStruct((tokens, head_dim), f32),
            jax.ShapeDtypeStruct((tokens, width), bf),
        ),
        in_specs=[vmem, anywhere, vmem, vmem] + [anywhere] * 6 + [vmem] * 7,
        out_specs=(vmem, vmem, vmem, anywhere) + (vmem,) * 7,
        scratch_shapes=[
            pltpu.VMEM(query_weight.shape, bf),
            pltpu.VMEM(key_weight.shape, bf),
            pltpu.VMEM(value_weight.shape, bf),
            pltpu.VMEM(out_weight.shape, bf),
            pltpu.VMEM((tokens, width), bf),
            pltpu.VMEM((2, quarter, width), bf),
            pltpu.VMEM((quarter, width), bf),
            pltpu.VMEM((quarter, width), bf),
            dma((2, 2, size - 1, 2)),
            dma((2, 2, size - 1, 2)),
            dma((2, 3)),
            dma((5,)),
            dma((2, 3 * local)),
            dma((2, 6 * local)),
            dma((2, 6 * local)),
        ],
        compiler_params=pltpu.CompilerParams(
            collective_id=0, has_side_effects=True, vmem_limit_bytes=VMEM_LIMIT
        ),
        name="start_layer",
    )(*arguments)


def run_experts_body(
    size,
    local_experts,
    experts,
    inputs_hbm,
    packs_hbm,
    gate_up_ref,
    down_ref,
    others_ref,
    member_ref,
    middle_ref,
    gain_ref,
    hidden_out,
    kept_ref,
    given_ref,
    cross_ref,
    landing_ref,
    gmid_ref,
    gmid_all,
    gain_out,
    weights,
    hidden,
    grad_parts,
    mix_parts,
    grad_slots,
    mix_slots,
    turned,
    stage,
    landed,
    totals,
    load_sems,
    grad_sems,
    mix_sems,
    side_sems,
    store_sems,
    give_sems,
    land_sems,
    token_sems,
    inputs_ref,
    packs_ref,
):
    f32, bf = jnp.float32, jnp.bfloat16
    dp = lax.axis_index("dp")
    own, partner, across = tensor_peers()
    width = inputs_ref.shape[1]
    quarter = inputs_ref.shape[0] // size
    pair = 2 * quarter
    half = size // 2
    units = weights.shape[1]
    members = others_ref.shape[0] + 1
    span = units // members
    cut = width // 2
    wide = 512
    place = ring_place(dp, size)

    def token_loads(index):
        rows = pl.ds(pl.multiple_of(index * pair, pair), pair)
        return (
            pltpu.make_async_copy(inputs_hbm.at[rows], inputs_ref.at[rows], token_sems.at[0, index]),
            pltpu.make_async_copy(packs_hbm.at[rows], packs_ref.at[rows], token_sems.at[1, index]),
        )

    for copy in token_loads(0):
        copy.start()
    forward = (ring_index(place + 1, size), own)
    backward = (ring_index(place + size - 1, size), own)
    greet([forward, backward, (dp, partner), (dp, across)])
    part_units = span // local_experts
    loads = []
    for expert in range(local_experts):
        rows = pl.ds(expert * part_units, part_units)
        for kind in range(3):
            source = gate_up_ref.at[expert, kind] if kind < 2 else down_ref.at[expert]
            loads.append((expert * part_units, source, weights.at[kind, rows]))
    for other in range(members - 1):
        for first in range(0, span, LANES):
            at = (other + 1) * span + first
            source = others_ref.at[other, :, pl.ds(first, LANES)]
            loads.append((at, source, weights.at[:, pl.ds(at, LANES)]))
    loads = [
        (at, pltpu.make_async_copy(source, target, load_sems.at[number]))
        for number, (at, source, target) in enumerate(loads)
    ]
    for _, copy in loads:
        copy.start()
    for index in range(1, half):
        for copy in token_loads(index):
            copy.start()

    grad_ring = (grad_parts, grad_slots, grad_sems)
    mix_ring = (mix_parts, mix_slots, mix_sems)

    ring_parts = 2
    piece_rows = quarter // ring_parts

    def ring_copy(ring, way, step, part, source):
        device = forward if way == 0 else backward
        _, slots, sems = ring
        rows = pl.ds(part * piece_rows, piece_rows)
        return push(
            source.at[rows],
            slots.at[way, step, rows],
            (sems.at[0, way, step, part], sems.at[1, way, step, part]),
            device,
        )

    def columns_of(way):
        return pl.ds(way * cut, cut)

    def ring_step(ring, step, blocks, first=False):
        parts, slots, _ = ring
        for part in range(ring_parts):
            for way in (0, 1):
                if first:
                    source = parts.at[blocks[way], :, columns_of(way)]
                else:
                    source = slots.at[way, step - 1]
                    ring_copy(ring, way, step - 1, part, source).wait_recv()

                    def add(rows):
                        rows = pl.ds(pl.multiple_of(rows.start + part * piece_rows, 16), rows.size)
                        slots[way, step - 1, rows, :] = (
                            slots[way, step - 1, rows, :].astype(f32)
                            + parts[blocks[way], rows, columns_of(way)].astype(f32)
                        ).astype(bf)

                    row_loop(piece_rows, 16, add)
                ring_copy(ring, way, step, part, source).start()

    def ring_last(ring):
        for part in range(ring_parts):
            for way in (0, 1):
                ring_copy(ring, way, size - 2, part, ring[1].at[way, size - 2]).wait_recv()

    def do_pair(index, carry):
        rows = pl.ds(pl.multiple_of(index * pair, pair), pair)
        for copy in token_loads(index):
            copy.wait()
        tail = packs_ref[rows, width:].astype(f32)
        lane = lax.broadcasted_iota(jnp.int32, tail.shape, 1)
        shares = []
        for expert in range(local_experts):
            name = dp * local_experts + expert
            picked = (lane == name) | (lane == experts + name)
            shares.append(jnp.sum(jnp.where(picked, tail, 0.0), axis=1, keepdims=True))

        def do_units(tile, carry):
            here = pl.ds(pl.multiple_of(tile * wide, wide), wide)

            for number in range(units // wide):

                @pl.when((index == 0) & (tile == number))
                def _():
                    for at, copy in loads:
                        if at // wide == number:
                            copy.wait()

            scale = shares[0] * member_ref[0:1, here]
            for expert in range(1, local_experts):
                scale = scale + shares[expert] * member_ref[expert : expert + 1, here]
            tokens = inputs_ref[rows, :]
            gate = matmul_nt(tokens, weights[0, here, :])
            upward = matmul_nt(tokens, weights[1, here, :])
            grads = scale * matmul_nt(packs_ref[rows, :width], weights[2, here, :])
            share = jax.nn.sigmoid(gate)
            silu = gate * share
            hidden[0, rows, here] = (grads * upward * share * (1.0 + gate * (1.0 - share))).astype(bf)
            hidden[1, rows, here] = (grads * silu).astype(bf)
            hidden[2, rows, here] = (scale * silu * upward).astype(bf)
            return carry

        lax.fori_loop(0, units // wide, do_units, 0)

        def do_columns(tile, carry):
            here = pl.ds(pl.multiple_of(tile * wide, wide), wide)
            sums = matmul(hidden[0, rows, :], weights[0, :, here]) + matmul(
                hidden[1, rows, :], weights[1, :, here]
            )
            low = sums.astype(bf)
            grad_parts[2 * index, :, here] = low[:quarter]
            grad_parts[2 * index + 1, :, here] = low[quarter:]
            return carry

        def do_mix(tile, carry):
            here = pl.ds(pl.multiple_of(tile * wide, wide), wide)
            low = matmul(hidden[2, rows, :], weights[2, :, here]).astype(bf)
            mix_parts[2 * index, :, here] = low[:quarter]
            mix_parts[2 * index + 1, :, here] = low[quarter:]
            return carry

        lax.fori_loop(0, width // wide, do_columns, 0)

        def go_on(ring):
            @pl.when(index == 0)
            def _():
                ring_step(ring, 0, (0, 1), first=True)

            @pl.when(index > 0)
            def _():
                ring_step(ring, index, (2 * index, 2 * index + 1 - index // (half - 1)))

        go_on(grad_ring)
        lax.fori_loop(0, width // wide, do_mix, 0)
        go_on(mix_ring)
        return carry

    lax.fori_loop(0, half, do_pair, 0)
    group_units = (3, 1, 2, 0)
    targets = (landing_ref, given_ref, cross_ref, kept_ref)

    def tile_copies(group, kind, slot):
        copies = []
        for expert in range(local_experts):
            at = expert + 2 * local_experts if isinstance(kind, int) else 2 * expert + kind
            source = stage.at[slot, pl.ds(expert * part_units, part_units)]
            target = targets[group].at[at]
            if group < 2:
                sems = (give_sems.at[0, group, at], give_sems.at[1, group, at])
                copies.append(push(source, target, sems, (dp, partner)))
            else:
                copies.append(pltpu.make_async_copy(source, target, store_sems.at[group - 2, at]))
        return copies

    def tile_left(group, kind, slot):
        for copy in tile_copies(group, kind, slot):
            if group < 2:
                copy.wait_send()
            else:
                copy.wait()

    def land(kind):
        copies = []
        for expert in range(local_experts):
            at = expert + 2 * local_experts if isinstance(kind, int) else 2 * expert + kind
            rows = pl.ds(expert * part_units, part_units)
            copies.append(
                pltpu.make_async_copy(landing_ref.at[at], landed.at[rows], land_sems.at[expert])
            )
        return copies

    def tile(group, kind, source, before):
        number = 3 * group + kind
        slot = number % 2
        if before is not None:
            before(slot)
        if group == 2:
            for copy in tile_copies(0, kind, slot):
                copy.wait_recv()
            for copy in land(kind):
                copy.start()
        rows = pl.ds(group_units[group] * span, span)
        for chunk in range(half):
            some = pl.ds(chunk * pair, pair)
            turned[:, some] = hidden[kind, some, rows].T
        if group == 2:
            for copy in land(kind):
                copy.wait()

        def do_columns(tile, carry):
            here = pl.ds(pl.multiple_of(tile * wide, wide), wide)
            sums = matmul(turned[...], source[:, here])
            if group == 2:
                sums = sums + landed[:, here].astype(f32)
            stage[slot, :, here] = sums.astype(bf)
            return carry

        lax.fori_loop(0, width // wide, do_columns, 0)
        for copy in tile_copies(group, kind, slot):
            copy.start()

    def token_tiles(group):
        def run(kind, carry):
            if group == 0:
                before = None
            else:
                def before(slot):
                    @pl.when(kind == 0)
                    def _():
                        tile_left(group - 1, kind + 1, slot)

                    @pl.when(kind == 1)
                    def _():
                        tile_left(group - 1, 2, slot)

            tile(group, kind, inputs_ref, before)
            return carry

        lax.fori_loop(0, 2, run, 0)

    def grad_tile(group):
        def before(slot):
            tile_left(group, jnp.int32(0), slot)

        tile(group, 2, packs_ref, before)

    def final_sum():
        totals[...] = jnp.zeros_like(totals)
        ring_last(grad_ring)
        base = own * quarter

        def finish(rows):
            sums = jnp.concatenate(
                [
                    grad_slots[0, size - 2, rows, :].astype(f32),
                    grad_slots[1, size - 2, rows, :].astype(f32),
                ],
                axis=-1,
            ) + grad_parts[size - 1, rows, :].astype(f32)
            middle = middle_ref[rows, :]
            inverse = lax.rsqrt(jnp.mean(middle * middle, axis=-1, keepdims=True) + EPSILON)
            hat = middle * inverse
            product = sums * hat
            totals[...] += product[:8] + product[8:]
            scaled = sums * gain_ref[...]
            back = inverse * (scaled - hat * jnp.mean(scaled * hat, axis=-1, keepdims=True))
            above = packs_ref[
                pl.ds(pl.multiple_of((size - 1) * quarter + rows.start, 16), rows.size), :width
            ]
            grad = above.astype(f32) + back
            gmid_ref[rows, :] = grad
            gmid_all[pl.ds(pl.multiple_of(base + rows.start, 16), rows.size), :] = grad.astype(bf)

        row_loop(quarter, 16, finish)
        gain_out[...] = jnp.sum(totals[...], axis=0, keepdims=True)

    def rows_of(index):
        return pl.ds(pl.multiple_of(index * quarter, quarter), quarter)

    def spread(index, whose, device):
        ref = gmid_all.at[rows_of(whose)]
        return push(ref, ref, (side_sems.at[0, index], side_sems.at[1, index]), device)

    def first_spread():
        spread(0, own, (dp, across)).start()
        spread(1, own, (dp, partner)).start()

    def second_spread():
        spread(0, own, (dp, across)).wait_recv()
        spread(2, across, (dp, partner)).start()

    def final_mix():
        ring_last(mix_ring)

        def finish(rows):
            for way in (0, 1):
                columns = columns_of(way)
                hidden_out[rows, columns] = (
                    middle_ref[rows, columns]
                    + mix_slots[way, size - 2, rows, :].astype(f32)
                    + mix_parts[size - 1, rows, columns].astype(f32)
                ).astype(bf)

        row_loop(quarter, 16, finish)

    def closing():
        final_sum()
        first_spread()

    grad_events, mix_events = [], []
    for step in range(half, size - 1):
        delta = -(1 + step)
        blocks = (slot_of(delta, size), slot_of(-delta, size))
        grad_events.append(functools.partial(ring_step, grad_ring, step, blocks))
        mix_events.append(functools.partial(ring_step, mix_ring, step, blocks))
    events = grad_events[:-1]
    events += [grad_events[-1], mix_events[0], closing] + mix_events[1:2] + [second_spread]
    events += mix_events[2:] + [final_mix]
    work = []
    for group in range(4):
        work.append(functools.partial(token_tiles, group))
        work.append(functools.partial(grad_tile, group))
    done = 0
    for number, piece in enumerate(work):
        piece()
        upto = -(-(number + 1) * len(events) // len(work))
        while done < upto:
            events[done]()
            done += 1
    tile_left(3, jnp.int32(1), 0)
    tile_left(3, 2, 1)
    for kind in (jnp.int32(0), jnp.int32(1), 2):
        for copy in tile_copies(1, kind, 0):
            copy.wait_recv()
    spread(1, own, (dp, partner)).wait_recv()
    spread(2, across, (dp, partner)).wait_recv()
    for index, device in ((0, across), (1, partner), (2, partner)):
        spread(index, own, (dp, device)).wait_send()
    for ring in (grad_ring, mix_ring):
        for way in (0, 1):
            for step in range(size - 1):
                for part in range(ring_parts):
                    ring_copy(ring, way, step, part, ring[1].at[way, step]).wait_send()


def run_experts(size, inputs, packs, gate_up, down, others, middle, gain, experts):
    bf, f32 = jnp.bfloat16, jnp.float32
    local_experts, _, part_units, width = gate_up.shape
    others = others.reshape(3, 3, local_experts * part_units, width)
    members, span = 4, local_experts * part_units
    rows = inputs.shape[0]
    quarter = rows // size
    units = members * span
    expert_of = (jnp.arange(units, dtype=jnp.int32) // (span // local_experts)) % local_experts
    member = (expert_of[None, :] == jnp.arange(local_experts, dtype=jnp.int32)[:, None]).astype(f32)
    vmem = pl.BlockSpec(memory_space=pltpu.VMEM)
    anywhere = pl.BlockSpec(memory_space=pl.ANY)
    dma = pltpu.SemaphoreType.DMA
    return pl.pallas_call(
        functools.partial(run_experts_body, size, local_experts, experts),
        out_shape=(
            jax.ShapeDtypeStruct((quarter, width), bf),
            jax.ShapeDtypeStruct((3 * local_experts, part_units, width), bf),
            jax.ShapeDtypeStruct((3 * local_experts, part_units, width), bf),
            jax.ShapeDtypeStruct((3 * local_experts, part_units, width), bf),
            jax.ShapeDtypeStruct((3 * local_experts, part_units, width), bf),
            jax.ShapeDtypeStruct((quarter, width), f32),
            jax.ShapeDtypeStruct((members * quarter, width), bf),
            jax.ShapeDtypeStruct((1, width), f32),
        ),
        in_specs=[anywhere] * 5 + [vmem] * 3,
        out_specs=(vmem,) + (anywhere,) * 4 + (vmem,) * 3,
        scratch_shapes=[
            pltpu.VMEM((3, units, width), bf),
            pltpu.VMEM((3, rows, units), bf),
            pltpu.VMEM((size, quarter, width), bf),
            pltpu.VMEM((size, quarter, width), bf),
            pltpu.VMEM((2, size - 1, quarter, width // 2), bf),
            pltpu.VMEM((2, size - 1, quarter, width // 2), bf),
            pltpu.VMEM((span, rows), bf),
            pltpu.VMEM((2, span, width), bf),
            pltpu.VMEM((span, width), bf),
            pltpu.VMEM((8, width), f32),
            dma((3 * local_experts + 3 * span // LANES,)),
            dma((2, 2, size - 1, 2)),
            dma((2, 2, size - 1, 2)),
            dma((2, 3)),
            dma((2, 3 * local_experts)),
            dma((2, 2, 3 * local_experts)),
            dma((local_experts,)),
            dma((2, size // 2)),
            pltpu.VMEM(inputs.shape, bf),
            pltpu.VMEM(packs.shape, bf),
        ],
        compiler_params=pltpu.CompilerParams(
            collective_id=2, has_side_effects=True, vmem_limit_bytes=VMEM_LIMIT
        ),
        name="run_experts",
    )(inputs, packs, gate_up, down, others, member, middle, gain.reshape(1, -1))


def back_through_head(grads, raw, gain, cosine, sine):
    hat_grads = grads * cosine - pltpu.roll(grads, grads.shape[1] // 2, 1) * sine
    inverse = lax.rsqrt(jnp.mean(raw * raw, axis=-1, keepdims=True) + EPSILON)
    hat = raw * inverse
    terms = hat_grads * hat
    scaled = hat_grads * gain
    back = inverse * (scaled - hat * jnp.mean(scaled * hat, axis=-1, keepdims=True))
    return back.astype(jnp.bfloat16), terms


def finish_layer_body(
    size,
    gmid_low_hbm,
    out_weight_hbm,
    mixed_hbm,
    query_hbm,
    key_hbm,
    value_hbm,
    raw_query_hbm,
    raw_key_hbm,
    normed_hbm,
    query_weight_hbm,
    key_weight_hbm,
    value_weight_hbm,
    cosine_ref,
    sine_ref,
    start_ref,
    query_gain_ref,
    key_gain_ref,
    middle_ref,
    token_hbm,
    hidden_ref,
    cross_ref,
    gain_ref,
    gains_ref,
    hidden_all,
    crossed_ref,
    grad_all,
    query_out,
    key_out,
    value_out,
    gather_b_hbm,
    gains_out,
    qkv_ref,
    out_ref,
    slots_a,
    slots_b,
    grad_mixed,
    grad_heads,
    key_sums,
    value_sums,
    turned,
    partial,
    from_partner,
    from_across,
    joined,
    totals,
    head_totals,
    pair_gains,
    ring_gains,
    sems_a,
    sems_b,
    ring_sems,
    side_sems,
    load_sems,
    store_sems,
    gather_a,
    gather_b,
    token_ref,
    gmid_low_ref,
    out_weight_ref,
    mixed_ref,
    query_ref,
    key_ref,
    value_ref,
    raw_query_ref,
    raw_key_ref,
    normed_ref,
    query_weight_ref,
    key_weight_ref,
    value_weight_ref,
):
    f32, bf = jnp.float32, jnp.bfloat16
    dp = lax.axis_index("dp")
    own, partner, across = tensor_peers()
    far_partner = (partner + 2) % 4
    quarter, width = token_ref.shape
    tokens = normed_ref.shape[0]
    head_dim = key_ref.shape[1]
    lead = query_ref.shape[1]
    heads = lead // head_dim
    scale = head_dim**-0.5
    place = ring_place(dp, size)
    forward = (ring_index(place + 1, size), own)
    backward = (ring_index(place + size - 1, size), own)
    ways = ((forward, 1), (backward, -1))
    mine = pl.ds(pl.multiple_of(own * quarter, quarter), quarter)
    home = own * quarter
    loads = {}
    for source, target in (
        (gmid_low_hbm, gmid_low_ref),
        (mixed_hbm, mixed_ref),
        (out_weight_hbm, out_weight_ref),
        (query_hbm, query_ref),
        (key_hbm, key_ref),
        (value_hbm, value_ref),
        (raw_query_hbm, raw_query_ref),
        (raw_key_hbm, raw_key_ref),
        (normed_hbm, normed_ref),
        (query_weight_hbm, query_weight_ref),
        (key_weight_hbm, key_weight_ref),
        (value_weight_hbm, value_weight_ref),
        (token_hbm.at[mine], token_ref),
    ):
        copy = pltpu.make_async_copy(source, target, load_sems.at[len(loads)])
        copy.start()
        loads[id(target)] = copy

    def loaded(*targets):
        for target in targets:
            loads[id(target)].wait()

    greet([forward, backward, (dp, partner), (dp, across)])
    waits = []

    def start(copy):
        copy.start()
        waits.append(copy)
        return copy

    sets = (
        (qkv_ref, slots_a, gather_a, sems_a),
        (out_ref, slots_b, gather_b, sems_b),
    )

    def block_of(ref, block, way):
        rows = ref.shape[0] // size
        cut = ref.shape[1] // 2
        return (pl.ds(pl.multiple_of(block * rows, rows), rows), pl.ds(way * cut, cut))

    def wrap(value):
        return (value + 2 * size) % size

    live = {}

    ring_parts = 2
    stores = []

    def add_own(which, way, step, part):
        ref, slots, blocks, _ = sets[which]
        live[which, way, step, part].wait_recv()
        sign = ways[way][1]
        rows, columns = block_of(ref, wrap(place - sign * (2 + step)), way)
        base = rows.start
        count = ref.shape[0] // size // ring_parts

        def add(inner):
            inner = pl.ds(pl.multiple_of(inner.start + part * count, 16), inner.size)
            there = pl.ds(pl.multiple_of(base + inner.start, 16), inner.size)
            sums = (slots[way, step, inner, :].astype(f32) + ref[there, columns].astype(f32)).astype(bf)
            if step == size - 2:
                blocks[place, inner, columns] = sums
            else:
                slots[way, step, inner, :] = sums

        row_loop(count, 16, add)

    def keep_block(which, way, block, part):
        ref, _, blocks, _ = sets[which]
        count, cut = ref.shape[0] // size // ring_parts, ref.shape[1] // 2
        inner = pl.ds(part * count, count)
        at = pl.multiple_of(block * (ref.shape[0] // size) + part * count, 16)
        rows = pl.ds(at, count)
        if which == 1:
            targets = [(gather_b_hbm.at[rows, pl.ds(way * cut, cut)], way * cut, cut)]
        elif way == 0:
            targets = [(query_out.at[rows, pl.ds(0, cut)], 0, cut)]
        else:
            targets = [
                (query_out.at[rows, pl.ds(cut, lead - cut)], cut, lead - cut),
                (key_out.at[rows], lead, head_dim),
                (value_out.at[rows], lead + head_dim, head_dim),
            ]
        for target, first, columns in targets:
            source = blocks.at[block, inner, pl.ds(first, columns)]
            copy = pltpu.make_async_copy(source, target, store_sems.at[len(stores)])
            copy.start()
            stores.append(copy)

    def ring_event(which, step):
        ref, slots, blocks, sems = sets[which]
        cut = ref.shape[1] // 2
        count = ref.shape[0] // size // ring_parts
        for part in range(ring_parts):
            inner = pl.ds(part * count, count)
            for way, (device, sign) in enumerate(ways):
                if step == 0:
                    rows, columns = block_of(ref, wrap(place - sign), way)
                    rows = pl.ds(pl.multiple_of(rows.start + part * count, 16), count)
                    source = ref.at[rows, columns]
                elif step < size:
                    add_own(which, way, step - 1, part)
                    source = slots.at[way, step - 1, inner] if step < size - 1 else None
                else:
                    live[which, way, step - 1, part].wait_recv()
                block = wrap(place - sign * (step - size + 1))
                if step >= size - 1:
                    keep_block(which, way, block, part)
                if step >= 2 * size - 2:
                    continue
                if step >= size - 1:
                    source = blocks.at[block, inner, pl.ds(way * cut, cut)]
                    target = source
                else:
                    target = slots.at[way, step, inner]
                sem = (sems.at[0, way, step, part], sems.at[1, way, step, part])
                live[which, way, step, part] = start(push(source, target, sem, device))

    def part_rows(index):
        return pl.ds(pl.multiple_of(index * quarter, quarter), quarter)

    def side(index):
        return (side_sems.at[0, index], side_sems.at[1, index])

    step_rows = 2 * LANES
    wide = 4 * LANES

    def out_rows(index, carry):
        rows = pl.ds(pl.multiple_of(index * step_rows, step_rows), step_rows)
        turned[...] = mixed_ref[:, rows].T

        def columns(tile, carry):
            here = pl.ds(pl.multiple_of(tile * wide, wide), wide)
            out_ref[rows, here] = matmul(turned[...], gmid_low_ref[:, here]).astype(bf)
            return carry

        return lax.fori_loop(0, width // wide, columns, carry)

    loaded(gmid_low_ref, mixed_ref)
    lax.fori_loop(0, lead // step_rows, out_rows, 0)
    ring_event(1, 0)

    def keep(rows):
        hidden_all[pl.ds(pl.multiple_of(home + rows.start, 16), rows.size), :] = hidden_ref[rows, :]

    row_loop(quarter, 16, keep)
    shown = [start(push(hidden_ref, hidden_all.at[mine], side(9), (dp, across)))]
    shown.append(start(push(hidden_ref, hidden_all.at[mine], side(10), (dp, partner))))

    def mixed_columns(tile, carry):
        here = pl.ds(pl.multiple_of(tile * wide, wide), wide)
        grad_mixed[:, here] = matmul_nt(gmid_low_ref[...], out_weight_ref[here, :]).astype(bf)
        return carry

    loaded(out_weight_ref)
    lax.fori_loop(0, lead // wide, mixed_columns, 0)
    loaded(query_ref, key_ref, value_ref, raw_query_ref, raw_key_ref)
    key_sums[...] = jnp.zeros_like(key_sums)
    value_sums[...] = jnp.zeros_like(value_sums)
    head_totals[...] = jnp.zeros_like(head_totals)
    block = tokens // 2

    def do_head(head, carry):
        lanes = pl.ds(pl.multiple_of(head * head_dim, head_dim), head_dim)
        for part in (0, 1):
            rows = pl.ds(part * block, block)
            count = (part + 1) * block
            keys = pl.ds(0, count)
            queries = query_ref[rows, lanes]
            outer = grad_mixed[rows, lanes]
            scores = matmul_nt(key_ref[keys, :], queries)
            key_at = lax.broadcasted_iota(jnp.int32, scores.shape, 0)
            query_at = lax.broadcasted_iota(jnp.int32, scores.shape, 1) + part * block
            seen = (key_at <= query_at) & (key_at >= start_ref[:, rows])
            exponent = jnp.where(seen, jnp.exp(scores * scale), 0.0)
            soft = exponent * (1.0 / jnp.sum(exponent, axis=0, keepdims=True))
            grad_soft = matmul_nt(value_ref[keys, :], outer)
            inner = jnp.sum(soft * grad_soft, axis=0, keepdims=True)
            grad_scores = (soft * (grad_soft - inner)).astype(bf)
            value_sums[keys, :] += matmul(soft.astype(bf), outer)
            key_sums[keys, :] += matmul(grad_scores, queries)
            grad_query = scale * lax.dot_general(
                grad_scores, key_ref[keys, :], (((0,), (0,)), ((), ())), preferred_element_type=f32
            )
            low, terms = back_through_head(
                grad_query, raw_query_ref[rows, lanes], query_gain_ref[...], cosine_ref[rows, :], sine_ref[rows, :]
            )
            grad_heads[rows, lanes] = low
            head_totals[0] += jnp.sum(terms.reshape(-1, 8, head_dim), axis=0)
        return carry

    lax.fori_loop(0, heads // 2, do_head, 0)
    ring_event(1, 1)
    lax.fori_loop(heads // 2, heads, do_head, 0)
    ring_event(1, 2)
    low, terms = back_through_head(
        scale * key_sums[...], raw_key_ref[...], key_gain_ref[...], cosine_ref[...], sine_ref[...]
    )
    grad_heads[:, pl.ds(lead, head_dim)] = low
    head_totals[1] += jnp.sum(terms.reshape(-1, 8, head_dim), axis=0)
    grad_heads[:, pl.ds(lead + head_dim, head_dim)] = value_sums[...].astype(bf)

    def in_rows(index, carry):
        rows = pl.ds(pl.multiple_of(index * step_rows, step_rows), step_rows)
        turned[...] = normed_ref[:, rows].T
        qkv_ref[rows, :] = matmul(turned[...], grad_heads[...]).astype(bf)
        return carry

    loaded(normed_ref)
    lax.fori_loop(0, width // step_rows, in_rows, 0)
    ring_event(1, 3)
    ring_event(0, 0)

    def token_columns(tile, carry):
        here = pl.ds(pl.multiple_of(tile * wide, wide), wide)
        sums = matmul_nt(grad_heads[:, :lead], query_weight_ref[here, :])
        sums = sums + matmul_nt(grad_heads[:, lead : lead + head_dim], key_weight_ref[here, :])
        sums = sums + matmul_nt(grad_heads[:, lead + head_dim :], value_weight_ref[here, :])
        partial[:, here] = sums.astype(bf)
        return carry

    loaded(query_weight_ref, key_weight_ref, value_weight_ref)
    lax.fori_loop(0, width // wide, token_columns, 0)
    first = start(push(partial.at[part_rows(far_partner)], from_partner.at[1], side(0), (dp, partner)))
    second = start(push(partial.at[part_rows(partner)], from_partner.at[0], side(1), (dp, partner)))
    ring_event(1, 4)
    first.wait_recv()
    away = across * quarter

    def join(rows):
        there = pl.ds(pl.multiple_of(away + rows.start, 16), rows.size)
        joined[rows, :] = (partial[there, :].astype(f32) + from_partner[1, rows, :].astype(f32)).astype(bf)

    row_loop(quarter, 16, join)
    third = start(push(joined, from_across, side(2), (dp, across)))
    ring_event(0, 1)
    ring_event(1, 5)
    second.wait_recv()
    third.wait_recv()
    totals[...] = jnp.zeros_like(totals)

    def finish(rows):
        there = pl.ds(pl.multiple_of(home + rows.start, 16), rows.size)
        grads = (
            partial[there, :].astype(f32)
            + from_partner[0, rows, :].astype(f32)
            + from_across[rows, :].astype(f32)
        )
        hidden = token_ref[rows, :].astype(f32)
        inverse = lax.rsqrt(jnp.mean(hidden * hidden, axis=-1, keepdims=True) + EPSILON)
        hat = hidden * inverse
        product = grads * hat
        totals[...] += product[:8] + product[8:]
        scaled = grads * gain_ref[...]
        back = inverse * (scaled - hat * jnp.mean(scaled * hat, axis=-1, keepdims=True))
        grad_all[there, :] = (middle_ref[rows, :] + back).astype(bf)

    loaded(token_ref)
    row_loop(quarter, 16, finish)
    spread = [start(push(grad_all.at[mine], grad_all.at[mine], side(3), (dp, across)))]
    spread.append(start(push(grad_all.at[mine], grad_all.at[mine], side(4), (dp, partner))))
    pair_gains[0, :, :width] = jnp.sum(totals[...], axis=0, keepdims=True)
    pair_gains[0, :, width : 2 * width] = gains_ref[...]
    pair_gains[0, :, 2 * width : 2 * width + head_dim] = jnp.sum(head_totals[0], axis=0, keepdims=True)
    pair_gains[0, :, 2 * width + head_dim :] = jnp.sum(head_totals[1], axis=0, keepdims=True)
    swap = start(push(pair_gains.at[0], pair_gains.at[1], side(5), (dp, partner)))
    ring_event(0, 2)
    ring_event(1, 6)
    far = part_rows(across)
    shown[0].wait_recv()
    shown.append(start(push(hidden_all.at[far], hidden_all.at[far], side(11), (dp, partner))))
    spread[0].wait_recv()
    spread.append(start(push(grad_all.at[far], grad_all.at[far], side(6), (dp, partner))))
    swap.wait_recv()
    pair_gains[2] = pair_gains[0] + pair_gains[1]
    swap = start(push(pair_gains.at[2], pair_gains.at[3], side(7), (dp, across)))
    ring_event(0, 3)
    ring_event(1, 7)
    swap.wait_recv()
    crossing = start(push(cross_ref, crossed_ref, side(8), (dp, across)))
    ring_gains[place] = pair_gains[2] + pair_gains[3]
    small = None
    for step in range(4, 2 * size - 1):
        ring_event(0, step)
        if step + 4 < 2 * size - 1:
            ring_event(1, step + 4)
        if step - 4 < size - 1:
            if small is not None:
                small.wait_recv()
            ref = ring_gains.at[wrap(place - step + 4)]
            sem = (ring_sems.at[0, step - 4], ring_sems.at[1, step - 4])
            small = start(push(ref, ref, sem, forward))
    small.wait_recv()
    gains_out[...] = jnp.sum(ring_gains[...], axis=0)
    for copy in (spread[1], spread[2], shown[1], shown[2], crossing):
        copy.wait_recv()
    for copy in waits:
        copy.wait_send()
    for copy in stores:
        copy.wait()


def finish_layer(size, *arguments):
    bf, f32 = jnp.bfloat16, jnp.float32
    (
        _, out_weight, mixed, query, key, _, _, _, normed, query_weight, _, _, _, _, _, _, _, _, token_rows, _,
        cross, _, _,
    ) = arguments
    tokens, width = token_rows.shape
    quarter = tokens // 4
    lead, head_dim = query.shape[1], key.shape[1]
    vmem = pl.BlockSpec(memory_space=pltpu.VMEM)
    anywhere = pl.BlockSpec(memory_space=pl.ANY)
    dma = pltpu.SemaphoreType.DMA
    columns = lead + 2 * head_dim
    rows_a, rows_b = width // size, lead // size
    count = 2 * width + 2 * head_dim
    return pl.pallas_call(
        functools.partial(finish_layer_body, size),
        out_shape=(
            jax.ShapeDtypeStruct((tokens, width), bf),
            jax.ShapeDtypeStruct(cross.shape, bf),
            jax.ShapeDtypeStruct((tokens, width), bf),
            jax.ShapeDtypeStruct((width, lead), bf),
            jax.ShapeDtypeStruct((width, head_dim), bf),
            jax.ShapeDtypeStruct((width, head_dim), bf),
            jax.ShapeDtypeStruct((lead, width), bf),
            jax.ShapeDtypeStruct((1, count), f32),
        ),
        in_specs=[anywhere] * 12 + [vmem] * 6 + [anywhere, vmem, anywhere, vmem, vmem],
        out_specs=(vmem, anywhere, vmem) + (anywhere,) * 4 + (vmem,),
        scratch_shapes=[
            pltpu.VMEM((width, columns), bf),
            pltpu.VMEM((lead, width), bf),
            pltpu.VMEM((2, size - 1, rows_a, columns // 2), bf),
            pltpu.VMEM((2, size - 1, rows_b, width // 2), bf),
            pltpu.VMEM((tokens, lead), bf),
            pltpu.VMEM((tokens, columns), bf),
            pltpu.VMEM((tokens, head_dim), f32),
            pltpu.VMEM((tokens, head_dim), f32),
            pltpu.VMEM((2 * LANES, tokens), bf),
            pltpu.VMEM((tokens, width), bf),
            pltpu.VMEM((2, quarter, width), bf),
            pltpu.VMEM((quarter, width), bf),
            pltpu.VMEM((quarter, width), bf),
            pltpu.VMEM((8, width), f32),
            pltpu.VMEM((2, 8, head_dim), f32),
            pltpu.VMEM((4, 1, count), f32),
            pltpu.VMEM((size, 1, count), f32),
            dma((2, 2, 2 * size - 2, 2)),
            dma((2, 2, 2 * size - 2, 2)),
            dma((2, size - 1)),
            dma((2, 12)),
            dma((13,)),
            dma((12 * size,)),
            pltpu.VMEM((size, rows_a, columns), bf),
            pltpu.VMEM((size, rows_b, width), bf),
            pltpu.VMEM((quarter, width), bf),
        ]
        + [pltpu.VMEM(argument.shape, argument.dtype) for argument in arguments[:12]],
        compiler_params=pltpu.CompilerParams(
            collective_id=1, has_side_effects=True, vmem_limit_bytes=VMEM_LIMIT
        ),
        name="finish_layer",
    )(*arguments)


def large_experts(size, inputs, packs, gate_up, down, others, middle, gain, experts):
    f32, bf = jnp.float32, jnp.bfloat16
    model_width = inputs.shape[1]
    own_weights = jnp.stack([gate_up[:, 0], gate_up[:, 1], down])
    all_weights = jnp.concatenate([own_weights[None], others])
    members = all_weights.shape[0]
    order = jnp.arange(members, dtype=jnp.int32) ^ lax.axis_index("tensor")
    all_weights = all_weights.reshape(members, 3, -1, model_width)[order]
    units = all_weights.shape[2]
    local_experts = experts // size
    indices = jnp.arange(size, dtype=jnp.int32)
    half = size // 2
    delta = (ring_place(indices, size) - ring_place(lax.axis_index("dp"), size)) % size
    ahead = jnp.where(delta == half, size - 2, jnp.where(delta == 0, size - 1, 2 * delta - 1))
    slots = jnp.where(delta > half, 2 * (size - delta) - 2, ahead)
    quarter = middle.shape[0]
    out_rows = packs[-quarter:, :model_width]
    inputs = inputs.reshape(size, quarter, -1)[slots].reshape(-1, model_width)
    packs = packs.reshape(size, quarter, -1)[slots].reshape(inputs.shape[0], -1)
    grads_all = packs[:, :model_width]
    shares = packs[:, model_width : model_width + 2 * experts].astype(f32)
    shares = shares[:, :experts] + shares[:, experts:]
    shares = lax.dynamic_slice_in_dim(
        shares, lax.axis_index("dp") * local_experts, local_experts, 1
    )
    weight_cols = jnp.broadcast_to(
        shares[:, None, :, None],
        (shares.shape[0], members, local_experts, units // local_experts),
    ).reshape(-1, members, units)

    def project(left, which):
        return jnp.einsum("td,rud->tru", left, all_weights[:, which], preferred_element_type=f32)

    gate_act = project(inputs, 0)
    upward = project(inputs, 1)
    sigmoid_gate = jax.nn.sigmoid(gate_act)
    active = gate_act * sigmoid_gate * upward
    weighted_low = (weight_cols * active).astype(bf)
    mixture_part = jnp.einsum(
        "tru,rud->td", weighted_low, all_weights[:, 2], preferred_element_type=f32
    ).astype(bf)
    grad_active = weight_cols * project(grads_all, 2)
    grad_gate = (
        grad_active * upward * sigmoid_gate * (1.0 + gate_act * (1.0 - sigmoid_gate))
    ).astype(bf)
    grad_up = (grad_active * gate_act * sigmoid_gate).astype(bf)
    grad_normed_part = jnp.einsum(
        "tru,rud->td", grad_gate, all_weights[:, 0], preferred_element_type=f32
    ) + jnp.einsum("tru,rud->td", grad_up, all_weights[:, 1], preferred_element_type=f32)
    grad_normed_two = lax.psum_scatter(grad_normed_part.astype(bf), "dp", tiled=True).astype(f32)
    weight_grads = jnp.stack(
        [
            jnp.einsum("tru,td->rud", grad_gate, inputs, preferred_element_type=f32).astype(bf),
            jnp.einsum("tru,td->rud", grad_up, inputs, preferred_element_type=f32).astype(bf),
            jnp.einsum("tru,td->rud", weighted_low, grads_all, preferred_element_type=f32).astype(bf),
        ],
        axis=1,
    )
    hat_two, inv_two = rms_parts(middle)
    grad_gain_two = jnp.sum(grad_normed_two * hat_two, axis=0)
    grad_middle = out_rows.astype(f32) + rms_back(grad_normed_two * gain, hat_two, inv_two)
    grad_mid_low = lax.all_gather(grad_middle.astype(bf), "tensor", tiled=True)
    mixture = lax.psum_scatter(mixture_part, "dp", tiled=True).astype(f32)
    hidden_out = (middle + mixture).astype(bf)
    sums = lax.psum_scatter(weight_grads.reshape(-1, model_width), "tensor", tiled=True)
    sums = sums.reshape(3, local_experts, -1, model_width)
    kept = jnp.concatenate(
        [jnp.swapaxes(sums[:2], 0, 1).reshape(2 * local_experts, -1, model_width), sums[2]]
    )
    zero = jnp.zeros_like(kept)
    return (hidden_out, kept, zero, zero, zero, grad_middle, grad_mid_low, grad_gain_two)


def local(
    hidden_in,
    seq_lens,
    norm1_gain,
    query_weight,
    key_weight,
    value_weight,
    query_gain,
    key_gain,
    out_weight,
    norm2_gain,
    w_gate_up,
    w_down,
    routes,
    route_weights,
    out_grad,
):
    bf = jnp.bfloat16
    f32 = jnp.float32
    tokens, model_width = hidden_in.shape
    local_experts = w_gate_up.shape[0]
    hidden_part = w_gate_up.shape[3]
    head_dim = query_gain.shape[0]
    data_size = lax.axis_size("dp")
    quarter = tokens // lax.axis_size("tensor")
    experts = local_experts * data_size
    rows = data_size * quarter
    places, starts = sequence_layout(seq_lens[0], tokens)
    cosine_table, sine_table = rotary_tables(places - starts, head_dim)
    cosines = jnp.concatenate([cosine_table, cosine_table], axis=1)
    sines = jnp.concatenate([-sine_table, sine_table], axis=1)
    starts = starts.reshape(1, -1).astype(jnp.int32)
    gate_up = jnp.transpose(w_gate_up, (0, 2, 3, 1))
    (
        middle,
        inputs,
        gathered,
        others,
        mixed_low,
        query_low,
        key_low,
        value_low,
        raw_query,
        raw_key,
        normed,
    ) = start_layer(
        data_size,
        experts,
        hidden_in,
        out_grad,
        routes,
        route_weights,
        query_weight,
        key_weight,
        value_weight,
        out_weight,
        gate_up,
        w_down,
        cosines,
        sines,
        starts,
        norm1_gain.reshape(1, -1),
        norm2_gain.reshape(1, -1),
        query_gain.reshape(1, -1),
        key_gain.reshape(1, -1),
    )
    stage = run_experts if data_size <= 8 else large_experts
    hidden_out, kept, given, joined, _, grad_middle, grad_mid_low, grad_gain_two = stage(
        data_size,
        inputs.reshape(rows, model_width),
        gathered.reshape(rows, -1),
        gate_up,
        w_down,
        others,
        middle,
        norm2_gain,
        experts,
    )
    hidden_out, crossed, grad_hidden, query_sum, key_sum, value_sum, out_sum, gains = finish_layer(
        data_size,
        grad_mid_low,
        out_weight,
        mixed_low,
        query_low,
        key_low,
        value_low,
        raw_query,
        raw_key,
        normed,
        query_weight,
        key_weight,
        value_weight,
        cosines,
        sines,
        starts,
        query_gain.reshape(1, -1),
        key_gain.reshape(1, -1),
        grad_middle,
        hidden_in,
        hidden_out,
        joined,
        norm1_gain.reshape(1, -1),
        grad_gain_two.reshape(1, -1),
    )
    def whole(first, last):
        parts = (kept[first:last], given[first:last], crossed[first:last])
        return parts[0].astype(f32) + parts[1].astype(f32) + parts[2].astype(f32)

    grad_w_gate_up = jnp.transpose(
        whole(0, 2 * local_experts).reshape(local_experts, 2, hidden_part, model_width), (0, 3, 1, 2)
    )
    grad_w_down = whole(2 * local_experts, 3 * local_experts)
    gains = gains.reshape(-1)
    return (
        hidden_out,
        grad_hidden,
        gains[:model_width],
        query_sum.astype(f32),
        key_sum.astype(f32),
        value_sum.astype(f32),
        gains[2 * model_width : 2 * model_width + head_dim],
        gains[2 * model_width + head_dim :],
        out_sum.astype(f32),
        gains[model_width : 2 * model_width],
        grad_w_gate_up,
        grad_w_down,
    )


def solution(mesh):
    in_specs = (
        P("dp", None),
        P("dp", None),
        P(),
        P(None, "tensor"),
        P(None, "tensor"),
        P(None, "tensor"),
        P(),
        P(),
        P("tensor", None),
        P(),
        P("dp", None, None, "tensor"),
        P("dp", "tensor", None),
        P("dp", None),
        P("dp", None),
        P("dp", None),
    )
    out_specs = (
        P("dp", None),
        P("dp", None),
        P(),
        P(None, "tensor"),
        P(None, "tensor"),
        P(None, "tensor"),
        P(),
        P(),
        P("tensor", None),
        P(),
        P("dp", None, None, "tensor"),
        P("dp", "tensor", None),
    )
    return jax.shard_map(local, mesh=mesh, in_specs=in_specs, out_specs=out_specs, check_vma=False)
```

```python
import functools
import math

import jax
import jax.numpy as jnp
from jax import lax
from jax.experimental import pallas as pl
from jax.experimental.pallas import tpu as pltpu
from jax.sharding import PartitionSpec as P

EPSILON = 1e-06
ROPE_BASE = 1000000.0


def rms_parts(values):
    inverse = lax.rsqrt(jnp.mean(values * values, axis=-1, keepdims=True) + EPSILON)
    return (values * inverse, inverse)


def rms_back(grad_hat, normal_hat, inverse):
    return inverse * (
        grad_hat - normal_hat * jnp.mean(grad_hat * normal_hat, axis=-1, keepdims=True)
    )


def rotary_tables(positions, head_dim):
    halves = jnp.arange(head_dim // 2, dtype=jnp.float32)
    inverse = jnp.exp(halves * (-2.0 * math.log(ROPE_BASE) / head_dim))
    angles = positions.astype(jnp.float32)[:, None] * inverse[None, :]
    return (jnp.cos(angles), jnp.sin(angles))


def sequence_layout(lengths, token_count):
    endings = jnp.cumsum(lengths)
    places = jnp.arange(token_count, dtype=jnp.int32)
    starts = jnp.sum(jnp.where(endings[None, :] <= places[:, None], lengths[None, :], 0), axis=1)
    return (places, starts)


LANES = 128
MESH = pl.DeviceIdType.MESH
VMEM_LIMIT = 127 * 512 * 1024


def ring_place(index, size):
    return jnp.where(index % 2 == 0, index // 2, size - (index + 1) // 2)


def ring_index(place, size):
    place = place % size
    return jnp.where(place < size // 2, 2 * place, 2 * size - 1 - 2 * place)


def tensor_peers():
    own = lax.axis_index("tensor")
    partner = own + 1 - 2 * (own % 2)
    across = (own + 2) % 4
    return own, partner, across


def greet(devices):
    barrier = pltpu.get_barrier_semaphore()
    for device in devices:
        pl.semaphore_signal(barrier, inc=1, device_id=device, device_id_type=MESH)
    pl.semaphore_wait(barrier, len(devices))


def push(source, target, sems, device):
    return pltpu.make_async_remote_copy(
        src_ref=source,
        dst_ref=target,
        send_sem=sems[0],
        recv_sem=sems[1],
        device_id=device,
        device_id_type=MESH,
    )


def slot_of(delta, size):
    delta = (delta + size // 2 - 1) % size - (size // 2 - 1)
    if delta == 0:
        return size - 1
    if delta == size // 2:
        return size - 2
    return 2 * delta - 1 if delta > 0 else -2 * delta - 2


class GatherRing:
    def __init__(self, size, blocks, sems, parts=2):
        self.size, self.blocks, self.sems, self.parts = size, blocks, sems, parts
        self.place = ring_place(lax.axis_index("dp"), size)
        self.sent = []
        self.live = {}

    def send(self, step):
        size, half = self.size, self.blocks.shape[1] // 2
        piece = half // self.parts
        for part in range(self.parts):
            for way in (0, 1):
                sign = 1 - 2 * way
                rows = pl.ds(way * half + part * piece, piece)
                source = self.blocks.at[slot_of(-sign * step, size), rows]
                target = self.blocks.at[slot_of(-sign * (step + 1), size), rows]
                device = (ring_index(self.place + size + sign, size), lax.axis_index("tensor"))
                copy = push(
                    source,
                    target,
                    (self.sems.at[0, way, step, part], self.sems.at[1, way, step, part]),
                    device,
                )
                if step > 0:
                    self.live[step - 1, part, way].wait_recv()
                copy.start()
                self.live[step, part, way] = copy
                self.sent.append(copy)

    def step(self, step):
        if step + 1 < self.size - 1:
            self.send(step + 1)
        else:
            for part in range(self.parts):
                for way in (0, 1):
                    self.live[step, part, way].wait_recv()

    def finish(self):
        for copy in self.sent:
            copy.wait_send()


def row_loop(total, rows, body):
    def run(index, carry):
        body(pl.ds(pl.multiple_of(index * rows, rows), rows))
        return carry

    lax.fori_loop(0, total // rows, run, 0)


def matmul_nt(left, right):
    return lax.dot_general(left, right, (((1,), (1,)), ((), ())), preferred_element_type=jnp.float32)


def matmul(left, right):
    return lax.dot_general(left, right, (((1,), (0,)), ((), ())), preferred_element_type=jnp.float32)


def rms_rows(values):
    return lax.rsqrt(jnp.mean(values * values, axis=-1, keepdims=True) + EPSILON)


def turn(values, cosine, sine):
    return values * cosine + pltpu.roll(values, values.shape[1] // 2, 1) * sine


def start_layer_body(
    size,
    experts,
    token_ref,
    above_ref,
    route_ref,
    share_ref,
    query_weight_ref,
    key_weight_ref,
    value_weight_ref,
    out_weight_ref,
    gate_up_ref,
    down_ref,
    cosine_ref,
    sine_ref,
    start_ref,
    first_gain_ref,
    second_gain_ref,
    query_gain_ref,
    key_gain_ref,
    middle_ref,
    inputs_out,
    packs_out,
    others_ref,
    mixed_out,
    query_out,
    key_ref,
    value_ref,
    raw_query_out,
    raw_key_ref,
    normed_out,
    query_weight,
    key_weight,
    value_weight,
    out_weight,
    part_ref,
    from_partner,
    from_across,
    joined,
    ring_sems,
    pack_sems,
    side_sems,
    load_sems,
    near_sems,
    far_sems,
    pass_sems,
    store_sems,
    inputs_ref,
    packs_ref,
    mixed_ref,
    query_ref,
    raw_query_ref,
    normed_ref,
):
    f32, bf = jnp.float32, jnp.bfloat16
    dp = lax.axis_index("dp")
    own, partner, across = tensor_peers()
    far_partner = (partner + 2) % 4
    quarter, width = middle_ref.shape
    tokens = token_ref.shape[0]
    head_dim = key_ref.shape[1]
    lead = query_weight_ref.shape[1]
    heads = lead // head_dim
    place = ring_place(dp, size)
    loads = []
    for index, (source, target) in enumerate(
        (
            (query_weight_ref, query_weight),
            (key_weight_ref, key_weight),
            (value_weight_ref, value_weight),
            (out_weight_ref, out_weight),
        )
    ):
        copy = pltpu.make_async_copy(source, target, load_sems.at[index])
        copy.start()
        loads.append(copy)
    mine = pl.ds(pl.multiple_of(own * quarter, quarter), quarter)
    base = own * quarter
    above = pltpu.make_async_copy(
        above_ref.at[mine], packs_ref.at[size - 1, :, pl.ds(0, width)], load_sems.at[4]
    )
    above.start()
    neighbours = [(ring_index(place + 1, size), own), (ring_index(place + size - 1, size), own)]
    greet(neighbours + [(dp, partner), (dp, across)])

    halves = 2
    pieces = []
    for kind in range(3):
        for expert in range(gate_up_ref.shape[0]):
            for half in range(halves):
                pieces.append((kind, expert, half))
    span = gate_up_ref.shape[2] // halves

    def piece_of(number):
        kind, expert, half = pieces[number]
        rows = pl.ds(half * span, span)
        source = gate_up_ref.at[expert, kind, rows] if kind < 2 else down_ref.at[expert, rows]
        return source, (kind, expert, rows)

    near = []
    for kind in range(3):
        for expert in range(gate_up_ref.shape[0]):
            number = len(near)
            source = gate_up_ref.at[expert, kind] if kind < 2 else down_ref.at[expert]
            copy = push(
                source,
                others_ref.at[0, kind, expert],
                (near_sems.at[0, number], near_sems.at[1, number]),
                (dp, partner),
            )
            copy.start()
            near.append(copy)
    far, passed = [], []

    def pump(passing=True):
        number = len(far)
        if number >= 3:
            old = far[number - 3]
            if number - 3 < len(pieces):
                old.wait_recv()
                kind, expert, rows = piece_of(number - 3)[1]
                copy = push(
                    others_ref.at[1, kind, expert, rows],
                    others_ref.at[2, kind, expert, rows],
                    (pass_sems.at[0, number - 3], pass_sems.at[1, number - 3]),
                    (dp, partner),
                )
                copy.start()
                passed.append(copy)
                old.wait_send()
        if number < len(pieces):
            source, (kind, expert, rows) = piece_of(number)
            copy = push(
                source,
                others_ref.at[1, kind, expert, rows],
                (far_sems.at[0, number], far_sems.at[1, number]),
                (dp, across),
            )
            copy.start()
            far.append(copy)
        else:
            far.append(None)

    pump()
    pump()
    pump()

    tail = packs_ref.shape[2] - width
    line = lax.broadcasted_iota(jnp.int32, (tail, quarter), 0)
    name = jnp.where(line < experts, line, line - experts)
    dense = jnp.zeros((tail, quarter), f32)
    for choice in range(route_ref.shape[0]):
        named = route_ref[choice : choice + 1, mine]
        dense = dense + jnp.where(named == name, share_ref[choice : choice + 1, mine], 0.0)
    high = dense.astype(bf).astype(f32)
    both = jnp.where(line < experts, high, jnp.where(line < 2 * experts, dense - high, 0.0))
    packs_ref[size - 1, :, width:] = both.T.astype(bf)
    above.wait()
    packs = GatherRing(size, packs_ref, pack_sems)
    packs.send(0)

    def norm_first(rows):
        hidden = token_ref[rows, :].astype(f32)
        normed_ref[rows, :] = (hidden * rms_rows(hidden) * first_gain_ref[...]).astype(bf)

    row_loop(tokens, 16, norm_first)
    loads[0].wait()
    wide = 4 * LANES

    def project(tile, carry):
        here = pl.ds(pl.multiple_of(tile * wide, wide), wide)
        raw_query_ref[:, here] = matmul(normed_ref[...], query_weight[:, here])
        return carry

    lax.fori_loop(0, lead // wide, project, 0)
    loads[1].wait()
    loads[2].wait()
    raw_key = matmul(normed_ref[...], key_weight[...])
    raw_key_ref[...] = raw_key
    key_ref[...] = turn(
        raw_key * rms_rows(raw_key) * key_gain_ref[...], cosine_ref[...], sine_ref[...]
    ).astype(bf)
    value_ref[...] = matmul(normed_ref[...], value_weight[...]).astype(bf)
    packs.step(0)
    scale = head_dim**-0.5
    block = tokens // 2

    def do_head(head, carry):
        lanes = pl.ds(pl.multiple_of(head * head_dim, head_dim), head_dim)
        for part in (0, 1):
            rows = pl.ds(part * block, block)
            keys = pl.ds(0, (part + 1) * block)
            raw = raw_query_ref[rows, lanes]
            queries = turn(
                raw * rms_rows(raw) * query_gain_ref[...], cosine_ref[rows, :], sine_ref[rows, :]
            ).astype(bf)
            query_ref[rows, lanes] = queries
            scores = matmul_nt(key_ref[keys, :], queries)
            key_at = lax.broadcasted_iota(jnp.int32, scores.shape, 0)
            query_at = lax.broadcasted_iota(jnp.int32, scores.shape, 1) + part * block
            seen = (key_at <= query_at) & (key_at >= start_ref[:, rows])
            exponent = jnp.where(seen, jnp.exp(scores * scale), 0.0)
            soft = (exponent * (1.0 / jnp.sum(exponent, axis=0, keepdims=True))).astype(bf)
            mixed_ref[rows, lanes] = lax.dot_general(
                soft, value_ref[keys, :], (((0,), (0,)), ((), ())), preferred_element_type=f32
            ).astype(bf)
        return carry

    lax.fori_loop(0, heads // 2, do_head, 0)
    packs.step(1)
    pump()
    lax.fori_loop(heads // 2, heads, do_head, 0)
    stores = []

    def leave(*pairs):
        for source, target in pairs:
            copy = pltpu.make_async_copy(source, target, store_sems.at[len(stores)])
            copy.start()
            stores.append(copy)

    leave((raw_query_ref, raw_query_out), (query_ref, query_out))
    leave((normed_ref, normed_out), (mixed_ref, mixed_out))
    packs.step(2)
    loads[3].wait()

    def share(tile, carry):
        here = pl.ds(pl.multiple_of(tile * wide, wide), wide)
        part_ref[:, here] = matmul(mixed_ref[...], out_weight[:, here]).astype(bf)
        return carry

    lax.fori_loop(0, width // wide, share, 0)

    def part_rows(index):
        return pl.ds(pl.multiple_of(index * quarter, quarter), quarter)

    def side(index):
        return (side_sems.at[0, index], side_sems.at[1, index])

    first = push(part_ref.at[part_rows(far_partner)], from_partner.at[1], side(0), (dp, partner))
    second = push(part_ref.at[part_rows(partner)], from_partner.at[0], side(1), (dp, partner))
    first.start()
    second.start()
    packs.step(3)
    first.wait_recv()
    away = across * quarter

    def join(rows):
        there = pl.ds(pl.multiple_of(away + rows.start, 16), rows.size)
        joined[rows, :] = (part_ref[there, :].astype(f32) + from_partner[1, rows, :].astype(f32)).astype(bf)

    row_loop(quarter, 16, join)
    third = push(joined, from_across, side(2), (dp, across))
    third.start()
    pump()
    second.wait_recv()
    third.wait_recv()

    def norm_second(rows):
        there = pl.ds(pl.multiple_of(base + rows.start, 16), rows.size)
        middle = (
            token_ref[there, :].astype(f32)
            + part_ref[there, :].astype(f32)
            + from_partner[0, rows, :].astype(f32)
            + from_across[rows, :].astype(f32)
        )
        middle_ref[rows, :] = middle
        inputs_ref[size - 1, rows, :] = (middle * rms_rows(middle) * second_gain_ref[...]).astype(bf)

    row_loop(quarter, 16, norm_second)
    ring = GatherRing(size, inputs_ref, ring_sems)
    ring.send(0)
    for step in range(size - 1):
        if step + 4 < size - 1:
            packs.step(step + 4)
        if step + 4 == size - 1:
            leave((packs_ref, packs_out))
        pump()
        ring.step(step)
        if step % 2 == 1:
            pump()
    leave((inputs_ref, inputs_out))
    while len(far) < len(pieces) + 3:
        pump()
    packs.finish()
    ring.finish()
    first.wait_send()
    second.wait_send()
    third.wait_send()
    for copy in near + passed + stores:
        copy.wait()


def start_layer(size, experts, *arguments):
    tokens_rows, _, _, _, query_weight, key_weight, value_weight, out_weight, gate_up = arguments[:9]
    bf, f32 = jnp.bfloat16, jnp.float32
    tokens, width = tokens_rows.shape
    quarter = tokens // 4
    lead, head_dim = query_weight.shape[1], key_weight.shape[1]
    columns = width + -(-2 * experts // LANES) * LANES
    local, _, units, _ = gate_up.shape
    vmem = pl.BlockSpec(memory_space=pltpu.VMEM)
    anywhere = pl.BlockSpec(memory_space=pl.ANY)
    dma = pltpu.SemaphoreType.DMA
    return pl.pallas_call(
        functools.partial(start_layer_body, size, experts),
        out_shape=(
            jax.ShapeDtypeStruct((quarter, width), f32),
            jax.ShapeDtypeStruct((size, quarter, width), bf),
            jax.ShapeDtypeStruct((size, quarter, columns), bf),
            jax.ShapeDtypeStruct((3, 3, local, units, width), bf),
            jax.ShapeDtypeStruct((tokens, lead), bf),
            jax.ShapeDtypeStruct((tokens, lead), bf),
            jax.ShapeDtypeStruct((tokens, head_dim), bf),
            jax.ShapeDtypeStruct((tokens, head_dim), bf),
            jax.ShapeDtypeStruct((tokens, lead), f32),
            jax.ShapeDtypeStruct((tokens, head_dim), f32),
            jax.ShapeDtypeStruct((tokens, width), bf),
        ),
        in_specs=[vmem, anywhere, vmem, vmem] + [anywhere] * 6 + [vmem] * 7,
        out_specs=(vmem,) + (anywhere,) * 5 + (vmem, vmem, anywhere, vmem, anywhere),
        scratch_shapes=[
            pltpu.VMEM(query_weight.shape, bf),
            pltpu.VMEM(key_weight.shape, bf),
            pltpu.VMEM(value_weight.shape, bf),
            pltpu.VMEM(out_weight.shape, bf),
            pltpu.VMEM((tokens, width), bf),
            pltpu.VMEM((2, quarter, width), bf),
            pltpu.VMEM((quarter, width), bf),
            pltpu.VMEM((quarter, width), bf),
            dma((2, 2, size - 1, 2)),
            dma((2, 2, size - 1, 2)),
            dma((2, 3)),
            dma((5,)),
            dma((2, 3 * local)),
            dma((2, 6 * local)),
            dma((2, 6 * local)),
            dma((6,)),
            pltpu.VMEM((size, quarter, width), bf),
            pltpu.VMEM((size, quarter, columns), bf),
            pltpu.VMEM((tokens, lead), bf),
            pltpu.VMEM((tokens, lead), bf),
            pltpu.VMEM((tokens, lead), f32),
            pltpu.VMEM((tokens, width), bf),
        ],
        compiler_params=pltpu.CompilerParams(
            collective_id=0, has_side_effects=True, vmem_limit_bytes=VMEM_LIMIT
        ),
        name="start_layer",
    )(*arguments)


def run_experts_body(
    size,
    local_experts,
    experts,
    inputs_hbm,
    packs_hbm,
    gate_up_ref,
    down_ref,
    others_ref,
    member_ref,
    middle_ref,
    gain_ref,
    hidden_out,
    kept_ref,
    given_ref,
    cross_ref,
    landing_ref,
    gmid_ref,
    gmid_all,
    gain_out,
    weights,
    hidden,
    grad_parts,
    mix_parts,
    grad_slots,
    mix_slots,
    turned,
    stage,
    landed,
    totals,
    load_sems,
    grad_sems,
    mix_sems,
    side_sems,
    store_sems,
    give_sems,
    land_sems,
    token_sems,
    inputs_ref,
    packs_ref,
):
    f32, bf = jnp.float32, jnp.bfloat16
    dp = lax.axis_index("dp")
    own, partner, across = tensor_peers()
    width = inputs_ref.shape[1]
    quarter = inputs_ref.shape[0] // size
    pair = 2 * quarter
    half = size // 2
    units = weights.shape[1]
    members = others_ref.shape[0] + 1
    span = units // members
    wide = 512
    place = ring_place(dp, size)

    def token_loads(index):
        rows = pl.ds(pl.multiple_of(index * pair, pair), pair)
        return (
            pltpu.make_async_copy(inputs_hbm.at[rows], inputs_ref.at[rows], token_sems.at[0, index]),
            pltpu.make_async_copy(packs_hbm.at[rows], packs_ref.at[rows], token_sems.at[1, index]),
        )

    for copy in token_loads(0):
        copy.start()
    forward = (ring_index(place + 1, size), own)
    backward = (ring_index(place + size - 1, size), own)
    greet([forward, backward, (dp, partner), (dp, across)])
    part_units = span // local_experts
    loads = []
    for expert in range(local_experts):
        rows = pl.ds(expert * part_units, part_units)
        for kind in range(3):
            source = gate_up_ref.at[expert, kind] if kind < 2 else down_ref.at[expert]
            loads.append((expert * part_units, source, weights.at[kind, rows]))
    for other in range(members - 1):
        for first in range(0, span, LANES):
            at = (other + 1) * span + first
            source = others_ref.at[other, :, pl.ds(first, LANES)]
            loads.append((at, source, weights.at[:, pl.ds(at, LANES)]))
    loads = [
        (at, pltpu.make_async_copy(source, target, load_sems.at[number]))
        for number, (at, source, target) in enumerate(loads)
    ]
    for _, copy in loads:
        copy.start()
    for index in range(1, half):
        for copy in token_loads(index):
            copy.start()

    grad_ring = (grad_parts, grad_slots, grad_sems)
    mix_ring = (mix_parts, mix_slots, mix_sems)

    ring_parts = 2
    way_rows = quarter // 2
    piece_rows = way_rows // ring_parts

    def ring_copy(ring, way, step, part, source):
        device = forward if way == 0 else backward
        _, slots, sems = ring
        rows = pl.ds(part * piece_rows, piece_rows)
        return push(
            source.at[rows],
            slots.at[way, step, rows],
            (sems.at[0, way, step, part], sems.at[1, way, step, part]),
            device,
        )

    def ring_step(ring, step, blocks, first=False):
        parts, slots, _ = ring
        for part in range(ring_parts):
            for way in (0, 1):
                if first:
                    source = parts.at[blocks[way], pl.ds(way * way_rows, way_rows)]
                else:
                    source = slots.at[way, step - 1]
                    ring_copy(ring, way, step - 1, part, source).wait_recv()

                    def add(rows):
                        rows = pl.ds(pl.multiple_of(rows.start + part * piece_rows, 16), rows.size)
                        there = pl.ds(pl.multiple_of(rows.start + way * way_rows, 16), rows.size)
                        slots[way, step - 1, rows, :] = (
                            slots[way, step - 1, rows, :].astype(f32)
                            + parts[blocks[way], there, :].astype(f32)
                        ).astype(bf)

                    row_loop(piece_rows, 16, add)
                ring_copy(ring, way, step, part, source).start()

    def ring_last(ring):
        for part in range(ring_parts):
            for way in (0, 1):
                ring_copy(ring, way, size - 2, part, ring[1].at[way, size - 2]).wait_recv()

    def do_pair(index, carry):
        rows = pl.ds(pl.multiple_of(index * pair, pair), pair)
        for copy in token_loads(index):
            copy.wait()
        tail = packs_ref[rows, width:].astype(f32)
        lane = lax.broadcasted_iota(jnp.int32, tail.shape, 1)
        shares = []
        for expert in range(local_experts):
            name = dp * local_experts + expert
            picked = (lane == name) | (lane == experts + name)
            shares.append(jnp.sum(jnp.where(picked, tail, 0.0), axis=1, keepdims=True))

        def do_units(tile, carry):
            here = pl.ds(pl.multiple_of(tile * wide, wide), wide)

            for number in range(units // wide):

                @pl.when((index == 0) & (tile == number))
                def _():
                    for at, copy in loads:
                        if at // wide == number:
                            copy.wait()

            scale = shares[0] * member_ref[0:1, here]
            for expert in range(1, local_experts):
                scale = scale + shares[expert] * member_ref[expert : expert + 1, here]
            tokens = inputs_ref[rows, :]
            gate = matmul_nt(tokens, weights[0, here, :])
            upward = matmul_nt(tokens, weights[1, here, :])
            grads = scale * matmul_nt(packs_ref[rows, :width], weights[2, here, :])
            share = jax.nn.sigmoid(gate)
            silu = gate * share
            hidden[0, rows, here] = (grads * upward * share * (1.0 + gate * (1.0 - share))).astype(bf)
            hidden[1, rows, here] = (grads * silu).astype(bf)
            hidden[2, rows, here] = (scale * silu * upward).astype(bf)
            return carry

        lax.fori_loop(0, units // wide, do_units, 0)

        def do_columns(tile, carry):
            here = pl.ds(pl.multiple_of(tile * wide, wide), wide)
            sums = matmul(hidden[0, rows, :], weights[0, :, here]) + matmul(
                hidden[1, rows, :], weights[1, :, here]
            )
            low = sums.astype(bf)
            grad_parts[2 * index, :, here] = low[:quarter]
            grad_parts[2 * index + 1, :, here] = low[quarter:]
            return carry

        def do_mix(tile, carry):
            here = pl.ds(pl.multiple_of(tile * wide, wide), wide)
            low = matmul(hidden[2, rows, :], weights[2, :, here]).astype(bf)
            mix_parts[2 * index, :, here] = low[:quarter]
            mix_parts[2 * index + 1, :, here] = low[quarter:]
            return carry

        lax.fori_loop(0, width // wide, do_columns, 0)

        def go_on(ring):
            @pl.when(index == 0)
            def _():
                ring_step(ring, 0, (0, 1), first=True)

            @pl.when(index > 0)
            def _():
                ring_step(ring, index, (2 * index, 2 * index + 1 - index // (half - 1)))

        go_on(grad_ring)
        lax.fori_loop(0, width // wide, do_mix, 0)
        go_on(mix_ring)
        return carry

    lax.fori_loop(0, half, do_pair, 0)
    group_units = (3, 1, 2, 0)
    targets = (landing_ref, given_ref, cross_ref, kept_ref)

    def tile_copies(group, kind, slot):
        copies = []
        for expert in range(local_experts):
            at = expert + 2 * local_experts if isinstance(kind, int) else 2 * expert + kind
            source = stage.at[slot, pl.ds(expert * part_units, part_units)]
            target = targets[group].at[at]
            if group < 2:
                sems = (give_sems.at[0, group, at], give_sems.at[1, group, at])
                copies.append(push(source, target, sems, (dp, partner)))
            else:
                copies.append(pltpu.make_async_copy(source, target, store_sems.at[group - 2, at]))
        return copies

    def tile_left(group, kind, slot):
        for copy in tile_copies(group, kind, slot):
            if group < 2:
                copy.wait_send()
            else:
                copy.wait()

    def land(kind):
        copies = []
        for expert in range(local_experts):
            at = expert + 2 * local_experts if isinstance(kind, int) else 2 * expert + kind
            rows = pl.ds(expert * part_units, part_units)
            copies.append(
                pltpu.make_async_copy(landing_ref.at[at], landed.at[rows], land_sems.at[expert])
            )
        return copies

    def tile(group, kind, source, before):
        number = 3 * group + kind
        slot = number % 2
        if before is not None:
            before(slot)
        if group == 2:
            for copy in tile_copies(0, kind, slot):
                copy.wait_recv()
            for copy in land(kind):
                copy.start()
        rows = pl.ds(group_units[group] * span, span)
        for chunk in range(half):
            some = pl.ds(chunk * pair, pair)
            turned[:, some] = hidden[kind, some, rows].T
        if group == 2:
            for copy in land(kind):
                copy.wait()

        def do_columns(tile, carry):
            here = pl.ds(pl.multiple_of(tile * wide, wide), wide)
            sums = matmul(turned[...], source[:, here])
            if group == 2:
                sums = sums + landed[:, here].astype(f32)
            stage[slot, :, here] = sums.astype(bf)
            return carry

        lax.fori_loop(0, width // wide, do_columns, 0)
        for copy in tile_copies(group, kind, slot):
            copy.start()

    def token_tiles(group):
        def run(kind, carry):
            if group == 0:
                before = None
            else:
                def before(slot):
                    @pl.when(kind == 0)
                    def _():
                        tile_left(group - 1, kind + 1, slot)

                    @pl.when(kind == 1)
                    def _():
                        tile_left(group - 1, 2, slot)

            tile(group, kind, inputs_ref, before)
            return carry

        lax.fori_loop(0, 2, run, 0)

    def grad_tile(group):
        def before(slot):
            tile_left(group, jnp.int32(0), slot)

        tile(group, 2, packs_ref, before)

    def final_sum():
        totals[...] = jnp.zeros_like(totals)
        ring_last(grad_ring)
        base = own * quarter

        def finish(way, inner):
            rows = pl.ds(pl.multiple_of(inner.start + way * way_rows, 16), inner.size)
            sums = grad_slots[way, size - 2, inner, :].astype(f32) + grad_parts[
                size - 1, rows, :
            ].astype(f32)
            middle = middle_ref[rows, :]
            inverse = lax.rsqrt(jnp.mean(middle * middle, axis=-1, keepdims=True) + EPSILON)
            hat = middle * inverse
            product = sums * hat
            totals[...] += product[:8] + product[8:]
            scaled = sums * gain_ref[...]
            back = inverse * (scaled - hat * jnp.mean(scaled * hat, axis=-1, keepdims=True))
            above = packs_ref[
                pl.ds(pl.multiple_of((size - 1) * quarter + rows.start, 16), rows.size), :width
            ]
            grad = above.astype(f32) + back
            gmid_ref[rows, :] = grad
            gmid_all[pl.ds(pl.multiple_of(base + rows.start, 16), rows.size), :] = grad.astype(bf)

        for way in (0, 1):
            row_loop(way_rows, 16, functools.partial(finish, way))
        gain_out[...] = jnp.sum(totals[...], axis=0, keepdims=True)

    def rows_of(index):
        return pl.ds(pl.multiple_of(index * quarter, quarter), quarter)

    def spread(index, whose, device):
        ref = gmid_all.at[rows_of(whose)]
        return push(ref, ref, (side_sems.at[0, index], side_sems.at[1, index]), device)

    def first_spread():
        spread(0, own, (dp, across)).start()
        spread(1, own, (dp, partner)).start()

    def second_spread():
        spread(0, own, (dp, across)).wait_recv()
        spread(2, across, (dp, partner)).start()

    def final_mix():
        ring_last(mix_ring)

        def finish(way, inner):
            rows = pl.ds(pl.multiple_of(inner.start + way * way_rows, 16), inner.size)
            hidden_out[rows, :] = (
                middle_ref[rows, :]
                + mix_slots[way, size - 2, inner, :].astype(f32)
                + mix_parts[size - 1, rows, :].astype(f32)
            ).astype(bf)

        for way in (0, 1):
            row_loop(way_rows, 16, functools.partial(finish, way))

    def closing():
        final_sum()
        first_spread()

    grad_events, mix_events = [], []
    for step in range(half, size - 1):
        delta = -(1 + step)
        blocks = (slot_of(delta, size), slot_of(-delta, size))
        grad_events.append(functools.partial(ring_step, grad_ring, step, blocks))
        mix_events.append(functools.partial(ring_step, mix_ring, step, blocks))
    events = grad_events[:-1]
    events += [grad_events[-1], mix_events[0], closing] + mix_events[1:2] + [second_spread]
    events += mix_events[2:] + [final_mix]
    work = []
    for group in range(4):
        work.append(functools.partial(token_tiles, group))
        work.append(functools.partial(grad_tile, group))
    done = 0
    for number, piece in enumerate(work):
        piece()
        upto = -(-(number + 1) * len(events) // len(work))
        while done < upto:
            events[done]()
            done += 1
    tile_left(3, jnp.int32(1), 0)
    tile_left(3, 2, 1)
    for kind in (jnp.int32(0), jnp.int32(1), 2):
        for copy in tile_copies(1, kind, 0):
            copy.wait_recv()
    spread(1, own, (dp, partner)).wait_recv()
    spread(2, across, (dp, partner)).wait_recv()
    for index, device in ((0, across), (1, partner), (2, partner)):
        spread(index, own, (dp, device)).wait_send()
    for ring in (grad_ring, mix_ring):
        for way in (0, 1):
            for step in range(size - 1):
                for part in range(ring_parts):
                    ring_copy(ring, way, step, part, ring[1].at[way, step]).wait_send()


def run_experts(size, inputs, packs, gate_up, down, others, middle, gain, experts):
    bf, f32 = jnp.bfloat16, jnp.float32
    local_experts, _, part_units, width = gate_up.shape
    others = others.reshape(3, 3, local_experts * part_units, width)
    members, span = 4, local_experts * part_units
    rows = inputs.shape[0]
    quarter = rows // size
    units = members * span
    expert_of = (jnp.arange(units, dtype=jnp.int32) // (span // local_experts)) % local_experts
    member = (expert_of[None, :] == jnp.arange(local_experts, dtype=jnp.int32)[:, None]).astype(f32)
    vmem = pl.BlockSpec(memory_space=pltpu.VMEM)
    anywhere = pl.BlockSpec(memory_space=pl.ANY)
    dma = pltpu.SemaphoreType.DMA
    return pl.pallas_call(
        functools.partial(run_experts_body, size, local_experts, experts),
        out_shape=(
            jax.ShapeDtypeStruct((quarter, width), bf),
            jax.ShapeDtypeStruct((3 * local_experts, part_units, width), bf),
            jax.ShapeDtypeStruct((3 * local_experts, part_units, width), bf),
            jax.ShapeDtypeStruct((3 * local_experts, part_units, width), bf),
            jax.ShapeDtypeStruct((3 * local_experts, part_units, width), bf),
            jax.ShapeDtypeStruct((quarter, width), f32),
            jax.ShapeDtypeStruct((members * quarter, width), bf),
            jax.ShapeDtypeStruct((1, width), f32),
        ),
        in_specs=[anywhere] * 5 + [vmem] * 3,
        out_specs=(vmem,) + (anywhere,) * 4 + (vmem,) * 3,
        scratch_shapes=[
            pltpu.VMEM((3, units, width), bf),
            pltpu.VMEM((3, rows, units), bf),
            pltpu.VMEM((size, quarter, width), bf),
            pltpu.VMEM((size, quarter, width), bf),
            pltpu.VMEM((2, size - 1, quarter // 2, width), bf),
            pltpu.VMEM((2, size - 1, quarter // 2, width), bf),
            pltpu.VMEM((span, rows), bf),
            pltpu.VMEM((2, span, width), bf),
            pltpu.VMEM((span, width), bf),
            pltpu.VMEM((8, width), f32),
            dma((3 * local_experts + 3 * span // LANES,)),
            dma((2, 2, size - 1, 2)),
            dma((2, 2, size - 1, 2)),
            dma((2, 3)),
            dma((2, 3 * local_experts)),
            dma((2, 2, 3 * local_experts)),
            dma((local_experts,)),
            dma((2, size // 2)),
            pltpu.VMEM(inputs.shape, bf),
            pltpu.VMEM(packs.shape, bf),
        ],
        compiler_params=pltpu.CompilerParams(
            collective_id=2, has_side_effects=True, vmem_limit_bytes=VMEM_LIMIT
        ),
        name="run_experts",
    )(inputs, packs, gate_up, down, others, member, middle, gain.reshape(1, -1))


def back_through_head(grads, raw, gain, cosine, sine):
    hat_grads = grads * cosine - pltpu.roll(grads, grads.shape[1] // 2, 1) * sine
    inverse = lax.rsqrt(jnp.mean(raw * raw, axis=-1, keepdims=True) + EPSILON)
    hat = raw * inverse
    terms = hat_grads * hat
    scaled = hat_grads * gain
    back = inverse * (scaled - hat * jnp.mean(scaled * hat, axis=-1, keepdims=True))
    return back.astype(jnp.bfloat16), terms


def finish_layer_body(
    size,
    gmid_low_hbm,
    out_weight_hbm,
    mixed_hbm,
    query_hbm,
    key_hbm,
    value_hbm,
    raw_query_hbm,
    raw_key_hbm,
    normed_hbm,
    query_weight_hbm,
    key_weight_hbm,
    value_weight_hbm,
    cosine_ref,
    sine_ref,
    start_ref,
    query_gain_ref,
    key_gain_ref,
    middle_ref,
    token_hbm,
    hidden_ref,
    cross_ref,
    gain_ref,
    gains_ref,
    hidden_all,
    crossed_ref,
    grad_all,
    query_out,
    key_out,
    value_out,
    outer_out,
    first_out,
    second_out,
    query_gain_out,
    key_gain_out,
    qkv_ref,
    out_ref,
    slots_a,
    slots_b,
    grad_mixed,
    grad_heads,
    key_sums,
    value_sums,
    turned,
    partial,
    from_partner,
    from_across,
    joined,
    totals,
    head_totals,
    pair_gains,
    ring_gains,
    sems_a,
    sems_b,
    ring_sems,
    side_sems,
    load_sems,
    store_sems,
    gather_a,
    gather_b,
    token_ref,
    gmid_low_ref,
    out_weight_ref,
    mixed_ref,
    query_ref,
    key_ref,
    value_ref,
    raw_query_ref,
    raw_key_ref,
    normed_ref,
    query_weight_ref,
    key_weight_ref,
    value_weight_ref,
):
    f32, bf = jnp.float32, jnp.bfloat16
    dp = lax.axis_index("dp")
    own, partner, across = tensor_peers()
    far_partner = (partner + 2) % 4
    quarter, width = token_ref.shape
    tokens = normed_ref.shape[0]
    head_dim = key_ref.shape[1]
    lead = query_ref.shape[1]
    heads = lead // head_dim
    scale = head_dim**-0.5
    place = ring_place(dp, size)
    forward = (ring_index(place + 1, size), own)
    backward = (ring_index(place + size - 1, size), own)
    ways = ((forward, 1), (backward, -1))
    mine = pl.ds(pl.multiple_of(own * quarter, quarter), quarter)
    home = own * quarter
    loads = {}
    for source, target in (
        (gmid_low_hbm, gmid_low_ref),
        (mixed_hbm, mixed_ref),
        (out_weight_hbm, out_weight_ref),
        (query_hbm, query_ref),
        (key_hbm, key_ref),
        (value_hbm, value_ref),
        (raw_query_hbm, raw_query_ref),
        (raw_key_hbm, raw_key_ref),
        (normed_hbm, normed_ref),
        (query_weight_hbm, query_weight_ref),
        (key_weight_hbm, key_weight_ref),
        (value_weight_hbm, value_weight_ref),
        (token_hbm.at[mine], token_ref),
    ):
        copy = pltpu.make_async_copy(source, target, load_sems.at[len(loads)])
        copy.start()
        loads[id(target)] = copy

    def loaded(*targets):
        for target in targets:
            loads[id(target)].wait()

    greet([forward, backward, (dp, partner), (dp, across)])
    waits = []

    def start(copy):
        copy.start()
        waits.append(copy)
        return copy

    sets = (
        (qkv_ref, slots_a, gather_a, sems_a),
        (out_ref, slots_b, gather_b, sems_b),
    )

    def wrap(value):
        return (value + 2 * size) % size

    live = {}

    ring_parts = 2 if lead // size % 64 == 0 else 1
    stores = []

    def ring_rows(ref):
        rows = ref.shape[0] // size
        return rows, rows // 2, rows // 2 // ring_parts

    def add_own(which, way, step, part):
        ref, slots, blocks, _ = sets[which]
        live[which, way, step, part].wait_recv()
        rows, half, count = ring_rows(ref)
        base = wrap(place - ways[way][1] * (2 + step)) * rows + way * half

        def add(inner):
            inner = pl.ds(pl.multiple_of(inner.start + part * count, 16), inner.size)
            there = pl.ds(pl.multiple_of(base + inner.start, 16), inner.size)
            sums = (slots[way, step, inner, :].astype(f32) + ref[there, :].astype(f32)).astype(bf)
            if step == size - 2:
                final = pl.ds(pl.multiple_of(inner.start + way * half, 16), inner.size)
                blocks[place, final, :] = sums
            else:
                slots[way, step, inner, :] = sums

        row_loop(count, 16, add)

    def keep_block(which, way, block, part):
        ref, _, blocks, _ = sets[which]
        rows, half, count = ring_rows(ref)
        inner = pl.ds(way * half + part * count, count)
        there = pl.ds(pl.multiple_of(block * rows + way * half + part * count, 16), count)
        if which == 1:
            targets = [(outer_out, 0, width)]
        else:
            targets = [
                (query_out, 0, lead),
                (key_out, lead, head_dim),
                (value_out, lead + head_dim, head_dim),
            ]
        for target, first, columns in targets:
            source = blocks.at[block, inner, pl.ds(first, columns)]
            copy = pltpu.make_async_copy(source, target.at[there], store_sems.at[len(stores)])
            copy.start()
            stores.append(copy)

    def ring_event(which, step):
        ref, slots, blocks, sems = sets[which]
        rows, half, count = ring_rows(ref)
        for part in range(ring_parts):
            inner = pl.ds(part * count, count)
            for way, (device, sign) in enumerate(ways):
                if step == 0:
                    at = wrap(place - sign) * rows + way * half + part * count
                    source = ref.at[pl.ds(pl.multiple_of(at, 16), count)]
                elif step < size:
                    add_own(which, way, step - 1, part)
                    source = slots.at[way, step - 1, inner] if step < size - 1 else None
                else:
                    live[which, way, step - 1, part].wait_recv()
                block = wrap(place - sign * (step - size + 1))
                if step >= size - 1:
                    keep_block(which, way, block, part)
                if step >= 2 * size - 2:
                    continue
                if step >= size - 1:
                    source = blocks.at[block, pl.ds(way * half + part * count, count)]
                    target = source
                else:
                    target = slots.at[way, step, inner]
                sem = (sems.at[0, way, step, part], sems.at[1, way, step, part])
                live[which, way, step, part] = start(push(source, target, sem, device))

    def part_rows(index):
        return pl.ds(pl.multiple_of(index * quarter, quarter), quarter)

    def side(index):
        return (side_sems.at[0, index], side_sems.at[1, index])

    step_rows = 2 * LANES
    wide = 4 * LANES

    def out_rows(index, carry):
        rows = pl.ds(pl.multiple_of(index * step_rows, step_rows), step_rows)
        turned[...] = mixed_ref[:, rows].T

        def columns(tile, carry):
            here = pl.ds(pl.multiple_of(tile * wide, wide), wide)
            out_ref[rows, here] = matmul(turned[...], gmid_low_ref[:, here]).astype(bf)
            return carry

        return lax.fori_loop(0, width // wide, columns, carry)

    loaded(gmid_low_ref, mixed_ref)
    lax.fori_loop(0, lead // step_rows, out_rows, 0)
    ring_event(1, 0)

    def keep(rows):
        hidden_all[pl.ds(pl.multiple_of(home + rows.start, 16), rows.size), :] = hidden_ref[rows, :]

    row_loop(quarter, 16, keep)
    shown = [start(push(hidden_ref, hidden_all.at[mine], side(9), (dp, across)))]
    shown.append(start(push(hidden_ref, hidden_all.at[mine], side(10), (dp, partner))))

    def mixed_columns(tile, carry):
        here = pl.ds(pl.multiple_of(tile * wide, wide), wide)
        grad_mixed[:, here] = matmul_nt(gmid_low_ref[...], out_weight_ref[here, :]).astype(bf)
        return carry

    loaded(out_weight_ref)
    lax.fori_loop(0, lead // wide, mixed_columns, 0)
    loaded(query_ref, key_ref, value_ref, raw_query_ref, raw_key_ref)
    key_sums[...] = jnp.zeros_like(key_sums)
    value_sums[...] = jnp.zeros_like(value_sums)
    head_totals[...] = jnp.zeros_like(head_totals)
    block = tokens // 2

    def do_head(head, carry):
        lanes = pl.ds(pl.multiple_of(head * head_dim, head_dim), head_dim)
        for part in (0, 1):
            rows = pl.ds(part * block, block)
            count = (part + 1) * block
            keys = pl.ds(0, count)
            queries = query_ref[rows, lanes]
            outer = grad_mixed[rows, lanes]
            scores = matmul_nt(key_ref[keys, :], queries)
            key_at = lax.broadcasted_iota(jnp.int32, scores.shape, 0)
            query_at = lax.broadcasted_iota(jnp.int32, scores.shape, 1) + part * block
            seen = (key_at <= query_at) & (key_at >= start_ref[:, rows])
            exponent = jnp.where(seen, jnp.exp(scores * scale), 0.0)
            soft = exponent * (1.0 / jnp.sum(exponent, axis=0, keepdims=True))
            grad_soft = matmul_nt(value_ref[keys, :], outer)
            inner = jnp.sum(soft * grad_soft, axis=0, keepdims=True)
            grad_scores = (soft * (grad_soft - inner)).astype(bf)
            value_sums[keys, :] += matmul(soft.astype(bf), outer)
            key_sums[keys, :] += matmul(grad_scores, queries)
            grad_query = scale * lax.dot_general(
                grad_scores, key_ref[keys, :], (((0,), (0,)), ((), ())), preferred_element_type=f32
            )
            low, terms = back_through_head(
                grad_query, raw_query_ref[rows, lanes], query_gain_ref[...], cosine_ref[rows, :], sine_ref[rows, :]
            )
            grad_heads[rows, lanes] = low
            head_totals[0] += jnp.sum(terms.reshape(-1, 8, head_dim), axis=0)
        return carry

    lax.fori_loop(0, heads // 2, do_head, 0)
    ring_event(1, 1)
    lax.fori_loop(heads // 2, heads, do_head, 0)
    ring_event(1, 2)
    low, terms = back_through_head(
        scale * key_sums[...], raw_key_ref[...], key_gain_ref[...], cosine_ref[...], sine_ref[...]
    )
    grad_heads[:, pl.ds(lead, head_dim)] = low
    head_totals[1] += jnp.sum(terms.reshape(-1, 8, head_dim), axis=0)
    grad_heads[:, pl.ds(lead + head_dim, head_dim)] = value_sums[...].astype(bf)

    def in_rows(index, carry):
        rows = pl.ds(pl.multiple_of(index * step_rows, step_rows), step_rows)
        turned[...] = normed_ref[:, rows].T
        qkv_ref[rows, :] = matmul(turned[...], grad_heads[...]).astype(bf)
        return carry

    loaded(normed_ref)
    lax.fori_loop(0, width // step_rows, in_rows, 0)
    ring_event(1, 3)
    ring_event(0, 0)

    def token_columns(tile, carry):
        here = pl.ds(pl.multiple_of(tile * wide, wide), wide)
        sums = matmul_nt(grad_heads[:, :lead], query_weight_ref[here, :])
        sums = sums + matmul_nt(grad_heads[:, lead : lead + head_dim], key_weight_ref[here, :])
        sums = sums + matmul_nt(grad_heads[:, lead + head_dim :], value_weight_ref[here, :])
        partial[:, here] = sums.astype(bf)
        return carry

    loaded(query_weight_ref, key_weight_ref, value_weight_ref)
    lax.fori_loop(0, width // wide, token_columns, 0)
    first = start(push(partial.at[part_rows(far_partner)], from_partner.at[1], side(0), (dp, partner)))
    second = start(push(partial.at[part_rows(partner)], from_partner.at[0], side(1), (dp, partner)))
    ring_event(1, 4)
    first.wait_recv()
    away = across * quarter

    def join(rows):
        there = pl.ds(pl.multiple_of(away + rows.start, 16), rows.size)
        joined[rows, :] = (partial[there, :].astype(f32) + from_partner[1, rows, :].astype(f32)).astype(bf)

    row_loop(quarter, 16, join)
    third = start(push(joined, from_across, side(2), (dp, across)))
    ring_event(0, 1)
    ring_event(1, 5)
    second.wait_recv()
    third.wait_recv()
    totals[...] = jnp.zeros_like(totals)

    def finish(rows):
        there = pl.ds(pl.multiple_of(home + rows.start, 16), rows.size)
        grads = (
            partial[there, :].astype(f32)
            + from_partner[0, rows, :].astype(f32)
            + from_across[rows, :].astype(f32)
        )
        hidden = token_ref[rows, :].astype(f32)
        inverse = lax.rsqrt(jnp.mean(hidden * hidden, axis=-1, keepdims=True) + EPSILON)
        hat = hidden * inverse
        product = grads * hat
        totals[...] += product[:8] + product[8:]
        scaled = grads * gain_ref[...]
        back = inverse * (scaled - hat * jnp.mean(scaled * hat, axis=-1, keepdims=True))
        grad_all[there, :] = (middle_ref[rows, :] + back).astype(bf)

    loaded(token_ref)
    row_loop(quarter, 16, finish)
    spread = [start(push(grad_all.at[mine], grad_all.at[mine], side(3), (dp, across)))]
    spread.append(start(push(grad_all.at[mine], grad_all.at[mine], side(4), (dp, partner))))
    pair_gains[0, :, :width] = jnp.sum(totals[...], axis=0, keepdims=True)
    pair_gains[0, :, width : 2 * width] = gains_ref[...]
    pair_gains[0, :, 2 * width : 2 * width + head_dim] = jnp.sum(head_totals[0], axis=0, keepdims=True)
    pair_gains[0, :, 2 * width + head_dim :] = jnp.sum(head_totals[1], axis=0, keepdims=True)
    swap = start(push(pair_gains.at[0], pair_gains.at[1], side(5), (dp, partner)))
    ring_event(0, 2)
    ring_event(1, 6)
    far = part_rows(across)
    shown[0].wait_recv()
    shown.append(start(push(hidden_all.at[far], hidden_all.at[far], side(11), (dp, partner))))
    spread[0].wait_recv()
    spread.append(start(push(grad_all.at[far], grad_all.at[far], side(6), (dp, partner))))
    swap.wait_recv()
    pair_gains[2] = pair_gains[0] + pair_gains[1]
    swap = start(push(pair_gains.at[2], pair_gains.at[3], side(7), (dp, across)))
    ring_event(0, 3)
    ring_event(1, 7)
    swap.wait_recv()
    crossing = start(push(cross_ref, crossed_ref, side(8), (dp, across)))
    ring_gains[place] = pair_gains[2] + pair_gains[3]
    small = None
    for step in range(4, 2 * size - 1):
        ring_event(0, step)
        if step + 4 < 2 * size - 1:
            ring_event(1, step + 4)
        if step - 4 < size - 1:
            if small is not None:
                small.wait_recv()
            ref = ring_gains.at[wrap(place - step + 4)]
            sem = (ring_sems.at[0, step - 4], ring_sems.at[1, step - 4])
            small = start(push(ref, ref, sem, forward))
    small.wait_recv()
    gains = jnp.sum(ring_gains[...], axis=0)
    first_out[...] = gains[:, :width]
    second_out[...] = gains[:, width : 2 * width]
    query_gain_out[...] = gains[:, 2 * width : 2 * width + head_dim]
    key_gain_out[...] = gains[:, 2 * width + head_dim :]
    for copy in (spread[1], spread[2], shown[1], shown[2], crossing):
        copy.wait_recv()
    for copy in waits:
        copy.wait_send()
    for copy in stores:
        copy.wait()


def finish_layer(size, *arguments):
    bf, f32 = jnp.bfloat16, jnp.float32
    (
        _, out_weight, mixed, query, key, _, _, _, normed, query_weight, _, _, _, _, _, _, _, _, token_rows, _,
        cross, _, _,
    ) = arguments
    tokens, width = token_rows.shape
    quarter = tokens // 4
    lead, head_dim = query.shape[1], key.shape[1]
    vmem = pl.BlockSpec(memory_space=pltpu.VMEM)
    anywhere = pl.BlockSpec(memory_space=pl.ANY)
    dma = pltpu.SemaphoreType.DMA
    columns = lead + 2 * head_dim
    rows_a, rows_b = width // size, lead // size
    count = 2 * width + 2 * head_dim
    return pl.pallas_call(
        functools.partial(finish_layer_body, size),
        out_shape=(
            jax.ShapeDtypeStruct((tokens, width), bf),
            jax.ShapeDtypeStruct(cross.shape, bf),
            jax.ShapeDtypeStruct((tokens, width), bf),
            jax.ShapeDtypeStruct((width, lead), bf),
            jax.ShapeDtypeStruct((width, head_dim), bf),
            jax.ShapeDtypeStruct((width, head_dim), bf),
            jax.ShapeDtypeStruct((lead, width), bf),
            jax.ShapeDtypeStruct((1, width), f32),
            jax.ShapeDtypeStruct((1, width), f32),
            jax.ShapeDtypeStruct((1, head_dim), f32),
            jax.ShapeDtypeStruct((1, head_dim), f32),
        ),
        in_specs=[anywhere] * 12 + [vmem] * 6 + [anywhere, vmem, anywhere, vmem, vmem],
        out_specs=(vmem, anywhere, vmem) + (anywhere,) * 4 + (vmem,) * 4,
        scratch_shapes=[
            pltpu.VMEM((width, columns), bf),
            pltpu.VMEM((lead, width), bf),
            pltpu.VMEM((2, size - 1, rows_a // 2, columns), bf),
            pltpu.VMEM((2, size - 1, rows_b // 2, width), bf),
            pltpu.VMEM((tokens, lead), bf),
            pltpu.VMEM((tokens, columns), bf),
            pltpu.VMEM((tokens, head_dim), f32),
            pltpu.VMEM((tokens, head_dim), f32),
            pltpu.VMEM((2 * LANES, tokens), bf),
            pltpu.VMEM((tokens, width), bf),
            pltpu.VMEM((2, quarter, width), bf),
            pltpu.VMEM((quarter, width), bf),
            pltpu.VMEM((quarter, width), bf),
            pltpu.VMEM((8, width), f32),
            pltpu.VMEM((2, 8, head_dim), f32),
            pltpu.VMEM((4, 1, count), f32),
            pltpu.VMEM((size, 1, count), f32),
            dma((2, 2, 2 * size - 2, 2)),
            dma((2, 2, 2 * size - 2, 2)),
            dma((2, size - 1)),
            dma((2, 12)),
            dma((13,)),
            dma((16 * size,)),
            pltpu.VMEM((size, rows_a, columns), bf),
            pltpu.VMEM((size, rows_b, width), bf),
            pltpu.VMEM((quarter, width), bf),
        ]
        + [pltpu.VMEM(argument.shape, argument.dtype) for argument in arguments[:12]],
        compiler_params=pltpu.CompilerParams(
            collective_id=1, has_side_effects=True, vmem_limit_bytes=VMEM_LIMIT
        ),
        name="finish_layer",
    )(*arguments)


def widen_body(refs):
    f32 = jnp.float32
    for source, target in zip(refs[:4], refs[12:16]):
        target[...] = source[...].astype(f32)
    for first, target in ((4, refs[16]), (7, refs[17])):
        sums = refs[first][...].astype(f32) + refs[first + 1][...].astype(f32)
        target[...] = sums + refs[first + 2][...].astype(f32)
    refs[18][...] = refs[10][...]
    refs[19][...] = refs[11][...]


def widen(query, key, value, outer, shares, split, hidden, grads):
    f32 = jnp.float32
    steps = 8
    width = outer.shape[1]
    shares = [share.reshape(-1, width) for share in shares]
    rest = shares[0].shape[0] - split

    def rows(count, columns, first=0):
        block = count // steps
        assert count % steps == 0 and block % 16 == 0 and first % block == 0
        return pl.BlockSpec((block, columns), lambda step: (step + first // block, 0))

    plain = [rows(*array.shape) for array in (query, key, value, outer)]
    pair = [rows(*array.shape) for array in (hidden, grads)]
    first, second = rows(split, width), rows(rest, width)
    return pl.pallas_call(
        lambda *refs: widen_body(refs),
        grid=(steps,),
        out_shape=[jax.ShapeDtypeStruct(a.shape, f32) for a in (query, key, value, outer)]
        + [jax.ShapeDtypeStruct((split, width), f32), jax.ShapeDtypeStruct((rest, width), f32)]
        + [jax.ShapeDtypeStruct(a.shape, a.dtype) for a in (hidden, grads)],
        in_specs=plain + [first] * 3 + [rows(rest, width, split)] * 3 + pair,
        out_specs=plain + [first, second] + pair,
        compiler_params=pltpu.CompilerParams(vmem_limit_bytes=VMEM_LIMIT),
        name="widen",
    )(query, key, value, outer, *shares, *shares, hidden, grads)


def large_experts(size, inputs, packs, gate_up, down, others, middle, gain, experts):
    f32, bf = jnp.float32, jnp.bfloat16
    model_width = inputs.shape[1]
    own_weights = jnp.stack([gate_up[:, 0], gate_up[:, 1], down])
    all_weights = jnp.concatenate([own_weights[None], others])
    members = all_weights.shape[0]
    order = jnp.arange(members, dtype=jnp.int32) ^ lax.axis_index("tensor")
    all_weights = all_weights.reshape(members, 3, -1, model_width)[order]
    units = all_weights.shape[2]
    local_experts = experts // size
    indices = jnp.arange(size, dtype=jnp.int32)
    half = size // 2
    delta = (ring_place(indices, size) - ring_place(lax.axis_index("dp"), size)) % size
    ahead = jnp.where(delta == half, size - 2, jnp.where(delta == 0, size - 1, 2 * delta - 1))
    slots = jnp.where(delta > half, 2 * (size - delta) - 2, ahead)
    quarter = middle.shape[0]
    out_rows = packs[-quarter:, :model_width]
    inputs = inputs.reshape(size, quarter, -1)[slots].reshape(-1, model_width)
    packs = packs.reshape(size, quarter, -1)[slots].reshape(inputs.shape[0], -1)
    grads_all = packs[:, :model_width]
    shares = packs[:, model_width : model_width + 2 * experts].astype(f32)
    shares = shares[:, :experts] + shares[:, experts:]
    shares = lax.dynamic_slice_in_dim(
        shares, lax.axis_index("dp") * local_experts, local_experts, 1
    )
    weight_cols = jnp.broadcast_to(
        shares[:, None, :, None],
        (shares.shape[0], members, local_experts, units // local_experts),
    ).reshape(-1, members, units)

    def project(left, which):
        return jnp.einsum("td,rud->tru", left, all_weights[:, which], preferred_element_type=f32)

    gate_act = project(inputs, 0)
    upward = project(inputs, 1)
    sigmoid_gate = jax.nn.sigmoid(gate_act)
    active = gate_act * sigmoid_gate * upward
    weighted_low = (weight_cols * active).astype(bf)
    mixture_part = jnp.einsum(
        "tru,rud->td", weighted_low, all_weights[:, 2], preferred_element_type=f32
    ).astype(bf)
    grad_active = weight_cols * project(grads_all, 2)
    grad_gate = (
        grad_active * upward * sigmoid_gate * (1.0 + gate_act * (1.0 - sigmoid_gate))
    ).astype(bf)
    grad_up = (grad_active * gate_act * sigmoid_gate).astype(bf)
    grad_normed_part = jnp.einsum(
        "tru,rud->td", grad_gate, all_weights[:, 0], preferred_element_type=f32
    ) + jnp.einsum("tru,rud->td", grad_up, all_weights[:, 1], preferred_element_type=f32)
    grad_normed_two = lax.psum_scatter(grad_normed_part.astype(bf), "dp", tiled=True).astype(f32)
    weight_grads = jnp.stack(
        [
            jnp.einsum("tru,td->rud", grad_gate, inputs, preferred_element_type=f32).astype(bf),
            jnp.einsum("tru,td->rud", grad_up, inputs, preferred_element_type=f32).astype(bf),
            jnp.einsum("tru,td->rud", weighted_low, grads_all, preferred_element_type=f32).astype(bf),
        ],
        axis=1,
    )
    hat_two, inv_two = rms_parts(middle)
    grad_gain_two = jnp.sum(grad_normed_two * hat_two, axis=0)
    grad_middle = out_rows.astype(f32) + rms_back(grad_normed_two * gain, hat_two, inv_two)
    grad_mid_low = lax.all_gather(grad_middle.astype(bf), "tensor", tiled=True)
    mixture = lax.psum_scatter(mixture_part, "dp", tiled=True).astype(f32)
    hidden_out = (middle + mixture).astype(bf)
    sums = lax.psum_scatter(weight_grads.reshape(-1, model_width), "tensor", tiled=True)
    sums = sums.reshape(3, local_experts, -1, model_width)
    kept = jnp.concatenate(
        [jnp.swapaxes(sums[:2], 0, 1).reshape(2 * local_experts, -1, model_width), sums[2]]
    )
    zero = jnp.zeros_like(kept)
    return (hidden_out, kept, zero, zero, zero, grad_middle, grad_mid_low, grad_gain_two)


def local(
    hidden_in,
    seq_lens,
    norm1_gain,
    query_weight,
    key_weight,
    value_weight,
    query_gain,
    key_gain,
    out_weight,
    norm2_gain,
    w_gate_up,
    w_down,
    routes,
    route_weights,
    out_grad,
):
    bf = jnp.bfloat16
    f32 = jnp.float32
    tokens, model_width = hidden_in.shape
    local_experts = w_gate_up.shape[0]
    hidden_part = w_gate_up.shape[3]
    head_dim = query_gain.shape[0]
    data_size = lax.axis_size("dp")
    quarter = tokens // lax.axis_size("tensor")
    experts = local_experts * data_size
    rows = data_size * quarter
    places, starts = sequence_layout(seq_lens[0], tokens)
    cosine_table, sine_table = rotary_tables(places - starts, head_dim)
    cosines = jnp.concatenate([cosine_table, cosine_table], axis=1)
    sines = jnp.concatenate([-sine_table, sine_table], axis=1)
    starts = starts.reshape(1, -1).astype(jnp.int32)
    gate_up = jnp.transpose(w_gate_up, (0, 2, 3, 1))
    (
        middle,
        inputs,
        gathered,
        others,
        mixed_low,
        query_low,
        key_low,
        value_low,
        raw_query,
        raw_key,
        normed,
    ) = start_layer(
        data_size,
        experts,
        hidden_in,
        out_grad,
        routes.T,
        route_weights.T,
        query_weight,
        key_weight,
        value_weight,
        out_weight,
        gate_up,
        w_down,
        cosines,
        sines,
        starts,
        norm1_gain.reshape(1, -1),
        norm2_gain.reshape(1, -1),
        query_gain.reshape(1, -1),
        key_gain.reshape(1, -1),
    )
    stage = run_experts if data_size <= 8 else large_experts
    hidden_out, kept, given, joined, _, grad_middle, grad_mid_low, grad_gain_two = stage(
        data_size,
        inputs.reshape(rows, model_width),
        gathered.reshape(rows, -1),
        gate_up,
        w_down,
        others,
        middle,
        norm2_gain,
        experts,
    )
    hidden_out, crossed, grad_hidden, query_sum, key_sum, value_sum, out_sum, *gains = finish_layer(
        data_size,
        grad_mid_low,
        out_weight,
        mixed_low,
        query_low,
        key_low,
        value_low,
        raw_query,
        raw_key,
        normed,
        query_weight,
        key_weight,
        value_weight,
        cosines,
        sines,
        starts,
        query_gain.reshape(1, -1),
        key_gain.reshape(1, -1),
        grad_middle,
        hidden_in,
        hidden_out,
        joined,
        norm1_gain.reshape(1, -1),
        grad_gain_two.reshape(1, -1),
    )
    split = 2 * local_experts * hidden_part
    query_sum, key_sum, value_sum, out_sum, gate_up_sum, down_sum, hidden_out, grad_hidden = widen(
        query_sum, key_sum, value_sum, out_sum, (kept, given, crossed), split, hidden_out, grad_hidden
    )
    grad_w_gate_up = jnp.transpose(
        gate_up_sum.reshape(local_experts, 2, hidden_part, model_width), (0, 3, 1, 2)
    )
    grad_w_down = down_sum.reshape(local_experts, hidden_part, model_width)
    gains = [gain.reshape(-1) for gain in gains]
    return (
        hidden_out,
        grad_hidden,
        gains[0],
        query_sum,
        key_sum,
        value_sum,
        gains[2],
        gains[3],
        out_sum,
        gains[1],
        grad_w_gate_up,
        grad_w_down,
    )


def solution(mesh):
    in_specs = (
        P("dp", None),
        P("dp", None),
        P(),
        P(None, "tensor"),
        P(None, "tensor"),
        P(None, "tensor"),
        P(),
        P(),
        P("tensor", None),
        P(),
        P("dp", None, None, "tensor"),
        P("dp", "tensor", None),
        P("dp", None),
        P("dp", None),
        P("dp", None),
    )
    out_specs = (
        P("dp", None),
        P("dp", None),
        P(),
        P(None, "tensor"),
        P(None, "tensor"),
        P(None, "tensor"),
        P(),
        P(),
        P("tensor", None),
        P(),
        P("dp", None, None, "tensor"),
        P("dp", "tensor", None),
    )
    return jax.shard_map(local, mesh=mesh, in_specs=in_specs, out_specs=out_specs, check_vma=False)
```

```python
import functools
import math

import jax
import jax.numpy as jnp
import numpy as np
from jax import lax
from jax.experimental import pallas as pl
from jax.experimental.pallas import tpu as pltpu
from jax.sharding import PartitionSpec as P

EPSILON = 1e-06
ROPE_BASE = 1000000.0


def rms_parts(values):
    inverse = lax.rsqrt(jnp.mean(values * values, axis=-1, keepdims=True) + EPSILON)
    return (values * inverse, inverse)


def rms_back(grad_hat, normal_hat, inverse):
    return inverse * (
        grad_hat - normal_hat * jnp.mean(grad_hat * normal_hat, axis=-1, keepdims=True)
    )


def rotary_tables(positions, head_dim):
    lane = jnp.arange(head_dim, dtype=jnp.int32)
    halves = (lane % (head_dim // 2)).astype(jnp.float32)
    inverse = jnp.exp(halves * (-2.0 * math.log(ROPE_BASE) / head_dim))
    angles = positions.astype(jnp.float32)[:, None] * inverse[None, :]
    sines = jnp.sin(angles)
    return (jnp.cos(angles), jnp.where(lane[None, :] < head_dim // 2, -sines, sines))


def sequence_layout(lengths, token_count):
    order = jnp.arange(lengths.shape[0], dtype=jnp.int32)
    endings = jnp.sum(jnp.where(order[:, None] <= order[None, :], lengths[:, None], 0), axis=0)
    places = jnp.arange(token_count, dtype=jnp.int32)
    starts = jnp.sum(jnp.where(endings[None, :] <= places[:, None], lengths[None, :], 0), axis=1)
    return (places, starts)


LANES = 128
MESH = pl.DeviceIdType.MESH
VMEM_LIMIT = 127 * 512 * 1024


def ring_place(index, size):
    return jnp.where(index % 2 == 0, index // 2, size - (index + 1) // 2)


def ring_index(place, size):
    place = place % size
    return jnp.where(place < size // 2, 2 * place, 2 * size - 1 - 2 * place)


def tensor_peers():
    own = lax.axis_index("tensor")
    partner = own + 1 - 2 * (own % 2)
    across = (own + 2) % 4
    return own, partner, across


def greet(devices):
    barrier = pltpu.get_barrier_semaphore()
    for device in devices:
        pl.semaphore_signal(barrier, inc=1, device_id=device, device_id_type=MESH)
    pl.semaphore_wait(barrier, len(devices))


def push(source, target, sems, device):
    return pltpu.make_async_remote_copy(
        src_ref=source,
        dst_ref=target,
        send_sem=sems[0],
        recv_sem=sems[1],
        device_id=device,
        device_id_type=MESH,
    )


def slot_of(delta, size):
    delta = (delta + size // 2 - 1) % size - (size // 2 - 1)
    if delta == 0:
        return size - 1
    if delta == size // 2:
        return size - 2
    return 2 * delta - 1 if delta > 0 else -2 * delta - 2


class GatherRing:
    def __init__(self, size, blocks, sems, parts=2):
        self.size, self.blocks, self.sems, self.parts = size, blocks, sems, parts
        self.place = ring_place(lax.axis_index("dp"), size)
        self.sent = []
        self.live = {}

    def send(self, step):
        size, half = self.size, self.blocks.shape[1] // 2
        piece = half // self.parts
        for part in range(self.parts):
            for way in (0, 1):
                sign = 1 - 2 * way
                rows = pl.ds(way * half + part * piece, piece)
                source = self.blocks.at[slot_of(-sign * step, size), rows]
                target = self.blocks.at[slot_of(-sign * (step + 1), size), rows]
                device = (ring_index(self.place + size + sign, size), lax.axis_index("tensor"))
                copy = push(
                    source,
                    target,
                    (self.sems.at[0, way, step, part], self.sems.at[1, way, step, part]),
                    device,
                )
                if step > 0:
                    self.live[step - 1, part, way].wait_recv()
                copy.start()
                self.live[step, part, way] = copy
                self.sent.append(copy)

    def step(self, step):
        if step + 1 < self.size - 1:
            self.send(step + 1)
        else:
            for part in range(self.parts):
                for way in (0, 1):
                    self.live[step, part, way].wait_recv()

    def finish(self):
        for copy in self.sent:
            copy.wait_send()


def row_loop(total, rows, body):
    def run(index, carry):
        body(pl.ds(pl.multiple_of(index * rows, rows), rows))
        return carry

    lax.fori_loop(0, total // rows, run, 0)


def matmul_nt(left, right):
    return lax.dot_general(left, right, (((1,), (1,)), ((), ())), preferred_element_type=jnp.float32)


def matmul(left, right):
    return lax.dot_general(left, right, (((1,), (0,)), ((), ())), preferred_element_type=jnp.float32)


def rms_rows(values):
    return lax.rsqrt(jnp.mean(values * values, axis=-1, keepdims=True) + EPSILON)


def turn(values, cosine, sine):
    return values * cosine + pltpu.roll(values, values.shape[1] // 2, 1) * sine


def start_layer_body(
    size,
    experts,
    token_ref,
    above_ref,
    route_ref,
    share_ref,
    query_weight_ref,
    key_weight_ref,
    value_weight_ref,
    out_weight_ref,
    gate_up_ref,
    down_ref,
    cosine_ref,
    sine_ref,
    start_ref,
    first_gain_ref,
    second_gain_ref,
    query_gain_ref,
    key_gain_ref,
    middle_ref,
    inputs_out,
    packs_out,
    others_ref,
    mixed_out,
    query_out,
    key_ref,
    value_ref,
    raw_query_out,
    raw_key_ref,
    normed_out,
    query_weight,
    key_weight,
    value_weight,
    out_weight,
    part_ref,
    from_partner,
    from_across,
    joined,
    ring_sems,
    pack_sems,
    side_sems,
    load_sems,
    near_sems,
    far_sems,
    pass_sems,
    store_sems,
    inputs_ref,
    packs_ref,
    mixed_ref,
    query_ref,
    raw_query_ref,
    normed_ref,
):
    f32, bf = jnp.float32, jnp.bfloat16
    dp = lax.axis_index("dp")
    own, partner, across = tensor_peers()
    far_partner = (partner + 2) % 4
    quarter, width = middle_ref.shape
    tokens = token_ref.shape[0]
    head_dim = key_ref.shape[1]
    lead = query_weight_ref.shape[1]
    heads = lead // head_dim
    place = ring_place(dp, size)
    loads = []
    for index, (source, target) in enumerate(
        (
            (query_weight_ref, query_weight),
            (key_weight_ref, key_weight),
            (value_weight_ref, value_weight),
            (out_weight_ref, out_weight),
        )
    ):
        copy = pltpu.make_async_copy(source, target, load_sems.at[index])
        copy.start()
        loads.append(copy)
    mine = pl.ds(pl.multiple_of(own * quarter, quarter), quarter)
    base = own * quarter
    above = pltpu.make_async_copy(
        above_ref.at[mine], packs_ref.at[size - 1, :, pl.ds(0, width)], load_sems.at[4]
    )
    above.start()
    neighbours = [(ring_index(place + 1, size), own), (ring_index(place + size - 1, size), own)]
    greet(neighbours + [(dp, partner), (dp, across)])

    halves = 2
    pieces = []
    for kind in range(3):
        for expert in range(gate_up_ref.shape[0]):
            for half in range(halves):
                pieces.append((kind, expert, half))
    span = gate_up_ref.shape[2] // halves

    def piece_of(number):
        kind, expert, half = pieces[number]
        rows = pl.ds(half * span, span)
        source = gate_up_ref.at[expert, kind, rows] if kind < 2 else down_ref.at[expert, rows]
        return source, (kind, expert, rows)

    near = []
    for kind in range(3):
        for expert in range(gate_up_ref.shape[0]):
            number = len(near)
            source = gate_up_ref.at[expert, kind] if kind < 2 else down_ref.at[expert]
            copy = push(
                source,
                others_ref.at[0, kind, expert],
                (near_sems.at[0, number], near_sems.at[1, number]),
                (dp, partner),
            )
            copy.start()
            near.append(copy)
    far, passed = [], []

    def pump(passing=True):
        number = len(far)
        if number >= 3:
            old = far[number - 3]
            if number - 3 < len(pieces):
                old.wait_recv()
                kind, expert, rows = piece_of(number - 3)[1]
                copy = push(
                    others_ref.at[1, kind, expert, rows],
                    others_ref.at[2, kind, expert, rows],
                    (pass_sems.at[0, number - 3], pass_sems.at[1, number - 3]),
                    (dp, partner),
                )
                copy.start()
                passed.append(copy)
                old.wait_send()
        if number < len(pieces):
            source, (kind, expert, rows) = piece_of(number)
            copy = push(
                source,
                others_ref.at[1, kind, expert, rows],
                (far_sems.at[0, number], far_sems.at[1, number]),
                (dp, across),
            )
            copy.start()
            far.append(copy)
        else:
            far.append(None)

    pump()
    pump()
    pump()

    tail = packs_ref.shape[2] - width
    line = lax.broadcasted_iota(jnp.int32, (tail, quarter), 0)
    name = jnp.where(line < experts, line, line - experts)
    dense = jnp.zeros((tail, quarter), f32)
    for choice in range(route_ref.shape[0]):
        named = route_ref[choice : choice + 1, mine]
        dense = dense + jnp.where(named == name, share_ref[choice : choice + 1, mine], 0.0)
    high = dense.astype(bf).astype(f32)
    both = jnp.where(line < experts, high, jnp.where(line < 2 * experts, dense - high, 0.0))
    packs_ref[size - 1, :, width:] = both.T.astype(bf)
    above.wait()
    packs = GatherRing(size, packs_ref, pack_sems)
    packs.send(0)

    def norm_first(rows):
        hidden = token_ref[rows, :].astype(f32)
        normed_ref[rows, :] = (hidden * rms_rows(hidden) * first_gain_ref[...]).astype(bf)

    row_loop(tokens, 16, norm_first)
    loads[0].wait()
    wide = 4 * LANES

    def project(tile, carry):
        here = pl.ds(pl.multiple_of(tile * wide, wide), wide)
        raw_query_ref[:, here] = matmul(normed_ref[...], query_weight[:, here])
        return carry

    lax.fori_loop(0, lead // wide, project, 0)
    loads[1].wait()
    loads[2].wait()
    raw_key = matmul(normed_ref[...], key_weight[...])
    raw_key_ref[...] = raw_key
    key_ref[...] = turn(
        raw_key * rms_rows(raw_key) * key_gain_ref[...], cosine_ref[...], sine_ref[...]
    ).astype(bf)
    value_ref[...] = matmul(normed_ref[...], value_weight[...]).astype(bf)
    packs.step(0)
    scale = head_dim**-0.5
    block = tokens // 2

    def do_head(head, carry):
        lanes = pl.ds(pl.multiple_of(head * head_dim, head_dim), head_dim)
        for part in (0, 1):
            rows = pl.ds(part * block, block)
            keys = pl.ds(0, (part + 1) * block)
            raw = raw_query_ref[rows, lanes]
            queries = turn(
                raw * rms_rows(raw) * query_gain_ref[...], cosine_ref[rows, :], sine_ref[rows, :]
            ).astype(bf)
            query_ref[rows, lanes] = queries
            scores = matmul_nt(key_ref[keys, :], queries)
            key_at = lax.broadcasted_iota(jnp.int32, scores.shape, 0)
            query_at = lax.broadcasted_iota(jnp.int32, scores.shape, 1) + part * block
            seen = (key_at <= query_at) & (key_at >= start_ref[:, rows])
            exponent = jnp.where(seen, jnp.exp(scores * scale), 0.0)
            soft = (exponent * (1.0 / jnp.sum(exponent, axis=0, keepdims=True))).astype(bf)
            mixed_ref[rows, lanes] = lax.dot_general(
                soft, value_ref[keys, :], (((0,), (0,)), ((), ())), preferred_element_type=f32
            ).astype(bf)
        return carry

    lax.fori_loop(0, heads // 2, do_head, 0)
    packs.step(1)
    pump()
    lax.fori_loop(heads // 2, heads, do_head, 0)
    stores = []

    def leave(*pairs):
        for source, target in pairs:
            copy = pltpu.make_async_copy(source, target, store_sems.at[len(stores)])
            copy.start()
            stores.append(copy)

    leave((raw_query_ref, raw_query_out), (query_ref, query_out))
    leave((normed_ref, normed_out), (mixed_ref, mixed_out))
    packs.step(2)
    loads[3].wait()

    def share(tile, carry):
        here = pl.ds(pl.multiple_of(tile * wide, wide), wide)
        part_ref[:, here] = matmul(mixed_ref[...], out_weight[:, here]).astype(bf)
        return carry

    lax.fori_loop(0, width // wide, share, 0)

    def part_rows(index):
        return pl.ds(pl.multiple_of(index * quarter, quarter), quarter)

    def side(index):
        return (side_sems.at[0, index], side_sems.at[1, index])

    first = push(part_ref.at[part_rows(far_partner)], from_partner.at[1], side(0), (dp, partner))
    second = push(part_ref.at[part_rows(partner)], from_partner.at[0], side(1), (dp, partner))
    first.start()
    second.start()
    packs.step(3)
    first.wait_recv()
    away = across * quarter

    def join(rows):
        there = pl.ds(pl.multiple_of(away + rows.start, 16), rows.size)
        joined[rows, :] = (part_ref[there, :].astype(f32) + from_partner[1, rows, :].astype(f32)).astype(bf)

    row_loop(quarter, 16, join)
    third = push(joined, from_across, side(2), (dp, across))
    third.start()
    pump()
    second.wait_recv()
    third.wait_recv()

    def norm_second(rows):
        there = pl.ds(pl.multiple_of(base + rows.start, 16), rows.size)
        middle = (
            token_ref[there, :].astype(f32)
            + part_ref[there, :].astype(f32)
            + from_partner[0, rows, :].astype(f32)
            + from_across[rows, :].astype(f32)
        )
        middle_ref[rows, :] = middle
        inputs_ref[size - 1, rows, :] = (middle * rms_rows(middle) * second_gain_ref[...]).astype(bf)

    row_loop(quarter, 16, norm_second)
    ring = GatherRing(size, inputs_ref, ring_sems)
    ring.send(0)
    for step in range(size - 1):
        if step + 4 < size - 1:
            packs.step(step + 4)
        if step + 4 == size - 1:
            leave((packs_ref, packs_out))
        pump()
        ring.step(step)
        if step % 2 == 1:
            pump()
    leave((inputs_ref, inputs_out))
    while len(far) < len(pieces) + 3:
        pump()
    packs.finish()
    ring.finish()
    first.wait_send()
    second.wait_send()
    third.wait_send()
    for copy in near + passed + stores:
        copy.wait()


def start_layer(size, experts, *arguments):
    tokens_rows, _, _, _, query_weight, key_weight, value_weight, out_weight, gate_up = arguments[:9]
    bf, f32 = jnp.bfloat16, jnp.float32
    tokens, width = tokens_rows.shape
    quarter = tokens // 4
    lead, head_dim = query_weight.shape[1], key_weight.shape[1]
    columns = width + -(-2 * experts // LANES) * LANES
    local, _, units, _ = gate_up.shape
    vmem = pl.BlockSpec(memory_space=pltpu.VMEM)
    anywhere = pl.BlockSpec(memory_space=pl.ANY)
    dma = pltpu.SemaphoreType.DMA
    return pl.pallas_call(
        functools.partial(start_layer_body, size, experts),
        out_shape=(
            jax.ShapeDtypeStruct((quarter, width), f32),
            jax.ShapeDtypeStruct((size, quarter, width), bf),
            jax.ShapeDtypeStruct((size, quarter, columns), bf),
            jax.ShapeDtypeStruct((3, 3, local, units, width), bf),
            jax.ShapeDtypeStruct((tokens, lead), bf),
            jax.ShapeDtypeStruct((tokens, lead), bf),
            jax.ShapeDtypeStruct((tokens, head_dim), bf),
            jax.ShapeDtypeStruct((tokens, head_dim), bf),
            jax.ShapeDtypeStruct((tokens, lead), f32),
            jax.ShapeDtypeStruct((tokens, head_dim), f32),
            jax.ShapeDtypeStruct((tokens, width), bf),
        ),
        in_specs=[vmem, anywhere, vmem, vmem] + [anywhere] * 6 + [vmem] * 7,
        out_specs=(vmem,) + (anywhere,) * 5 + (vmem, vmem, anywhere, vmem, anywhere),
        scratch_shapes=[
            pltpu.VMEM(query_weight.shape, bf),
            pltpu.VMEM(key_weight.shape, bf),
            pltpu.VMEM(value_weight.shape, bf),
            pltpu.VMEM(out_weight.shape, bf),
            pltpu.VMEM((tokens, width), bf),
            pltpu.VMEM((2, quarter, width), bf),
            pltpu.VMEM((quarter, width), bf),
            pltpu.VMEM((quarter, width), bf),
            dma((2, 2, size - 1, 2)),
            dma((2, 2, size - 1, 2)),
            dma((2, 3)),
            dma((5,)),
            dma((2, 3 * local)),
            dma((2, 6 * local)),
            dma((2, 6 * local)),
            dma((6,)),
            pltpu.VMEM((size, quarter, width), bf),
            pltpu.VMEM((size, quarter, columns), bf),
            pltpu.VMEM((tokens, lead), bf),
            pltpu.VMEM((tokens, lead), bf),
            pltpu.VMEM((tokens, lead), f32),
            pltpu.VMEM((tokens, width), bf),
        ],
        compiler_params=pltpu.CompilerParams(
            collective_id=0, has_side_effects=True, vmem_limit_bytes=VMEM_LIMIT
        ),
        name="start_layer",
    )(*arguments)


def run_experts_body(
    size,
    local_experts,
    experts,
    inputs_hbm,
    packs_hbm,
    gate_up_ref,
    down_ref,
    others_ref,
    member_ref,
    middle_ref,
    gain_ref,
    hidden_out,
    kept_ref,
    given_ref,
    cross_ref,
    landing_ref,
    gmid_ref,
    gmid_all,
    gain_out,
    weights,
    hidden,
    grad_parts,
    mix_parts,
    grad_slots,
    mix_slots,
    turned,
    stage,
    landed,
    totals,
    load_sems,
    grad_sems,
    mix_sems,
    side_sems,
    store_sems,
    give_sems,
    land_sems,
    token_sems,
    inputs_ref,
    packs_ref,
):
    f32, bf = jnp.float32, jnp.bfloat16
    dp = lax.axis_index("dp")
    own, partner, across = tensor_peers()
    width = inputs_ref.shape[1]
    quarter = inputs_ref.shape[0] // size
    pair = 2 * quarter
    half = size // 2
    units = weights.shape[1]
    members = others_ref.shape[0] + 1
    span = units // members
    wide = 512
    place = ring_place(dp, size)

    def token_loads(index):
        rows = pl.ds(pl.multiple_of(index * pair, pair), pair)
        return (
            pltpu.make_async_copy(inputs_hbm.at[rows], inputs_ref.at[rows], token_sems.at[0, index]),
            pltpu.make_async_copy(packs_hbm.at[rows], packs_ref.at[rows], token_sems.at[1, index]),
        )

    for copy in token_loads(0):
        copy.start()
    forward = (ring_index(place + 1, size), own)
    backward = (ring_index(place + size - 1, size), own)
    greet([forward, backward, (dp, partner), (dp, across)])
    part_units = span // local_experts
    loads = []
    for expert in range(local_experts):
        rows = pl.ds(expert * part_units, part_units)
        for kind in range(3):
            source = gate_up_ref.at[expert, kind] if kind < 2 else down_ref.at[expert]
            loads.append((expert * part_units, source, weights.at[kind, rows]))
    for other in range(members - 1):
        for first in range(0, span, LANES):
            at = (other + 1) * span + first
            source = others_ref.at[other, :, pl.ds(first, LANES)]
            loads.append((at, source, weights.at[:, pl.ds(at, LANES)]))
    loads = [
        (at, pltpu.make_async_copy(source, target, load_sems.at[number]))
        for number, (at, source, target) in enumerate(loads)
    ]
    for _, copy in loads:
        copy.start()
    for index in range(1, half):
        for copy in token_loads(index):
            copy.start()

    grad_ring = (grad_parts, grad_slots, grad_sems)
    mix_ring = (mix_parts, mix_slots, mix_sems)

    ring_parts = 2
    way_rows = quarter // 2
    piece_rows = way_rows // ring_parts

    def ring_copy(ring, way, step, part, source):
        device = forward if way == 0 else backward
        _, slots, sems = ring
        rows = pl.ds(part * piece_rows, piece_rows)
        return push(
            source.at[rows],
            slots.at[way, step, rows],
            (sems.at[0, way, step, part], sems.at[1, way, step, part]),
            device,
        )

    def ring_step(ring, step, blocks, first=False):
        parts, slots, _ = ring
        for part in range(ring_parts):
            for way in (0, 1):
                if first:
                    source = parts.at[blocks[way], pl.ds(way * way_rows, way_rows)]
                else:
                    source = slots.at[way, step - 1]
                    ring_copy(ring, way, step - 1, part, source).wait_recv()

                    def add(rows):
                        rows = pl.ds(pl.multiple_of(rows.start + part * piece_rows, 16), rows.size)
                        there = pl.ds(pl.multiple_of(rows.start + way * way_rows, 16), rows.size)
                        slots[way, step - 1, rows, :] = (
                            slots[way, step - 1, rows, :].astype(f32)
                            + parts[blocks[way], there, :].astype(f32)
                        ).astype(bf)

                    row_loop(piece_rows, 16, add)
                ring_copy(ring, way, step, part, source).start()

    def ring_last(ring):
        for part in range(ring_parts):
            for way in (0, 1):
                ring_copy(ring, way, size - 2, part, ring[1].at[way, size - 2]).wait_recv()

    def do_pair(index, carry):
        rows = pl.ds(pl.multiple_of(index * pair, pair), pair)
        for copy in token_loads(index):
            copy.wait()
        tail = packs_ref[rows, width:].astype(f32)
        lane = lax.broadcasted_iota(jnp.int32, tail.shape, 1)
        shares = []
        for expert in range(local_experts):
            name = dp * local_experts + expert
            picked = (lane == name) | (lane == experts + name)
            shares.append(jnp.sum(jnp.where(picked, tail, 0.0), axis=1, keepdims=True))

        def do_units(tile, carry):
            here = pl.ds(pl.multiple_of(tile * wide, wide), wide)

            for number in range(units // wide):

                @pl.when((index == 0) & (tile == number))
                def _():
                    for at, copy in loads:
                        if at // wide == number:
                            copy.wait()

            scale = shares[0] * member_ref[0:1, here]
            for expert in range(1, local_experts):
                scale = scale + shares[expert] * member_ref[expert : expert + 1, here]
            tokens = inputs_ref[rows, :]
            gate = matmul_nt(tokens, weights[0, here, :])
            upward = matmul_nt(tokens, weights[1, here, :])
            grads = scale * matmul_nt(packs_ref[rows, :width], weights[2, here, :])
            share = jax.nn.sigmoid(gate)
            silu = gate * share
            hidden[0, rows, here] = (grads * upward * share * (1.0 + gate * (1.0 - share))).astype(bf)
            hidden[1, rows, here] = (grads * silu).astype(bf)
            hidden[2, rows, here] = (scale * silu * upward).astype(bf)
            return carry

        lax.fori_loop(0, units // wide, do_units, 0)

        def do_columns(tile, carry):
            here = pl.ds(pl.multiple_of(tile * wide, wide), wide)
            sums = matmul(hidden[0, rows, :], weights[0, :, here]) + matmul(
                hidden[1, rows, :], weights[1, :, here]
            )
            low = sums.astype(bf)
            grad_parts[2 * index, :, here] = low[:quarter]
            grad_parts[2 * index + 1, :, here] = low[quarter:]
            return carry

        def do_mix(tile, carry):
            here = pl.ds(pl.multiple_of(tile * wide, wide), wide)
            low = matmul(hidden[2, rows, :], weights[2, :, here]).astype(bf)
            mix_parts[2 * index, :, here] = low[:quarter]
            mix_parts[2 * index + 1, :, here] = low[quarter:]
            return carry

        lax.fori_loop(0, width // wide, do_columns, 0)

        def go_on(ring):
            @pl.when(index == 0)
            def _():
                ring_step(ring, 0, (0, 1), first=True)

            @pl.when(index > 0)
            def _():
                ring_step(ring, index, (2 * index, 2 * index + 1 - index // (half - 1)))

        go_on(grad_ring)
        lax.fori_loop(0, width // wide, do_mix, 0)
        go_on(mix_ring)
        return carry

    lax.fori_loop(0, half, do_pair, 0)
    group_units = (3, 1, 2, 0)
    targets = (landing_ref, given_ref, cross_ref, kept_ref)

    def tile_copies(group, kind, slot):
        copies = []
        for expert in range(local_experts):
            at = expert + 2 * local_experts if isinstance(kind, int) else 2 * expert + kind
            source = stage.at[slot, pl.ds(expert * part_units, part_units)]
            target = targets[group].at[at]
            if group < 2:
                sems = (give_sems.at[0, group, at], give_sems.at[1, group, at])
                copies.append(push(source, target, sems, (dp, partner)))
            else:
                copies.append(pltpu.make_async_copy(source, target, store_sems.at[group - 2, at]))
        return copies

    def tile_left(group, kind, slot):
        for copy in tile_copies(group, kind, slot):
            if group < 2:
                copy.wait_send()
            else:
                copy.wait()

    def land(kind):
        copies = []
        for expert in range(local_experts):
            at = expert + 2 * local_experts if isinstance(kind, int) else 2 * expert + kind
            rows = pl.ds(expert * part_units, part_units)
            copies.append(
                pltpu.make_async_copy(landing_ref.at[at], landed.at[rows], land_sems.at[expert])
            )
        return copies

    def tile(group, kind, source, before):
        number = 3 * group + kind
        slot = number % 2
        if before is not None:
            before(slot)
        if group == 2:
            for copy in tile_copies(0, kind, slot):
                copy.wait_recv()
            for copy in land(kind):
                copy.start()
        rows = pl.ds(group_units[group] * span, span)
        for chunk in range(half):
            some = pl.ds(chunk * pair, pair)
            turned[:, some] = hidden[kind, some, rows].T
        if group == 2:
            for copy in land(kind):
                copy.wait()

        def do_columns(tile, carry):
            here = pl.ds(pl.multiple_of(tile * wide, wide), wide)
            sums = matmul(turned[...], source[:, here])
            if group == 2:
                sums = sums + landed[:, here].astype(f32)
            stage[slot, :, here] = sums.astype(bf)
            return carry

        lax.fori_loop(0, width // wide, do_columns, 0)
        for copy in tile_copies(group, kind, slot):
            copy.start()

    def token_tiles(group):
        def run(kind, carry):
            if group == 0:
                before = None
            else:
                def before(slot):
                    @pl.when(kind == 0)
                    def _():
                        tile_left(group - 1, kind + 1, slot)

                    @pl.when(kind == 1)
                    def _():
                        tile_left(group - 1, 2, slot)

            tile(group, kind, inputs_ref, before)
            return carry

        lax.fori_loop(0, 2, run, 0)

    def grad_tile(group):
        def before(slot):
            tile_left(group, jnp.int32(0), slot)

        tile(group, 2, packs_ref, before)

    def final_sum():
        totals[...] = jnp.zeros_like(totals)
        ring_last(grad_ring)
        base = own * quarter

        def finish(way, inner):
            rows = pl.ds(pl.multiple_of(inner.start + way * way_rows, 16), inner.size)
            sums = grad_slots[way, size - 2, inner, :].astype(f32) + grad_parts[
                size - 1, rows, :
            ].astype(f32)
            middle = middle_ref[rows, :]
            inverse = lax.rsqrt(jnp.mean(middle * middle, axis=-1, keepdims=True) + EPSILON)
            hat = middle * inverse
            product = sums * hat
            totals[...] += product[:8] + product[8:]
            scaled = sums * gain_ref[...]
            back = inverse * (scaled - hat * jnp.mean(scaled * hat, axis=-1, keepdims=True))
            above = packs_ref[
                pl.ds(pl.multiple_of((size - 1) * quarter + rows.start, 16), rows.size), :width
            ]
            grad = above.astype(f32) + back
            gmid_ref[rows, :] = grad
            gmid_all[pl.ds(pl.multiple_of(base + rows.start, 16), rows.size), :] = grad.astype(bf)

        for way in (0, 1):
            row_loop(way_rows, 16, functools.partial(finish, way))
        gain_out[...] = jnp.sum(totals[...], axis=0, keepdims=True)

    def rows_of(index):
        return pl.ds(pl.multiple_of(index * quarter, quarter), quarter)

    def spread(index, whose, device):
        ref = gmid_all.at[rows_of(whose)]
        return push(ref, ref, (side_sems.at[0, index], side_sems.at[1, index]), device)

    def first_spread():
        spread(0, own, (dp, across)).start()
        spread(1, own, (dp, partner)).start()

    def second_spread():
        spread(0, own, (dp, across)).wait_recv()
        spread(2, across, (dp, partner)).start()

    def final_mix():
        ring_last(mix_ring)

        def finish(way, inner):
            rows = pl.ds(pl.multiple_of(inner.start + way * way_rows, 16), inner.size)
            hidden_out[rows, :] = (
                middle_ref[rows, :]
                + mix_slots[way, size - 2, inner, :].astype(f32)
                + mix_parts[size - 1, rows, :].astype(f32)
            ).astype(bf)

        for way in (0, 1):
            row_loop(way_rows, 16, functools.partial(finish, way))

    def closing():
        final_sum()
        first_spread()

    grad_events, mix_events = [], []
    for step in range(half, size - 1):
        delta = -(1 + step)
        blocks = (slot_of(delta, size), slot_of(-delta, size))
        grad_events.append(functools.partial(ring_step, grad_ring, step, blocks))
        mix_events.append(functools.partial(ring_step, mix_ring, step, blocks))
    events = [grad_events[0]]
    for first, second in zip(grad_events[1:], mix_events):
        events += [first, second]
    events += [closing, mix_events[-1], second_spread, final_mix]
    work = []
    for group in range(4):
        work.append(functools.partial(token_tiles, group))
        work.append(functools.partial(grad_tile, group))
    done = 0
    for number, piece in enumerate(work):
        piece()
        upto = -(-(number + 1) * len(events) // len(work))
        while done < upto:
            events[done]()
            done += 1
    tile_left(3, jnp.int32(1), 0)
    tile_left(3, 2, 1)
    for kind in (jnp.int32(0), jnp.int32(1), 2):
        for copy in tile_copies(1, kind, 0):
            copy.wait_recv()
    spread(1, own, (dp, partner)).wait_recv()
    spread(2, across, (dp, partner)).wait_recv()
    for index, device in ((0, across), (1, partner), (2, partner)):
        spread(index, own, (dp, device)).wait_send()
    for ring in (grad_ring, mix_ring):
        for way in (0, 1):
            for step in range(size - 1):
                for part in range(ring_parts):
                    ring_copy(ring, way, step, part, ring[1].at[way, step]).wait_send()


def run_experts(size, inputs, packs, gate_up, down, others, middle, gain, experts):
    bf, f32 = jnp.bfloat16, jnp.float32
    local_experts, _, part_units, width = gate_up.shape
    others = others.reshape(3, 3, local_experts * part_units, width)
    members, span = 4, local_experts * part_units
    rows = inputs.shape[0]
    quarter = rows // size
    units = members * span
    expert_of = (np.arange(units) // (span // local_experts)) % local_experts
    member = jnp.asarray(expert_of[None, :] == np.arange(local_experts)[:, None], f32)
    vmem = pl.BlockSpec(memory_space=pltpu.VMEM)
    anywhere = pl.BlockSpec(memory_space=pl.ANY)
    dma = pltpu.SemaphoreType.DMA
    return pl.pallas_call(
        functools.partial(run_experts_body, size, local_experts, experts),
        out_shape=(
            jax.ShapeDtypeStruct((quarter, width), bf),
            jax.ShapeDtypeStruct((3 * local_experts, part_units, width), bf),
            jax.ShapeDtypeStruct((3 * local_experts, part_units, width), bf),
            jax.ShapeDtypeStruct((3 * local_experts, part_units, width), bf),
            jax.ShapeDtypeStruct((3 * local_experts, part_units, width), bf),
            jax.ShapeDtypeStruct((quarter, width), f32),
            jax.ShapeDtypeStruct((members * quarter, width), bf),
            jax.ShapeDtypeStruct((1, width), f32),
        ),
        in_specs=[anywhere] * 5 + [vmem] * 3,
        out_specs=(vmem,) + (anywhere,) * 4 + (vmem,) * 3,
        scratch_shapes=[
            pltpu.VMEM((3, units, width), bf),
            pltpu.VMEM((3, rows, units), bf),
            pltpu.VMEM((size, quarter, width), bf),
            pltpu.VMEM((size, quarter, width), bf),
            pltpu.VMEM((2, size - 1, quarter // 2, width), bf),
            pltpu.VMEM((2, size - 1, quarter // 2, width), bf),
            pltpu.VMEM((span, rows), bf),
            pltpu.VMEM((2, span, width), bf),
            pltpu.VMEM((span, width), bf),
            pltpu.VMEM((8, width), f32),
            dma((3 * local_experts + 3 * span // LANES,)),
            dma((2, 2, size - 1, 2)),
            dma((2, 2, size - 1, 2)),
            dma((2, 3)),
            dma((2, 3 * local_experts)),
            dma((2, 2, 3 * local_experts)),
            dma((local_experts,)),
            dma((2, size // 2)),
            pltpu.VMEM(inputs.shape, bf),
            pltpu.VMEM(packs.shape, bf),
        ],
        compiler_params=pltpu.CompilerParams(
            collective_id=2, has_side_effects=True, vmem_limit_bytes=VMEM_LIMIT
        ),
        name="run_experts",
    )(inputs, packs, gate_up, down, others, member, middle, gain.reshape(1, -1))


def back_through_head(grads, raw, gain, cosine, sine):
    hat_grads = grads * cosine - pltpu.roll(grads, grads.shape[1] // 2, 1) * sine
    inverse = lax.rsqrt(jnp.mean(raw * raw, axis=-1, keepdims=True) + EPSILON)
    hat = raw * inverse
    terms = hat_grads * hat
    scaled = hat_grads * gain
    back = inverse * (scaled - hat * jnp.mean(scaled * hat, axis=-1, keepdims=True))
    return back.astype(jnp.bfloat16), terms


def finish_layer_body(
    size,
    gmid_low_hbm,
    out_weight_hbm,
    mixed_hbm,
    query_hbm,
    key_hbm,
    value_hbm,
    raw_query_hbm,
    raw_key_hbm,
    normed_hbm,
    query_weight_hbm,
    key_weight_hbm,
    value_weight_hbm,
    cosine_ref,
    sine_ref,
    start_ref,
    query_gain_ref,
    key_gain_ref,
    middle_ref,
    token_hbm,
    hidden_ref,
    cross_ref,
    gain_ref,
    gains_ref,
    hidden_all,
    crossed_ref,
    grad_all,
    query_out,
    key_out,
    value_out,
    outer_out,
    first_out,
    second_out,
    query_gain_out,
    key_gain_out,
    qkv_ref,
    out_ref,
    slots_a,
    slots_b,
    grad_mixed,
    grad_heads,
    key_sums,
    value_sums,
    turned,
    partial,
    from_partner,
    from_across,
    joined,
    totals,
    head_totals,
    pair_gains,
    ring_gains,
    sems_a,
    sems_b,
    ring_sems,
    side_sems,
    load_sems,
    store_sems,
    gather_a,
    gather_b,
    token_ref,
    gmid_low_ref,
    out_weight_ref,
    mixed_ref,
    query_ref,
    key_ref,
    value_ref,
    raw_query_ref,
    raw_key_ref,
    normed_ref,
    query_weight_ref,
    key_weight_ref,
    value_weight_ref,
):
    f32, bf = jnp.float32, jnp.bfloat16
    dp = lax.axis_index("dp")
    own, partner, across = tensor_peers()
    far_partner = (partner + 2) % 4
    quarter, width = token_ref.shape
    tokens = normed_ref.shape[0]
    head_dim = key_ref.shape[1]
    lead = query_ref.shape[1]
    heads = lead // head_dim
    scale = head_dim**-0.5
    place = ring_place(dp, size)
    forward = (ring_index(place + 1, size), own)
    backward = (ring_index(place + size - 1, size), own)
    ways = ((forward, 1), (backward, -1))
    mine = pl.ds(pl.multiple_of(own * quarter, quarter), quarter)
    home = own * quarter
    loads = {}
    for source, target in (
        (gmid_low_hbm, gmid_low_ref),
        (mixed_hbm, mixed_ref),
        (out_weight_hbm, out_weight_ref),
        (query_hbm, query_ref),
        (key_hbm, key_ref),
        (value_hbm, value_ref),
        (raw_query_hbm, raw_query_ref),
        (raw_key_hbm, raw_key_ref),
        (normed_hbm, normed_ref),
        (query_weight_hbm, query_weight_ref),
        (key_weight_hbm, key_weight_ref),
        (value_weight_hbm, value_weight_ref),
        (token_hbm.at[mine], token_ref),
    ):
        copy = pltpu.make_async_copy(source, target, load_sems.at[len(loads)])
        copy.start()
        loads[id(target)] = copy

    def loaded(*targets):
        for target in targets:
            loads[id(target)].wait()

    greet([forward, backward, (dp, partner), (dp, across)])
    waits = []

    def start(copy):
        copy.start()
        waits.append(copy)
        return copy

    sets = (
        (qkv_ref, slots_a, gather_a, sems_a),
        (out_ref, slots_b, gather_b, sems_b),
    )

    def wrap(value):
        return (value + 2 * size) % size

    live = {}

    ring_parts = 2 if lead // size % 64 == 0 else 1
    stores = []

    def ring_rows(ref):
        rows = ref.shape[0] // size
        return rows, rows // 2, rows // 2 // ring_parts

    def add_own(which, way, step, part):
        ref, slots, blocks, _ = sets[which]
        live[which, way, step, part].wait_recv()
        rows, half, count = ring_rows(ref)
        base = wrap(place - ways[way][1] * (2 + step)) * rows + way * half

        def add(inner):
            inner = pl.ds(pl.multiple_of(inner.start + part * count, 16), inner.size)
            there = pl.ds(pl.multiple_of(base + inner.start, 16), inner.size)
            sums = (slots[way, step, inner, :].astype(f32) + ref[there, :].astype(f32)).astype(bf)
            if step == size - 2:
                final = pl.ds(pl.multiple_of(inner.start + way * half, 16), inner.size)
                blocks[place, final, :] = sums
            else:
                slots[way, step, inner, :] = sums

        row_loop(count, 16, add)

    def keep_block(which, way, block, part):
        ref, _, blocks, _ = sets[which]
        rows, half, count = ring_rows(ref)
        inner = pl.ds(way * half + part * count, count)
        there = pl.ds(pl.multiple_of(block * rows + way * half + part * count, 16), count)
        if which == 1:
            targets = [(outer_out, 0, width)]
        else:
            targets = [
                (query_out, 0, lead),
                (key_out, lead, head_dim),
                (value_out, lead + head_dim, head_dim),
            ]
        for target, first, columns in targets:
            source = blocks.at[block, inner, pl.ds(first, columns)]
            copy = pltpu.make_async_copy(source, target.at[there], store_sems.at[len(stores)])
            copy.start()
            stores.append(copy)

    def ring_event(which, step):
        ref, slots, blocks, sems = sets[which]
        rows, half, count = ring_rows(ref)
        for part in range(ring_parts):
            inner = pl.ds(part * count, count)
            for way, (device, sign) in enumerate(ways):
                if step == 0:
                    at = wrap(place - sign) * rows + way * half + part * count
                    source = ref.at[pl.ds(pl.multiple_of(at, 16), count)]
                elif step < size:
                    add_own(which, way, step - 1, part)
                    source = slots.at[way, step - 1, inner] if step < size - 1 else None
                else:
                    live[which, way, step - 1, part].wait_recv()
                block = wrap(place - sign * (step - size + 1))
                if step >= size - 1:
                    keep_block(which, way, block, part)
                if step >= 2 * size - 2:
                    continue
                if step >= size - 1:
                    source = blocks.at[block, pl.ds(way * half + part * count, count)]
                    target = source
                else:
                    target = slots.at[way, step, inner]
                sem = (sems.at[0, way, step, part], sems.at[1, way, step, part])
                live[which, way, step, part] = start(push(source, target, sem, device))

    def part_rows(index):
        return pl.ds(pl.multiple_of(index * quarter, quarter), quarter)

    def side(index):
        return (side_sems.at[0, index], side_sems.at[1, index])

    step_rows = 2 * LANES
    wide = 4 * LANES

    def out_rows(index, carry):
        rows = pl.ds(pl.multiple_of(index * step_rows, step_rows), step_rows)
        turned[...] = mixed_ref[:, rows].T

        def columns(tile, carry):
            here = pl.ds(pl.multiple_of(tile * wide, wide), wide)
            out_ref[rows, here] = matmul(turned[...], gmid_low_ref[:, here]).astype(bf)
            return carry

        return lax.fori_loop(0, width // wide, columns, carry)

    loaded(gmid_low_ref, mixed_ref)
    lax.fori_loop(0, lead // step_rows, out_rows, 0)
    ring_event(1, 0)

    def keep(rows):
        hidden_all[pl.ds(pl.multiple_of(home + rows.start, 16), rows.size), :] = hidden_ref[rows, :]

    row_loop(quarter, 16, keep)
    shown = [start(push(hidden_ref, hidden_all.at[mine], side(9), (dp, across)))]
    shown.append(start(push(hidden_ref, hidden_all.at[mine], side(10), (dp, partner))))

    def mixed_columns(tile, carry):
        here = pl.ds(pl.multiple_of(tile * wide, wide), wide)
        grad_mixed[:, here] = matmul_nt(gmid_low_ref[...], out_weight_ref[here, :]).astype(bf)
        return carry

    loaded(out_weight_ref)
    lax.fori_loop(0, lead // wide, mixed_columns, 0)
    loaded(query_ref, key_ref, value_ref, raw_query_ref, raw_key_ref)
    key_sums[...] = jnp.zeros_like(key_sums)
    value_sums[...] = jnp.zeros_like(value_sums)
    head_totals[...] = jnp.zeros_like(head_totals)
    block = tokens // 2

    def do_head(head, carry):
        lanes = pl.ds(pl.multiple_of(head * head_dim, head_dim), head_dim)
        for part in (0, 1):
            rows = pl.ds(part * block, block)
            count = (part + 1) * block
            keys = pl.ds(0, count)
            queries = query_ref[rows, lanes]
            outer = grad_mixed[rows, lanes]
            scores = matmul_nt(key_ref[keys, :], queries)
            key_at = lax.broadcasted_iota(jnp.int32, scores.shape, 0)
            query_at = lax.broadcasted_iota(jnp.int32, scores.shape, 1) + part * block
            seen = (key_at <= query_at) & (key_at >= start_ref[:, rows])
            exponent = jnp.where(seen, jnp.exp(scores * scale), 0.0)
            soft = exponent * (1.0 / jnp.sum(exponent, axis=0, keepdims=True))
            grad_soft = matmul_nt(value_ref[keys, :], outer)
            inner = jnp.sum(soft * grad_soft, axis=0, keepdims=True)
            grad_scores = (soft * (grad_soft - inner)).astype(bf)
            value_sums[keys, :] += matmul(soft.astype(bf), outer)
            key_sums[keys, :] += matmul(grad_scores, queries)
            grad_query = scale * lax.dot_general(
                grad_scores, key_ref[keys, :], (((0,), (0,)), ((), ())), preferred_element_type=f32
            )
            low, terms = back_through_head(
                grad_query, raw_query_ref[rows, lanes], query_gain_ref[...], cosine_ref[rows, :], sine_ref[rows, :]
            )
            grad_heads[rows, lanes] = low
            head_totals[0] += jnp.sum(terms.reshape(-1, 8, head_dim), axis=0)
        return carry

    lax.fori_loop(0, heads // 4, do_head, 0)
    ring_event(1, 1)
    lax.fori_loop(heads // 4, 5 * heads // 8, do_head, 0)
    ring_event(1, 2)
    lax.fori_loop(5 * heads // 8, heads, do_head, 0)
    ring_event(1, 3)
    low, terms = back_through_head(
        scale * key_sums[...], raw_key_ref[...], key_gain_ref[...], cosine_ref[...], sine_ref[...]
    )
    grad_heads[:, pl.ds(lead, head_dim)] = low
    head_totals[1] += jnp.sum(terms.reshape(-1, 8, head_dim), axis=0)
    grad_heads[:, pl.ds(lead + head_dim, head_dim)] = value_sums[...].astype(bf)

    def in_rows(index, carry):
        rows = pl.ds(pl.multiple_of(index * step_rows, step_rows), step_rows)
        turned[...] = normed_ref[:, rows].T
        qkv_ref[rows, :] = matmul(turned[...], grad_heads[...]).astype(bf)
        return carry

    loaded(normed_ref)
    lax.fori_loop(0, width // step_rows, in_rows, 0)
    ring_event(1, 4)
    ring_event(0, 0)

    def token_columns(tile, carry):
        here = pl.ds(pl.multiple_of(tile * wide, wide), wide)
        sums = matmul_nt(grad_heads[:, :lead], query_weight_ref[here, :])
        sums = sums + matmul_nt(grad_heads[:, lead : lead + head_dim], key_weight_ref[here, :])
        sums = sums + matmul_nt(grad_heads[:, lead + head_dim :], value_weight_ref[here, :])
        partial[:, here] = sums.astype(bf)
        return carry

    loaded(query_weight_ref, key_weight_ref, value_weight_ref)
    lax.fori_loop(0, width // wide, token_columns, 0)
    first = start(push(partial.at[part_rows(far_partner)], from_partner.at[1], side(0), (dp, partner)))
    second = start(push(partial.at[part_rows(partner)], from_partner.at[0], side(1), (dp, partner)))
    ring_event(1, 5)
    first.wait_recv()
    away = across * quarter

    def join(rows):
        there = pl.ds(pl.multiple_of(away + rows.start, 16), rows.size)
        joined[rows, :] = (partial[there, :].astype(f32) + from_partner[1, rows, :].astype(f32)).astype(bf)

    row_loop(quarter, 16, join)
    third = start(push(joined, from_across, side(2), (dp, across)))
    ring_event(0, 1)
    ring_event(1, 6)
    second.wait_recv()
    third.wait_recv()
    totals[...] = jnp.zeros_like(totals)

    def finish(rows):
        there = pl.ds(pl.multiple_of(home + rows.start, 16), rows.size)
        grads = (
            partial[there, :].astype(f32)
            + from_partner[0, rows, :].astype(f32)
            + from_across[rows, :].astype(f32)
        )
        hidden = token_ref[rows, :].astype(f32)
        inverse = lax.rsqrt(jnp.mean(hidden * hidden, axis=-1, keepdims=True) + EPSILON)
        hat = hidden * inverse
        product = grads * hat
        totals[...] += product[:8] + product[8:]
        scaled = grads * gain_ref[...]
        back = inverse * (scaled - hat * jnp.mean(scaled * hat, axis=-1, keepdims=True))
        grad_all[there, :] = (middle_ref[rows, :] + back).astype(bf)

    loaded(token_ref)
    row_loop(quarter, 16, finish)
    spread = [start(push(grad_all.at[mine], grad_all.at[mine], side(3), (dp, across)))]
    spread.append(start(push(grad_all.at[mine], grad_all.at[mine], side(4), (dp, partner))))
    pair_gains[0, :, :width] = jnp.sum(totals[...], axis=0, keepdims=True)
    pair_gains[0, :, width : 2 * width] = gains_ref[...]
    pair_gains[0, :, 2 * width : 2 * width + head_dim] = jnp.sum(head_totals[0], axis=0, keepdims=True)
    pair_gains[0, :, 2 * width + head_dim :] = jnp.sum(head_totals[1], axis=0, keepdims=True)
    swap = start(push(pair_gains.at[0], pair_gains.at[1], side(5), (dp, partner)))
    ring_event(0, 2)
    ring_event(1, 7)
    far = part_rows(across)
    shown[0].wait_recv()
    shown.append(start(push(hidden_all.at[far], hidden_all.at[far], side(11), (dp, partner))))
    spread[0].wait_recv()
    spread.append(start(push(grad_all.at[far], grad_all.at[far], side(6), (dp, partner))))
    swap.wait_recv()
    pair_gains[2] = pair_gains[0] + pair_gains[1]
    swap = start(push(pair_gains.at[2], pair_gains.at[3], side(7), (dp, across)))
    ring_event(0, 3)
    ring_event(1, 8)
    swap.wait_recv()
    crossing = start(push(cross_ref, crossed_ref, side(8), (dp, across)))
    ring_gains[place] = pair_gains[2] + pair_gains[3]
    small = None
    for step in range(4, 2 * size - 1):
        ring_event(0, step)
        if step + 5 < 2 * size - 1:
            ring_event(1, step + 5)
        if step - 4 < size - 1:
            if small is not None:
                small.wait_recv()
            ref = ring_gains.at[wrap(place - step + 4)]
            sem = (ring_sems.at[0, step - 4], ring_sems.at[1, step - 4])
            small = start(push(ref, ref, sem, forward))
    small.wait_recv()
    gains = jnp.sum(ring_gains[...], axis=0)
    first_out[...] = gains[:, :width]
    second_out[...] = gains[:, width : 2 * width]
    query_gain_out[...] = gains[:, 2 * width : 2 * width + head_dim]
    key_gain_out[...] = gains[:, 2 * width + head_dim :]
    for copy in (spread[1], spread[2], shown[1], shown[2], crossing):
        copy.wait_recv()
    for copy in waits:
        copy.wait_send()
    for copy in stores:
        copy.wait()


def finish_layer(size, *arguments):
    bf, f32 = jnp.bfloat16, jnp.float32
    (
        _, out_weight, mixed, query, key, _, _, _, normed, query_weight, _, _, _, _, _, _, _, _, token_rows, _,
        cross, _, _,
    ) = arguments
    tokens, width = token_rows.shape
    quarter = tokens // 4
    lead, head_dim = query.shape[1], key.shape[1]
    vmem = pl.BlockSpec(memory_space=pltpu.VMEM)
    anywhere = pl.BlockSpec(memory_space=pl.ANY)
    dma = pltpu.SemaphoreType.DMA
    columns = lead + 2 * head_dim
    rows_a, rows_b = width // size, lead // size
    count = 2 * width + 2 * head_dim
    return pl.pallas_call(
        functools.partial(finish_layer_body, size),
        out_shape=(
            jax.ShapeDtypeStruct((tokens, width), bf),
            jax.ShapeDtypeStruct(cross.shape, bf),
            jax.ShapeDtypeStruct((tokens, width), bf),
            jax.ShapeDtypeStruct((width, lead), bf),
            jax.ShapeDtypeStruct((width, head_dim), bf),
            jax.ShapeDtypeStruct((width, head_dim), bf),
            jax.ShapeDtypeStruct((lead, width), bf),
            jax.ShapeDtypeStruct((1, width), f32),
            jax.ShapeDtypeStruct((1, width), f32),
            jax.ShapeDtypeStruct((1, head_dim), f32),
            jax.ShapeDtypeStruct((1, head_dim), f32),
        ),
        in_specs=[anywhere] * 12 + [vmem] * 6 + [anywhere, vmem, anywhere, vmem, vmem],
        out_specs=(vmem, anywhere, vmem) + (anywhere,) * 4 + (vmem,) * 4,
        scratch_shapes=[
            pltpu.VMEM((width, columns), bf),
            pltpu.VMEM((lead, width), bf),
            pltpu.VMEM((2, size - 1, rows_a // 2, columns), bf),
            pltpu.VMEM((2, size - 1, rows_b // 2, width), bf),
            pltpu.VMEM((tokens, lead), bf),
            pltpu.VMEM((tokens, columns), bf),
            pltpu.VMEM((tokens, head_dim), f32),
            pltpu.VMEM((tokens, head_dim), f32),
            pltpu.VMEM((2 * LANES, tokens), bf),
            pltpu.VMEM((tokens, width), bf),
            pltpu.VMEM((2, quarter, width), bf),
            pltpu.VMEM((quarter, width), bf),
            pltpu.VMEM((quarter, width), bf),
            pltpu.VMEM((8, width), f32),
            pltpu.VMEM((2, 8, head_dim), f32),
            pltpu.VMEM((4, 1, count), f32),
            pltpu.VMEM((size, 1, count), f32),
            dma((2, 2, 2 * size - 2, 2)),
            dma((2, 2, 2 * size - 2, 2)),
            dma((2, size - 1)),
            dma((2, 12)),
            dma((13,)),
            dma((16 * size,)),
            pltpu.VMEM((size, rows_a, columns), bf),
            pltpu.VMEM((size, rows_b, width), bf),
            pltpu.VMEM((quarter, width), bf),
        ]
        + [pltpu.VMEM(argument.shape, argument.dtype) for argument in arguments[:12]],
        compiler_params=pltpu.CompilerParams(
            collective_id=1, has_side_effects=True, vmem_limit_bytes=VMEM_LIMIT
        ),
        name="finish_layer",
    )(*arguments)


def widen_body(refs):
    f32 = jnp.float32
    for source, target in zip(refs[:4], refs[12:16]):
        target[...] = source[...].astype(f32)
    for first, target in ((4, refs[16]), (7, refs[17])):
        sums = refs[first][...].astype(f32) + refs[first + 1][...].astype(f32)
        target[...] = sums + refs[first + 2][...].astype(f32)
    refs[18][...] = refs[10][...]
    refs[19][...] = refs[11][...]


def widen(query, key, value, outer, shares, split, hidden, grads):
    f32 = jnp.float32
    steps = 8
    width = outer.shape[1]
    shares = [share.reshape(-1, width) for share in shares]
    rest = shares[0].shape[0] - split

    def rows(count, columns, first=0):
        block = count // steps
        assert count % steps == 0 and block % 16 == 0 and first % block == 0
        return pl.BlockSpec((block, columns), lambda step: (step + first // block, 0))

    plain = [rows(*array.shape) for array in (query, key, value, outer)]
    pair = [rows(*array.shape) for array in (hidden, grads)]
    first, second = rows(split, width), rows(rest, width)
    return pl.pallas_call(
        lambda *refs: widen_body(refs),
        grid=(steps,),
        out_shape=[jax.ShapeDtypeStruct(a.shape, f32) for a in (query, key, value, outer)]
        + [jax.ShapeDtypeStruct((split, width), f32), jax.ShapeDtypeStruct((rest, width), f32)]
        + [jax.ShapeDtypeStruct(a.shape, a.dtype) for a in (hidden, grads)],
        in_specs=plain + [first] * 3 + [rows(rest, width, split)] * 3 + pair,
        out_specs=plain + [first, second] + pair,
        compiler_params=pltpu.CompilerParams(vmem_limit_bytes=VMEM_LIMIT),
        name="widen",
    )(query, key, value, outer, *shares, *shares, hidden, grads)


def large_experts(size, inputs, packs, gate_up, down, others, middle, gain, experts):
    f32, bf = jnp.float32, jnp.bfloat16
    model_width = inputs.shape[1]
    own_weights = jnp.stack([gate_up[:, 0], gate_up[:, 1], down])
    all_weights = jnp.concatenate([own_weights[None], others])
    members = all_weights.shape[0]
    order = jnp.arange(members, dtype=jnp.int32) ^ lax.axis_index("tensor")
    all_weights = all_weights.reshape(members, 3, -1, model_width)[order]
    units = all_weights.shape[2]
    local_experts = experts // size
    indices = jnp.arange(size, dtype=jnp.int32)
    half = size // 2
    delta = (ring_place(indices, size) - ring_place(lax.axis_index("dp"), size)) % size
    ahead = jnp.where(delta == half, size - 2, jnp.where(delta == 0, size - 1, 2 * delta - 1))
    slots = jnp.where(delta > half, 2 * (size - delta) - 2, ahead)
    quarter = middle.shape[0]
    out_rows = packs[-quarter:, :model_width]
    inputs = inputs.reshape(size, quarter, -1)[slots].reshape(-1, model_width)
    packs = packs.reshape(size, quarter, -1)[slots].reshape(inputs.shape[0], -1)
    grads_all = packs[:, :model_width]
    shares = packs[:, model_width : model_width + 2 * experts].astype(f32)
    shares = shares[:, :experts] + shares[:, experts:]
    shares = lax.dynamic_slice_in_dim(
        shares, lax.axis_index("dp") * local_experts, local_experts, 1
    )
    weight_cols = jnp.broadcast_to(
        shares[:, None, :, None],
        (shares.shape[0], members, local_experts, units // local_experts),
    ).reshape(-1, members, units)

    def project(left, which):
        return jnp.einsum("td,rud->tru", left, all_weights[:, which], preferred_element_type=f32)

    gate_act = project(inputs, 0)
    upward = project(inputs, 1)
    sigmoid_gate = jax.nn.sigmoid(gate_act)
    active = gate_act * sigmoid_gate * upward
    weighted_low = (weight_cols * active).astype(bf)
    mixture_part = jnp.einsum(
        "tru,rud->td", weighted_low, all_weights[:, 2], preferred_element_type=f32
    ).astype(bf)
    grad_active = weight_cols * project(grads_all, 2)
    grad_gate = (
        grad_active * upward * sigmoid_gate * (1.0 + gate_act * (1.0 - sigmoid_gate))
    ).astype(bf)
    grad_up = (grad_active * gate_act * sigmoid_gate).astype(bf)
    grad_normed_part = jnp.einsum(
        "tru,rud->td", grad_gate, all_weights[:, 0], preferred_element_type=f32
    ) + jnp.einsum("tru,rud->td", grad_up, all_weights[:, 1], preferred_element_type=f32)
    grad_normed_two = lax.psum_scatter(grad_normed_part.astype(bf), "dp", tiled=True).astype(f32)
    weight_grads = jnp.stack(
        [
            jnp.einsum("tru,td->rud", grad_gate, inputs, preferred_element_type=f32).astype(bf),
            jnp.einsum("tru,td->rud", grad_up, inputs, preferred_element_type=f32).astype(bf),
            jnp.einsum("tru,td->rud", weighted_low, grads_all, preferred_element_type=f32).astype(bf),
        ],
        axis=1,
    )
    hat_two, inv_two = rms_parts(middle)
    grad_gain_two = jnp.sum(grad_normed_two * hat_two, axis=0)
    grad_middle = out_rows.astype(f32) + rms_back(grad_normed_two * gain, hat_two, inv_two)
    grad_mid_low = lax.all_gather(grad_middle.astype(bf), "tensor", tiled=True)
    mixture = lax.psum_scatter(mixture_part, "dp", tiled=True).astype(f32)
    hidden_out = (middle + mixture).astype(bf)
    sums = lax.psum_scatter(weight_grads.reshape(-1, model_width), "tensor", tiled=True)
    sums = sums.reshape(3, local_experts, -1, model_width)
    kept = jnp.concatenate(
        [jnp.swapaxes(sums[:2], 0, 1).reshape(2 * local_experts, -1, model_width), sums[2]]
    )
    zero = jnp.zeros_like(kept)
    return (hidden_out, kept, zero, zero, zero, grad_middle, grad_mid_low, grad_gain_two)


def local(
    hidden_in,
    seq_lens,
    norm1_gain,
    query_weight,
    key_weight,
    value_weight,
    query_gain,
    key_gain,
    out_weight,
    norm2_gain,
    w_gate_up,
    w_down,
    routes,
    route_weights,
    out_grad,
):
    bf = jnp.bfloat16
    f32 = jnp.float32
    tokens, model_width = hidden_in.shape
    local_experts = w_gate_up.shape[0]
    hidden_part = w_gate_up.shape[3]
    head_dim = query_gain.shape[0]
    data_size = lax.axis_size("dp")
    quarter = tokens // lax.axis_size("tensor")
    experts = local_experts * data_size
    rows = data_size * quarter
    places, starts = sequence_layout(seq_lens[0], tokens)
    cosines, sines = rotary_tables(places - starts, head_dim)
    starts = starts.reshape(1, -1).astype(jnp.int32)
    gate_up = jnp.transpose(w_gate_up, (0, 2, 3, 1))
    (
        middle,
        inputs,
        gathered,
        others,
        mixed_low,
        query_low,
        key_low,
        value_low,
        raw_query,
        raw_key,
        normed,
    ) = start_layer(
        data_size,
        experts,
        hidden_in,
        out_grad,
        routes.T,
        route_weights.T,
        query_weight,
        key_weight,
        value_weight,
        out_weight,
        gate_up,
        w_down,
        cosines,
        sines,
        starts,
        norm1_gain.reshape(1, -1),
        norm2_gain.reshape(1, -1),
        query_gain.reshape(1, -1),
        key_gain.reshape(1, -1),
    )
    stage = run_experts if data_size <= 8 else large_experts
    hidden_out, kept, given, joined, _, grad_middle, grad_mid_low, grad_gain_two = stage(
        data_size,
        inputs.reshape(rows, model_width),
        gathered.reshape(rows, -1),
        gate_up,
        w_down,
        others,
        middle,
        norm2_gain,
        experts,
    )
    hidden_out, crossed, grad_hidden, query_sum, key_sum, value_sum, out_sum, *gains = finish_layer(
        data_size,
        grad_mid_low,
        out_weight,
        mixed_low,
        query_low,
        key_low,
        value_low,
        raw_query,
        raw_key,
        normed,
        query_weight,
        key_weight,
        value_weight,
        cosines,
        sines,
        starts,
        query_gain.reshape(1, -1),
        key_gain.reshape(1, -1),
        grad_middle,
        hidden_in,
        hidden_out,
        joined,
        norm1_gain.reshape(1, -1),
        grad_gain_two.reshape(1, -1),
    )
    split = 2 * local_experts * hidden_part
    query_sum, key_sum, value_sum, out_sum, gate_up_sum, down_sum, hidden_out, grad_hidden = widen(
        query_sum, key_sum, value_sum, out_sum, (kept, given, crossed), split, hidden_out, grad_hidden
    )
    grad_w_gate_up = jnp.transpose(
        gate_up_sum.reshape(local_experts, 2, hidden_part, model_width), (0, 3, 1, 2)
    )
    grad_w_down = down_sum.reshape(local_experts, hidden_part, model_width)
    gains = [gain.reshape(-1) for gain in gains]
    return (
        hidden_out,
        grad_hidden,
        gains[0],
        query_sum,
        key_sum,
        value_sum,
        gains[2],
        gains[3],
        out_sum,
        gains[1],
        grad_w_gate_up,
        grad_w_down,
    )


def solution(mesh):
    in_specs = (
        P("dp", None),
        P("dp", None),
        P(),
        P(None, "tensor"),
        P(None, "tensor"),
        P(None, "tensor"),
        P(),
        P(),
        P("tensor", None),
        P(),
        P("dp", None, None, "tensor"),
        P("dp", "tensor", None),
        P("dp", None),
        P("dp", None),
        P("dp", None),
    )
    out_specs = (
        P("dp", None),
        P("dp", None),
        P(),
        P(None, "tensor"),
        P(None, "tensor"),
        P(None, "tensor"),
        P(),
        P(),
        P("tensor", None),
        P(),
        P("dp", None, None, "tensor"),
        P("dp", "tensor", None),
    )
    return jax.shard_map(local, mesh=mesh, in_specs=in_specs, out_specs=out_specs, check_vma=False)
```

```python
import functools
import math

import jax
import jax.numpy as jnp
import numpy as np
from jax import lax
from jax.experimental import pallas as pl
from jax.experimental.pallas import tpu as pltpu
from jax.sharding import PartitionSpec as P

EPSILON = 1e-06
ROPE_BASE = 1000000.0


def rms_parts(values):
    inverse = lax.rsqrt(jnp.mean(values * values, axis=-1, keepdims=True) + EPSILON)
    return (values * inverse, inverse)


def rms_back(grad_hat, normal_hat, inverse):
    return inverse * (
        grad_hat - normal_hat * jnp.mean(grad_hat * normal_hat, axis=-1, keepdims=True)
    )


def rotary_tables(positions, head_dim):
    lane = jnp.arange(head_dim, dtype=jnp.int32)
    halves = (lane % (head_dim // 2)).astype(jnp.float32)
    inverse = jnp.exp(halves * (-2.0 * math.log(ROPE_BASE) / head_dim))
    angles = positions.astype(jnp.float32)[:, None] * inverse[None, :]
    sines = jnp.sin(angles)
    return (jnp.cos(angles), jnp.where(lane[None, :] < head_dim // 2, -sines, sines))


def sequence_layout(lengths, token_count):
    order = jnp.arange(lengths.shape[0], dtype=jnp.int32)
    endings = jnp.sum(jnp.where(order[:, None] <= order[None, :], lengths[:, None], 0), axis=0)
    places = jnp.arange(token_count, dtype=jnp.int32)
    starts = jnp.sum(jnp.where(endings[None, :] <= places[:, None], lengths[None, :], 0), axis=1)
    return (places, starts)


LANES = 128
MESH = pl.DeviceIdType.MESH
VMEM_LIMIT = 127 * 512 * 1024


def ring_place(index, size):
    return jnp.where(index % 2 == 0, index // 2, size - (index + 1) // 2)


def ring_index(place, size):
    place = place % size
    return jnp.where(place < size // 2, 2 * place, 2 * size - 1 - 2 * place)


def tensor_peers():
    own = lax.axis_index("tensor")
    partner = own + 1 - 2 * (own % 2)
    across = (own + 2) % 4
    return own, partner, across


def greet(devices):
    barrier = pltpu.get_barrier_semaphore()
    for device in devices:
        pl.semaphore_signal(barrier, inc=1, device_id=device, device_id_type=MESH)
    pl.semaphore_wait(barrier, len(devices))


def push(source, target, sems, device):
    return pltpu.make_async_remote_copy(
        src_ref=source,
        dst_ref=target,
        send_sem=sems[0],
        recv_sem=sems[1],
        device_id=device,
        device_id_type=MESH,
    )


def slot_of(delta, size):
    delta = (delta + size // 2 - 1) % size - (size // 2 - 1)
    if delta == 0:
        return size - 1
    if delta == size // 2:
        return size - 2
    return 2 * delta - 1 if delta > 0 else -2 * delta - 2


class GatherRing:
    def __init__(self, size, blocks, sems, parts=2):
        self.size, self.blocks, self.sems, self.parts = size, blocks, sems, parts
        self.place = ring_place(lax.axis_index("dp"), size)
        self.sent = []
        self.live = {}

    def send(self, step):
        size, half = self.size, self.blocks.shape[1] // 2
        piece = half // self.parts
        for part in range(self.parts):
            for way in (0, 1):
                sign = 1 - 2 * way
                rows = pl.ds(way * half + part * piece, piece)
                source = self.blocks.at[slot_of(-sign * step, size), rows]
                target = self.blocks.at[slot_of(-sign * (step + 1), size), rows]
                device = (ring_index(self.place + size + sign, size), lax.axis_index("tensor"))
                copy = push(
                    source,
                    target,
                    (self.sems.at[0, way, step, part], self.sems.at[1, way, step, part]),
                    device,
                )
                if step > 0:
                    self.live[step - 1, part, way].wait_recv()
                copy.start()
                self.live[step, part, way] = copy
                self.sent.append(copy)

    def step(self, step):
        if step + 1 < self.size - 1:
            self.send(step + 1)
        else:
            for part in range(self.parts):
                for way in (0, 1):
                    self.live[step, part, way].wait_recv()

    def finish(self):
        for copy in self.sent:
            copy.wait_send()


def row_loop(total, rows, body):
    def run(index, carry):
        body(pl.ds(pl.multiple_of(index * rows, rows), rows))
        return carry

    lax.fori_loop(0, total // rows, run, 0)


def matmul_nt(left, right):
    return lax.dot_general(left, right, (((1,), (1,)), ((), ())), preferred_element_type=jnp.float32)


def matmul(left, right):
    return lax.dot_general(left, right, (((1,), (0,)), ((), ())), preferred_element_type=jnp.float32)


def rms_rows(values):
    return lax.rsqrt(jnp.mean(values * values, axis=-1, keepdims=True) + EPSILON)


def turn(values, cosine, sine):
    return values * cosine + pltpu.roll(values, values.shape[1] // 2, 1) * sine


def start_layer_body(
    size,
    experts,
    token_ref,
    above_ref,
    route_ref,
    share_ref,
    query_weight_ref,
    key_weight_ref,
    value_weight_ref,
    out_weight_ref,
    gate_up_ref,
    down_ref,
    cosine_ref,
    sine_ref,
    start_ref,
    first_gain_ref,
    second_gain_ref,
    query_gain_ref,
    key_gain_ref,
    middle_ref,
    inputs_out,
    packs_out,
    others_ref,
    mixed_out,
    query_out,
    key_ref,
    value_ref,
    raw_query_out,
    raw_key_ref,
    normed_out,
    query_weight,
    key_weight,
    value_weight,
    out_weight,
    part_ref,
    from_partner,
    from_across,
    joined,
    ring_sems,
    pack_sems,
    side_sems,
    load_sems,
    near_sems,
    far_sems,
    pass_sems,
    store_sems,
    inputs_ref,
    packs_ref,
    mixed_ref,
    query_ref,
    raw_query_ref,
    normed_ref,
):
    f32, bf = jnp.float32, jnp.bfloat16
    dp = lax.axis_index("dp")
    own, partner, across = tensor_peers()
    far_partner = (partner + 2) % 4
    quarter, width = middle_ref.shape
    tokens = token_ref.shape[0]
    head_dim = key_ref.shape[1]
    lead = query_weight_ref.shape[1]
    heads = lead // head_dim
    place = ring_place(dp, size)
    loads = []
    for index, (source, target) in enumerate(
        (
            (query_weight_ref, query_weight),
            (key_weight_ref, key_weight),
            (value_weight_ref, value_weight),
            (out_weight_ref, out_weight),
        )
    ):
        copy = pltpu.make_async_copy(source, target, load_sems.at[index])
        copy.start()
        loads.append(copy)
    mine = pl.ds(pl.multiple_of(own * quarter, quarter), quarter)
    base = own * quarter
    above = pltpu.make_async_copy(
        above_ref.at[mine], packs_ref.at[size - 1, :, pl.ds(0, width)], load_sems.at[4]
    )
    above.start()
    neighbours = [(ring_index(place + 1, size), own), (ring_index(place + size - 1, size), own)]
    greet(neighbours + [(dp, partner), (dp, across)])

    halves = 2
    pieces = []
    for kind in range(3):
        for expert in range(gate_up_ref.shape[0]):
            for half in range(halves):
                pieces.append((kind, expert, half))
    span = gate_up_ref.shape[2] // halves

    def piece_of(number):
        kind, expert, half = pieces[number]
        rows = pl.ds(half * span, span)
        source = gate_up_ref.at[expert, kind, rows] if kind < 2 else down_ref.at[expert, rows]
        return source, (kind, expert, rows)

    near = []
    for kind in range(3):
        for expert in range(gate_up_ref.shape[0]):
            number = len(near)
            source = gate_up_ref.at[expert, kind] if kind < 2 else down_ref.at[expert]
            copy = push(
                source,
                others_ref.at[0, kind, expert],
                (near_sems.at[0, number], near_sems.at[1, number]),
                (dp, partner),
            )
            copy.start()
            near.append(copy)
    far, passed = [], []

    def pump(passing=True):
        number = len(far)
        if number >= 3:
            old = far[number - 3]
            if number - 3 < len(pieces):
                old.wait_recv()
                kind, expert, rows = piece_of(number - 3)[1]
                copy = push(
                    others_ref.at[1, kind, expert, rows],
                    others_ref.at[2, kind, expert, rows],
                    (pass_sems.at[0, number - 3], pass_sems.at[1, number - 3]),
                    (dp, partner),
                )
                copy.start()
                passed.append(copy)
                old.wait_send()
        if number < len(pieces):
            source, (kind, expert, rows) = piece_of(number)
            copy = push(
                source,
                others_ref.at[1, kind, expert, rows],
                (far_sems.at[0, number], far_sems.at[1, number]),
                (dp, across),
            )
            copy.start()
            far.append(copy)
        else:
            far.append(None)

    pump()
    pump()
    pump()

    tail = packs_ref.shape[2] - width
    line = lax.broadcasted_iota(jnp.int32, (tail, quarter), 0)
    name = jnp.where(line < experts, line, line - experts)
    dense = jnp.zeros((tail, quarter), f32)
    for choice in range(route_ref.shape[0]):
        named = route_ref[choice : choice + 1, mine]
        dense = dense + jnp.where(named == name, share_ref[choice : choice + 1, mine], 0.0)
    high = dense.astype(bf).astype(f32)
    both = jnp.where(line < experts, high, jnp.where(line < 2 * experts, dense - high, 0.0))
    packs_ref[size - 1, :, width:] = both.T.astype(bf)
    above.wait()
    packs = GatherRing(size, packs_ref, pack_sems)
    packs.send(0)

    def norm_first(rows):
        hidden = token_ref[rows, :].astype(f32)
        normed_ref[rows, :] = (hidden * rms_rows(hidden) * first_gain_ref[...]).astype(bf)

    row_loop(tokens, 16, norm_first)
    loads[0].wait()
    wide = 4 * LANES

    def project(tile, carry):
        here = pl.ds(pl.multiple_of(tile * wide, wide), wide)
        raw_query_ref[:, here] = matmul(normed_ref[...], query_weight[:, here])
        return carry

    lax.fori_loop(0, lead // wide, project, 0)
    loads[1].wait()
    loads[2].wait()
    raw_key = matmul(normed_ref[...], key_weight[...])
    raw_key_ref[...] = raw_key
    key_ref[...] = turn(
        raw_key * rms_rows(raw_key) * key_gain_ref[...], cosine_ref[...], sine_ref[...]
    ).astype(bf)
    value_ref[...] = matmul(normed_ref[...], value_weight[...]).astype(bf)
    packs.step(0)
    scale = head_dim**-0.5
    block = tokens // 2

    def do_head(head, carry):
        lanes = pl.ds(pl.multiple_of(head * head_dim, head_dim), head_dim)
        for part in (0, 1):
            rows = pl.ds(part * block, block)
            keys = pl.ds(0, (part + 1) * block)
            raw = raw_query_ref[rows, lanes]
            queries = turn(
                raw * rms_rows(raw) * query_gain_ref[...], cosine_ref[rows, :], sine_ref[rows, :]
            ).astype(bf)
            query_ref[rows, lanes] = queries
            scores = matmul_nt(key_ref[keys, :], queries)
            key_at = lax.broadcasted_iota(jnp.int32, scores.shape, 0)
            query_at = lax.broadcasted_iota(jnp.int32, scores.shape, 1) + part * block
            seen = (key_at <= query_at) & (key_at >= start_ref[:, rows])
            exponent = jnp.where(seen, jnp.exp(scores * scale), 0.0)
            soft = (exponent * (1.0 / jnp.sum(exponent, axis=0, keepdims=True))).astype(bf)
            mixed_ref[rows, lanes] = lax.dot_general(
                soft, value_ref[keys, :], (((0,), (0,)), ((), ())), preferred_element_type=f32
            ).astype(bf)
        return carry

    lax.fori_loop(0, heads // 2, do_head, 0)
    packs.step(1)
    pump()
    lax.fori_loop(heads // 2, heads, do_head, 0)
    stores = []

    def leave(*pairs):
        for source, target in pairs:
            copy = pltpu.make_async_copy(source, target, store_sems.at[len(stores)])
            copy.start()
            stores.append(copy)

    leave((raw_query_ref, raw_query_out), (query_ref, query_out))
    leave((normed_ref, normed_out), (mixed_ref, mixed_out))
    packs.step(2)
    loads[3].wait()

    def share(tile, carry):
        here = pl.ds(pl.multiple_of(tile * wide, wide), wide)
        part_ref[:, here] = matmul(mixed_ref[...], out_weight[:, here]).astype(bf)
        return carry

    lax.fori_loop(0, width // wide, share, 0)

    def part_rows(index):
        return pl.ds(pl.multiple_of(index * quarter, quarter), quarter)

    def side(index):
        return (side_sems.at[0, index], side_sems.at[1, index])

    first = push(part_ref.at[part_rows(far_partner)], from_partner.at[1], side(0), (dp, partner))
    second = push(part_ref.at[part_rows(partner)], from_partner.at[0], side(1), (dp, partner))
    first.start()
    second.start()
    packs.step(3)
    first.wait_recv()
    away = across * quarter

    def join(rows):
        there = pl.ds(pl.multiple_of(away + rows.start, 16), rows.size)
        joined[rows, :] = (part_ref[there, :].astype(f32) + from_partner[1, rows, :].astype(f32)).astype(bf)

    row_loop(quarter, 16, join)
    third = push(joined, from_across, side(2), (dp, across))
    third.start()
    pump()
    second.wait_recv()
    third.wait_recv()

    def norm_second(rows):
        there = pl.ds(pl.multiple_of(base + rows.start, 16), rows.size)
        middle = (
            token_ref[there, :].astype(f32)
            + part_ref[there, :].astype(f32)
            + from_partner[0, rows, :].astype(f32)
            + from_across[rows, :].astype(f32)
        )
        middle_ref[rows, :] = middle
        inputs_ref[size - 1, rows, :] = (middle * rms_rows(middle) * second_gain_ref[...]).astype(bf)

    row_loop(quarter, 16, norm_second)
    ring = GatherRing(size, inputs_ref, ring_sems)
    ring.send(0)
    for step in range(size - 1):
        if step + 4 < size - 1:
            packs.step(step + 4)
        if step + 4 == size - 1:
            leave((packs_ref, packs_out))
        pump()
        ring.step(step)
        if step % 2 == 1:
            pump()
    leave((inputs_ref, inputs_out))
    while len(far) < len(pieces) + 3:
        pump()
    packs.finish()
    ring.finish()
    first.wait_send()
    second.wait_send()
    third.wait_send()
    for copy in near + passed + stores:
        copy.wait()


def start_layer(size, experts, *arguments):
    tokens_rows, _, _, _, query_weight, key_weight, value_weight, out_weight, gate_up = arguments[:9]
    bf, f32 = jnp.bfloat16, jnp.float32
    tokens, width = tokens_rows.shape
    quarter = tokens // 4
    lead, head_dim = query_weight.shape[1], key_weight.shape[1]
    columns = width + -(-2 * experts // LANES) * LANES
    local, _, units, _ = gate_up.shape
    vmem = pl.BlockSpec(memory_space=pltpu.VMEM)
    anywhere = pl.BlockSpec(memory_space=pl.ANY)
    dma = pltpu.SemaphoreType.DMA
    return pl.pallas_call(
        functools.partial(start_layer_body, size, experts),
        out_shape=(
            jax.ShapeDtypeStruct((quarter, width), f32),
            jax.ShapeDtypeStruct((size, quarter, width), bf),
            jax.ShapeDtypeStruct((size, quarter, columns), bf),
            jax.ShapeDtypeStruct((3, 3, local, units, width), bf),
            jax.ShapeDtypeStruct((tokens, lead), bf),
            jax.ShapeDtypeStruct((tokens, lead), bf),
            jax.ShapeDtypeStruct((tokens, head_dim), bf),
            jax.ShapeDtypeStruct((tokens, head_dim), bf),
            jax.ShapeDtypeStruct((tokens, lead), f32),
            jax.ShapeDtypeStruct((tokens, head_dim), f32),
            jax.ShapeDtypeStruct((tokens, width), bf),
        ),
        in_specs=[vmem, anywhere, vmem, vmem] + [anywhere] * 6 + [vmem] * 7,
        out_specs=(vmem,) + (anywhere,) * 5 + (vmem, vmem, anywhere, vmem, anywhere),
        scratch_shapes=[
            pltpu.VMEM(query_weight.shape, bf),
            pltpu.VMEM(key_weight.shape, bf),
            pltpu.VMEM(value_weight.shape, bf),
            pltpu.VMEM(out_weight.shape, bf),
            pltpu.VMEM((tokens, width), bf),
            pltpu.VMEM((2, quarter, width), bf),
            pltpu.VMEM((quarter, width), bf),
            pltpu.VMEM((quarter, width), bf),
            dma((2, 2, size - 1, 2)),
            dma((2, 2, size - 1, 2)),
            dma((2, 3)),
            dma((5,)),
            dma((2, 3 * local)),
            dma((2, 6 * local)),
            dma((2, 6 * local)),
            dma((6,)),
            pltpu.VMEM((size, quarter, width), bf),
            pltpu.VMEM((size, quarter, columns), bf),
            pltpu.VMEM((tokens, lead), bf),
            pltpu.VMEM((tokens, lead), bf),
            pltpu.VMEM((tokens, lead), f32),
            pltpu.VMEM((tokens, width), bf),
        ],
        compiler_params=pltpu.CompilerParams(
            collective_id=0, has_side_effects=True, vmem_limit_bytes=VMEM_LIMIT
        ),
        name="start_layer",
    )(*arguments)


def run_experts_body(
    size,
    local_experts,
    experts,
    inputs_hbm,
    packs_hbm,
    gate_up_ref,
    down_ref,
    others_ref,
    member_ref,
    middle_ref,
    gain_ref,
    hidden_out,
    kept_ref,
    given_ref,
    cross_ref,
    landing_ref,
    gmid_ref,
    gmid_all,
    gain_out,
    weights,
    hidden,
    grad_parts,
    mix_parts,
    grad_slots,
    mix_slots,
    turned,
    stage,
    landed,
    totals,
    load_sems,
    grad_sems,
    mix_sems,
    side_sems,
    store_sems,
    give_sems,
    land_sems,
    token_sems,
    inputs_ref,
    packs_ref,
):
    f32, bf = jnp.float32, jnp.bfloat16
    dp = lax.axis_index("dp")
    own, partner, across = tensor_peers()
    width = inputs_ref.shape[1]
    quarter = inputs_ref.shape[0] // size
    pair = 2 * quarter
    half = size // 2
    units = weights.shape[1]
    members = others_ref.shape[0] + 1
    span = units // members
    wide = 512
    place = ring_place(dp, size)

    def token_loads(index):
        rows = pl.ds(pl.multiple_of(index * pair, pair), pair)
        return (
            pltpu.make_async_copy(inputs_hbm.at[rows], inputs_ref.at[rows], token_sems.at[0, index]),
            pltpu.make_async_copy(packs_hbm.at[rows], packs_ref.at[rows], token_sems.at[1, index]),
        )

    for copy in token_loads(0):
        copy.start()
    forward = (ring_index(place + 1, size), own)
    backward = (ring_index(place + size - 1, size), own)
    greet([forward, backward, (dp, partner), (dp, across)])
    part_units = span // local_experts
    loads = []
    for expert in range(local_experts):
        rows = pl.ds(expert * part_units, part_units)
        for kind in range(3):
            source = gate_up_ref.at[expert, kind] if kind < 2 else down_ref.at[expert]
            loads.append((expert * part_units, source, weights.at[kind, rows]))
    for other in range(members - 1):
        for first in range(0, span, LANES):
            at = (other + 1) * span + first
            source = others_ref.at[other, :, pl.ds(first, LANES)]
            loads.append((at, source, weights.at[:, pl.ds(at, LANES)]))
    loads = [
        (at, pltpu.make_async_copy(source, target, load_sems.at[number]))
        for number, (at, source, target) in enumerate(loads)
    ]
    for _, copy in loads:
        copy.start()
    for index in range(1, half):
        for copy in token_loads(index):
            copy.start()

    grad_ring = (grad_parts, grad_slots, grad_sems)
    mix_ring = (mix_parts, mix_slots, mix_sems)

    ring_parts = 2
    way_rows = quarter // 2
    piece_rows = way_rows // ring_parts

    def ring_copy(ring, way, step, part, source):
        device = forward if way == 0 else backward
        _, slots, sems = ring
        rows = pl.ds(part * piece_rows, piece_rows)
        return push(
            source.at[rows],
            slots.at[way, step, rows],
            (sems.at[0, way, step, part], sems.at[1, way, step, part]),
            device,
        )

    def ring_step(ring, step, blocks, first=False):
        parts, slots, _ = ring
        for part in range(ring_parts):
            for way in (0, 1):
                if first:
                    source = parts.at[blocks[way], pl.ds(way * way_rows, way_rows)]
                else:
                    source = slots.at[way, step - 1]
                    ring_copy(ring, way, step - 1, part, source).wait_recv()

                    def add(rows):
                        rows = pl.ds(pl.multiple_of(rows.start + part * piece_rows, 16), rows.size)
                        there = pl.ds(pl.multiple_of(rows.start + way * way_rows, 16), rows.size)
                        slots[way, step - 1, rows, :] = (
                            slots[way, step - 1, rows, :].astype(f32)
                            + parts[blocks[way], there, :].astype(f32)
                        ).astype(bf)

                    row_loop(piece_rows, 16, add)
                ring_copy(ring, way, step, part, source).start()

    def ring_last(ring):
        for part in range(ring_parts):
            for way in (0, 1):
                ring_copy(ring, way, size - 2, part, ring[1].at[way, size - 2]).wait_recv()

    def do_pair(index, carry):
        rows = pl.ds(pl.multiple_of(index * pair, pair), pair)
        for copy in token_loads(index):
            copy.wait()
        tail = packs_ref[rows, width:].astype(f32)
        lane = lax.broadcasted_iota(jnp.int32, tail.shape, 1)
        shares = []
        for expert in range(local_experts):
            name = dp * local_experts + expert
            picked = (lane == name) | (lane == experts + name)
            shares.append(jnp.sum(jnp.where(picked, tail, 0.0), axis=1, keepdims=True))

        def do_units(tile, carry):
            here = pl.ds(pl.multiple_of(tile * wide, wide), wide)

            for number in range(units // wide):

                @pl.when((index == 0) & (tile == number))
                def _():
                    for at, copy in loads:
                        if at // wide == number:
                            copy.wait()

            scale = shares[0] * member_ref[0:1, here]
            for expert in range(1, local_experts):
                scale = scale + shares[expert] * member_ref[expert : expert + 1, here]
            tokens = inputs_ref[rows, :]
            gate = matmul_nt(tokens, weights[0, here, :])
            upward = matmul_nt(tokens, weights[1, here, :])
            grads = scale * matmul_nt(packs_ref[rows, :width], weights[2, here, :])
            share = jax.nn.sigmoid(gate)
            silu = gate * share
            hidden[0, rows, here] = (grads * upward * share * (1.0 + gate * (1.0 - share))).astype(bf)
            hidden[1, rows, here] = (grads * silu).astype(bf)
            hidden[2, rows, here] = (scale * silu * upward).astype(bf)
            return carry

        lax.fori_loop(0, units // wide, do_units, 0)

        def do_columns(tile, carry):
            here = pl.ds(pl.multiple_of(tile * wide, wide), wide)
            sums = matmul(hidden[0, rows, :], weights[0, :, here]) + matmul(
                hidden[1, rows, :], weights[1, :, here]
            )
            low = sums.astype(bf)
            grad_parts[2 * index, :, here] = low[:quarter]
            grad_parts[2 * index + 1, :, here] = low[quarter:]
            return carry

        def do_mix(tile, carry):
            here = pl.ds(pl.multiple_of(tile * wide, wide), wide)
            low = matmul(hidden[2, rows, :], weights[2, :, here]).astype(bf)
            mix_parts[2 * index, :, here] = low[:quarter]
            mix_parts[2 * index + 1, :, here] = low[quarter:]
            return carry

        lax.fori_loop(0, width // wide, do_columns, 0)

        def go_on(ring):
            @pl.when(index == 0)
            def _():
                ring_step(ring, 0, (0, 1), first=True)

            @pl.when(index > 0)
            def _():
                ring_step(ring, index, (2 * index, 2 * index + 1 - index // (half - 1)))

        go_on(grad_ring)
        lax.fori_loop(0, width // wide, do_mix, 0)
        go_on(mix_ring)
        return carry

    lax.fori_loop(0, half, do_pair, 0)
    group_units = (3, 1, 2, 0)
    targets = (landing_ref, given_ref, cross_ref, kept_ref)

    def tile_copies(group, kind, slot):
        copies = []
        for expert in range(local_experts):
            at = expert + 2 * local_experts if isinstance(kind, int) else 2 * expert + kind
            source = stage.at[slot, pl.ds(expert * part_units, part_units)]
            target = targets[group].at[at]
            if group < 2:
                sems = (give_sems.at[0, group, at], give_sems.at[1, group, at])
                copies.append(push(source, target, sems, (dp, partner)))
            else:
                copies.append(pltpu.make_async_copy(source, target, store_sems.at[group - 2, at]))
        return copies

    def tile_left(group, kind, slot):
        for copy in tile_copies(group, kind, slot):
            if group < 2:
                copy.wait_send()
            else:
                copy.wait()

    def land(kind):
        copies = []
        for expert in range(local_experts):
            at = expert + 2 * local_experts if isinstance(kind, int) else 2 * expert + kind
            rows = pl.ds(expert * part_units, part_units)
            copies.append(
                pltpu.make_async_copy(landing_ref.at[at], landed.at[rows], land_sems.at[expert])
            )
        return copies

    def tile(group, kind, source, before):
        number = 3 * group + kind
        slot = number % 2
        if before is not None:
            before(slot)
        if group == 2:
            for copy in tile_copies(0, kind, slot):
                copy.wait_recv()
            for copy in land(kind):
                copy.start()
        rows = pl.ds(group_units[group] * span, span)
        for chunk in range(half):
            some = pl.ds(chunk * pair, pair)
            turned[:, some] = hidden[kind, some, rows].T
        if group == 2:
            for copy in land(kind):
                copy.wait()

        def do_columns(tile, carry):
            here = pl.ds(pl.multiple_of(tile * wide, wide), wide)
            sums = matmul(turned[...], source[:, here])
            if group == 2:
                sums = sums + landed[:, here].astype(f32)
            stage[slot, :, here] = sums.astype(bf)
            return carry

        lax.fori_loop(0, width // wide, do_columns, 0)
        for copy in tile_copies(group, kind, slot):
            copy.start()

    def token_tiles(group):
        def run(kind, carry):
            if group == 0:
                before = None
            else:
                def before(slot):
                    @pl.when(kind == 0)
                    def _():
                        tile_left(group - 1, kind + 1, slot)

                    @pl.when(kind == 1)
                    def _():
                        tile_left(group - 1, 2, slot)

            tile(group, kind, inputs_ref, before)
            return carry

        lax.fori_loop(0, 2, run, 0)

    def grad_tile(group):
        def before(slot):
            tile_left(group, jnp.int32(0), slot)

        tile(group, 2, packs_ref, before)

    def final_sum():
        totals[...] = jnp.zeros_like(totals)
        ring_last(grad_ring)
        base = own * quarter

        def finish(way, inner):
            rows = pl.ds(pl.multiple_of(inner.start + way * way_rows, 16), inner.size)
            sums = grad_slots[way, size - 2, inner, :].astype(f32) + grad_parts[
                size - 1, rows, :
            ].astype(f32)
            middle = middle_ref[rows, :]
            inverse = lax.rsqrt(jnp.mean(middle * middle, axis=-1, keepdims=True) + EPSILON)
            hat = middle * inverse
            product = sums * hat
            totals[...] += product[:8] + product[8:]
            scaled = sums * gain_ref[...]
            back = inverse * (scaled - hat * jnp.mean(scaled * hat, axis=-1, keepdims=True))
            above = packs_ref[
                pl.ds(pl.multiple_of((size - 1) * quarter + rows.start, 16), rows.size), :width
            ]
            grad = above.astype(f32) + back
            gmid_ref[rows, :] = grad
            gmid_all[pl.ds(pl.multiple_of(base + rows.start, 16), rows.size), :] = grad.astype(bf)

        for way in (0, 1):
            row_loop(way_rows, 16, functools.partial(finish, way))
        gain_out[...] = jnp.sum(totals[...], axis=0, keepdims=True)

    def rows_of(index):
        return pl.ds(pl.multiple_of(index * quarter, quarter), quarter)

    def spread(index, whose, device):
        ref = gmid_all.at[rows_of(whose)]
        return push(ref, ref, (side_sems.at[0, index], side_sems.at[1, index]), device)

    def first_spread():
        spread(0, own, (dp, across)).start()
        spread(1, own, (dp, partner)).start()

    def second_spread():
        spread(0, own, (dp, across)).wait_recv()
        spread(2, across, (dp, partner)).start()

    def final_mix():
        ring_last(mix_ring)

        def finish(way, inner):
            rows = pl.ds(pl.multiple_of(inner.start + way * way_rows, 16), inner.size)
            hidden_out[rows, :] = (
                middle_ref[rows, :]
                + mix_slots[way, size - 2, inner, :].astype(f32)
                + mix_parts[size - 1, rows, :].astype(f32)
            ).astype(bf)

        for way in (0, 1):
            row_loop(way_rows, 16, functools.partial(finish, way))

    def closing():
        final_sum()
        first_spread()

    grad_events, mix_events = [], []
    for step in range(half, size - 1):
        delta = -(1 + step)
        blocks = (slot_of(delta, size), slot_of(-delta, size))
        grad_events.append(functools.partial(ring_step, grad_ring, step, blocks))
        mix_events.append(functools.partial(ring_step, mix_ring, step, blocks))
    events = [grad_events[0]]
    for first, second in zip(grad_events[1:], mix_events):
        events += [first, second]
    events += [closing, mix_events[-1], second_spread, final_mix]
    work = []
    for group in range(4):
        work.append(functools.partial(token_tiles, group))
        work.append(functools.partial(grad_tile, group))
    done = 0
    for number, piece in enumerate(work):
        piece()
        upto = -(-(number + 1) * len(events) // len(work))
        while done < upto:
            events[done]()
            done += 1
    tile_left(3, jnp.int32(1), 0)
    tile_left(3, 2, 1)
    for kind in (jnp.int32(0), jnp.int32(1), 2):
        for copy in tile_copies(1, kind, 0):
            copy.wait_recv()
    spread(1, own, (dp, partner)).wait_recv()
    spread(2, across, (dp, partner)).wait_recv()
    for index, device in ((0, across), (1, partner), (2, partner)):
        spread(index, own, (dp, device)).wait_send()
    for ring in (grad_ring, mix_ring):
        for way in (0, 1):
            for step in range(size - 1):
                for part in range(ring_parts):
                    ring_copy(ring, way, step, part, ring[1].at[way, step]).wait_send()


def run_experts(size, inputs, packs, gate_up, down, others, middle, gain, experts):
    bf, f32 = jnp.bfloat16, jnp.float32
    local_experts, _, part_units, width = gate_up.shape
    others = others.reshape(3, 3, local_experts * part_units, width)
    members, span = 4, local_experts * part_units
    rows = inputs.shape[0]
    quarter = rows // size
    units = members * span
    expert_of = (np.arange(units) // (span // local_experts)) % local_experts
    member = jnp.asarray(expert_of[None, :] == np.arange(local_experts)[:, None], f32)
    vmem = pl.BlockSpec(memory_space=pltpu.VMEM)
    anywhere = pl.BlockSpec(memory_space=pl.ANY)
    dma = pltpu.SemaphoreType.DMA
    return pl.pallas_call(
        functools.partial(run_experts_body, size, local_experts, experts),
        out_shape=(
            jax.ShapeDtypeStruct((quarter, width), bf),
            jax.ShapeDtypeStruct((3 * local_experts, part_units, width), bf),
            jax.ShapeDtypeStruct((3 * local_experts, part_units, width), bf),
            jax.ShapeDtypeStruct((3 * local_experts, part_units, width), bf),
            jax.ShapeDtypeStruct((3 * local_experts, part_units, width), bf),
            jax.ShapeDtypeStruct((quarter, width), f32),
            jax.ShapeDtypeStruct((members * quarter, width), bf),
            jax.ShapeDtypeStruct((1, width), f32),
        ),
        in_specs=[anywhere] * 5 + [vmem] * 3,
        out_specs=(vmem,) + (anywhere,) * 4 + (vmem,) * 3,
        scratch_shapes=[
            pltpu.VMEM((3, units, width), bf),
            pltpu.VMEM((3, rows, units), bf),
            pltpu.VMEM((size, quarter, width), bf),
            pltpu.VMEM((size, quarter, width), bf),
            pltpu.VMEM((2, size - 1, quarter // 2, width), bf),
            pltpu.VMEM((2, size - 1, quarter // 2, width), bf),
            pltpu.VMEM((span, rows), bf),
            pltpu.VMEM((2, span, width), bf),
            pltpu.VMEM((span, width), bf),
            pltpu.VMEM((8, width), f32),
            dma((3 * local_experts + 3 * span // LANES,)),
            dma((2, 2, size - 1, 2)),
            dma((2, 2, size - 1, 2)),
            dma((2, 3)),
            dma((2, 3 * local_experts)),
            dma((2, 2, 3 * local_experts)),
            dma((local_experts,)),
            dma((2, size // 2)),
            pltpu.VMEM(inputs.shape, bf),
            pltpu.VMEM(packs.shape, bf),
        ],
        compiler_params=pltpu.CompilerParams(
            collective_id=2, has_side_effects=True, vmem_limit_bytes=VMEM_LIMIT
        ),
        name="run_experts",
    )(inputs, packs, gate_up, down, others, member, middle, gain.reshape(1, -1))


def back_through_head(grads, raw, gain, cosine, sine):
    hat_grads = grads * cosine - pltpu.roll(grads, grads.shape[1] // 2, 1) * sine
    inverse = lax.rsqrt(jnp.mean(raw * raw, axis=-1, keepdims=True) + EPSILON)
    hat = raw * inverse
    terms = hat_grads * hat
    scaled = hat_grads * gain
    back = inverse * (scaled - hat * jnp.mean(scaled * hat, axis=-1, keepdims=True))
    return back.astype(jnp.bfloat16), terms


def finish_layer_body(
    size,
    gmid_low_hbm,
    out_weight_hbm,
    mixed_hbm,
    query_hbm,
    key_hbm,
    value_hbm,
    raw_query_hbm,
    raw_key_hbm,
    normed_hbm,
    query_weight_hbm,
    key_weight_hbm,
    value_weight_hbm,
    cosine_ref,
    sine_ref,
    start_ref,
    query_gain_ref,
    key_gain_ref,
    middle_ref,
    token_hbm,
    hidden_ref,
    cross_ref,
    gain_ref,
    gains_ref,
    hidden_all,
    crossed_ref,
    grad_all,
    query_out,
    key_out,
    value_out,
    outer_out,
    first_out,
    second_out,
    query_gain_out,
    key_gain_out,
    qkv_ref,
    out_ref,
    slots_a,
    slots_b,
    grad_mixed,
    grad_heads,
    key_sums,
    value_sums,
    turned,
    partial,
    from_partner,
    from_across,
    joined,
    totals,
    head_totals,
    pair_gains,
    ring_gains,
    sems_a,
    sems_b,
    ring_sems,
    side_sems,
    load_sems,
    store_sems,
    gather_a,
    gather_b,
    token_ref,
    gmid_low_ref,
    out_weight_ref,
    mixed_ref,
    query_ref,
    key_ref,
    value_ref,
    raw_query_ref,
    raw_key_ref,
    normed_ref,
    query_weight_ref,
    key_weight_ref,
    value_weight_ref,
):
    f32, bf = jnp.float32, jnp.bfloat16
    dp = lax.axis_index("dp")
    own, partner, across = tensor_peers()
    far_partner = (partner + 2) % 4
    quarter, width = token_ref.shape
    tokens = normed_ref.shape[0]
    head_dim = key_ref.shape[1]
    lead = query_ref.shape[1]
    heads = lead // head_dim
    scale = head_dim**-0.5
    place = ring_place(dp, size)
    forward = (ring_index(place + 1, size), own)
    backward = (ring_index(place + size - 1, size), own)
    ways = ((forward, 1), (backward, -1))
    mine = pl.ds(pl.multiple_of(own * quarter, quarter), quarter)
    home = own * quarter
    loads = {}
    for source, target in (
        (gmid_low_hbm, gmid_low_ref),
        (mixed_hbm, mixed_ref),
        (out_weight_hbm, out_weight_ref),
        (query_hbm, query_ref),
        (key_hbm, key_ref),
        (value_hbm, value_ref),
        (raw_query_hbm, raw_query_ref),
        (raw_key_hbm, raw_key_ref),
        (normed_hbm, normed_ref),
        (query_weight_hbm, query_weight_ref),
        (key_weight_hbm, key_weight_ref),
        (value_weight_hbm, value_weight_ref),
        (token_hbm.at[mine], token_ref),
    ):
        copy = pltpu.make_async_copy(source, target, load_sems.at[len(loads)])
        copy.start()
        loads[id(target)] = copy

    def loaded(*targets):
        for target in targets:
            loads[id(target)].wait()

    greet([forward, backward, (dp, partner), (dp, across)])
    waits = []

    def start(copy):
        copy.start()
        waits.append(copy)
        return copy

    sets = (
        (qkv_ref, slots_a, gather_a, sems_a),
        (out_ref, slots_b, gather_b, sems_b),
    )

    def wrap(value):
        return (value + 2 * size) % size

    live = {}

    ring_parts = 2 if lead // size % 64 == 0 else 1
    stores = []

    def ring_rows(ref):
        rows = ref.shape[0] // size
        return rows, rows // 2, rows // 2 // ring_parts

    def add_own(which, way, step, part):
        ref, slots, blocks, _ = sets[which]
        live[which, way, step, part].wait_recv()
        rows, half, count = ring_rows(ref)
        base = wrap(place - ways[way][1] * (2 + step)) * rows + way * half

        def add(inner):
            inner = pl.ds(pl.multiple_of(inner.start + part * count, 16), inner.size)
            there = pl.ds(pl.multiple_of(base + inner.start, 16), inner.size)
            sums = (slots[way, step, inner, :].astype(f32) + ref[there, :].astype(f32)).astype(bf)
            if step == size - 2:
                final = pl.ds(pl.multiple_of(inner.start + way * half, 16), inner.size)
                blocks[place, final, :] = sums
            else:
                slots[way, step, inner, :] = sums

        row_loop(count, 16, add)

    def keep_block(which, way, block, part):
        ref, _, blocks, _ = sets[which]
        rows, half, count = ring_rows(ref)
        inner = pl.ds(way * half + part * count, count)
        there = pl.ds(pl.multiple_of(block * rows + way * half + part * count, 16), count)
        if which == 1:
            targets = [(outer_out, 0, width)]
        else:
            targets = [
                (query_out, 0, lead),
                (key_out, lead, head_dim),
                (value_out, lead + head_dim, head_dim),
            ]
        for target, first, columns in targets:
            source = blocks.at[block, inner, pl.ds(first, columns)]
            copy = pltpu.make_async_copy(source, target.at[there], store_sems.at[len(stores)])
            copy.start()
            stores.append(copy)

    def ring_event(which, step):
        ref, slots, blocks, sems = sets[which]
        rows, half, count = ring_rows(ref)
        for part in range(ring_parts):
            inner = pl.ds(part * count, count)
            for way, (device, sign) in enumerate(ways):
                if step == 0:
                    at = wrap(place - sign) * rows + way * half + part * count
                    source = ref.at[pl.ds(pl.multiple_of(at, 16), count)]
                elif step < size:
                    add_own(which, way, step - 1, part)
                    source = slots.at[way, step - 1, inner] if step < size - 1 else None
                else:
                    live[which, way, step - 1, part].wait_recv()
                block = wrap(place - sign * (step - size + 1))
                if step >= size - 1:
                    keep_block(which, way, block, part)
                if step >= 2 * size - 2:
                    continue
                if step >= size - 1:
                    source = blocks.at[block, pl.ds(way * half + part * count, count)]
                    target = source
                else:
                    target = slots.at[way, step, inner]
                sem = (sems.at[0, way, step, part], sems.at[1, way, step, part])
                live[which, way, step, part] = start(push(source, target, sem, device))

    def part_rows(index):
        return pl.ds(pl.multiple_of(index * quarter, quarter), quarter)

    def side(index):
        return (side_sems.at[0, index], side_sems.at[1, index])

    step_rows = 2 * LANES
    wide = 4 * LANES

    def out_rows(index, carry):
        rows = pl.ds(pl.multiple_of(index * step_rows, step_rows), step_rows)
        turned[...] = mixed_ref[:, rows].T

        def columns(tile, carry):
            here = pl.ds(pl.multiple_of(tile * wide, wide), wide)
            out_ref[rows, here] = matmul(turned[...], gmid_low_ref[:, here]).astype(bf)
            return carry

        return lax.fori_loop(0, width // wide, columns, carry)

    loaded(gmid_low_ref, mixed_ref)
    lax.fori_loop(0, lead // step_rows, out_rows, 0)
    ring_event(1, 0)

    def keep(rows):
        hidden_all[pl.ds(pl.multiple_of(home + rows.start, 16), rows.size), :] = hidden_ref[rows, :]

    row_loop(quarter, 16, keep)
    shown = [start(push(hidden_ref, hidden_all.at[mine], side(9), (dp, across)))]
    shown.append(start(push(hidden_ref, hidden_all.at[mine], side(10), (dp, partner))))

    def mixed_columns(tile, carry):
        here = pl.ds(pl.multiple_of(tile * wide, wide), wide)
        grad_mixed[:, here] = matmul_nt(gmid_low_ref[...], out_weight_ref[here, :]).astype(bf)
        return carry

    loaded(out_weight_ref)
    lax.fori_loop(0, lead // wide, mixed_columns, 0)
    loaded(query_ref, key_ref, value_ref, raw_query_ref, raw_key_ref)
    key_sums[...] = jnp.zeros_like(key_sums)
    value_sums[...] = jnp.zeros_like(value_sums)
    head_totals[...] = jnp.zeros_like(head_totals)
    block = tokens // 2

    def do_head(head, carry):
        lanes = pl.ds(pl.multiple_of(head * head_dim, head_dim), head_dim)
        for part in (0, 1):
            rows = pl.ds(part * block, block)
            count = (part + 1) * block
            keys = pl.ds(0, count)
            queries = query_ref[rows, lanes]
            outer = grad_mixed[rows, lanes]
            scores = matmul_nt(key_ref[keys, :], queries)
            key_at = lax.broadcasted_iota(jnp.int32, scores.shape, 0)
            query_at = lax.broadcasted_iota(jnp.int32, scores.shape, 1) + part * block
            seen = (key_at <= query_at) & (key_at >= start_ref[:, rows])
            exponent = jnp.where(seen, jnp.exp(scores * scale), 0.0)
            soft = exponent * (1.0 / jnp.sum(exponent, axis=0, keepdims=True))
            grad_soft = matmul_nt(value_ref[keys, :], outer)
            inner = jnp.sum(soft * grad_soft, axis=0, keepdims=True)
            grad_scores = (soft * (grad_soft - inner)).astype(bf)
            value_sums[keys, :] += matmul(soft.astype(bf), outer)
            key_sums[keys, :] += matmul(grad_scores, queries)
            grad_query = scale * lax.dot_general(
                grad_scores, key_ref[keys, :], (((0,), (0,)), ((), ())), preferred_element_type=f32
            )
            low, terms = back_through_head(
                grad_query, raw_query_ref[rows, lanes], query_gain_ref[...], cosine_ref[rows, :], sine_ref[rows, :]
            )
            grad_heads[rows, lanes] = low
            head_totals[0] += jnp.sum(terms.reshape(-1, 8, head_dim), axis=0)
        return carry

    lax.fori_loop(0, heads // 4, do_head, 0)
    ring_event(1, 1)
    lax.fori_loop(heads // 4, 5 * heads // 8, do_head, 0)
    ring_event(1, 2)
    lax.fori_loop(5 * heads // 8, heads, do_head, 0)
    ring_event(1, 3)
    low, terms = back_through_head(
        scale * key_sums[...], raw_key_ref[...], key_gain_ref[...], cosine_ref[...], sine_ref[...]
    )
    grad_heads[:, pl.ds(lead, head_dim)] = low
    head_totals[1] += jnp.sum(terms.reshape(-1, 8, head_dim), axis=0)
    grad_heads[:, pl.ds(lead + head_dim, head_dim)] = value_sums[...].astype(bf)

    def in_rows(index, carry):
        rows = pl.ds(pl.multiple_of(index * step_rows, step_rows), step_rows)
        turned[...] = normed_ref[:, rows].T
        qkv_ref[rows, :] = matmul(turned[...], grad_heads[...]).astype(bf)
        return carry

    loaded(normed_ref)
    lax.fori_loop(0, width // step_rows, in_rows, 0)
    ring_event(1, 4)
    ring_event(0, 0)

    def token_columns(tile, carry):
        here = pl.ds(pl.multiple_of(tile * wide, wide), wide)
        sums = matmul_nt(grad_heads[:, :lead], query_weight_ref[here, :])
        sums = sums + matmul_nt(grad_heads[:, lead : lead + head_dim], key_weight_ref[here, :])
        sums = sums + matmul_nt(grad_heads[:, lead + head_dim :], value_weight_ref[here, :])
        partial[:, here] = sums.astype(bf)
        return carry

    loaded(query_weight_ref, key_weight_ref, value_weight_ref)
    lax.fori_loop(0, width // wide, token_columns, 0)
    first = start(push(partial.at[part_rows(far_partner)], from_partner.at[1], side(0), (dp, partner)))
    second = start(push(partial.at[part_rows(partner)], from_partner.at[0], side(1), (dp, partner)))
    ring_event(1, 5)
    first.wait_recv()
    away = across * quarter

    def join(rows):
        there = pl.ds(pl.multiple_of(away + rows.start, 16), rows.size)
        joined[rows, :] = (partial[there, :].astype(f32) + from_partner[1, rows, :].astype(f32)).astype(bf)

    row_loop(quarter, 16, join)
    third = start(push(joined, from_across, side(2), (dp, across)))
    ring_event(0, 1)
    ring_event(1, 6)
    second.wait_recv()
    third.wait_recv()
    totals[...] = jnp.zeros_like(totals)

    def finish(rows):
        there = pl.ds(pl.multiple_of(home + rows.start, 16), rows.size)
        grads = (
            partial[there, :].astype(f32)
            + from_partner[0, rows, :].astype(f32)
            + from_across[rows, :].astype(f32)
        )
        hidden = token_ref[rows, :].astype(f32)
        inverse = lax.rsqrt(jnp.mean(hidden * hidden, axis=-1, keepdims=True) + EPSILON)
        hat = hidden * inverse
        product = grads * hat
        totals[...] += product[:8] + product[8:]
        scaled = grads * gain_ref[...]
        back = inverse * (scaled - hat * jnp.mean(scaled * hat, axis=-1, keepdims=True))
        grad_all[there, :] = (middle_ref[rows, :] + back).astype(bf)

    loaded(token_ref)
    row_loop(quarter, 16, finish)
    spread = [start(push(grad_all.at[mine], grad_all.at[mine], side(3), (dp, across)))]
    spread.append(start(push(grad_all.at[mine], grad_all.at[mine], side(4), (dp, partner))))
    pair_gains[0, :, :width] = jnp.sum(totals[...], axis=0, keepdims=True)
    pair_gains[0, :, width : 2 * width] = gains_ref[...]
    pair_gains[0, :, 2 * width : 2 * width + head_dim] = jnp.sum(head_totals[0], axis=0, keepdims=True)
    pair_gains[0, :, 2 * width + head_dim :] = jnp.sum(head_totals[1], axis=0, keepdims=True)
    swap = start(push(pair_gains.at[0], pair_gains.at[1], side(5), (dp, partner)))
    ring_event(0, 2)
    ring_event(1, 7)
    far = part_rows(across)
    shown[0].wait_recv()
    shown.append(start(push(hidden_all.at[far], hidden_all.at[far], side(11), (dp, partner))))
    spread[0].wait_recv()
    spread.append(start(push(grad_all.at[far], grad_all.at[far], side(6), (dp, partner))))
    swap.wait_recv()
    pair_gains[2] = pair_gains[0] + pair_gains[1]
    swap = start(push(pair_gains.at[2], pair_gains.at[3], side(7), (dp, across)))
    ring_event(0, 3)
    ring_event(1, 8)
    swap.wait_recv()
    crossing = start(push(cross_ref, crossed_ref, side(8), (dp, across)))
    ring_gains[place] = pair_gains[2] + pair_gains[3]
    small = None
    for step in range(4, 2 * size - 1):
        ring_event(0, step)
        if step + 5 < 2 * size - 1:
            ring_event(1, step + 5)
        if step - 4 < size - 1:
            if small is not None:
                small.wait_recv()
            ref = ring_gains.at[wrap(place - step + 4)]
            sem = (ring_sems.at[0, step - 4], ring_sems.at[1, step - 4])
            small = start(push(ref, ref, sem, forward))
    small.wait_recv()
    gains = jnp.sum(ring_gains[...], axis=0)
    first_out[...] = gains[:, :width]
    second_out[...] = gains[:, width : 2 * width]
    query_gain_out[...] = gains[:, 2 * width : 2 * width + head_dim]
    key_gain_out[...] = gains[:, 2 * width + head_dim :]
    for copy in (spread[1], spread[2], shown[1], shown[2], crossing):
        copy.wait_recv()
    for copy in waits:
        copy.wait_send()
    for copy in stores:
        copy.wait()


def finish_layer(size, *arguments):
    bf, f32 = jnp.bfloat16, jnp.float32
    (
        _, out_weight, mixed, query, key, _, _, _, normed, query_weight, _, _, _, _, _, _, _, _, token_rows, _,
        cross, _, _,
    ) = arguments
    tokens, width = token_rows.shape
    quarter = tokens // 4
    lead, head_dim = query.shape[1], key.shape[1]
    vmem = pl.BlockSpec(memory_space=pltpu.VMEM)
    anywhere = pl.BlockSpec(memory_space=pl.ANY)
    dma = pltpu.SemaphoreType.DMA
    columns = lead + 2 * head_dim
    rows_a, rows_b = width // size, lead // size
    count = 2 * width + 2 * head_dim
    return pl.pallas_call(
        functools.partial(finish_layer_body, size),
        out_shape=(
            jax.ShapeDtypeStruct((tokens, width), bf),
            jax.ShapeDtypeStruct(cross.shape, bf),
            jax.ShapeDtypeStruct((tokens, width), bf),
            jax.ShapeDtypeStruct((width, lead), bf),
            jax.ShapeDtypeStruct((width, head_dim), bf),
            jax.ShapeDtypeStruct((width, head_dim), bf),
            jax.ShapeDtypeStruct((lead, width), bf),
            jax.ShapeDtypeStruct((1, width), f32),
            jax.ShapeDtypeStruct((1, width), f32),
            jax.ShapeDtypeStruct((1, head_dim), f32),
            jax.ShapeDtypeStruct((1, head_dim), f32),
        ),
        in_specs=[anywhere] * 12 + [vmem] * 6 + [anywhere, vmem, anywhere, vmem, vmem],
        out_specs=(vmem, anywhere, vmem) + (anywhere,) * 4 + (vmem,) * 4,
        scratch_shapes=[
            pltpu.VMEM((width, columns), bf),
            pltpu.VMEM((lead, width), bf),
            pltpu.VMEM((2, size - 1, rows_a // 2, columns), bf),
            pltpu.VMEM((2, size - 1, rows_b // 2, width), bf),
            pltpu.VMEM((tokens, lead), bf),
            pltpu.VMEM((tokens, columns), bf),
            pltpu.VMEM((tokens, head_dim), f32),
            pltpu.VMEM((tokens, head_dim), f32),
            pltpu.VMEM((2 * LANES, tokens), bf),
            pltpu.VMEM((tokens, width), bf),
            pltpu.VMEM((2, quarter, width), bf),
            pltpu.VMEM((quarter, width), bf),
            pltpu.VMEM((quarter, width), bf),
            pltpu.VMEM((8, width), f32),
            pltpu.VMEM((2, 8, head_dim), f32),
            pltpu.VMEM((4, 1, count), f32),
            pltpu.VMEM((size, 1, count), f32),
            dma((2, 2, 2 * size - 2, 2)),
            dma((2, 2, 2 * size - 2, 2)),
            dma((2, size - 1)),
            dma((2, 12)),
            dma((13,)),
            dma((16 * size,)),
            pltpu.VMEM((size, rows_a, columns), bf),
            pltpu.VMEM((size, rows_b, width), bf),
            pltpu.VMEM((quarter, width), bf),
        ]
        + [pltpu.VMEM(argument.shape, argument.dtype) for argument in arguments[:12]],
        compiler_params=pltpu.CompilerParams(
            collective_id=1, has_side_effects=True, vmem_limit_bytes=VMEM_LIMIT
        ),
        name="finish_layer",
    )(*arguments)


def widen_body(refs):
    f32 = jnp.float32
    for source, target in zip(refs[:4], refs[12:16]):
        target[...] = source[...].astype(f32)
    for first, target in ((4, refs[16]), (7, refs[17])):
        sums = refs[first][...].astype(f32) + refs[first + 1][...].astype(f32)
        target[...] = sums + refs[first + 2][...].astype(f32)
    refs[18][...] = refs[10][...]
    refs[19][...] = refs[11][...]


def widen(query, key, value, outer, shares, split, hidden, grads):
    f32 = jnp.float32
    steps = 4
    width = outer.shape[1]
    shares = [share.reshape(-1, width) for share in shares]
    rest = shares[0].shape[0] - split

    def rows(count, columns, first=0):
        block = count // steps
        assert count % steps == 0 and block % 16 == 0 and first % block == 0
        return pl.BlockSpec((block, columns), lambda step: (step + first // block, 0))

    plain = [rows(*array.shape) for array in (query, key, value, outer)]
    pair = [rows(*array.shape) for array in (hidden, grads)]
    first, second = rows(split, width), rows(rest, width)
    return pl.pallas_call(
        lambda *refs: widen_body(refs),
        grid=(steps,),
        out_shape=[jax.ShapeDtypeStruct(a.shape, f32) for a in (query, key, value, outer)]
        + [jax.ShapeDtypeStruct((split, width), f32), jax.ShapeDtypeStruct((rest, width), f32)]
        + [jax.ShapeDtypeStruct(a.shape, a.dtype) for a in (hidden, grads)],
        in_specs=plain + [first] * 3 + [rows(rest, width, split)] * 3 + pair,
        out_specs=plain + [first, second] + pair,
        compiler_params=pltpu.CompilerParams(vmem_limit_bytes=VMEM_LIMIT),
        name="widen",
    )(query, key, value, outer, *shares, *shares, hidden, grads)


def large_experts(size, inputs, packs, gate_up, down, others, middle, gain, experts):
    f32, bf = jnp.float32, jnp.bfloat16
    model_width = inputs.shape[1]
    own_weights = jnp.stack([gate_up[:, 0], gate_up[:, 1], down])
    all_weights = jnp.concatenate([own_weights[None], others])
    members = all_weights.shape[0]
    order = jnp.arange(members, dtype=jnp.int32) ^ lax.axis_index("tensor")
    all_weights = all_weights.reshape(members, 3, -1, model_width)[order]
    units = all_weights.shape[2]
    local_experts = experts // size
    indices = jnp.arange(size, dtype=jnp.int32)
    half = size // 2
    delta = (ring_place(indices, size) - ring_place(lax.axis_index("dp"), size)) % size
    ahead = jnp.where(delta == half, size - 2, jnp.where(delta == 0, size - 1, 2 * delta - 1))
    slots = jnp.where(delta > half, 2 * (size - delta) - 2, ahead)
    quarter = middle.shape[0]
    out_rows = packs[-quarter:, :model_width]
    inputs = inputs.reshape(size, quarter, -1)[slots].reshape(-1, model_width)
    packs = packs.reshape(size, quarter, -1)[slots].reshape(inputs.shape[0], -1)
    grads_all = packs[:, :model_width]
    shares = packs[:, model_width : model_width + 2 * experts].astype(f32)
    shares = shares[:, :experts] + shares[:, experts:]
    shares = lax.dynamic_slice_in_dim(
        shares, lax.axis_index("dp") * local_experts, local_experts, 1
    )
    weight_cols = jnp.broadcast_to(
        shares[:, None, :, None],
        (shares.shape[0], members, local_experts, units // local_experts),
    ).reshape(-1, members, units)

    def project(left, which):
        return jnp.einsum("td,rud->tru", left, all_weights[:, which], preferred_element_type=f32)

    gate_act = project(inputs, 0)
    upward = project(inputs, 1)
    sigmoid_gate = jax.nn.sigmoid(gate_act)
    active = gate_act * sigmoid_gate * upward
    weighted_low = (weight_cols * active).astype(bf)
    mixture_part = jnp.einsum(
        "tru,rud->td", weighted_low, all_weights[:, 2], preferred_element_type=f32
    ).astype(bf)
    grad_active = weight_cols * project(grads_all, 2)
    grad_gate = (
        grad_active * upward * sigmoid_gate * (1.0 + gate_act * (1.0 - sigmoid_gate))
    ).astype(bf)
    grad_up = (grad_active * gate_act * sigmoid_gate).astype(bf)
    grad_normed_part = jnp.einsum(
        "tru,rud->td", grad_gate, all_weights[:, 0], preferred_element_type=f32
    ) + jnp.einsum("tru,rud->td", grad_up, all_weights[:, 1], preferred_element_type=f32)
    grad_normed_two = lax.psum_scatter(grad_normed_part.astype(bf), "dp", tiled=True).astype(f32)
    weight_grads = jnp.stack(
        [
            jnp.einsum("tru,td->rud", grad_gate, inputs, preferred_element_type=f32).astype(bf),
            jnp.einsum("tru,td->rud", grad_up, inputs, preferred_element_type=f32).astype(bf),
            jnp.einsum("tru,td->rud", weighted_low, grads_all, preferred_element_type=f32).astype(bf),
        ],
        axis=1,
    )
    hat_two, inv_two = rms_parts(middle)
    grad_gain_two = jnp.sum(grad_normed_two * hat_two, axis=0)
    grad_middle = out_rows.astype(f32) + rms_back(grad_normed_two * gain, hat_two, inv_two)
    grad_mid_low = lax.all_gather(grad_middle.astype(bf), "tensor", tiled=True)
    mixture = lax.psum_scatter(mixture_part, "dp", tiled=True).astype(f32)
    hidden_out = (middle + mixture).astype(bf)
    sums = lax.psum_scatter(weight_grads.reshape(-1, model_width), "tensor", tiled=True)
    sums = sums.reshape(3, local_experts, -1, model_width)
    kept = jnp.concatenate(
        [jnp.swapaxes(sums[:2], 0, 1).reshape(2 * local_experts, -1, model_width), sums[2]]
    )
    zero = jnp.zeros_like(kept)
    return (hidden_out, kept, zero, zero, zero, grad_middle, grad_mid_low, grad_gain_two)


def local(
    hidden_in,
    seq_lens,
    norm1_gain,
    query_weight,
    key_weight,
    value_weight,
    query_gain,
    key_gain,
    out_weight,
    norm2_gain,
    w_gate_up,
    w_down,
    routes,
    route_weights,
    out_grad,
):
    bf = jnp.bfloat16
    f32 = jnp.float32
    tokens, model_width = hidden_in.shape
    local_experts = w_gate_up.shape[0]
    hidden_part = w_gate_up.shape[3]
    head_dim = query_gain.shape[0]
    data_size = lax.axis_size("dp")
    quarter = tokens // lax.axis_size("tensor")
    experts = local_experts * data_size
    rows = data_size * quarter
    places, starts = sequence_layout(seq_lens[0], tokens)
    cosines, sines = rotary_tables(places - starts, head_dim)
    starts = starts.reshape(1, -1).astype(jnp.int32)
    gate_up = jnp.transpose(w_gate_up, (0, 2, 3, 1))
    (
        middle,
        inputs,
        gathered,
        others,
        mixed_low,
        query_low,
        key_low,
        value_low,
        raw_query,
        raw_key,
        normed,
    ) = start_layer(
        data_size,
        experts,
        hidden_in,
        out_grad,
        routes.T,
        route_weights.T,
        query_weight,
        key_weight,
        value_weight,
        out_weight,
        gate_up,
        w_down,
        cosines,
        sines,
        starts,
        norm1_gain.reshape(1, -1),
        norm2_gain.reshape(1, -1),
        query_gain.reshape(1, -1),
        key_gain.reshape(1, -1),
    )
    stage = run_experts if data_size <= 8 else large_experts
    hidden_out, kept, given, joined, _, grad_middle, grad_mid_low, grad_gain_two = stage(
        data_size,
        inputs.reshape(rows, model_width),
        gathered.reshape(rows, -1),
        gate_up,
        w_down,
        others,
        middle,
        norm2_gain,
        experts,
    )
    hidden_out, crossed, grad_hidden, query_sum, key_sum, value_sum, out_sum, *gains = finish_layer(
        data_size,
        grad_mid_low,
        out_weight,
        mixed_low,
        query_low,
        key_low,
        value_low,
        raw_query,
        raw_key,
        normed,
        query_weight,
        key_weight,
        value_weight,
        cosines,
        sines,
        starts,
        query_gain.reshape(1, -1),
        key_gain.reshape(1, -1),
        grad_middle,
        hidden_in,
        hidden_out,
        joined,
        norm1_gain.reshape(1, -1),
        grad_gain_two.reshape(1, -1),
    )
    split = 2 * local_experts * hidden_part
    query_sum, key_sum, value_sum, out_sum, gate_up_sum, down_sum, hidden_out, grad_hidden = widen(
        query_sum, key_sum, value_sum, out_sum, (kept, given, crossed), split, hidden_out, grad_hidden
    )
    grad_w_gate_up = jnp.transpose(
        gate_up_sum.reshape(local_experts, 2, hidden_part, model_width), (0, 3, 1, 2)
    )
    grad_w_down = down_sum.reshape(local_experts, hidden_part, model_width)
    gains = [gain.reshape(-1) for gain in gains]
    return (
        hidden_out,
        grad_hidden,
        gains[0],
        query_sum,
        key_sum,
        value_sum,
        gains[2],
        gains[3],
        out_sum,
        gains[1],
        grad_w_gate_up,
        grad_w_down,
    )


def solution(mesh):
    in_specs = (
        P("dp", None),
        P("dp", None),
        P(),
        P(None, "tensor"),
        P(None, "tensor"),
        P(None, "tensor"),
        P(),
        P(),
        P("tensor", None),
        P(),
        P("dp", None, None, "tensor"),
        P("dp", "tensor", None),
        P("dp", None),
        P("dp", None),
        P("dp", None),
    )
    out_specs = (
        P("dp", None),
        P("dp", None),
        P(),
        P(None, "tensor"),
        P(None, "tensor"),
        P(None, "tensor"),
        P(),
        P(),
        P("tensor", None),
        P(),
        P("dp", None, None, "tensor"),
        P("dp", "tensor", None),
    )
    return jax.shard_map(local, mesh=mesh, in_specs=in_specs, out_specs=out_specs, check_vma=False)
```
